32 devices in a mesh: row: 4 (over y, x), col: 8 (over z, core).
Axes of the slice: x: 2, y: 2, z: 4, core: 2. Of those that a mesh axis runs over, the one named last changes fastest.
Arguments:
- hidden_states: bfloat16 [1536, 4096], P('col', 'row'), may hold values from -50 to 50
- out_grad: bfloat16 [1536, 4096], P('col', 'row'), may hold values from -6 to 6
- lengths: int32 [4, 4], P('row'), may hold values from 1 to 512, 1024 in all within a row
- norm_gains: bfloat16 [2, 2, 1536], P(None, None, 'col'), may hold values from 0.099609375 to 1.8984375
- qkv_weight: bfloat16 [2, 1536, 2048], P(None, 'row', 'col'), may hold values from -0.15625 to 0.15625
- qkv_bias: bfloat16 [2, 16, 128], P(None, 'col', 'row'), may hold values from -2 to 2
- out_weight: bfloat16 [2, 1536, 1536], P(None, 'col', 'row'), may hold values from -0.625 to 0.625
- gate_weight: bfloat16 [2, 1536, 8960], P(None, 'row', 'col'), may hold values from -0.15625 to 0.15625
- up_weight: bfloat16 [2, 1536, 8960], P(None, 'row', 'col'), may hold values from -0.15625 to 0.15625
- down_weight: bfloat16 [2, 8960, 1536], P(None, 'col', 'row'), may hold values from -0.0625 to 0.0625
Outputs:
- out_states: bfloat16 [1536, 4096], P('col', 'row')
- input_grad: float32 [1536, 4096], P('col', 'row')
- norm_gains_grad: float32 [2, 2, 1536], P(None, None, 'col')
- qkv_weight_grad: float32 [2, 1536, 2048], P(None, 'row', 'col')
- qkv_bias_grad: float32 [2, 16, 128], P(None, 'col', 'row')
- out_weight_grad: float32 [2, 1536, 1536], P(None, 'col', 'row')
- gate_weight_grad: float32 [2, 1536, 8960], P(None, 'row', 'col')
- up_weight_grad: float32 [2, 1536, 8960], P(None, 'row', 'col')
- down_weight_grad: float32 [2, 8960, 1536], P(None, 'col', 'row')
The draws below stay inside these ranges and needn't reach their ends.
Inputs may be any that keep to these rules, and one draw needn't show every extreme that they name: Row g lists, in order, the lengths of the sequences packed into row group g; each row sums to 1024 and holds one length of exactly 512.
All inputs are finite; a program needn't handle non-finite values.
Results may differ from the reference program's by a relative error of at most 0.017.
Values may be sent and summed in bfloat16 or wider, within the bound.
A program may use at most 256 MiB of HBM per device.

```python
import math
import jax
import jax.numpy as jnp
import numpy as np
from jax import lax

D = 1536
HEADS = 12
KV_HEADS = 2
HD = 128
FF = 8960
LAYERS = 2
SEQ_MAX = 512
GROUPS = 4
TOK_ROW = 1024
TOKENS = 4096
SEQS = 4


def draw_hidden_states(key, part):
    noise_key, col_key, tok_key = jax.random.split(key, 3)
    place = jnp.arange(D, dtype=jnp.float32) / D
    col_scale = jnp.exp(jax.random.uniform(col_key, (D, 1), jnp.float32, -0.7, 0.7)) * jnp.exp(place * 1.1)[:, None]
    tok_scale = jnp.exp(jax.random.uniform(tok_key, (1, TOKENS), jnp.float32, -0.7, 0.7))
    base = jnp.clip(jax.random.normal(noise_key, (D, TOKENS), jnp.float32), -4.0, 4.0)
    return (base * col_scale * tok_scale).astype(jnp.bfloat16)


def draw_qkv_bias(key, part):
    return (jnp.clip(jax.random.normal(key, (LAYERS, HEADS + 2 * KV_HEADS, HD), jnp.float32), -4.0, 4.0) * 0.5).astype(jnp.bfloat16)


def shard_levels(key, shape, cuts, low, top_value):
    def one(dim, shards_of):
        heights = jax.random.uniform(jax.random.fold_in(jax.random.fold_in(key, 6), dim), (shards_of,), jnp.float32, low / len(cuts), top_value / len(cuts))
        return jnp.repeat(jnp.exp(heights), shape[dim] // shards_of).reshape((-1,) + (1,) * (len(shape) - dim - 1))

    gain = one(*cuts[0])
    for cut in cuts[1:]:
        gain = gain * one(*cut)
    return gain


def profile(amount, total, most, skew):
    portions = [(1 << 20) // math.isqrt(standing ** skew) + 1 for standing in range(2, amount + 1)]
    surplus, given = total - most - (amount - 1), [1] * (amount - 1)
    while surplus > 0:
        candidates = [i for i in range(amount - 1) if given[i] < most]
        mass, budget = sum([portions[i] for i in candidates]), surplus
        for i in candidates:
            addition = min(most - given[i], max(1, budget * portions[i] // mass), surplus)
            given[i] = given[i] + addition
            surplus = surplus - addition
    return np.array([most] + given)


def uneven(stream_key, count, total, most, slope):
    if count == 2:
        one = jax.random.randint(stream_key, (), max(1, total - most), min(most, total - 1) + 1)
        return jnp.stack([one, total - one])
    sizes = jnp.asarray(profile(count, total, most, slope), jnp.int32)
    twos = (count - 1) // 2
    giver, receiver = sizes[1:1 + 2 * twos:2], sizes[2:2 + 2 * twos:2]
    margin = jnp.minimum(giver - 1, most - receiver)
    passed = jax.random.randint(jax.random.fold_in(stream_key, 1), (twos,), 0, 1 << 20) % (margin + 1)
    sizes = sizes.at[1:1 + 2 * twos:2].set(giver - passed).at[2:2 + 2 * twos:2].set(receiver + passed)
    return sizes[jax.random.permutation(jax.random.fold_in(stream_key, 2), count)]


def noise(stream_key, extent, scale, limit, cuts=(), held_as=jnp.bfloat16):
    level = shard_levels(stream_key, extent, cuts, -0.22, 0.18) if cuts else 1.0
    values = jax.random.normal(stream_key, extent, jnp.float32) * scale * level
    return jnp.minimum(jnp.maximum(values, -limit), limit).astype(held_as)


def setup_inputs(seed: int = 0) -> dict:
    key_list = jax.random.split(jax.random.key(seed), 11)
    return {
        "hidden_states": draw_hidden_states(jax.random.fold_in(key_list[10], 71), 0),
        "out_grad": noise(key_list[1], (D, TOKENS), 1.0, 6.0, ((0, 8), (1, 4))),
        "lengths": jax.vmap(lambda own: uneven(own, SEQS, TOK_ROW, SEQ_MAX, 2))(jax.random.split(key_list[2], GROUPS)).reshape((GROUPS, SEQS)).astype(jnp.int32),
        "norm_gains": jnp.clip(1.0 + 0.18 * jax.random.normal(key_list[3], (LAYERS, 2, D), jnp.float32), 0.099609375, 1.8984375).astype(jnp.bfloat16),
        "qkv_weight": noise(key_list[4], (LAYERS, D, (HEADS + 2 * KV_HEADS) * HD), D ** -0.5, 0.15625, ((1, 4), (2, 8))),
        "qkv_bias": draw_qkv_bias(jax.random.fold_in(key_list[10], 71), 0),
        "out_weight": noise(key_list[6], (LAYERS, HEADS * HD, D), (HEADS * HD // 16) ** -0.5, 0.625, ((1, 8), (2, 4))),
        "gate_weight": noise(key_list[7], (LAYERS, D, FF), D ** -0.5, 0.15625, ((1, 4), (2, 8))),
        "up_weight": noise(key_list[8], (LAYERS, D, FF), D ** -0.5, 0.15625, ((1, 4), (2, 8))),
        "down_weight": noise(key_list[9], (LAYERS, FF, D), FF ** -0.5, 0.0625, ((1, 8), (2, 4))),
    }


eps_norm = 1e-06
rope_base = 1000000.0
neg_fill = -1e+30
highest = lax.Precision.HIGHEST

@jax.custom_vjp
def low(v):
    return lax.optimization_barrier(v.astype(jnp.bfloat16)).astype(jnp.float32)

@jax.custom_vjp
def low_back(v):
    return v

def low_keep(v):
    return (low(v), None)

def low_pass(kept, grad):
    return (grad,)

def back_keep(v):
    return (v, None)

def back_low(kept, grad):
    return (low(grad),)
low.defvjp(low_keep, low_pass)
low_back.defvjp(back_keep, back_low)

def row_starts(sizes, count):
    ends = jnp.cumsum(sizes)
    firsts = ends - sizes
    places = jnp.arange(count, dtype=jnp.int32)
    inside = (places[None, :] >= firsts[:, None]) & (places[None, :] < ends[:, None])
    return lax.optimization_barrier(jnp.sum(jnp.where(inside, firsts[:, None], 0), axis=0)).astype(jnp.int32)

def rope_tables(positions):
    half = HD // 2
    freq = rope_base ** (-(jnp.arange(half, dtype=jnp.float32) * (2.0 / HD)))
    angle = positions.astype(jnp.float32)[:, None] * freq[None, :]
    cosine = jnp.concatenate([jnp.cos(angle), jnp.cos(angle)], axis=-1)
    sine = jnp.concatenate([jnp.sin(angle), jnp.sin(angle)], axis=-1)
    return (cosine, sine)

def layer_forward(residual, params, layer, cosine, sine, mask):
    gains, w_qkv, b_qkv, w_out, w_gate, w_up, w_down = params
    count = residual.shape[0]
    group = HEADS // KV_HEADS
    rotary = HEADS + KV_HEADS
    half = HD // 2
    scale_one = lax.rsqrt(lax.optimization_barrier(jnp.mean(residual * residual, axis=1, keepdims=True)) + eps_norm)
    normed_one = low(residual * scale_one * gains[layer, 0])
    raw = low_back(jnp.dot(normed_one, w_qkv[layer], precision=highest) + b_qkv[layer].reshape(-1))
    heads = raw.reshape(count, HEADS + 2 * KV_HEADS, HD)
    rotating = heads[:, :rotary]
    turned = jnp.concatenate([-rotating[..., half:], rotating[..., :half]], axis=-1)
    rotating = rotating * cosine[:, None, :] + turned * sine[:, None, :]
    every = low(jnp.concatenate([rotating, heads[:, rotary:]], axis=1))
    queries = every[:, :HEADS].reshape(count, KV_HEADS, group, HD)
    keys = every[:, HEADS:rotary]
    values = every[:, rotary:]
    scores = low_back(jnp.einsum('tkgh,skh->kgts', queries, keys, precision=highest) * HD ** (-0.5))
    masked = jnp.where(mask[None, None], scores, neg_fill)
    row_top = lax.optimization_barrier(jnp.max(masked, axis=-1, keepdims=True))
    lifted = jnp.exp(masked - row_top)
    probs = lifted / lax.optimization_barrier(jnp.sum(lifted, axis=-1, keepdims=True))
    mixed = jnp.einsum('kgts,skh->tkgh', low(probs), values, precision=highest).reshape(count, HEADS * HD)
    mixed = low(low_back(mixed))
    residual_mid = residual + low_back(jnp.dot(mixed, w_out[layer], precision=highest))
    scale_two = lax.rsqrt(lax.optimization_barrier(jnp.mean(residual_mid * residual_mid, axis=1, keepdims=True)) + eps_norm)
    normed_two = low(residual_mid * scale_two * gains[layer, 1])
    gate = low_back(jnp.dot(normed_two, w_gate[layer], precision=highest))
    up = low_back(jnp.dot(normed_two, w_up[layer], precision=highest))
    hidden = low(gate * jax.nn.sigmoid(gate) * up)
    return residual_mid + low_back(jnp.dot(hidden, w_down[layer], precision=highest))

def group_forward(tokens, sizes, params):
    count = tokens.shape[0]
    starts = row_starts(sizes, count)
    places = jnp.arange(count, dtype=jnp.int32)
    cosine, sine = rope_tables(places - starts)
    mask = (places[None, :] >= starts[:, None]) & (places[None, :] <= places[:, None])
    residual = tokens
    for layer in range(LAYERS):
        residual = layer_forward(residual, params, layer, cosine, sine, mask)
    return residual

def reference(hidden_states, out_grad, lengths, norm_gains, qkv_weight, qkv_bias, out_weight, gate_weight, up_weight, down_weight):
    params = tuple((item.astype(jnp.float32) for item in (norm_gains, qkv_weight, qkv_bias, out_weight, gate_weight, up_weight, down_weight)))
    groups = lengths.shape[0]
    tokens = hidden_states.astype(jnp.float32).T
    count = tokens.shape[0] // groups

    def whole(flat, weights):

        def one_group(item):
            return group_forward(item[0], item[1], weights)
        pieces = lax.map(jax.checkpoint(one_group), (flat.reshape(groups, count, D), lengths))
        return pieces.reshape(groups * count, D)
    result, pull = jax.vjp(whole, tokens, params)
    d_tokens, d_params = pull(out_grad.astype(jnp.float32).T)
    return (result.T.astype(jnp.bfloat16), d_tokens.T, d_params[0], d_params[1], d_params[2], d_params[3], d_params[4], d_params[5], d_params[6])
```

```python
from functools import partial

import jax
import jax.numpy as jnp
from jax import lax
from jax.experimental import pallas as pl
from jax.experimental.pallas import tpu as pltpu
from jax.sharding import PartitionSpec as P

D = 1536
HEADS = 12
KV_HEADS = 2
HD = 128
LAYERS = 2
SEQ_MAX = 512
QB = 128
MESH = pl.DeviceIdType.MESH
LOW = jnp.bfloat16
F32 = jnp.float32
ANY = pl.BlockSpec(memory_space=pl.ANY)
ONCHIP = pl.BlockSpec(memory_space=pltpu.VMEM)
HALF = 208


class Place:
    def __init__(self):
        self.r = lax.axis_index("row")
        self.k = lax.axis_index("col")
        self.z = self.k // 2
        self.c = self.k % 2

    def at(self, z, c):
        return (self.r, 2 * z + c)

    def rows(self):
        x, y = self.r % 2, self.r // 2
        return (2 * y + (1 - x), 2 * (1 - y) + x, 2 * (1 - y) + (1 - x))


def remote(src, dst, send, recv, device):
    return pltpu.make_async_remote_copy(
        src_ref=src, dst_ref=dst, send_sem=send, recv_sem=recv, device_id=device, device_id_type=MESH
    )


class Later:
    def __init__(self):
        self.todo = []

    def add(self, wait, cond=None):
        self.todo.append((wait, cond))

    def run(self):
        for wait, cond in self.todo:
            if cond is None:
                wait()
            else:
                pl.when(cond)(wait)


def greet(place, reach):
    barrier = pltpu.get_barrier_semaphore()

    def hail(device):
        pl.semaphore_signal(barrier, inc=1, device_id=device, device_id_type=MESH)

    if "all" in reach:
        for rr in range(4):
            for kk in range(8):
                pl.when((place.r != rr) | (place.k != kk))(partial(hail, (rr, kk)))
        pl.semaphore_wait(barrier, 31)
        return
    count = 0
    if "rows" in reach:
        for row in place.rows():
            hail((row, place.k))
        count += 3
    if "col" in reach:
        for kk in range(8):
            pl.when(place.k != kk)(partial(hail, (place.r, kk)))
        pl.semaphore_wait(barrier, count + 7)
        return
    hail(place.at(place.z, 1 - place.c))
    count += 1
    if "line" not in reach:
        pl.semaphore_wait(barrier, count)
        return
    pl.when(place.z < 3)(partial(hail, place.at(jnp.minimum(place.z + 1, 3), place.c)))
    pl.when(place.z > 0)(partial(hail, place.at(jnp.maximum(place.z - 1, 0), place.c)))
    edge = (place.z == 0) | (place.z == 3)
    pl.when(edge)(lambda: pl.semaphore_wait(barrier, count + 1))
    pl.when(jnp.logical_not(edge))(lambda: pl.semaphore_wait(barrier, count + 2))


class Cargo:
    arrays = ()
    outs = ()
    scratch = ()
    reach = "rows"
    slow = False

    def middle(self, place, ins, outs, scratch, later):
        pass


def part_of(ref, dim, row, size):
    cut = pl.ds(pl.multiple_of(row * size, 128 if dim else 16), size)
    return ref.at[:, cut] if dim else ref.at[cut, :]


class GatherRows(Cargo):
    def __init__(self, block, dim):
        self.dim = dim
        self.arrays = (block,)
        full = list(block.shape)
        full[dim] *= 4
        self.size = block.shape[dim]
        self.half = block.shape[0] // 32 * 16
        self.rest = block.shape[0] - self.half
        self.outs = (jax.ShapeDtypeStruct(tuple(full), block.dtype),)
        self.scratch = (pltpu.SemaphoreType.DMA((6,)), pltpu.SemaphoreType.DMA((6,)), pltpu.SemaphoreType.DMA((1,)))

    def halves(self, ref):
        return ref.at[0 : self.half, :], ref.at[self.half :, :]

    def spots(self, full, row):
        if self.dim:
            cut = pl.ds(pl.multiple_of(row * self.size, 128), self.size)
            return full.at[0 : self.half, cut], full.at[self.half :, cut]
        first = pl.multiple_of(row * self.size, 16)
        return full.at[pl.ds(first, self.half), :], full.at[pl.ds(first + self.half, self.rest), :]

    def copies(self, place, ins, outs, scratch):
        (src,), (dst,), (send, recv, _) = ins, outs, scratch
        x, y, d = place.rows()
        block, mine = self.halves(src), self.spots(dst, place.r)
        from_x, from_y = self.spots(dst, x), self.spots(dst, y)
        out = [
            remote(block[0], mine[0], send.at[0], recv.at[0], (x, place.k)),
            remote(block[1], mine[1], send.at[1], recv.at[3], (y, place.k)),
            remote(block[1], mine[1], send.at[2], recv.at[1], (x, place.k)),
            remote(block[0], mine[0], send.at[3], recv.at[2], (y, place.k)),
        ]
        onward = [
            remote(from_x[0], from_x[0], send.at[4], recv.at[4], (y, place.k)),
            remote(from_y[1], from_y[1], send.at[5], recv.at[5], (x, place.k)),
        ]
        return out, onward

    def start(self, place, ins, outs, scratch, later):
        (src,), (dst,), (_, _, keep_sem) = ins, outs, scratch
        for copy in self.copies(place, ins, outs, scratch)[0]:
            copy.start()
        keep = pltpu.make_async_copy(src, part_of(dst, self.dim, place.r, self.size), keep_sem.at[0])
        keep.start()
        later.add(keep.wait)

    def middle(self, place, ins, outs, scratch, later):
        (src,), (dst,), (send, recv, _) = ins, outs, scratch
        x, y, d = place.rows()
        from_x, from_y, from_d = self.spots(dst, x), self.spots(dst, y), self.spots(dst, d)
        block = self.halves(src)

        def arrived(view, sem, device):
            return remote(view, view, send.at[0], recv.at[sem], device)

        out, onward = self.copies(place, ins, outs, scratch)
        arrived(from_x[0], 0, (x, place.k)).wait_recv()
        onward[0].start()
        arrived(from_y[1], 3, (y, place.k)).wait_recv()
        onward[1].start()
        for view, sem, row in ((from_x[1], 1, x), (from_y[0], 2, y), (from_d[0], 4, y), (from_d[1], 5, x)):
            later.add(arrived(view, sem, (row, place.k)).wait_recv)
        for copy in (*out, *onward):
            later.add(copy.wait_send)


class ScatterRows(Cargo):
    def __init__(self, grad, dim):
        self.dim = dim
        self.arrays = (grad,)
        part = list(grad.shape)
        part[dim] //= 4
        self.size = part[dim]
        self.half = part[0] // 32 * 16
        self.rest = part[0] - self.half
        self.outs = (jax.ShapeDtypeStruct((2, *part), grad.dtype),)
        upper, lower = pltpu.VMEM((self.half, part[1]), grad.dtype), pltpu.VMEM((self.rest, part[1]), grad.dtype)
        self.scratch = (
            *(upper, lower, lower, upper, lower, upper),
            pltpu.SemaphoreType.DMA((6,)),
            pltpu.SemaphoreType.DMA((6,)),
            pltpu.SemaphoreType.DMA((2,)),
        )

    def spots(self, full, row):
        if self.dim:
            cut = pl.ds(pl.multiple_of(row * self.size, 128), self.size)
            return full.at[0 : self.half, cut], full.at[self.half :, cut]
        first = pl.multiple_of(row * self.size, 16)
        return full.at[pl.ds(first, self.half), :], full.at[pl.ds(first + self.half, self.rest), :]

    def copies(self, place, ins, outs, scratch):
        (src,), (dst,) = ins, outs
        via_x, via_y, own_x, own_y, sum_x, sum_y, send, recv, keep = scratch
        x, y, d = place.rows()
        for_x, for_y, for_d = self.spots(src, x), self.spots(src, y), self.spots(src, d)
        slot_x = dst.at[0, 0 : self.half, :], dst.at[0, self.half :, :]
        slot_y = dst.at[1, 0 : self.half, :], dst.at[1, self.half :, :]
        first = [
            remote(for_d[0], via_x, send.at[0], recv.at[0], (x, place.k)),
            remote(for_d[1], via_y, send.at[1], recv.at[1], (y, place.k)),
            remote(for_x[0], slot_x[0], send.at[2], recv.at[2], (x, place.k)),
            remote(for_y[1], slot_y[1], send.at[3], recv.at[3], (y, place.k)),
        ]
        held = [
            pltpu.make_async_copy(for_x[1], own_x, keep.at[0]),
            pltpu.make_async_copy(for_y[0], own_y, keep.at[1]),
        ]
        last = [
            remote(sum_x, slot_x[1], send.at[4], recv.at[4], (x, place.k)),
            remote(sum_y, slot_y[0], send.at[5], recv.at[5], (y, place.k)),
        ]
        return first, held, last

    def start(self, place, ins, outs, scratch, later):
        first, held, _ = self.copies(place, ins, outs, scratch)
        for copy in (*first, *held):
            copy.start()

    def middle(self, place, ins, outs, scratch, later):
        via_x, via_y, own_x, own_y, sum_x, sum_y, *_ = scratch
        first, held, last = self.copies(place, ins, outs, scratch)
        held[0].wait()
        first[1].wait_recv()
        add_into(sum_x, [own_x, via_y])
        last[0].start()
        held[1].wait()
        first[0].wait_recv()
        add_into(sum_y, [own_y, via_x])
        last[1].start()
        for copy in (*first, *last):
            later.add(copy.wait_send)
        for copy in (*first[2:], *last):
            later.add(copy.wait_recv)


class Swap(Cargo):
    reach = "line"

    def __init__(self, *arrays):
        self.arrays = arrays
        self.outs = tuple(jax.ShapeDtypeStruct(a.shape, a.dtype) for a in arrays)
        self.scratch = (pltpu.SemaphoreType.DMA((len(arrays),)), pltpu.SemaphoreType.DMA((len(arrays),)))

    def start(self, place, ins, outs, scratch, later):
        send, recv = scratch
        for i, (src, dst) in enumerate(zip(ins, outs)):
            copy = remote(src, dst, send.at[i], recv.at[i], place.at(place.z, 1 - place.c))
            copy.start()
            later.add(copy.wait)


def tile_owner(z, t):
    if t < 3:
        head = 3 * z + t
        return head // 2, head % 2
    return 3 + t, z // 2


class HeadsToChips(Cargo):
    reach = "col"

    def __init__(self, tiles):
        self.arrays = (tiles,)
        self.outs = (jax.ShapeDtypeStruct((HALF, 5 * HD), LOW),)
        self.scratch = (pltpu.SemaphoreType.DMA((2, 2, 2)), pltpu.SemaphoreType.DMA((5,)))

    def start(self, place, ins, outs, scratch, later):
        (tiles,), (slab,), (send, recv) = ins, outs, scratch
        r, k, z, c = place.r, place.k, place.z, place.c
        query = k < 6
        for second in range(2):
            for i in range(2):
                head = 2 * k + i
                chip = jnp.where(query, head // 3, 2 * i + second)
                t = jnp.where(query, head % 3, k - 3)
                spot = slab.at[:, pl.ds(pl.multiple_of(t * HD, HD), HD)]
                for core in range(2):
                    here = k == 2 * chip + core
                    away = jnp.logical_not(here)
                    if second == 1:
                        here, away = here & (k >= 6), away & (k >= 6)
                    sem = send.at[i, second, core]
                    copy = remote(tiles.at[i, core], spot, sem, recv.at[t], (r, 2 * chip + core))
                    pl.when(away)(copy.start)
                    later.add(copy.wait_send, away)
                    keep = pltpu.make_async_copy(tiles.at[i, core], spot, sem)
                    pl.when(here)(keep.start)
                    later.add(keep.wait, here)
        for t in range(5):
            owner, _ = tile_owner(z, t)
            came = remote(
                tiles.at[0, 0], slab.at[:, t * HD : (t + 1) * HD], send.at[0, 0, 0], recv.at[t], (r, owner)
            )
            later.add(came.wait_recv, k != owner)


class HeadsToOwners(Cargo):
    reach = "col"

    def __init__(self, slab):
        self.arrays = (slab,)
        self.outs = (jax.ShapeDtypeStruct((2, 2, 2, HALF, HD), LOW),)
        self.scratch = (pltpu.SemaphoreType.DMA((5,)), pltpu.SemaphoreType.DMA((2, 2, 2)))

    def start(self, place, ins, outs, scratch, later):
        (slab,), (tiles,), (send, recv) = ins, outs, scratch
        r, k, z, c = place.r, place.k, place.z, place.c
        for t in range(5):
            owner, i = tile_owner(z, t)
            which = z % 2 if t >= 3 else 0
            view, spot = slab.at[:, t * HD : (t + 1) * HD], tiles.at[i, c, which]
            here = k == owner
            copy = remote(view, spot, send.at[t], recv.at[i, c, which], (r, owner))
            pl.when(jnp.logical_not(here))(copy.start)
            later.add(copy.wait_send, jnp.logical_not(here))
            keep = pltpu.make_async_copy(view, spot, send.at[t])
            pl.when(here)(keep.start)
            later.add(keep.wait, here)
        for i in range(2):
            for which in range(2):
                chip = jnp.where(k < 6, (2 * k + i) // 3, 2 * i + which)
                for core in range(2):
                    wanted = k != 2 * chip + core
                    if which == 1:
                        wanted = wanted & (k >= 6)
                    came = remote(
                        slab.at[:, 0:HD],
                        tiles.at[i, core, which],
                        send.at[0],
                        recv.at[i, core, which],
                        (r, 2 * chip + core),
                    )
                    later.add(came.wait_recv, wanted)


class Exchange(Cargo):
    def __init__(self, chunks, every_row=False):
        self.arrays = (chunks,)
        self.rows_too = every_row
        self.reach = "all" if every_row else "col"
        lead = (4,) if every_row else ()
        self.outs = (jax.ShapeDtypeStruct((*lead, *chunks.shape), chunks.dtype),)
        self.scratch = (pltpu.SemaphoreType.DMA((4, 8)), pltpu.SemaphoreType.DMA((4, 8)))

    def start(self, place, ins, outs, sems, later):
        (src,), (dst,), (send, recv) = ins, outs, sems
        r, k = place.r, place.k
        for rr in range(4) if self.rows_too else (None,):
            to_row = r if rr is None else rr
            for kk in range(8):
                here = (k == kk) if rr is None else (k == kk) & (r == rr)
                mine = dst.at[k] if rr is None else dst.at[r, k]
                theirs = dst.at[kk] if rr is None else dst.at[rr, kk]
                at = 0 if rr is None else rr
                my_at = 0 if rr is None else r
                copy = remote(src.at[kk], mine, send.at[at, kk], recv.at[my_at, k], (to_row, kk))
                pl.when(jnp.logical_not(here))(copy.start)
                later.add(copy.wait_send, jnp.logical_not(here))
                came = remote(src.at[kk], theirs, send.at[at, kk], recv.at[at, kk], (to_row, kk))
                later.add(came.wait_recv, jnp.logical_not(here))
                keep = pltpu.make_async_copy(src.at[kk], mine, send.at[at, kk])
                pl.when(here)(keep.start)
                later.add(keep.wait, here)


def add_into(dst, views):
    rows = dst.shape[0]

    def step(i, carry):
        cut = pl.ds(pl.multiple_of(i * 16, 16), 16)
        total = views[0][cut, :].astype(F32)
        for view in views[1:]:
            total = total + view[cut, :].astype(F32)
        dst[cut, :] = total.astype(dst.dtype)
        return carry

    lax.fori_loop(0, rows // 16, step, 0)


def gather_line(place, block, full, sems, later, both, middle):
    send_r, send_l, send_p, recv, keep_sem = sems
    z, c = place.z, place.c

    def spot(zz, cc):
        return full.at[2 * zz + cc] if both else full.at[zz]

    def arrival(zz, cc):
        return recv.at[2 * zz + cc]

    def pass_on(src, zz, slot):
        dst, sem = spot(zz, c), arrival(zz, c)

        def go(send, device):
            return remote(src, dst, send.at[slot], sem, device)

        return (
            go(send_r, place.at(jnp.minimum(z + 1, 3), c)),
            go(send_l, place.at(jnp.maximum(z - 1, 0), c)),
            go(send_p, place.at(z, 1 - c)),
        )

    right, left, partner = pass_on(block, z, 0)
    pl.when(z < 3)(right.start)
    pl.when(z > 0)(left.start)
    later.add(right.wait_send, z < 3)
    later.add(left.wait_send, z > 0)
    if both:
        partner.start()
        later.add(partner.wait_send)
    keep = pltpu.make_async_copy(block, spot(z, c), keep_sem.at[0])
    keep.start()
    later.add(keep.wait)
    for t in range(1, 4):
        if t == 2:
            middle()
        for way in (-1, 1):
            there = z + way * t
            valid = (there >= 0) & (there <= 3)
            zz = jnp.clip(there, 0, 3)
            right, left, partner = pass_on(spot(zz, c), zz, t if way == -1 else 3 + t)
            onward, may = (right, z < 3) if way == -1 else (left, z > 0)

            @pl.when(valid)
            def _(onward=onward, may=may, partner=partner):
                onward.wait_recv()
                pl.when(may)(onward.start)
                if both:
                    partner.start()

            later.add(onward.wait_send, valid & may)
            if both:
                later.add(partner.wait_send, valid)
    if both:
        for zz in range(4):
            came = remote(block, spot(zz, 1 - c), send_p.at[0], arrival(zz, 1 - c), place.at(z, 1 - c))
            later.add(came.wait_recv)


def reduce_line(place, part, out, from_p, from_r, from_l, held, sems, later, both, middle):
    send_p, recv_p, send, recv_r, recv_l = sems
    z, c = place.z, place.c
    right_at, left_at = place.at(jnp.minimum(z + 1, 3), c), place.at(jnp.maximum(z - 1, 0), c)

    def own(j):
        return part.at[2 * j + c] if both else part.at[j]

    def partner(j):
        return remote(part.at[2 * j + 1 - c], from_p.at[j], send_p.at[j], recv_p.at[j], place.at(z, 1 - c))

    def moving(j, buffer, sem, device):
        return remote(held.at[j], buffer.at[j], send.at[j], sem.at[j], device)

    if both:
        for j in (3, 0, 2, 1):
            copy = partner(j)
            copy.start()
            later.add(copy.wait_send)

    def terms(j):
        if both:
            partner(j).wait_recv()
            return [own(j), from_p.at[j]]
        return [own(j)]

    for s in range(3):
        if s == 2:
            middle()
        for go_right in (True, False):
            if go_right:
                j, valid, first = 3 - s + z, z <= s, z == 0
                buffer, sem, device = from_r, recv_r, right_at
            else:
                j, valid, first = s - 3 + z, z >= 3 - s, z == 3
                buffer, sem, device = from_l, recv_l, left_at
            j = jnp.clip(j, 0, 3)
            copy = moving(j, buffer, sem, device)

            @pl.when(valid & first)
            def _(j=j, copy=copy):
                add_into(held.at[j], terms(j))
                copy.start()

            @pl.when(valid & jnp.logical_not(first))
            def _(j=j, copy=copy, buffer=buffer):
                views = terms(j)
                copy.wait_recv()
                add_into(held.at[j], [*views, buffer.at[j]])
                copy.start()

            later.add(copy.wait_send, valid)
    views = terms(z)
    last_r, last_l = moving(z, from_r, recv_r, right_at), moving(z, from_l, recv_l, left_at)

    @pl.when(z == 0)
    def _():
        last_l.wait_recv()
        add_into(out, [*views, from_l.at[z]])

    @pl.when(z == 3)
    def _():
        last_r.wait_recv()
        add_into(out, [*views, from_r.at[z]])

    @pl.when((z > 0) & (z < 3))
    def _():
        last_r.wait_recv()
        last_l.wait_recv()
        add_into(out, [*views, from_r.at[z], from_l.at[z]])


class Names:
    def __init__(self):
        self.next = 0

    def take(self):
        self.next += 1
        return self.next - 1


def carry_kernel(body, reach, n_in, n_out, n_scratch, cargo, *refs):
    refs = list(refs)

    def pop(n):
        taken = refs[:n]
        del refs[:n]
        return taken

    ins = pop(n_in)
    cargo_ins = [pop(len(item.arrays)) for item in cargo]
    outs = pop(n_out)
    cargo_outs = [pop(len(item.outs)) for item in cargo]
    scratch = pop(n_scratch)
    cargo_scratch = [pop(len(item.scratch)) for item in cargo]
    place = Place()
    later = Later()
    loads = list(zip(cargo, cargo_ins, cargo_outs, cargo_scratch))
    greet(place, {reach, *(item.reach for item in cargo)})
    for item, *theirs in loads:
        item.start(place, *theirs, later)

    def middle():
        for item, *theirs in loads:
            item.middle(place, *theirs, later)

    body(place, ins, outs, scratch, later, middle)
    later.run()


def carry_call(names, body, reach, arrays, in_specs, outs, out_specs, scratch, cargo, name=None):
    call = pl.pallas_call(
        partial(carry_kernel, body, reach, len(arrays), len(outs), len(scratch), cargo),
        out_shape=[*outs, *(o for item in cargo for o in item.outs)],
        in_specs=[*in_specs, *(ANY for item in cargo for _ in item.arrays)],
        out_specs=[*out_specs, *(ANY for item in cargo for _ in item.outs)],
        scratch_shapes=[*scratch, *(s for item in cargo for s in item.scratch)],
        compiler_params=pltpu.CompilerParams(
            collective_id=names.take(), has_side_effects=True, vmem_limit_bytes=40 * 2**20
        ),
        name=name,
    )
    results = list(call(*arrays, *(a for item in cargo for a in item.arrays)))
    main = results[: len(outs)]
    rest = results[len(outs) :]
    loads = []
    for item in cargo:
        loads.append(rest[: len(item.outs)])
        rest = rest[len(item.outs) :]
    return main, loads


def gather_tokens(names, block, cargo, both=True, name=None):
    tokens, width = block.shape
    blocks = 8 if both else 4

    def body(place, ins, outs, scratch, later, middle):
        gather_line(place, ins[0], outs[0], scratch, later, both, middle)

    (full,), loads = carry_call(
        names,
        body,
        "line",
        [block],
        [ONCHIP],
        [jax.ShapeDtypeStruct((blocks, tokens, width), block.dtype)],
        [ANY],
        [
            pltpu.SemaphoreType.DMA((7,)),
            pltpu.SemaphoreType.DMA((7,)),
            pltpu.SemaphoreType.DMA((7,)),
            pltpu.SemaphoreType.DMA((8,)),
            pltpu.SemaphoreType.DMA((1,)),
        ],
        cargo,
        name=name,
    )
    return full.reshape(blocks * tokens, width), loads


def reduce_tokens(names, part, cargo, both=True, name=None):
    blocks = 8 if both else 4
    tokens, width = part.shape[0] // blocks, part.shape[1]

    def body(place, ins, outs, scratch, later, middle):
        from_p, from_r, from_l, held, *sems = scratch
        reduce_line(place, ins[0], outs[0], from_p, from_r, from_l, held, sems, later, both, middle)

    (total,), loads = carry_call(
        names,
        body,
        "line",
        [part.reshape(blocks, tokens, width)],
        [ONCHIP],
        [jax.ShapeDtypeStruct((tokens, width), F32)],
        [ONCHIP],
        [
            *[pltpu.VMEM((4, tokens, width), LOW)] * 4,
            *[pltpu.SemaphoreType.DMA((4,))] * 5,
        ],
        cargo,
        name=name,
    )
    return total, loads


def stages_call(names, stages, name=None):
    cargo = [item for stage in stages for item in stage]
    arrays, outs, scratch = [], [], []
    for item in cargo:
        arrays += [a for a in item.arrays if not isinstance(a, From)]
        outs += item.outs
        scratch += item.scratch
    n_in, n_out = len(arrays), len(outs)

    def kernel(*refs):
        ins, made, held = list(refs[:n_in]), list(refs[n_in : n_in + n_out]), list(refs[n_in + n_out :])
        place = Place()
        greet(place, {item.reach for item in cargo})
        out_refs = {}
        last = Later()
        for stage in stages:
            later = Later()
            begun = []
            for item in stage:
                mine = [out_refs[a.item][a.at] if isinstance(a, From) else ins.pop(0) for a in item.arrays]
                out_refs[item] = [made.pop(0) for _ in item.outs]
                kept = [held.pop(0) for _ in item.scratch]
                begun.append((item, mine, out_refs[item], kept, last if item.slow else later))
            for item, *theirs in begun:
                item.start(place, *theirs)
            for item, *theirs in begun:
                item.middle(place, *theirs)
            later.run()
        last.run()

    results = list(
        pl.pallas_call(
            kernel,
            out_shape=outs,
            in_specs=[ANY] * n_in,
            out_specs=[ANY] * n_out,
            scratch_shapes=scratch,
            compiler_params=pltpu.CompilerParams(
                collective_id=names.take(), has_side_effects=True, vmem_limit_bytes=40 * 2**20
            ),
            name=name,
        )(*arrays)
    )
    loads = []
    for item in cargo:
        loads.append([results.pop(0) for _ in item.outs])
    return loads


class From:
    def __init__(self, item, at=0):
        self.item, self.at = item, at
        self.shape, self.dtype = item.outs[at].shape, item.outs[at].dtype


eps_norm = 1e-06
rope_base = 1000000.0
neg_fill = -1e30


def row_starts(sizes, count):
    ends = jnp.cumsum(sizes)
    firsts = ends - sizes
    places = jnp.arange(count, dtype=jnp.int32)
    inside = (places[None, :] >= firsts[:, None]) & (places[None, :] < ends[:, None])
    return jnp.sum(jnp.where(inside, firsts[:, None], 0), axis=0)


def rope_tables(positions):
    half = HD // 2
    freq = rope_base ** (-(jnp.arange(half, dtype=jnp.float32) * (2.0 / HD)))
    angle = freq[:, None] * positions.astype(jnp.float32)[None, :]
    cosine = jnp.concatenate([jnp.cos(angle), jnp.cos(angle)], axis=0)
    sine = jnp.concatenate([jnp.sin(angle), jnp.sin(angle)], axis=0)
    return (cosine, sine)


def rotate(values, cosine, sine):
    half = HD // 2
    turned = jnp.concatenate([-values[:, half:], values[:, :half]], axis=1)
    return values * cosine + turned * sine


def rotate_back(grads, cosine, sine):
    half = HD // 2
    lifted = grads * sine
    turned = jnp.concatenate([lifted[:, half:], -lifted[:, :half]], axis=1)
    return grads * cosine + turned


def contract_first(left, right):
    return lax.dot_general(
        left, right, (((0,), (0,)), ((), ())), preferred_element_type=jnp.float32
    )


def contract_last(left, right):
    return lax.dot_general(
        left, right, (((1,), (1,)), ((), ())), preferred_element_type=jnp.float32
    )


def feature_total(values):
    return lax.psum(jnp.sum(values, axis=0), "col")


def spread(values):
    return lax.all_gather(values, "col", axis=0, tiled=True)


def summed_rows(make_term, rows):
    return lax.psum_scatter(
        make_term(jnp.int32(0), lax.axis_size("col") * rows), "col", scatter_dimension=0, tiled=True
    )


def to_blocks(values):
    return lax.all_to_all(values, "col", split_axis=1, concat_axis=0, tiled=True)


def to_tokens(values):
    return lax.all_to_all(values, "col", split_axis=0, concat_axis=1, tiled=True)


def by_columns(weight, acts, start, count):
    return contract_first(weight, acts)


def by_rows(weight, grads, start, count):
    return jnp.dot(weight, grads, preferred_element_type=jnp.float32)


def by_rows_pair(first_weight, first_grads, second_weight, second_grads, start, count):
    return by_rows(first_weight, first_grads, start, count) + by_rows(
        second_weight, second_grads, start, count
    )


def norm_forward(residual, gain):
    totals = feature_total(residual * residual)
    scale = lax.rsqrt(totals / D + eps_norm)
    return (scale, (residual * scale * gain[:, None]).astype(jnp.bfloat16))


def norm_backward(d_normed, residual, scale, gain):
    weighted = d_normed * gain[:, None]
    inner = feature_total(weighted * residual)
    d_residual = weighted * scale - residual * (scale * scale * scale) * inner / D
    d_gain = jnp.sum(d_normed * residual * scale, axis=1)
    return (d_residual, d_gain)


def attend_scores(queries, keys, mask):
    scores = jnp.einsum(
        "kghq,khj->kgqj", queries, keys, preferred_element_type=jnp.float32
    ) * HD ** (-0.5)
    return jnp.where(mask[None, None], scores, neg_fill)


def per_device(
    hidden_states,
    out_grad,
    lengths,
    norm_gains,
    qkv_weight,
    qkv_bias,
    out_weight,
    gate_weight,
    up_weight,
    down_weight,
):
    feat_rows, tok_row = hidden_states.shape
    col_at = lax.axis_index("col")
    starts = row_starts(lengths[0], tok_row)
    positions = jnp.arange(tok_row, dtype=jnp.int32) - starts
    cosine, sine = rope_tables(positions)
    first = col_at * QB
    block_starts = lax.dynamic_slice_in_dim(starts, first, QB)
    cos_block = lax.dynamic_slice_in_dim(cosine, first, QB, 1)
    sin_block = lax.dynamic_slice_in_dim(sine, first, QB, 1)
    reach = QB + SEQ_MAX
    window = jnp.maximum(first - SEQ_MAX, 0)
    key_places = window + jnp.arange(reach, dtype=jnp.int32)
    query_places = first + jnp.arange(QB, dtype=jnp.int32)
    mask = (key_places[None, :] >= block_starts[:, None]) & (
        key_places[None, :] <= query_places[:, None]
    )
    group = HEADS // KV_HEADS
    rotary = HEADS + KV_HEADS
    query_rows = HEADS * HD
    kv_rows = KV_HEADS * HD
    gains = norm_gains.astype(jnp.float32)
    residual = hidden_states.astype(jnp.float32)
    saved = []
    for layer in range(LAYERS):
        w_qkv, b_qkv, w_out, w_gate, w_up, w_down = (
            lax.all_gather(qkv_weight[layer], "row", axis=0, tiled=True),
            lax.all_gather(qkv_bias[layer], "row", axis=1, tiled=True),
            lax.all_gather(out_weight[layer], "row", axis=1, tiled=True),
            lax.all_gather(gate_weight[layer], "row", axis=0, tiled=True),
            lax.all_gather(up_weight[layer], "row", axis=0, tiled=True),
            lax.all_gather(down_weight[layer], "row", axis=1, tiled=True),
        )
        scale_one, normed_one = norm_forward(residual, gains[layer, 0])
        full_one = spread(normed_one)
        raw = contract_first(w_qkv, full_one) + b_qkv.reshape(-1).astype(jnp.float32)[:, None]
        local_heads = raw.shape[0] // HD
        shaped = raw.reshape(local_heads, HD, tok_row)
        head_ids = col_at * local_heads + jnp.arange(local_heads)
        turned = jnp.where((head_ids < rotary)[:, None, None], rotate(shaped, cosine, sine), shaped)
        blocked = to_blocks(turned.reshape(raw.shape).astype(jnp.bfloat16))
        kv_full = lax.all_gather(blocked[query_rows:], "col", axis=1, tiled=True)
        kv_window = lax.dynamic_slice_in_dim(kv_full, window, reach, 1)
        queries = blocked[:query_rows].reshape(KV_HEADS, group, HD, QB)
        keys = kv_window[:kv_rows].reshape(KV_HEADS, HD, reach)
        values = kv_window[kv_rows:].reshape(KV_HEADS, HD, reach)
        masked = attend_scores(queries, keys, mask)
        row_top = jnp.max(masked, axis=-1, keepdims=True)
        lifted = jnp.exp(masked - row_top)
        row_mass = jnp.sum(lifted, axis=-1, keepdims=True)
        probs = lifted / row_mass
        log_mass = row_top + jnp.log(row_mass)
        mixed = (
            jnp.einsum(
                "kgqj,khj->kghq",
                probs.astype(jnp.bfloat16),
                values,
                preferred_element_type=jnp.float32,
            )
            .reshape(query_rows, QB)
            .astype(jnp.bfloat16)
        )
        carried = to_tokens(mixed)
        attention = summed_rows(partial(by_columns, w_out, carried), feat_rows)
        residual_mid = residual + attention
        scale_two, normed_two = norm_forward(residual_mid, gains[layer, 1])
        full_two = spread(normed_two)
        gate = contract_first(w_gate, full_two)
        up = contract_first(w_up, full_two)
        hidden = (gate * jax.nn.sigmoid(gate) * up).astype(jnp.bfloat16)
        feed = summed_rows(partial(by_columns, w_down, hidden), feat_rows)
        saved.append(
            (
                residual,
                scale_one,
                full_one,
                blocked,
                kv_window,
                log_mass,
                mixed,
                carried,
                residual_mid,
                scale_two,
                full_two,
                gate,
                up,
                hidden,
                (w_qkv, w_out, w_gate, w_up, w_down),
                local_heads,
            )
        )
        residual = residual_mid + feed
    out_states = residual.astype(jnp.bfloat16)
    grad = out_grad.astype(jnp.float32)
    layer_grads = [None] * LAYERS
    gain_terms = [None] * LAYERS
    for layer in reversed(range(LAYERS)):
        (
            residual_in,
            scale_one,
            full_one,
            blocked,
            kv_window,
            log_mass,
            mixed,
            carried,
            residual_mid,
            scale_two,
            full_two,
            gate,
            up,
            hidden,
            weights_full,
            local_heads,
        ) = saved[layer]
        w_qkv, w_out, w_gate, w_up, w_down = weights_full
        grad_full = spread(grad.astype(jnp.bfloat16))
        d_down = contract_last(hidden, grad_full)
        d_hidden = jnp.dot(w_down, grad_full, preferred_element_type=jnp.float32)
        squash = jax.nn.sigmoid(gate)
        d_gate = (d_hidden * up * squash * (1.0 + gate * (1.0 - squash))).astype(jnp.bfloat16)
        d_up = (d_hidden * gate * squash).astype(jnp.bfloat16)
        d_gate_w = contract_last(full_two, d_gate)
        d_up_w = contract_last(full_two, d_up)
        d_normed_two = summed_rows(partial(by_rows_pair, w_gate, d_gate, w_up, d_up), feat_rows)
        d_residual, d_gain_two = norm_backward(
            d_normed_two, residual_mid, scale_two, gains[layer, 1]
        )
        grad = grad + d_residual
        grad_full = spread(grad.astype(jnp.bfloat16))
        d_out_w = contract_last(carried, grad_full)
        d_mixed = to_blocks(
            jnp.dot(w_out, grad_full, preferred_element_type=jnp.float32).astype(jnp.bfloat16)
        )
        queries = blocked[:query_rows].reshape(KV_HEADS, group, HD, QB)
        keys = kv_window[:kv_rows].reshape(KV_HEADS, HD, reach)
        values = kv_window[kv_rows:].reshape(KV_HEADS, HD, reach)
        masked = attend_scores(queries, keys, mask)
        probs = jnp.exp(masked - log_mass)
        low_probs = probs.astype(jnp.bfloat16)
        d_heads_mix = d_mixed.reshape(KV_HEADS, group, HD, QB)
        d_probs = jnp.einsum(
            "kghq,khj->kgqj", d_heads_mix, values, preferred_element_type=jnp.float32
        )
        inner = jnp.sum(probs * d_probs, axis=-1, keepdims=True)
        d_scores = (probs * (d_probs - inner)).astype(jnp.bfloat16)
        d_queries = (
            jnp.einsum("kgqj,khj->kghq", d_scores, keys, preferred_element_type=jnp.float32)
            * HD ** (-0.5)
        ).reshape(query_rows, QB)
        d_keys = (
            jnp.einsum("kgqj,kghq->khj", d_scores, queries, preferred_element_type=jnp.float32)
            * HD ** (-0.5)
        ).reshape(kv_rows, reach)
        d_values = jnp.einsum(
            "kgqj,kghq->khj", low_probs, d_heads_mix, preferred_element_type=jnp.float32
        ).reshape(kv_rows, reach)
        d_window = jnp.concatenate([d_keys, d_values], axis=0)
        d_placed = lax.dynamic_update_slice_in_dim(
            jnp.zeros((2 * kv_rows, tok_row), jnp.float32), d_window, window, 1
        )
        d_kv = lax.psum_scatter(d_placed, "col", scatter_dimension=1, tiled=True)
        d_heads = jnp.concatenate([d_queries, d_kv], axis=0).reshape(HEADS + 2 * KV_HEADS, HD, QB)
        d_turned = jnp.concatenate(
            [rotate_back(d_heads[:rotary], cos_block, sin_block), d_heads[rotary:]], axis=0
        )
        d_raw = to_tokens(d_turned.reshape((HEADS + 2 * KV_HEADS) * HD, QB).astype(jnp.bfloat16))
        d_bias = jnp.sum(d_raw, axis=1, dtype=jnp.float32).reshape(local_heads, HD)
        d_qkv_w = contract_last(full_one, d_raw)
        d_normed_one = summed_rows(partial(by_rows, w_qkv, d_raw), feat_rows)
        d_residual, d_gain_one = norm_backward(
            d_normed_one, residual_in, scale_one, gains[layer, 0]
        )
        grad = grad + d_residual
        layer_grads[layer] = (
            lax.psum_scatter(d_qkv_w, "row", scatter_dimension=0, tiled=True),
            lax.psum_scatter(d_bias, "row", scatter_dimension=1, tiled=True),
            lax.psum_scatter(d_out_w, "row", scatter_dimension=1, tiled=True),
            lax.psum_scatter(d_gate_w, "row", scatter_dimension=0, tiled=True),
            lax.psum_scatter(d_up_w, "row", scatter_dimension=0, tiled=True),
            lax.psum_scatter(d_down, "row", scatter_dimension=1, tiled=True),
        )
        gain_terms[layer] = jnp.stack([d_gain_one, d_gain_two])
    gain_grads = lax.psum(jnp.stack(gain_terms), "row")
    stacked = [jnp.stack([entry[member] for entry in layer_grads]) for member in range(6)]
    return (
        out_states,
        grad,
        gain_grads,
        stacked[0],
        stacked[1],
        stacked[2],
        stacked[3],
        stacked[4],
        stacked[5],
    )


def softmax_scores(queries, keys, mask):
    scores = jnp.einsum("htd,ud->htu", queries, keys, preferred_element_type=F32) * HD ** (-0.5)
    return jnp.where(mask[None], scores, neg_fill)


def dot(a, b):
    return jnp.dot(a, b, preferred_element_type=F32)


def dot_t(a, b):
    return lax.dot_general(a, b, (((1,), (1,)), ((), ())), preferred_element_type=F32)


def t_dot(a, b):
    return lax.dot_general(a, b, (((0,), (0,)), ((), ())), preferred_element_type=F32)


def turn(values, cosine, sine):
    half = HD // 2
    turned = jnp.concatenate([-values[..., half:], values[..., :half]], axis=-1)
    return values * cosine + turned * sine


def turn_back(grads, cosine, sine):
    half = HD // 2
    lifted = grads * sine
    turned = jnp.concatenate([lifted[..., half:], -lifted[..., :half]], axis=-1)
    return grads * cosine + turned


def norm_on(residual, gain):
    scale = lax.rsqrt(jnp.mean(residual * residual, axis=1, keepdims=True) + eps_norm)
    return scale, (residual * scale * gain[None, :]).astype(LOW)


def norm_back(d_normed, residual, scale, gain):
    weighted = d_normed * gain[None, :]
    inner = jnp.sum(weighted * residual, axis=1, keepdims=True)
    d_residual = weighted * scale - residual * (scale * scale * scale) * inner / D
    d_gain = jnp.sum(d_normed * residual * scale, axis=0)
    return d_residual, d_gain


def per_device_line(
    hidden_states,
    out_grad,
    lengths,
    norm_gains,
    qkv_weight,
    qkv_bias,
    out_weight,
    gate_weight,
    up_weight,
    down_weight,
):
    names = Names()
    tok_row = hidden_states.shape[1]
    row_at = lax.axis_index("row")
    col_at = lax.axis_index("col")
    core = col_at % 2
    starts = row_starts(lengths[0], tok_row)
    places = jnp.arange(tok_row, dtype=jnp.int32)
    cosine, sine = rope_tables(places - starts)
    cosine, sine = cosine.T[:, None], sine.T[:, None]

    def own(values):
        cut = values.reshape(4, 2, QB, *values.shape[1:])
        return lax.dynamic_index_in_dim(cut, core, 1, keepdims=False).reshape(4 * QB, *values.shape[1:])

    mask = (places[None, :] >= own(starts)[:, None]) & (places[None, :] <= own(places)[:, None])

    def head_tiles(layer):
        biases = jnp.zeros((2, 1, 16, HD), LOW)
        biases = lax.dynamic_update_slice(biases, qkv_bias[layer][:, None, None], (0, 0, 0, row_at * (HD // 4)))
        tiles = qkv_weight[layer].reshape(2, D // 8, 2, HD).transpose(2, 0, 1, 3)
        return jnp.concatenate([tiles, jnp.broadcast_to(biases, (2, 2, 16, HD))], axis=2)

    def slab_of(mine, theirs, out_mine, out_theirs):
        first, second = jnp.where(core == 0, mine, theirs), jnp.where(core == 0, theirs, mine)
        both = jnp.stack([first.reshape(4, HALF, 5 * HD), second.reshape(4, HALF, 5 * HD)], axis=1)
        w_qkv = both[:, :, : D // 8].reshape(D, 5 * HD)
        bias = jnp.sum(both[:, 0, D // 8].astype(F32), axis=0)
        w_out = jnp.concatenate(
            [jnp.where(core == 0, out_mine, out_theirs), jnp.where(core == 0, out_theirs, out_mine)], axis=0
        )
        return w_qkv, bias, w_out

    arrivals = jnp.concatenate(
        [
            hidden_states.T.reshape(8, QB, D // 8),
            out_grad.T.reshape(8, QB, D // 8),
            jnp.broadcast_to(
                jnp.pad(norm_gains.reshape(2 * LAYERS, D // 8), ((0, 16 - 2 * LAYERS), (0, 0))), (8, 16, D // 8)
            ),
        ],
        axis=1,
    )
    spread = Exchange(arrivals)
    spread.slow = True
    to_chips = [HeadsToChips(head_tiles(layer)) for layer in range(LAYERS)]
    to_chips[1].slow = True
    slab_rows, out_rows = GatherRows(From(to_chips[0]), 0), GatherRows(out_weight[0], 1)
    swap = Swap(From(slab_rows), From(out_rows))
    loads = stages_call(
        names, [[to_chips[0]], [slab_rows, out_rows, spread, to_chips[1]], [swap]], name="open"
    )
    (_,), (mine,), (out_mine,), (came,), (slab_next,), (theirs, out_theirs) = loads
    load = (mine, theirs, out_mine, out_theirs)
    came = came.transpose(1, 0, 2).reshape(2 * QB + 16, D)
    residual = came[:QB].astype(F32)
    grad = came[QB : 2 * QB].astype(F32)
    gains = came[2 * QB : 2 * QB + 2 * LAYERS].astype(F32).reshape(LAYERS, 2, D)

    def weights_in(layer):
        return [GatherRows(gate_weight[layer], 0), GatherRows(up_weight[layer], 0), GatherRows(down_weight[layer], 1)]

    sent = weights_in(0)
    grad_full_last, ((w_gate,),) = gather_tokens(names, grad.astype(LOW), sent[:1], name="gather_three_1")
    saved = []
    for layer in range(LAYERS):
        if layer == 1:
            mine, out_mine, (w_gate,) = load
        scale_one, normed_one = norm_on(residual, gains[layer, 0])
        if layer == 0:
            normed_one, _ = lax.optimization_barrier((normed_one, grad_full_last))
        cargo = [sent[1]] if layer == 0 else [sent[1], Swap(mine, out_mine)]
        full_one, loads = gather_tokens(names, normed_one, cargo, name=f"gather_one_{layer}")
        w_up = loads[0][0]
        if layer == 1:
            load = (mine, loads[1][0], out_mine, loads[1][1])
        w_qkv, bias, w_out = slab_of(*load)
        raw = (dot(full_one, w_qkv) + bias[None]).reshape(tok_row, 5, HD)
        turned = jnp.concatenate([turn(raw[:, :4], cosine, sine), raw[:, 4:]], axis=1).astype(LOW)
        queries = own(turned[:, :3]).transpose(1, 0, 2)
        keys, values = turned[:, 3], turned[:, 4]
        masked = softmax_scores(queries, keys, mask)
        row_top = jnp.max(masked, axis=-1, keepdims=True)
        lifted = jnp.exp(masked - row_top)
        row_mass = jnp.sum(lifted, axis=-1, keepdims=True)
        probs = (lifted / row_mass).astype(LOW)
        log_mass = row_top + jnp.log(row_mass)
        mixed = jnp.einsum("htu,ud->thd", probs, values, preferred_element_type=F32)
        mixed = mixed.astype(LOW).reshape(4 * QB, 3 * HD)
        attention, ((w_down,),) = reduce_tokens(
            names, dot(mixed, w_out).astype(LOW), [sent[2]], both=False, name=f"reduce_one_{layer}"
        )
        residual_mid = residual + attention
        scale_two, normed_two = norm_on(residual_mid, gains[layer, 1])
        cargo = []
        if layer == 0:
            sent = weights_in(1)
            cargo = sent[:1]
        full_two, loads_two = gather_tokens(names, normed_two, cargo, name=f"gather_two_{layer}")
        gate = dot(full_two, w_gate)
        up = dot(full_two, w_up)
        hidden = (gate * jax.nn.sigmoid(gate) * up).astype(LOW)
        cargo = [GatherRows(slab_next, 0), GatherRows(out_weight[1], 1)] if layer == 0 else []
        feed, loads = reduce_tokens(names, dot(hidden, w_down).astype(LOW), cargo, name=f"reduce_two_{layer}")
        saved.append(
            (
                residual,
                scale_one,
                full_one,
                queries,
                keys,
                values,
                log_mass,
                mixed,
                residual_mid,
                scale_two,
                full_two,
                gate,
                up,
                hidden,
                (w_qkv, w_out, w_gate, w_up, w_down),
            )
        )
        residual = residual_mid + feed
        if layer == 0:
            load = (loads[0][0], loads[1][0], loads_two[0])
    states = residual.astype(LOW)

    def own_part(full, dim):
        size = full.shape[dim] // 4
        return lax.dynamic_slice_in_dim(full, row_at * size, size, dim)

    def settle(full, dim, slots):
        return jnp.sum(slots.astype(F32), axis=0) + own_part(full, dim).astype(F32)

    def settle_heads(tiles):
        total = tiles[:, :, 0].astype(F32) + jnp.where(col_at >= 6, tiles[:, :, 1].astype(F32), 0.0)
        weight = total[:, :, : D // 8].transpose(1, 2, 0, 3).reshape(D // 4, 2 * HD)
        bias = lax.dynamic_slice_in_dim(total[:, 0, D // 8], row_at * (HD // 4), HD // 4, 1)
        return weight, bias

    grads = {}
    gain_terms = [None] * LAYERS
    waiting = None
    for layer in reversed(range(LAYERS)):
        (
            residual_in,
            scale_one,
            full_one,
            queries,
            keys,
            values,
            log_mass,
            mixed,
            residual_mid,
            scale_two,
            full_two,
            gate,
            up,
            hidden,
            (w_qkv, w_out, w_gate, w_up, w_down),
        ) = saved[layer]
        if layer == LAYERS - 1:
            grad_full = grad_full_last
        else:
            grad_full, loads = gather_tokens(
                names,
                grad.astype(LOW),
                [ScatterRows(waiting[0], 0), ScatterRows(waiting[1], 1)],
                name=f"gather_three_{layer}",
            )
            slab_sum = settle(waiting[0], 0, loads[0][0]).astype(LOW)
            grads["out", layer + 1] = settle(waiting[1], 1, loads[1][0])
        d_down = t_dot(hidden, grad_full).astype(LOW)
        d_hidden = dot_t(grad_full, w_down)
        squash = jax.nn.sigmoid(gate)
        d_gate = (d_hidden * up * squash * (1.0 + gate * (1.0 - squash))).astype(LOW)
        d_up = (d_hidden * gate * squash).astype(LOW)
        d_normed = (dot_t(d_gate, w_gate) + dot_t(d_up, w_up)).astype(LOW)
        cargo = [ScatterRows(d_down, 1)]
        if layer < LAYERS - 1:
            cargo.append(HeadsToOwners(slab_sum))
        d_normed_two, loads = reduce_tokens(names, d_normed, cargo, name=f"reduce_three_{layer}")
        if layer < LAYERS - 1:
            grads["qkv", layer + 1] = settle_heads(loads[1][0])
        grads["down", layer] = settle(d_down, 1, loads[0][0])
        d_gate_w = t_dot(full_two, d_gate).astype(LOW)
        d_up_w = t_dot(full_two, d_up).astype(LOW)
        d_residual, d_gain_two = norm_back(d_normed_two, residual_mid, scale_two, gains[layer, 1])
        grad = grad + d_residual
        grad_own, loads = gather_tokens(
            names, grad.astype(LOW), [ScatterRows(d_gate_w, 0)], both=False, name=f"gather_four_{layer}"
        )
        grads["gate", layer] = settle(d_gate_w, 0, loads[0][0])
        d_out_w = t_dot(mixed, grad_own).astype(LOW)
        d_mixed = dot_t(grad_own, w_out).astype(LOW).reshape(4 * QB, 3, HD).transpose(1, 0, 2)
        masked = softmax_scores(queries, keys, mask)
        probs = jnp.exp(masked - log_mass)
        d_probs = jnp.einsum("htd,ud->htu", d_mixed, values, preferred_element_type=F32)
        inner = jnp.sum(probs * d_probs, axis=-1, keepdims=True)
        d_scores = (probs * (d_probs - inner)).astype(LOW)
        d_queries = jnp.einsum("htu,ud->thd", d_scores, keys, preferred_element_type=F32) * HD ** (-0.5)
        d_keys = jnp.einsum("htu,htd->ud", d_scores, queries, preferred_element_type=F32) * HD ** (-0.5)
        d_values = jnp.einsum("htu,htd->ud", probs.astype(LOW), d_mixed, preferred_element_type=F32)
        d_raw_q = turn_back(d_queries, own(cosine), own(sine)).astype(LOW).reshape(4, QB, 3 * HD)
        mine = (jnp.arange(2) == core)[None, :, None, None]
        d_raw_q = jnp.where(mine, d_raw_q[:, None], jnp.zeros((), LOW)).reshape(tok_row, 3 * HD)
        d_raw_k = turn_back(d_keys, cosine[:, 0], sine[:, 0]).astype(LOW)
        d_raw = jnp.concatenate([d_raw_q, d_raw_k, d_values.astype(LOW)], axis=1)
        d_bias = jnp.sum(d_raw, axis=0, dtype=F32).astype(LOW)
        d_qkv_w = t_dot(full_one, d_raw).astype(LOW).reshape(4, 2, D // 8, 5 * HD)
        tail = jnp.broadcast_to(jnp.pad(d_bias[None], ((0, 15), (0, 0))), (4, 2, 16, 5 * HD))
        d_slab = jnp.concatenate([d_qkv_w, tail], axis=2)
        d_out_w = d_out_w.reshape(2, D // 8, D)

        def half(full, dim, which):
            return lax.dynamic_index_in_dim(full, which, dim, keepdims=False)

        d_normed_one, loads = reduce_tokens(
            names,
            dot_t(d_raw, w_qkv).astype(LOW),
            [ScatterRows(d_up_w, 0), Swap(half(d_slab, 1, 1 - core), half(d_out_w, 0, 1 - core))],
            name=f"reduce_four_{layer}",
        )
        grads["up", layer] = settle(d_up_w, 0, loads[0][0])
        slab_part = (half(d_slab, 1, core).astype(F32) + loads[1][0].astype(F32)).astype(LOW)
        out_part = (half(d_out_w, 0, core).astype(F32) + loads[1][1].astype(F32)).astype(LOW)
        waiting = (slab_part.reshape(4 * HALF, 5 * HD), out_part)
        d_residual, d_gain_one = norm_back(d_normed_one, residual_in, scale_one, gains[layer, 0])
        grad = grad + d_residual
        gain_terms[layer] = jnp.stack([d_gain_one, d_gain_two])
    leaving = jnp.concatenate([states, grad.astype(LOW)], axis=0).reshape(2 * QB, 8, D // 8).transpose(1, 0, 2)
    gain_parts = jnp.pad(jnp.stack(gain_terms).reshape(2 * LAYERS, 8, D // 8), ((0, 8 - 2 * LAYERS), (0, 0), (0, 0)))
    (left,), (gain_all,), (slots,), (out_slots,) = stages_call(
        names,
        [
            [
                Exchange(leaving),
                Exchange(gain_parts.transpose(1, 0, 2), every_row=True),
                ScatterRows(waiting[0], 0),
                ScatterRows(waiting[1], 1),
            ]
        ],
        name="close",
    )
    ((tiles,),) = stages_call(names, [[HeadsToOwners(settle(waiting[0], 0, slots).astype(LOW))]], name="close_heads")
    grads["qkv", 0] = settle_heads(tiles)
    grads["out", 0] = settle(waiting[1], 1, out_slots)
    out_states = left[:, :QB].reshape(tok_row, D // 8).T
    input_grad = left[:, QB:].reshape(tok_row, D // 8).T.astype(F32)
    gain_grads = jnp.sum(gain_all, axis=(0, 1))[: 2 * LAYERS].reshape(LAYERS, 2, D // 8)

    def both_layers(kind):
        return jnp.stack([grads[kind, layer] for layer in range(LAYERS)])

    heads = [jnp.stack([grads["qkv", layer][i] for layer in range(LAYERS)]) for i in range(2)]
    return (
        out_states,
        input_grad,
        gain_grads,
        heads[0],
        heads[1],
        both_layers("out"),
        both_layers("gate"),
        both_layers("up"),
        both_layers("down"),
    )


def solution(mesh):
    placed = (
        P("col", "row"),
        P("col", "row"),
        P("row", None),
        P(None, None, "col"),
        P(None, "row", "col"),
        P(None, "col", "row"),
        P(None, "col", "row"),
        P(None, "row", "col"),
        P(None, "row", "col"),
        P(None, "col", "row"),
    )
    on_lines = mesh.shape["row"] == 4 and mesh.shape["col"] == 8
    return jax.shard_map(
        per_device_line if on_lines else per_device,
        mesh=mesh,
        in_specs=placed,
        out_specs=(
            P("col", "row"),
            P("col", "row"),
            P(None, None, "col"),
            P(None, "row", "col"),
            P(None, "col", "row"),
            P(None, "col", "row"),
            P(None, "row", "col"),
            P(None, "row", "col"),
            P(None, "col", "row"),
        ),
        check_vma=False,
    )
```

```python
from functools import partial

import jax
import jax.numpy as jnp
from jax import lax
from jax.experimental import pallas as pl
from jax.experimental.pallas import tpu as pltpu
from jax.sharding import PartitionSpec as P

D = 1536
HEADS = 12
KV_HEADS = 2
HD = 128
LAYERS = 2
SEQ_MAX = 512
QB = 128
MESH = pl.DeviceIdType.MESH
LOW = jnp.bfloat16
F32 = jnp.float32
ANY = pl.BlockSpec(memory_space=pl.ANY)
ONCHIP = pl.BlockSpec(memory_space=pltpu.VMEM)
HALF = 208


class Place:
    def __init__(self):
        self.r = lax.axis_index("row")
        self.k = lax.axis_index("col")
        self.z = self.k // 2
        self.c = self.k % 2

    def at(self, z, c):
        return (self.r, 2 * z + c)

    def rows(self):
        x, y = self.r % 2, self.r // 2
        return (2 * y + (1 - x), 2 * (1 - y) + x, 2 * (1 - y) + (1 - x))


def remote(src, dst, send, recv, device):
    return pltpu.make_async_remote_copy(
        src_ref=src, dst_ref=dst, send_sem=send, recv_sem=recv, device_id=device, device_id_type=MESH
    )


class Later:
    def __init__(self):
        self.todo = []

    def add(self, wait, cond=None):
        self.todo.append((wait, cond))

    def run(self):
        todo, self.todo = self.todo, []
        for wait, cond in todo:
            if cond is None:
                wait()
            else:
                pl.when(cond)(wait)


def greet(place, reach):
    barrier = pltpu.get_barrier_semaphore()

    def hail(device):
        pl.semaphore_signal(barrier, inc=1, device_id=device, device_id_type=MESH)

    if "all" in reach:
        for rr in range(4):
            for kk in range(8):
                pl.when((place.r != rr) | (place.k != kk))(partial(hail, (rr, kk)))
        pl.semaphore_wait(barrier, 31)
        return
    count = 0
    if "rows" in reach:
        for row in place.rows():
            hail((row, place.k))
        count += 3
    if "col" in reach:
        for kk in range(8):
            pl.when(place.k != kk)(partial(hail, (place.r, kk)))
        pl.semaphore_wait(barrier, count + 7)
        return
    hail(place.at(place.z, 1 - place.c))
    count += 1
    if "line" not in reach:
        pl.semaphore_wait(barrier, count)
        return
    pl.when(place.z < 3)(partial(hail, place.at(jnp.minimum(place.z + 1, 3), place.c)))
    pl.when(place.z > 0)(partial(hail, place.at(jnp.maximum(place.z - 1, 0), place.c)))
    edge = (place.z == 0) | (place.z == 3)
    pl.when(edge)(lambda: pl.semaphore_wait(barrier, count + 1))
    pl.when(jnp.logical_not(edge))(lambda: pl.semaphore_wait(barrier, count + 2))


class Cargo:
    arrays = ()
    outs = ()
    scratch = ()
    reach = "rows"
    phase = 0
    slow = False

    def middle(self, place, ins, outs, scratch):
        pass


def part_of(ref, dim, row, size):
    cut = pl.ds(pl.multiple_of(row * size, 128 if dim else 16), size)
    return ref.at[:, cut] if dim else ref.at[cut, :]


class GatherRows(Cargo):
    def __init__(self, block, dim):
        self.dim = dim
        self.arrays = (block,)
        full = list(block.shape)
        full[dim] *= 4
        self.size = block.shape[dim]
        self.half = block.shape[0] // 32 * 16
        self.rest = block.shape[0] - self.half
        self.outs = (jax.ShapeDtypeStruct(tuple(full), block.dtype),)
        self.scratch = (pltpu.SemaphoreType.DMA((6,)), pltpu.SemaphoreType.DMA((6,)), pltpu.SemaphoreType.DMA((1,)))

    def halves(self, ref):
        return ref.at[0 : self.half, :], ref.at[self.half :, :]

    def spots(self, full, row):
        if self.dim:
            cut = pl.ds(pl.multiple_of(row * self.size, 128), self.size)
            return full.at[0 : self.half, cut], full.at[self.half :, cut]
        first = pl.multiple_of(row * self.size, 16)
        return full.at[pl.ds(first, self.half), :], full.at[pl.ds(first + self.half, self.rest), :]

    def copies(self, place, ins, outs, scratch):
        (src,), (dst,), (send, recv, _) = ins, outs, scratch
        x, y, d = place.rows()
        block, mine = self.halves(src), self.spots(dst, place.r)
        from_x, from_y = self.spots(dst, x), self.spots(dst, y)
        out = [
            remote(block[0], mine[0], send.at[0], recv.at[0], (x, place.k)),
            remote(block[1], mine[1], send.at[1], recv.at[3], (y, place.k)),
            remote(block[1], mine[1], send.at[2], recv.at[1], (x, place.k)),
            remote(block[0], mine[0], send.at[3], recv.at[2], (y, place.k)),
        ]
        onward = [
            remote(from_x[0], from_x[0], send.at[4], recv.at[4], (y, place.k)),
            remote(from_y[1], from_y[1], send.at[5], recv.at[5], (x, place.k)),
        ]
        return out, onward

    def arrived(self, place, scratch, view, sem, row):
        return remote(view, view, scratch[0].at[0], scratch[1].at[sem], (row, place.k))

    def start(self, place, ins, outs, scratch, later):
        (src,), (dst,), (_, _, keep_sem) = ins, outs, scratch
        out, onward = self.copies(place, ins, outs, scratch)
        for copy in out:
            copy.start()
        keep = pltpu.make_async_copy(src, part_of(dst, self.dim, place.r, self.size), keep_sem.at[0])
        keep.start()
        later.add(keep.wait)
        x, y, d = place.rows()
        from_x, from_y, from_d = self.spots(dst, x), self.spots(dst, y), self.spots(dst, d)
        for view, sem, row in ((from_x[1], 1, x), (from_y[0], 2, y), (from_d[0], 4, y), (from_d[1], 5, x)):
            later.add(self.arrived(place, scratch, view, sem, row).wait_recv)
        for copy in (*out, *onward):
            later.add(copy.wait_send)

    def middle(self, place, ins, outs, scratch):
        (dst,) = outs
        x, y, d = place.rows()
        _, onward = self.copies(place, ins, outs, scratch)
        self.arrived(place, scratch, self.spots(dst, x)[0], 0, x).wait_recv()
        onward[0].start()
        self.arrived(place, scratch, self.spots(dst, y)[1], 3, y).wait_recv()
        onward[1].start()


class ScatterRows(Cargo):
    def __init__(self, grad, dim):
        self.dim = dim
        self.arrays = (grad,)
        part = list(grad.shape)
        part[dim] //= 4
        self.size = part[dim]
        self.half = part[0] // 32 * 16
        self.rest = part[0] - self.half
        self.outs = (jax.ShapeDtypeStruct((2, *part), grad.dtype),)
        upper, lower = pltpu.VMEM((self.half, part[1]), grad.dtype), pltpu.VMEM((self.rest, part[1]), grad.dtype)
        self.scratch = (
            *(upper, lower, lower, upper, lower, upper),
            pltpu.SemaphoreType.DMA((6,)),
            pltpu.SemaphoreType.DMA((6,)),
            pltpu.SemaphoreType.DMA((2,)),
        )

    def spots(self, full, row):
        if self.dim:
            cut = pl.ds(pl.multiple_of(row * self.size, 128), self.size)
            return full.at[0 : self.half, cut], full.at[self.half :, cut]
        first = pl.multiple_of(row * self.size, 16)
        return full.at[pl.ds(first, self.half), :], full.at[pl.ds(first + self.half, self.rest), :]

    def copies(self, place, ins, outs, scratch):
        (src,), (dst,) = ins, outs
        via_x, via_y, own_x, own_y, sum_x, sum_y, send, recv, keep = scratch
        x, y, d = place.rows()
        for_x, for_y, for_d = self.spots(src, x), self.spots(src, y), self.spots(src, d)
        slot_x = dst.at[0, 0 : self.half, :], dst.at[0, self.half :, :]
        slot_y = dst.at[1, 0 : self.half, :], dst.at[1, self.half :, :]
        first = [
            remote(for_d[0], via_x, send.at[0], recv.at[0], (x, place.k)),
            remote(for_d[1], via_y, send.at[1], recv.at[1], (y, place.k)),
            remote(for_x[0], slot_x[0], send.at[2], recv.at[2], (x, place.k)),
            remote(for_y[1], slot_y[1], send.at[3], recv.at[3], (y, place.k)),
        ]
        held = [
            pltpu.make_async_copy(for_x[1], own_x, keep.at[0]),
            pltpu.make_async_copy(for_y[0], own_y, keep.at[1]),
        ]
        last = [
            remote(sum_x, slot_x[1], send.at[4], recv.at[4], (x, place.k)),
            remote(sum_y, slot_y[0], send.at[5], recv.at[5], (y, place.k)),
        ]
        return first, held, last

    def start(self, place, ins, outs, scratch, later):
        first, held, last = self.copies(place, ins, outs, scratch)
        for copy in (*first, *held):
            copy.start()
        for copy in (*first, *last):
            later.add(copy.wait_send)
        for copy in (*first[2:], *last):
            later.add(copy.wait_recv)

    def middle(self, place, ins, outs, scratch):
        via_x, via_y, own_x, own_y, sum_x, sum_y, *_ = scratch
        first, held, last = self.copies(place, ins, outs, scratch)
        held[0].wait()
        first[1].wait_recv()
        add_into(sum_x, [own_x, via_y])
        last[0].start()
        held[1].wait()
        first[0].wait_recv()
        add_into(sum_y, [own_y, via_x])
        last[1].start()


class Swap(Cargo):
    reach = "line"

    def __init__(self, *arrays):
        self.arrays = arrays
        self.outs = tuple(jax.ShapeDtypeStruct(a.shape, a.dtype) for a in arrays)
        self.scratch = (pltpu.SemaphoreType.DMA((len(arrays),)), pltpu.SemaphoreType.DMA((len(arrays),)))

    def start(self, place, ins, outs, scratch, later):
        send, recv = scratch
        for i, (src, dst) in enumerate(zip(ins, outs)):
            copy = remote(src, dst, send.at[i], recv.at[i], place.at(place.z, 1 - place.c))
            copy.start()
            later.add(copy.wait)


def tile_owner(z, t):
    if t < 3:
        head = 3 * z + t
        return head // 2, head % 2
    return 3 + t, z // 2


class HeadsToChips(Cargo):
    reach = "col"

    def __init__(self, tiles):
        self.arrays = (tiles,)
        self.outs = (jax.ShapeDtypeStruct((HALF, 5 * HD), LOW),)
        self.scratch = (pltpu.SemaphoreType.DMA((2, 2, 2)), pltpu.SemaphoreType.DMA((5,)))

    def start(self, place, ins, outs, scratch, later):
        (tiles,), (slab,), (send, recv) = ins, outs, scratch
        r, k, z, c = place.r, place.k, place.z, place.c
        query = k < 6
        for second in range(2):
            for i in range(2):
                head = 2 * k + i
                chip = jnp.where(query, head // 3, 2 * i + second)
                t = jnp.where(query, head % 3, k - 3)
                spot = slab.at[:, pl.ds(pl.multiple_of(t * HD, HD), HD)]
                for core in range(2):
                    here = k == 2 * chip + core
                    away = jnp.logical_not(here)
                    if second == 1:
                        here, away = here & (k >= 6), away & (k >= 6)
                    sem = send.at[i, second, core]
                    copy = remote(tiles.at[i, core], spot, sem, recv.at[t], (r, 2 * chip + core))
                    pl.when(away)(copy.start)
                    later.add(copy.wait_send, away)
                    keep = pltpu.make_async_copy(tiles.at[i, core], spot, sem)
                    pl.when(here)(keep.start)
                    later.add(keep.wait, here)
        for t in range(5):
            owner, _ = tile_owner(z, t)
            came = remote(
                tiles.at[0, 0], slab.at[:, t * HD : (t + 1) * HD], send.at[0, 0, 0], recv.at[t], (r, owner)
            )
            later.add(came.wait_recv, k != owner)


class HeadsToOwners(Cargo):
    reach = "col"

    def __init__(self, slab):
        self.arrays = (slab,)
        self.outs = (jax.ShapeDtypeStruct((2, 2, 2, HALF, HD), LOW),)
        self.scratch = (pltpu.SemaphoreType.DMA((5,)), pltpu.SemaphoreType.DMA((2, 2, 2)))

    def start(self, place, ins, outs, scratch, later):
        (slab,), (tiles,), (send, recv) = ins, outs, scratch
        r, k, z, c = place.r, place.k, place.z, place.c
        for t in range(5):
            owner, i = tile_owner(z, t)
            which = z % 2 if t >= 3 else 0
            view, spot = slab.at[:, t * HD : (t + 1) * HD], tiles.at[i, c, which]
            here = k == owner
            copy = remote(view, spot, send.at[t], recv.at[i, c, which], (r, owner))
            pl.when(jnp.logical_not(here))(copy.start)
            later.add(copy.wait_send, jnp.logical_not(here))
            keep = pltpu.make_async_copy(view, spot, send.at[t])
            pl.when(here)(keep.start)
            later.add(keep.wait, here)
        for i in range(2):
            for which in range(2):
                chip = jnp.where(k < 6, (2 * k + i) // 3, 2 * i + which)
                for core in range(2):
                    wanted = k != 2 * chip + core
                    if which == 1:
                        wanted = wanted & (k >= 6)
                    came = remote(
                        slab.at[:, 0:HD],
                        tiles.at[i, core, which],
                        send.at[0],
                        recv.at[i, core, which],
                        (r, 2 * chip + core),
                    )
                    later.add(came.wait_recv, wanted)


class Exchange(Cargo):
    def __init__(self, chunks, every_row=False):
        self.arrays = (chunks,)
        self.rows_too = every_row
        self.reach = "all" if every_row else "col"
        lead = (4,) if every_row else ()
        self.outs = (jax.ShapeDtypeStruct((*lead, *chunks.shape), chunks.dtype),)
        self.scratch = (pltpu.SemaphoreType.DMA((4, 8)), pltpu.SemaphoreType.DMA((4, 8)))

    def start(self, place, ins, outs, sems, later):
        (src,), (dst,), (send, recv) = ins, outs, sems
        r, k = place.r, place.k
        for rr in range(4) if self.rows_too else (None,):
            to_row = r if rr is None else rr
            for kk in range(8):
                here = (k == kk) if rr is None else (k == kk) & (r == rr)
                mine = dst.at[k] if rr is None else dst.at[r, k]
                theirs = dst.at[kk] if rr is None else dst.at[rr, kk]
                at = 0 if rr is None else rr
                my_at = 0 if rr is None else r
                copy = remote(src.at[kk], mine, send.at[at, kk], recv.at[my_at, k], (to_row, kk))
                pl.when(jnp.logical_not(here))(copy.start)
                later.add(copy.wait_send, jnp.logical_not(here))
                came = remote(src.at[kk], theirs, send.at[at, kk], recv.at[at, kk], (to_row, kk))
                later.add(came.wait_recv, jnp.logical_not(here))
                keep = pltpu.make_async_copy(src.at[kk], mine, send.at[at, kk])
                pl.when(here)(keep.start)
                later.add(keep.wait, here)


def add_into(dst, views):
    rows = dst.shape[0]

    def step(i, carry):
        cut = pl.ds(pl.multiple_of(i * 16, 16), 16)
        total = views[0][cut, :].astype(F32)
        for view in views[1:]:
            total = total + view[cut, :].astype(F32)
        dst[cut, :] = total.astype(dst.dtype)
        return carry

    lax.fori_loop(0, rows // 16, step, 0)


def gather_line(place, block, full, sems, later, both, middle):
    send_r, send_l, send_p, recv, keep_sem = sems
    z, c = place.z, place.c

    def spot(zz, cc):
        return full.at[2 * zz + cc] if both else full.at[zz]

    def arrival(zz, cc):
        return recv.at[2 * zz + cc]

    def pass_on(src, zz, slot):
        dst, sem = spot(zz, c), arrival(zz, c)

        def go(send, device):
            return remote(src, dst, send.at[slot], sem, device)

        return (
            go(send_r, place.at(jnp.minimum(z + 1, 3), c)),
            go(send_l, place.at(jnp.maximum(z - 1, 0), c)),
            go(send_p, place.at(z, 1 - c)),
        )

    right, left, partner = pass_on(block, z, 0)
    pl.when(z < 3)(right.start)
    pl.when(z > 0)(left.start)
    later.add(right.wait_send, z < 3)
    later.add(left.wait_send, z > 0)
    if both:
        partner.start()
        later.add(partner.wait_send)
    keep = pltpu.make_async_copy(block, spot(z, c), keep_sem.at[0])
    keep.start()
    later.add(keep.wait)
    for t in range(1, 4):
        if t == 2:
            middle()
        for way in (-1, 1):
            there = z + way * t
            valid = (there >= 0) & (there <= 3)
            zz = jnp.clip(there, 0, 3)
            right, left, partner = pass_on(spot(zz, c), zz, t if way == -1 else 3 + t)
            onward, may = (right, z < 3) if way == -1 else (left, z > 0)

            @pl.when(valid)
            def _(onward=onward, may=may, partner=partner):
                onward.wait_recv()
                pl.when(may)(onward.start)
                if both:
                    partner.start()

            later.add(onward.wait_send, valid & may)
            if both:
                later.add(partner.wait_send, valid)
    if both:
        for zz in range(4):
            came = remote(block, spot(zz, 1 - c), send_p.at[0], arrival(zz, 1 - c), place.at(z, 1 - c))
            later.add(came.wait_recv)


def pair_copy(place, part, from_p, sems, j):
    return remote(part.at[2 * j + 1 - place.c], from_p.at[j], sems[0].at[j], sems[1].at[j], place.at(place.z, 1 - place.c))


def reduce_line(place, part, out, from_p, from_r, from_l, held, sems, later, both, middle, sent=False):
    send_p, recv_p, send, recv_r, recv_l = sems
    z, c = place.z, place.c
    right_at, left_at = place.at(jnp.minimum(z + 1, 3), c), place.at(jnp.maximum(z - 1, 0), c)

    def own(j):
        return part.at[2 * j + c] if both else part.at[j]

    def partner(j):
        return pair_copy(place, part, from_p, sems, j)

    def moving(j, buffer, sem, device):
        return remote(held.at[j], buffer.at[j], send.at[j], sem.at[j], device)

    if both:
        for j in (3, 0, 2, 1):
            copy = partner(j)
            if not sent:
                copy.start()
            later.add(copy.wait_send)

    def terms(j):
        if both:
            partner(j).wait_recv()
            return [own(j), from_p.at[j]]
        return [own(j)]

    for s in range(3):
        if s == 2:
            middle()
        for go_right in (True, False):
            if go_right:
                j, valid, first = 3 - s + z, z <= s, z == 0
                buffer, sem, device = from_r, recv_r, right_at
            else:
                j, valid, first = s - 3 + z, z >= 3 - s, z == 3
                buffer, sem, device = from_l, recv_l, left_at
            j = jnp.clip(j, 0, 3)
            copy = moving(j, buffer, sem, device)

            @pl.when(valid & first)
            def _(j=j, copy=copy):
                add_into(held.at[j], terms(j))
                copy.start()

            @pl.when(valid & jnp.logical_not(first))
            def _(j=j, copy=copy, buffer=buffer):
                views = terms(j)
                copy.wait_recv()
                add_into(held.at[j], [*views, buffer.at[j]])
                copy.start()

            later.add(copy.wait_send, valid)
    views = terms(z)
    last_r, last_l = moving(z, from_r, recv_r, right_at), moving(z, from_l, recv_l, left_at)

    @pl.when(z == 0)
    def _():
        last_l.wait_recv()
        add_into(out, [*views, from_l.at[z]])

    @pl.when(z == 3)
    def _():
        last_r.wait_recv()
        add_into(out, [*views, from_r.at[z]])

    @pl.when((z > 0) & (z < 3))
    def _():
        last_r.wait_recv()
        last_l.wait_recv()
        add_into(out, [*views, from_r.at[z], from_l.at[z]])


class Names:
    def __init__(self):
        self.next = 0

    def take(self):
        self.next += 1
        return self.next - 1


def carry_kernel(body, reach, n_in, n_out, n_scratch, cargo, *refs):
    refs = list(refs)

    def pop(n):
        taken = refs[:n]
        del refs[:n]
        return taken

    ins = pop(n_in)
    given = [pop(sum(not isinstance(a, From) for a in item.arrays)) for item in cargo]
    outs = pop(n_out)
    made = {item: pop(len(item.outs)) for item in cargo}
    scratch = pop(n_scratch)
    held = {item: pop(len(item.scratch)) for item in cargo}
    taken = {
        item: [made[a.item][a.at] if isinstance(a, From) else mine.pop(0) for a in item.arrays]
        for item, mine in zip(cargo, given)
    }
    place = Place()
    later = Later()
    owed = [Later(), Later()]
    greet(place, {reach, *(item.reach for item in cargo)})

    def start(phase):
        if phase == 1 and any(isinstance(a, From) for item in cargo for a in item.arrays):
            owed[0].run()
        for item in cargo:
            if item.phase == phase:
                item.start(place, taken[item], made[item], held[item], owed[phase])

    def middle(phase=0):
        for item in cargo:
            if item.phase == phase:
                item.middle(place, taken[item], made[item], held[item])

    start(0)
    body(place, ins, outs, scratch, later, middle, start)
    later.run()
    owed[0].run()
    owed[1].run()


def carry_call(names, body, reach, arrays, in_specs, outs, out_specs, scratch, cargo, name=None, vmem=40):
    given = [a for item in cargo for a in item.arrays if not isinstance(a, From)]
    call = pl.pallas_call(
        partial(carry_kernel, body, reach, len(arrays), len(outs), len(scratch), cargo),
        out_shape=[*outs, *(o for item in cargo for o in item.outs)],
        in_specs=[*in_specs, *(ANY for _ in given)],
        out_specs=[*out_specs, *(ANY for item in cargo for _ in item.outs)],
        scratch_shapes=[*scratch, *(s for item in cargo for s in item.scratch)],
        compiler_params=pltpu.CompilerParams(
            collective_id=names.take(), has_side_effects=True, vmem_limit_bytes=vmem * 2**20
        ),
        name=name,
    )
    results = list(call(*arrays, *given))
    main = results[: len(outs)]
    rest = results[len(outs) :]
    loads = []
    for item in cargo:
        loads.append(rest[: len(item.outs)])
        rest = rest[len(item.outs) :]
    return main, loads


def gather_tokens(names, block, cargo, both=True, name=None):
    tokens, width = block.shape
    blocks = 8 if both else 4

    def body(place, ins, outs, scratch, later, middle, start):
        gather_line(place, ins[0], outs[0], scratch, later, both, middle)

    (full,), loads = carry_call(
        names,
        body,
        "line",
        [block],
        [ONCHIP],
        [jax.ShapeDtypeStruct((blocks, tokens, width), block.dtype)],
        [ANY],
        [
            pltpu.SemaphoreType.DMA((7,)),
            pltpu.SemaphoreType.DMA((7,)),
            pltpu.SemaphoreType.DMA((7,)),
            pltpu.SemaphoreType.DMA((8,)),
            pltpu.SemaphoreType.DMA((1,)),
        ],
        cargo,
        name=name,
    )
    return full.reshape(blocks * tokens, width), loads


def reduce_tokens(names, part, cargo, both=True, name=None):
    blocks = 8 if both else 4
    tokens, width = part.shape[0] // blocks, part.shape[1]

    def body(place, ins, outs, scratch, later, middle, start):
        from_p, from_r, from_l, held, *sems = scratch
        reduce_line(place, ins[0], outs[0], from_p, from_r, from_l, held, sems, later, both, middle)

    (total,), loads = carry_call(
        names,
        body,
        "line",
        [part.reshape(blocks, tokens, width)],
        [ONCHIP],
        [jax.ShapeDtypeStruct((tokens, width), F32)],
        [ONCHIP],
        [
            *[pltpu.VMEM((4, tokens, width), LOW)] * 4,
            *[pltpu.SemaphoreType.DMA((4,))] * 5,
        ],
        cargo,
        name=name,
    )
    return total, loads


class Gather:
    scratch = (
        pltpu.SemaphoreType.DMA((4,)),
        pltpu.SemaphoreType.DMA((4,)),
        pltpu.SemaphoreType.DMA((8,)),
        pltpu.SemaphoreType.DMA((8,)),
        pltpu.SemaphoreType.DMA((1,)),
    )

    def __init__(self, place, block, full, sems, both=True):
        self.place, self.block, self.full, self.both = place, block, full, both
        self.send_r, self.send_l, self.send_p, self.recv, self.keep = sems

    def copies(self, src, zz, t, way):
        z, c = self.place.z, self.place.c
        spot, sem = self.full.at[2 * zz + c], self.recv.at[2 * zz + c]
        right = remote(src, spot, self.send_r.at[t], sem, self.place.at(jnp.minimum(z + 1, 3), c))
        left = remote(src, spot, self.send_l.at[t], sem, self.place.at(jnp.maximum(z - 1, 0), c))
        partner = remote(src, spot, self.send_p.at[2 * t + way], sem, self.place.at(z, 1 - c))
        return right, left, partner

    def start(self, later):
        z, c = self.place.z, self.place.c
        right, left, partner = self.copies(self.block, z, 0, 0)
        pl.when(z < 3)(right.start)
        pl.when(z > 0)(left.start)
        later.add(right.wait_send, z < 3)
        later.add(left.wait_send, z > 0)
        if self.both:
            partner.start()
            later.add(partner.wait_send)
        keep = pltpu.make_async_copy(self.block, self.full.at[2 * z + c], self.keep.at[0])
        keep.start()
        keep.wait()
        for t in range(1, 4):
            for way in (0, 1):
                zz, valid, onward, may, partner = self.step(t, way)
                later.add(onward.wait_send, valid & may)
                if self.both:
                    later.add(partner.wait_send, valid)

    def step(self, t, way):
        z = self.place.z
        there = z + (2 * way - 1) * t
        zz = jnp.clip(there, 0, 3)
        right, left, partner = self.copies(self.full.at[2 * zz + self.place.c], zz, t, way)
        onward, may = (left, z > 0) if way else (right, z < 3)
        return zz, (there >= 0) & (there <= 3), onward, may, partner

    def pass_on(self, t):
        for way in (0, 1):
            _, valid, onward, may, partner = self.step(t, way)

            @pl.when(valid)
            def _(onward=onward, may=may, partner=partner):
                onward.wait_recv()
                pl.when(may)(onward.start)
                if self.both:
                    partner.start()

    def chunk(self, p):
        z, c = self.place.z, self.place.c
        edge = (z == 0) | (z == 3)
        t = jnp.where(edge, p, (p + 1) // 2)
        pl.when((p >= 1) & (edge | (p != 2)))(lambda: self.pass_on(t))
        second = jnp.where(z == 0, 1, z - 1)
        third = jnp.where(z == 0, 2, jnp.where(z == 3, 1, z + 1))
        fourth = jnp.where(z <= 1, 3, 0)
        j = jnp.where(p == 0, z, jnp.where(p == 1, second, jnp.where(p == 2, third, fourth)))
        if self.both:
            spot = self.full.at[2 * j + 1 - c]
            remote(spot, spot, self.send_p.at[0], self.recv.at[2 * j + 1 - c], self.place.at(z, 1 - c)).wait_recv()
        return j


def forward_feed(names, block, w_gate, w_up, w_down, cargo, name):
    tokens, width = block.shape
    inner = w_gate.shape[1]

    def body(place, ins, outs, scratch, later, middle, start):
        block_ref, gate_hbm, up_hbm, down_hbm = ins
        total, full_out, gate_out, up_out = outs
        n = len(Gather.scratch)
        gather_sems, scratch = scratch[:n], scratch[n:]
        full, part, gate_w, up_w, down_w, gates, ups, load_sem, keep_sem = scratch[:9]
        from_p, from_r, from_l, held, *sems = scratch[9:]
        gather = Gather(place, block_ref, full, gather_sems)
        loads = [
            pltpu.make_async_copy(src, dst, load_sem.at[i])
            for i, (src, dst) in enumerate(((gate_hbm, gate_w), (up_hbm, up_w), (down_hbm, down_w)))
        ]
        for load in loads:
            load.start()
        gather.start(later)
        for load in loads:
            load.wait()

        def keep(j):
            rows = pl.ds(pl.multiple_of(2 * tokens * j, 2 * tokens), 2 * tokens)
            return [
                pltpu.make_async_copy(full.at[pl.ds(2 * j, 2)], full_out.at[pl.ds(2 * j, 2)], keep_sem.at[0, j]),
                pltpu.make_async_copy(gates.at[rows, :], gate_out.at[rows, :], keep_sem.at[1, j]),
                pltpu.make_async_copy(ups.at[rows, :], up_out.at[rows, :], keep_sem.at[2, j]),
            ]

        def step(p, carry):
            j = gather.chunk(p)
            pl.when(p == 2)(middle)
            acts = full[pl.ds(2 * j, 2)].reshape(2 * tokens, width)
            rows = pl.ds(pl.multiple_of(2 * tokens * j, 2 * tokens), 2 * tokens)
            gate = jnp.dot(acts, gate_w[...], preferred_element_type=F32)
            up = jnp.dot(acts, up_w[...], preferred_element_type=F32)
            gates[rows, :] = gate.astype(LOW)
            ups[rows, :] = up.astype(LOW)
            hidden = (gate * jax.nn.sigmoid(gate) * up).astype(LOW)
            sums = jnp.dot(hidden, down_w[...], preferred_element_type=F32).astype(LOW)
            part[pl.ds(2 * j, 2)] = sums.reshape(2, tokens, width)
            pair_copy(place, part, from_p, sems, j).start()
            for copy in keep(j):
                copy.start()
            return carry

        lax.fori_loop(0, 4, step, 0)
        start(1)
        reduce_line(place, part, total, from_p, from_r, from_l, held, sems, later, True, lambda: middle(1), sent=True)
        for j in range(4):
            for copy in keep(j):
                copy.wait()

    (total, full, gate, up), loads = carry_call(
        names,
        body,
        "line",
        [block, w_gate, w_up, w_down],
        [ONCHIP, ANY, ANY, ANY],
        [
            jax.ShapeDtypeStruct((tokens, width), F32),
            jax.ShapeDtypeStruct((8, tokens, width), LOW),
            jax.ShapeDtypeStruct((8 * tokens, inner), LOW),
            jax.ShapeDtypeStruct((8 * tokens, inner), LOW),
        ],
        [ONCHIP, ANY, ANY, ANY],
        [
            *Gather.scratch,
            pltpu.VMEM((8, tokens, width), LOW),
            pltpu.VMEM((8, tokens, width), LOW),
            pltpu.VMEM(w_gate.shape, LOW),
            pltpu.VMEM(w_up.shape, LOW),
            pltpu.VMEM(w_down.shape, LOW),
            pltpu.VMEM((8 * tokens, inner), LOW),
            pltpu.VMEM((8 * tokens, inner), LOW),
            pltpu.SemaphoreType.DMA((3,)),
            pltpu.SemaphoreType.DMA((3, 4)),
            *[pltpu.VMEM((4, tokens, width), LOW)] * 4,
            *[pltpu.SemaphoreType.DMA((4,))] * 5,
        ],
        cargo,
        name=name,
        vmem=58,
    )
    return total, full.reshape(8 * tokens, width), gate, up, loads


def stages_call(names, stages, name=None):
    cargo = [item for stage in stages for item in stage]
    arrays, outs, scratch = [], [], []
    for item in cargo:
        arrays += [a for a in item.arrays if not isinstance(a, From)]
        outs += item.outs
        scratch += item.scratch
    n_in, n_out = len(arrays), len(outs)

    def kernel(*refs):
        ins, made, held = list(refs[:n_in]), list(refs[n_in : n_in + n_out]), list(refs[n_in + n_out :])
        place = Place()
        greet(place, {item.reach for item in cargo})
        out_refs = {}
        last = Later()
        for stage in stages:
            later = Later()
            begun = []
            for item in stage:
                mine = [out_refs[a.item][a.at] if isinstance(a, From) else ins.pop(0) for a in item.arrays]
                out_refs[item] = [made.pop(0) for _ in item.outs]
                kept = [held.pop(0) for _ in item.scratch]
                begun.append((item, mine, out_refs[item], kept, last if item.slow else later))
            for item, *theirs in begun:
                item.start(place, *theirs)
            for item, *theirs in begun:
                item.middle(place, *theirs[:3])
            later.run()
        last.run()

    results = list(
        pl.pallas_call(
            kernel,
            out_shape=outs,
            in_specs=[ANY] * n_in,
            out_specs=[ANY] * n_out,
            scratch_shapes=scratch,
            compiler_params=pltpu.CompilerParams(
                collective_id=names.take(), has_side_effects=True, vmem_limit_bytes=40 * 2**20
            ),
            name=name,
        )(*arrays)
    )
    loads = []
    for item in cargo:
        loads.append([results.pop(0) for _ in item.outs])
    return loads


class From:
    def __init__(self, item, at=0):
        self.item, self.at = item, at
        self.shape, self.dtype = item.outs[at].shape, item.outs[at].dtype


eps_norm = 1e-06
rope_base = 1000000.0
neg_fill = -1e30


def row_starts(sizes, count):
    ends = jnp.cumsum(sizes)
    firsts = ends - sizes
    places = jnp.arange(count, dtype=jnp.int32)
    inside = (places[None, :] >= firsts[:, None]) & (places[None, :] < ends[:, None])
    return jnp.sum(jnp.where(inside, firsts[:, None], 0), axis=0)


def rope_tables(positions):
    half = HD // 2
    freq = rope_base ** (-(jnp.arange(half, dtype=jnp.float32) * (2.0 / HD)))
    angle = freq[:, None] * positions.astype(jnp.float32)[None, :]
    cosine = jnp.concatenate([jnp.cos(angle), jnp.cos(angle)], axis=0)
    sine = jnp.concatenate([jnp.sin(angle), jnp.sin(angle)], axis=0)
    return (cosine, sine)


def rotate(values, cosine, sine):
    half = HD // 2
    turned = jnp.concatenate([-values[:, half:], values[:, :half]], axis=1)
    return values * cosine + turned * sine


def rotate_back(grads, cosine, sine):
    half = HD // 2
    lifted = grads * sine
    turned = jnp.concatenate([lifted[:, half:], -lifted[:, :half]], axis=1)
    return grads * cosine + turned


def contract_first(left, right):
    return lax.dot_general(
        left, right, (((0,), (0,)), ((), ())), preferred_element_type=jnp.float32
    )


def contract_last(left, right):
    return lax.dot_general(
        left, right, (((1,), (1,)), ((), ())), preferred_element_type=jnp.float32
    )


def feature_total(values):
    return lax.psum(jnp.sum(values, axis=0), "col")


def spread(values):
    return lax.all_gather(values, "col", axis=0, tiled=True)


def summed_rows(make_term, rows):
    return lax.psum_scatter(
        make_term(jnp.int32(0), lax.axis_size("col") * rows), "col", scatter_dimension=0, tiled=True
    )


def to_blocks(values):
    return lax.all_to_all(values, "col", split_axis=1, concat_axis=0, tiled=True)


def to_tokens(values):
    return lax.all_to_all(values, "col", split_axis=0, concat_axis=1, tiled=True)


def by_columns(weight, acts, start, count):
    return contract_first(weight, acts)


def by_rows(weight, grads, start, count):
    return jnp.dot(weight, grads, preferred_element_type=jnp.float32)


def by_rows_pair(first_weight, first_grads, second_weight, second_grads, start, count):
    return by_rows(first_weight, first_grads, start, count) + by_rows(
        second_weight, second_grads, start, count
    )


def norm_forward(residual, gain):
    totals = feature_total(residual * residual)
    scale = lax.rsqrt(totals / D + eps_norm)
    return (scale, (residual * scale * gain[:, None]).astype(jnp.bfloat16))


def norm_backward(d_normed, residual, scale, gain):
    weighted = d_normed * gain[:, None]
    inner = feature_total(weighted * residual)
    d_residual = weighted * scale - residual * (scale * scale * scale) * inner / D
    d_gain = jnp.sum(d_normed * residual * scale, axis=1)
    return (d_residual, d_gain)


def attend_scores(queries, keys, mask):
    scores = jnp.einsum(
        "kghq,khj->kgqj", queries, keys, preferred_element_type=jnp.float32
    ) * HD ** (-0.5)
    return jnp.where(mask[None, None], scores, neg_fill)


def per_device(
    hidden_states,
    out_grad,
    lengths,
    norm_gains,
    qkv_weight,
    qkv_bias,
    out_weight,
    gate_weight,
    up_weight,
    down_weight,
):
    feat_rows, tok_row = hidden_states.shape
    col_at = lax.axis_index("col")
    starts = row_starts(lengths[0], tok_row)
    positions = jnp.arange(tok_row, dtype=jnp.int32) - starts
    cosine, sine = rope_tables(positions)
    first = col_at * QB
    block_starts = lax.dynamic_slice_in_dim(starts, first, QB)
    cos_block = lax.dynamic_slice_in_dim(cosine, first, QB, 1)
    sin_block = lax.dynamic_slice_in_dim(sine, first, QB, 1)
    reach = QB + SEQ_MAX
    window = jnp.maximum(first - SEQ_MAX, 0)
    key_places = window + jnp.arange(reach, dtype=jnp.int32)
    query_places = first + jnp.arange(QB, dtype=jnp.int32)
    mask = (key_places[None, :] >= block_starts[:, None]) & (
        key_places[None, :] <= query_places[:, None]
    )
    group = HEADS // KV_HEADS
    rotary = HEADS + KV_HEADS
    query_rows = HEADS * HD
    kv_rows = KV_HEADS * HD
    gains = norm_gains.astype(jnp.float32)
    residual = hidden_states.astype(jnp.float32)
    saved = []
    for layer in range(LAYERS):
        w_qkv, b_qkv, w_out, w_gate, w_up, w_down = (
            lax.all_gather(qkv_weight[layer], "row", axis=0, tiled=True),
            lax.all_gather(qkv_bias[layer], "row", axis=1, tiled=True),
            lax.all_gather(out_weight[layer], "row", axis=1, tiled=True),
            lax.all_gather(gate_weight[layer], "row", axis=0, tiled=True),
            lax.all_gather(up_weight[layer], "row", axis=0, tiled=True),
            lax.all_gather(down_weight[layer], "row", axis=1, tiled=True),
        )
        scale_one, normed_one = norm_forward(residual, gains[layer, 0])
        full_one = spread(normed_one)
        raw = contract_first(w_qkv, full_one) + b_qkv.reshape(-1).astype(jnp.float32)[:, None]
        local_heads = raw.shape[0] // HD
        shaped = raw.reshape(local_heads, HD, tok_row)
        head_ids = col_at * local_heads + jnp.arange(local_heads)
        turned = jnp.where((head_ids < rotary)[:, None, None], rotate(shaped, cosine, sine), shaped)
        blocked = to_blocks(turned.reshape(raw.shape).astype(jnp.bfloat16))
        kv_full = lax.all_gather(blocked[query_rows:], "col", axis=1, tiled=True)
        kv_window = lax.dynamic_slice_in_dim(kv_full, window, reach, 1)
        queries = blocked[:query_rows].reshape(KV_HEADS, group, HD, QB)
        keys = kv_window[:kv_rows].reshape(KV_HEADS, HD, reach)
        values = kv_window[kv_rows:].reshape(KV_HEADS, HD, reach)
        masked = attend_scores(queries, keys, mask)
        row_top = jnp.max(masked, axis=-1, keepdims=True)
        lifted = jnp.exp(masked - row_top)
        row_mass = jnp.sum(lifted, axis=-1, keepdims=True)
        probs = lifted / row_mass
        log_mass = row_top + jnp.log(row_mass)
        mixed = (
            jnp.einsum(
                "kgqj,khj->kghq",
                probs.astype(jnp.bfloat16),
                values,
                preferred_element_type=jnp.float32,
            )
            .reshape(query_rows, QB)
            .astype(jnp.bfloat16)
        )
        carried = to_tokens(mixed)
        attention = summed_rows(partial(by_columns, w_out, carried), feat_rows)
        residual_mid = residual + attention
        scale_two, normed_two = norm_forward(residual_mid, gains[layer, 1])
        full_two = spread(normed_two)
        gate = contract_first(w_gate, full_two)
        up = contract_first(w_up, full_two)
        hidden = (gate * jax.nn.sigmoid(gate) * up).astype(jnp.bfloat16)
        feed = summed_rows(partial(by_columns, w_down, hidden), feat_rows)
        saved.append(
            (
                residual,
                scale_one,
                full_one,
                blocked,
                kv_window,
                log_mass,
                mixed,
                carried,
                residual_mid,
                scale_two,
                full_two,
                gate,
                up,
                hidden,
                (w_qkv, w_out, w_gate, w_up, w_down),
                local_heads,
            )
        )
        residual = residual_mid + feed
    out_states = residual.astype(jnp.bfloat16)
    grad = out_grad.astype(jnp.float32)
    layer_grads = [None] * LAYERS
    gain_terms = [None] * LAYERS
    for layer in reversed(range(LAYERS)):
        (
            residual_in,
            scale_one,
            full_one,
            blocked,
            kv_window,
            log_mass,
            mixed,
            carried,
            residual_mid,
            scale_two,
            full_two,
            gate,
            up,
            hidden,
            weights_full,
            local_heads,
        ) = saved[layer]
        w_qkv, w_out, w_gate, w_up, w_down = weights_full
        grad_full = spread(grad.astype(jnp.bfloat16))
        d_down = contract_last(hidden, grad_full)
        d_hidden = jnp.dot(w_down, grad_full, preferred_element_type=jnp.float32)
        squash = jax.nn.sigmoid(gate)
        d_gate = (d_hidden * up * squash * (1.0 + gate * (1.0 - squash))).astype(jnp.bfloat16)
        d_up = (d_hidden * gate * squash).astype(jnp.bfloat16)
        d_gate_w = contract_last(full_two, d_gate)
        d_up_w = contract_last(full_two, d_up)
        d_normed_two = summed_rows(partial(by_rows_pair, w_gate, d_gate, w_up, d_up), feat_rows)
        d_residual, d_gain_two = norm_backward(
            d_normed_two, residual_mid, scale_two, gains[layer, 1]
        )
        grad = grad + d_residual
        grad_full = spread(grad.astype(jnp.bfloat16))
        d_out_w = contract_last(carried, grad_full)
        d_mixed = to_blocks(
            jnp.dot(w_out, grad_full, preferred_element_type=jnp.float32).astype(jnp.bfloat16)
        )
        queries = blocked[:query_rows].reshape(KV_HEADS, group, HD, QB)
        keys = kv_window[:kv_rows].reshape(KV_HEADS, HD, reach)
        values = kv_window[kv_rows:].reshape(KV_HEADS, HD, reach)
        masked = attend_scores(queries, keys, mask)
        probs = jnp.exp(masked - log_mass)
        low_probs = probs.astype(jnp.bfloat16)
        d_heads_mix = d_mixed.reshape(KV_HEADS, group, HD, QB)
        d_probs = jnp.einsum(
            "kghq,khj->kgqj", d_heads_mix, values, preferred_element_type=jnp.float32
        )
        inner = jnp.sum(probs * d_probs, axis=-1, keepdims=True)
        d_scores = (probs * (d_probs - inner)).astype(jnp.bfloat16)
        d_queries = (
            jnp.einsum("kgqj,khj->kghq", d_scores, keys, preferred_element_type=jnp.float32)
            * HD ** (-0.5)
        ).reshape(query_rows, QB)
        d_keys = (
            jnp.einsum("kgqj,kghq->khj", d_scores, queries, preferred_element_type=jnp.float32)
            * HD ** (-0.5)
        ).reshape(kv_rows, reach)
        d_values = jnp.einsum(
            "kgqj,kghq->khj", low_probs, d_heads_mix, preferred_element_type=jnp.float32
        ).reshape(kv_rows, reach)
        d_window = jnp.concatenate([d_keys, d_values], axis=0)
        d_placed = lax.dynamic_update_slice_in_dim(
            jnp.zeros((2 * kv_rows, tok_row), jnp.float32), d_window, window, 1
        )
        d_kv = lax.psum_scatter(d_placed, "col", scatter_dimension=1, tiled=True)
        d_heads = jnp.concatenate([d_queries, d_kv], axis=0).reshape(HEADS + 2 * KV_HEADS, HD, QB)
        d_turned = jnp.concatenate(
            [rotate_back(d_heads[:rotary], cos_block, sin_block), d_heads[rotary:]], axis=0
        )
        d_raw = to_tokens(d_turned.reshape((HEADS + 2 * KV_HEADS) * HD, QB).astype(jnp.bfloat16))
        d_bias = jnp.sum(d_raw, axis=1, dtype=jnp.float32).reshape(local_heads, HD)
        d_qkv_w = contract_last(full_one, d_raw)
        d_normed_one = summed_rows(partial(by_rows, w_qkv, d_raw), feat_rows)
        d_residual, d_gain_one = norm_backward(
            d_normed_one, residual_in, scale_one, gains[layer, 0]
        )
        grad = grad + d_residual
        layer_grads[layer] = (
            lax.psum_scatter(d_qkv_w, "row", scatter_dimension=0, tiled=True),
            lax.psum_scatter(d_bias, "row", scatter_dimension=1, tiled=True),
            lax.psum_scatter(d_out_w, "row", scatter_dimension=1, tiled=True),
            lax.psum_scatter(d_gate_w, "row", scatter_dimension=0, tiled=True),
            lax.psum_scatter(d_up_w, "row", scatter_dimension=0, tiled=True),
            lax.psum_scatter(d_down, "row", scatter_dimension=1, tiled=True),
        )
        gain_terms[layer] = jnp.stack([d_gain_one, d_gain_two])
    gain_grads = lax.psum(jnp.stack(gain_terms), "row")
    stacked = [jnp.stack([entry[member] for entry in layer_grads]) for member in range(6)]
    return (
        out_states,
        grad,
        gain_grads,
        stacked[0],
        stacked[1],
        stacked[2],
        stacked[3],
        stacked[4],
        stacked[5],
    )


def softmax_scores(queries, keys, mask):
    scores = jnp.einsum("htd,ud->htu", queries, keys, preferred_element_type=F32) * HD ** (-0.5)
    return jnp.where(mask[None], scores, neg_fill)


def dot(a, b):
    return jnp.dot(a, b, preferred_element_type=F32)


def dot_t(a, b):
    return lax.dot_general(a, b, (((1,), (1,)), ((), ())), preferred_element_type=F32)


def t_dot(a, b):
    return lax.dot_general(a, b, (((0,), (0,)), ((), ())), preferred_element_type=F32)


def turn(values, cosine, sine):
    half = HD // 2
    turned = jnp.concatenate([-values[..., half:], values[..., :half]], axis=-1)
    return values * cosine + turned * sine


def turn_back(grads, cosine, sine):
    half = HD // 2
    lifted = grads * sine
    turned = jnp.concatenate([lifted[..., half:], -lifted[..., :half]], axis=-1)
    return grads * cosine + turned


def norm_on(residual, gain):
    scale = lax.rsqrt(jnp.mean(residual * residual, axis=1, keepdims=True) + eps_norm)
    return scale, (residual * scale * gain[None, :]).astype(LOW)


def norm_back(d_normed, residual, scale, gain):
    weighted = d_normed * gain[None, :]
    inner = jnp.sum(weighted * residual, axis=1, keepdims=True)
    d_residual = weighted * scale - residual * (scale * scale * scale) * inner / D
    d_gain = jnp.sum(d_normed * residual * scale, axis=0)
    return d_residual, d_gain


def per_device_line(
    hidden_states,
    out_grad,
    lengths,
    norm_gains,
    qkv_weight,
    qkv_bias,
    out_weight,
    gate_weight,
    up_weight,
    down_weight,
):
    names = Names()
    tok_row = hidden_states.shape[1]
    row_at = lax.axis_index("row")
    col_at = lax.axis_index("col")
    core = col_at % 2
    starts = row_starts(lengths[0], tok_row)
    places = jnp.arange(tok_row, dtype=jnp.int32)
    cosine, sine = rope_tables(places - starts)
    cosine, sine = cosine.T[:, None], sine.T[:, None]

    def own(values):
        cut = values.reshape(4, 2, QB, *values.shape[1:])
        return lax.dynamic_index_in_dim(cut, core, 1, keepdims=False).reshape(4 * QB, *values.shape[1:])

    mask = (places[None, :] >= own(starts)[:, None]) & (places[None, :] <= own(places)[:, None])

    def head_tiles(layer):
        biases = jnp.zeros((2, 1, 16, HD), LOW)
        biases = lax.dynamic_update_slice(biases, qkv_bias[layer][:, None, None], (0, 0, 0, row_at * (HD // 4)))
        tiles = qkv_weight[layer].reshape(2, D // 8, 2, HD).transpose(2, 0, 1, 3)
        return jnp.concatenate([tiles, jnp.broadcast_to(biases, (2, 2, 16, HD))], axis=2)

    def slab_of(mine, theirs, out_mine, out_theirs):
        first, second = jnp.where(core == 0, mine, theirs), jnp.where(core == 0, theirs, mine)
        both = jnp.stack([first.reshape(4, HALF, 5 * HD), second.reshape(4, HALF, 5 * HD)], axis=1)
        w_qkv = both[:, :, : D // 8].reshape(D, 5 * HD)
        bias = jnp.sum(both[:, 0, D // 8].astype(F32), axis=0)
        w_out = jnp.concatenate(
            [jnp.where(core == 0, out_mine, out_theirs), jnp.where(core == 0, out_theirs, out_mine)], axis=0
        )
        return w_qkv, bias, w_out

    arrivals = jnp.concatenate(
        [
            hidden_states.T.reshape(8, QB, D // 8),
            out_grad.T.reshape(8, QB, D // 8),
            jnp.broadcast_to(
                jnp.pad(norm_gains.reshape(2 * LAYERS, D // 8), ((0, 16 - 2 * LAYERS), (0, 0))), (8, 16, D // 8)
            ),
        ],
        axis=1,
    )
    spread = Exchange(arrivals)
    spread.slow = True
    to_chips = [HeadsToChips(head_tiles(layer)) for layer in range(LAYERS)]
    to_chips[1].slow = True
    slab_rows, out_rows = GatherRows(From(to_chips[0]), 0), GatherRows(out_weight[0], 1)
    swap = Swap(From(slab_rows), From(out_rows))
    loads = stages_call(
        names, [[to_chips[0]], [slab_rows, out_rows, spread, to_chips[1]], [swap]], name="open"
    )
    (_,), (mine,), (out_mine,), (came,), (slab_next,), (theirs, out_theirs) = loads
    load = (mine, theirs, out_mine, out_theirs)
    came = came.transpose(1, 0, 2).reshape(2 * QB + 16, D)
    residual = came[:QB].astype(F32)
    grad = came[QB : 2 * QB].astype(F32)
    gains = came[2 * QB : 2 * QB + 2 * LAYERS].astype(F32).reshape(LAYERS, 2, D)

    def weights_in(layer):
        return [GatherRows(gate_weight[layer], 0), GatherRows(up_weight[layer], 0), GatherRows(down_weight[layer], 1)]

    sent = weights_in(0)
    grad_full_last, ((w_gate,),) = gather_tokens(names, grad.astype(LOW), sent[:1], name="gather_three_1")
    saved = []
    for layer in range(LAYERS):
        if layer == 1:
            mine, out_mine, (w_gate,) = load
        scale_one, normed_one = norm_on(residual, gains[layer, 0])
        if layer == 0:
            normed_one, _ = lax.optimization_barrier((normed_one, grad_full_last))
        cargo = [sent[1]] if layer == 0 else [sent[1], Swap(mine, out_mine)]
        full_one, loads = gather_tokens(names, normed_one, cargo, name=f"gather_one_{layer}")
        w_up = loads[0][0]
        if layer == 1:
            load = (mine, loads[1][0], out_mine, loads[1][1])
        w_qkv, bias, w_out = slab_of(*load)
        raw = (dot(full_one, w_qkv) + bias[None]).reshape(tok_row, 5, HD)
        turned = jnp.concatenate([turn(raw[:, :4], cosine, sine), raw[:, 4:]], axis=1).astype(LOW)
        queries = own(turned[:, :3]).transpose(1, 0, 2)
        keys, values = turned[:, 3], turned[:, 4]
        masked = softmax_scores(queries, keys, mask)
        row_top = jnp.max(masked, axis=-1, keepdims=True)
        lifted = jnp.exp(masked - row_top)
        row_mass = jnp.sum(lifted, axis=-1, keepdims=True)
        probs = (lifted / row_mass).astype(LOW)
        log_mass = row_top + jnp.log(row_mass)
        mixed = jnp.einsum("htu,ud->thd", probs, values, preferred_element_type=F32)
        mixed = mixed.astype(LOW).reshape(4 * QB, 3 * HD)
        attention, ((w_down,),) = reduce_tokens(
            names, dot(mixed, w_out).astype(LOW), [sent[2]], both=False, name=f"reduce_one_{layer}"
        )
        residual_mid = residual + attention
        scale_two, normed_two = norm_on(residual_mid, gains[layer, 1])
        cargo = []
        if layer == 0:
            sent = weights_in(1)
            cargo = sent[:1]
        if layer == 0:
            slab_rows, out_rows = GatherRows(slab_next, 0), GatherRows(out_weight[1], 1)
            sent[0].phase = 1
            cargo = [slab_rows, out_rows, sent[0]]
        feed, full_two, gate, up, loads = forward_feed(
            names, normed_two, w_gate, w_up, w_down, cargo, name=f"feed_{layer}"
        )
        saved.append(
            (
                residual,
                scale_one,
                full_one,
                queries,
                keys,
                values,
                log_mass,
                mixed,
                residual_mid,
                scale_two,
                full_two,
                gate,
                up,
                (w_qkv, w_out, w_gate, w_up, w_down),
            )
        )
        residual = residual_mid + feed
        if layer == 0:
            load = (loads[0][0], loads[1][0], loads[2])
    states = residual.astype(LOW)

    def own_part(full, dim):
        size = full.shape[dim] // 4
        return lax.dynamic_slice_in_dim(full, row_at * size, size, dim)

    def settle(full, dim, slots):
        return jnp.sum(slots.astype(F32), axis=0) + own_part(full, dim).astype(F32)

    def settle_heads(tiles):
        total = tiles[:, :, 0].astype(F32) + jnp.where(col_at >= 6, tiles[:, :, 1].astype(F32), 0.0)
        weight = total[:, :, : D // 8].transpose(1, 2, 0, 3).reshape(D // 4, 2 * HD)
        bias = lax.dynamic_slice_in_dim(total[:, 0, D // 8], row_at * (HD // 4), HD // 4, 1)
        return weight, bias

    grads = {}
    gain_terms = [None] * LAYERS
    waiting = None
    for layer in reversed(range(LAYERS)):
        (
            residual_in,
            scale_one,
            full_one,
            queries,
            keys,
            values,
            log_mass,
            mixed,
            residual_mid,
            scale_two,
            full_two,
            gate,
            up,
            (w_qkv, w_out, w_gate, w_up, w_down),
        ) = saved[layer]
        gate, up = gate.astype(F32), up.astype(F32)
        hidden = (gate * jax.nn.sigmoid(gate) * up).astype(LOW)
        if layer == LAYERS - 1:
            grad_full = grad_full_last
        else:
            grad_full, loads = gather_tokens(
                names,
                grad.astype(LOW),
                [ScatterRows(waiting[0], 0), ScatterRows(waiting[1], 1)],
                name=f"gather_three_{layer}",
            )
            slab_sum = settle(waiting[0], 0, loads[0][0]).astype(LOW)
            grads["out", layer + 1] = settle(waiting[1], 1, loads[1][0])
        d_down = t_dot(hidden, grad_full).astype(LOW)
        d_hidden = dot_t(grad_full, w_down)
        squash = jax.nn.sigmoid(gate)
        d_gate = (d_hidden * up * squash * (1.0 + gate * (1.0 - squash))).astype(LOW)
        d_up = (d_hidden * gate * squash).astype(LOW)
        d_normed = (dot_t(d_gate, w_gate) + dot_t(d_up, w_up)).astype(LOW)
        cargo = [ScatterRows(d_down, 1)]
        if layer < LAYERS - 1:
            cargo.append(HeadsToOwners(slab_sum))
        d_normed_two, loads = reduce_tokens(names, d_normed, cargo, name=f"reduce_three_{layer}")
        if layer < LAYERS - 1:
            grads["qkv", layer + 1] = settle_heads(loads[1][0])
        grads["down", layer] = settle(d_down, 1, loads[0][0])
        d_gate_w = t_dot(full_two, d_gate).astype(LOW)
        d_up_w = t_dot(full_two, d_up).astype(LOW)
        d_residual, d_gain_two = norm_back(d_normed_two, residual_mid, scale_two, gains[layer, 1])
        grad = grad + d_residual
        grad_own, loads = gather_tokens(
            names, grad.astype(LOW), [ScatterRows(d_gate_w, 0)], both=False, name=f"gather_four_{layer}"
        )
        grads["gate", layer] = settle(d_gate_w, 0, loads[0][0])
        d_out_w = t_dot(mixed, grad_own).astype(LOW)
        d_mixed = dot_t(grad_own, w_out).astype(LOW).reshape(4 * QB, 3, HD).transpose(1, 0, 2)
        masked = softmax_scores(queries, keys, mask)
        probs = jnp.exp(masked - log_mass)
        d_probs = jnp.einsum("htd,ud->htu", d_mixed, values, preferred_element_type=F32)
        inner = jnp.sum(probs * d_probs, axis=-1, keepdims=True)
        d_scores = (probs * (d_probs - inner)).astype(LOW)
        d_queries = jnp.einsum("htu,ud->thd", d_scores, keys, preferred_element_type=F32) * HD ** (-0.5)
        d_keys = jnp.einsum("htu,htd->ud", d_scores, queries, preferred_element_type=F32) * HD ** (-0.5)
        d_values = jnp.einsum("htu,htd->ud", probs.astype(LOW), d_mixed, preferred_element_type=F32)
        d_raw_q = turn_back(d_queries, own(cosine), own(sine)).astype(LOW).reshape(4, QB, 3 * HD)
        mine = (jnp.arange(2) == core)[None, :, None, None]
        d_raw_q = jnp.where(mine, d_raw_q[:, None], jnp.zeros((), LOW)).reshape(tok_row, 3 * HD)
        d_raw_k = turn_back(d_keys, cosine[:, 0], sine[:, 0]).astype(LOW)
        d_raw = jnp.concatenate([d_raw_q, d_raw_k, d_values.astype(LOW)], axis=1)
        d_bias = jnp.sum(d_raw, axis=0, dtype=F32).astype(LOW)
        d_qkv_w = t_dot(full_one, d_raw).astype(LOW).reshape(4, 2, D // 8, 5 * HD)
        tail = jnp.broadcast_to(jnp.pad(d_bias[None], ((0, 15), (0, 0))), (4, 2, 16, 5 * HD))
        d_slab = jnp.concatenate([d_qkv_w, tail], axis=2)
        d_out_w = d_out_w.reshape(2, D // 8, D)

        def half(full, dim, which):
            return lax.dynamic_index_in_dim(full, which, dim, keepdims=False)

        d_normed_one, loads = reduce_tokens(
            names,
            dot_t(d_raw, w_qkv).astype(LOW),
            [ScatterRows(d_up_w, 0), Swap(half(d_slab, 1, 1 - core), half(d_out_w, 0, 1 - core))],
            name=f"reduce_four_{layer}",
        )
        grads["up", layer] = settle(d_up_w, 0, loads[0][0])
        slab_part = (half(d_slab, 1, core).astype(F32) + loads[1][0].astype(F32)).astype(LOW)
        out_part = (half(d_out_w, 0, core).astype(F32) + loads[1][1].astype(F32)).astype(LOW)
        waiting = (slab_part.reshape(4 * HALF, 5 * HD), out_part)
        d_residual, d_gain_one = norm_back(d_normed_one, residual_in, scale_one, gains[layer, 0])
        grad = grad + d_residual
        gain_terms[layer] = jnp.stack([d_gain_one, d_gain_two])
    leaving = jnp.concatenate([states, grad.astype(LOW)], axis=0).reshape(2 * QB, 8, D // 8).transpose(1, 0, 2)
    gain_parts = jnp.pad(jnp.stack(gain_terms).reshape(2 * LAYERS, 8, D // 8), ((0, 8 - 2 * LAYERS), (0, 0), (0, 0)))
    (left,), (gain_all,), (slots,), (out_slots,) = stages_call(
        names,
        [
            [
                Exchange(leaving),
                Exchange(gain_parts.transpose(1, 0, 2), every_row=True),
                ScatterRows(waiting[0], 0),
                ScatterRows(waiting[1], 1),
            ]
        ],
        name="close",
    )
    ((tiles,),) = stages_call(names, [[HeadsToOwners(settle(waiting[0], 0, slots).astype(LOW))]], name="close_heads")
    grads["qkv", 0] = settle_heads(tiles)
    grads["out", 0] = settle(waiting[1], 1, out_slots)
    out_states = left[:, :QB].reshape(tok_row, D // 8).T
    input_grad = left[:, QB:].reshape(tok_row, D // 8).T.astype(F32)
    gain_grads = jnp.sum(gain_all, axis=(0, 1))[: 2 * LAYERS].reshape(LAYERS, 2, D // 8)

    def both_layers(kind):
        return jnp.stack([grads[kind, layer] for layer in range(LAYERS)])

    heads = [jnp.stack([grads["qkv", layer][i] for layer in range(LAYERS)]) for i in range(2)]
    return (
        out_states,
        input_grad,
        gain_grads,
        heads[0],
        heads[1],
        both_layers("out"),
        both_layers("gate"),
        both_layers("up"),
        both_layers("down"),
    )


def solution(mesh):
    placed = (
        P("col", "row"),
        P("col", "row"),
        P("row", None),
        P(None, None, "col"),
        P(None, "row", "col"),
        P(None, "col", "row"),
        P(None, "col", "row"),
        P(None, "row", "col"),
        P(None, "row", "col"),
        P(None, "col", "row"),
    )
    on_lines = mesh.shape["row"] == 4 and mesh.shape["col"] == 8
    return jax.shard_map(
        per_device_line if on_lines else per_device,
        mesh=mesh,
        in_specs=placed,
        out_specs=(
            P("col", "row"),
            P("col", "row"),
            P(None, None, "col"),
            P(None, "row", "col"),
            P(None, "col", "row"),
            P(None, "col", "row"),
            P(None, "row", "col"),
            P(None, "row", "col"),
            P(None, "col", "row"),
        ),
        check_vma=False,
    )
```

```python
from functools import partial

import jax
import jax.numpy as jnp
from jax import lax
from jax.experimental import pallas as pl
from jax.experimental.pallas import tpu as pltpu
from jax.sharding import PartitionSpec as P

D = 1536
HEADS = 12
KV_HEADS = 2
HD = 128
LAYERS = 2
SEQ_MAX = 512
QB = 128
MESH = pl.DeviceIdType.MESH
LOW = jnp.bfloat16
F32 = jnp.float32
ANY = pl.BlockSpec(memory_space=pl.ANY)
ONCHIP = pl.BlockSpec(memory_space=pltpu.VMEM)
HALF = 208


class Place:
    def __init__(self):
        self.r = lax.axis_index("row")
        self.k = lax.axis_index("col")
        self.z = self.k // 2
        self.c = self.k % 2

    def at(self, z, c):
        return (self.r, 2 * z + c)

    def rows(self):
        x, y = self.r % 2, self.r // 2
        return (2 * y + (1 - x), 2 * (1 - y) + x, 2 * (1 - y) + (1 - x))


def remote(src, dst, send, recv, device):
    return pltpu.make_async_remote_copy(
        src_ref=src, dst_ref=dst, send_sem=send, recv_sem=recv, device_id=device, device_id_type=MESH
    )


class Later:
    def __init__(self):
        self.todo = []

    def add(self, wait, cond=None):
        self.todo.append((wait, cond))

    def run(self):
        todo, self.todo = self.todo, []
        for wait, cond in todo:
            if cond is None:
                wait()
            else:
                pl.when(cond)(wait)


def greet(place, reach):
    barrier = pltpu.get_barrier_semaphore()

    def hail(device):
        pl.semaphore_signal(barrier, inc=1, device_id=device, device_id_type=MESH)

    if "all" in reach:
        for rr in range(4):
            for kk in range(8):
                pl.when((place.r != rr) | (place.k != kk))(partial(hail, (rr, kk)))
        pl.semaphore_wait(barrier, 31)
        return
    count = 0
    if "rows" in reach:
        for row in place.rows():
            hail((row, place.k))
        count += 3
    if "col" in reach:
        for kk in range(8):
            pl.when(place.k != kk)(partial(hail, (place.r, kk)))
        pl.semaphore_wait(barrier, count + 7)
        return
    hail(place.at(place.z, 1 - place.c))
    count += 1
    if "line" not in reach:
        pl.semaphore_wait(barrier, count)
        return
    pl.when(place.z < 3)(partial(hail, place.at(jnp.minimum(place.z + 1, 3), place.c)))
    pl.when(place.z > 0)(partial(hail, place.at(jnp.maximum(place.z - 1, 0), place.c)))
    edge = (place.z == 0) | (place.z == 3)
    pl.when(edge)(lambda: pl.semaphore_wait(barrier, count + 1))
    pl.when(jnp.logical_not(edge))(lambda: pl.semaphore_wait(barrier, count + 2))


class From:
    def __init__(self, item, at=0):
        self.item, self.at = item, at
        self.shape, self.dtype = item.outs[at].shape, item.outs[at].dtype


class Cargo:
    arrays = ()
    outs = ()
    scratch = ()
    reach = "rows"
    phase = 0
    slow = False

    def middle(self, place, ins, outs, scratch):
        pass


def part_of(ref, dim, row, size):
    cut = pl.ds(pl.multiple_of(row * size, 128 if dim else 16), size)
    return ref.at[:, cut] if dim else ref.at[cut, :]


class GatherRows(Cargo):
    def __init__(self, block, dim, layer=None, phase=0):
        self.dim, self.layer, self.phase = dim, layer, phase
        self.arrays = (block,)
        if layer is not None:
            block = jax.ShapeDtypeStruct(block.shape[1:], block.dtype)
        full = list(block.shape)
        full[dim] *= 4
        self.size = block.shape[dim]
        self.half = block.shape[0] // 32 * 16
        self.rest = block.shape[0] - self.half
        self.outs = (jax.ShapeDtypeStruct(tuple(full), block.dtype),)
        self.scratch = (pltpu.SemaphoreType.DMA((6,)), pltpu.SemaphoreType.DMA((6,)), pltpu.SemaphoreType.DMA((1,)))

    def halves(self, ref):
        return ref.at[0 : self.half, :], ref.at[self.half :, :]

    def spots(self, full, row):
        if self.dim:
            cut = pl.ds(pl.multiple_of(row * self.size, 128), self.size)
            return full.at[0 : self.half, cut], full.at[self.half :, cut]
        first = pl.multiple_of(row * self.size, 16)
        return full.at[pl.ds(first, self.half), :], full.at[pl.ds(first + self.half, self.rest), :]

    def source(self, ins):
        return ins[0] if self.layer is None else ins[0].at[self.layer]

    def copies(self, place, ins, outs, scratch):
        src, (dst,), (send, recv, _) = self.source(ins), outs, scratch
        x, y, d = place.rows()
        block, mine = self.halves(src), self.spots(dst, place.r)
        from_x, from_y = self.spots(dst, x), self.spots(dst, y)
        out = [
            remote(block[0], mine[0], send.at[0], recv.at[0], (x, place.k)),
            remote(block[1], mine[1], send.at[1], recv.at[3], (y, place.k)),
            remote(block[1], mine[1], send.at[2], recv.at[1], (x, place.k)),
            remote(block[0], mine[0], send.at[3], recv.at[2], (y, place.k)),
        ]
        onward = [
            remote(from_x[0], from_x[0], send.at[4], recv.at[4], (y, place.k)),
            remote(from_y[1], from_y[1], send.at[5], recv.at[5], (x, place.k)),
        ]
        return out, onward

    def arrived(self, place, scratch, view, sem, row):
        return remote(view, view, scratch[0].at[0], scratch[1].at[sem], (row, place.k))

    def start(self, place, ins, outs, scratch, later):
        src, (dst,), (_, _, keep_sem) = self.source(ins), outs, scratch
        out, onward = self.copies(place, ins, outs, scratch)
        for copy in out:
            copy.start()
        keep = pltpu.make_async_copy(src, part_of(dst, self.dim, place.r, self.size), keep_sem.at[0])
        keep.start()
        later.add(keep.wait)
        x, y, d = place.rows()
        from_x, from_y, from_d = self.spots(dst, x), self.spots(dst, y), self.spots(dst, d)
        for view, sem, row in ((from_x[1], 1, x), (from_y[0], 2, y), (from_d[0], 4, y), (from_d[1], 5, x)):
            later.add(self.arrived(place, scratch, view, sem, row).wait_recv)
        for copy in (*out, *onward):
            later.add(copy.wait_send)

    def middle(self, place, ins, outs, scratch):
        (dst,) = outs
        x, y, d = place.rows()
        _, onward = self.copies(place, ins, outs, scratch)
        self.arrived(place, scratch, self.spots(dst, x)[0], 0, x).wait_recv()
        onward[0].start()
        self.arrived(place, scratch, self.spots(dst, y)[1], 3, y).wait_recv()
        onward[1].start()


class ScatterRows(Cargo):
    def __init__(self, grad, dim, phase=0):
        self.dim, self.phase = dim, phase
        self.arrays = (grad,)
        part = list(grad.shape)
        part[dim] //= 4
        self.size = part[dim]
        self.half = part[0] // 32 * 16
        self.rest = part[0] - self.half
        self.outs = (jax.ShapeDtypeStruct((2, *part), grad.dtype),)
        upper, lower = pltpu.VMEM((self.half, part[1]), grad.dtype), pltpu.VMEM((self.rest, part[1]), grad.dtype)
        self.scratch = (
            *(upper, lower, lower, upper, lower, upper),
            pltpu.SemaphoreType.DMA((6,)),
            pltpu.SemaphoreType.DMA((6,)),
            pltpu.SemaphoreType.DMA((2,)),
        )

    def spots(self, full, row):
        if self.dim:
            cut = pl.ds(pl.multiple_of(row * self.size, 128), self.size)
            return full.at[0 : self.half, cut], full.at[self.half :, cut]
        first = pl.multiple_of(row * self.size, 16)
        return full.at[pl.ds(first, self.half), :], full.at[pl.ds(first + self.half, self.rest), :]

    def copies(self, place, ins, outs, scratch):
        (src,), (dst,) = ins, outs
        via_x, via_y, own_x, own_y, sum_x, sum_y, send, recv, keep = scratch
        x, y, d = place.rows()
        for_x, for_y, for_d = self.spots(src, x), self.spots(src, y), self.spots(src, d)
        slot_x = dst.at[0, 0 : self.half, :], dst.at[0, self.half :, :]
        slot_y = dst.at[1, 0 : self.half, :], dst.at[1, self.half :, :]
        first = [
            remote(for_d[0], via_x, send.at[0], recv.at[0], (x, place.k)),
            remote(for_d[1], via_y, send.at[1], recv.at[1], (y, place.k)),
            remote(for_x[0], slot_x[0], send.at[2], recv.at[2], (x, place.k)),
            remote(for_y[1], slot_y[1], send.at[3], recv.at[3], (y, place.k)),
        ]
        held = [
            pltpu.make_async_copy(for_x[1], own_x, keep.at[0]),
            pltpu.make_async_copy(for_y[0], own_y, keep.at[1]),
        ]
        last = [
            remote(sum_x, slot_x[1], send.at[4], recv.at[4], (x, place.k)),
            remote(sum_y, slot_y[0], send.at[5], recv.at[5], (y, place.k)),
        ]
        return first, held, last

    def start(self, place, ins, outs, scratch, later):
        first, held, last = self.copies(place, ins, outs, scratch)
        for copy in (*first, *held):
            copy.start()
        for copy in (*first, *last):
            later.add(copy.wait_send)
        for copy in (*first[2:], *last):
            later.add(copy.wait_recv)

    def middle(self, place, ins, outs, scratch):
        via_x, via_y, own_x, own_y, sum_x, sum_y, *_ = scratch
        first, held, last = self.copies(place, ins, outs, scratch)
        held[0].wait()
        first[1].wait_recv()
        add_into(sum_x, [own_x, via_y])
        last[0].start()
        held[1].wait()
        first[0].wait_recv()
        add_into(sum_y, [own_y, via_x])
        last[1].start()


class Swap(Cargo):
    reach = "line"

    def __init__(self, *arrays, phase=0):
        self.arrays, self.phase = arrays, phase
        self.outs = tuple(jax.ShapeDtypeStruct(a.shape, a.dtype) for a in arrays)
        self.scratch = (pltpu.SemaphoreType.DMA((len(arrays),)), pltpu.SemaphoreType.DMA((len(arrays),)))

    def start(self, place, ins, outs, scratch, later):
        send, recv = scratch
        for i, (src, dst) in enumerate(zip(ins, outs)):
            copy = remote(src, dst, send.at[i], recv.at[i], place.at(place.z, 1 - place.c))
            copy.start()
            later.add(copy.wait)


def tile_owner(z, t):
    if t < 3:
        head = 3 * z + t
        return head // 2, head % 2
    return 3 + t, z // 2


class HeadsToChips(Cargo):
    reach = "col"

    def __init__(self, weight, biases, layer):
        self.layer = layer
        self.arrays = (weight, biases)
        self.outs = (jax.ShapeDtypeStruct((HALF, 5 * HD), LOW),)
        self.scratch = (pltpu.SemaphoreType.DMA((2, 2, 2, 2)), pltpu.SemaphoreType.DMA((5, 2)))

    def start(self, place, ins, outs, scratch, later):
        (weight, biases), (slab,), (send, recv) = ins, outs, scratch
        r, k, z, c = place.r, place.k, place.z, place.c
        query = k < 6
        rows = D // 8
        for second in range(2):
            for i in range(2):
                head = 2 * k + i
                chip = jnp.where(query, head // 3, 2 * i + second)
                t = jnp.where(query, head % 3, k - 3)
                cut = pl.ds(pl.multiple_of(t * HD, HD), HD)
                spots = slab.at[0:rows, cut], slab.at[rows:HALF, cut]
                for core in range(2):
                    here = k == 2 * chip + core
                    away = jnp.logical_not(here)
                    if second == 1:
                        here, away = here & (k >= 6), away & (k >= 6)
                    views = (
                        weight.at[self.layer, core * rows : (core + 1) * rows, i * HD : (i + 1) * HD],
                        biases.at[self.layer, i],
                    )
                    for part in range(2):
                        sem = send.at[i, second, core, part]
                        copy = remote(views[part], spots[part], sem, recv.at[t, part], (r, 2 * chip + core))
                        pl.when(away)(copy.start)
                        later.add(copy.wait_send, away)
                        keep = pltpu.make_async_copy(views[part], spots[part], sem)
                        pl.when(here)(keep.start)
                        later.add(keep.wait, here)
        for t in range(5):
            owner, _ = tile_owner(z, t)
            cut = slice(t * HD, (t + 1) * HD)
            for part, spot in enumerate((slab.at[0:rows, cut], slab.at[rows:HALF, cut])):
                came = remote(spot, spot, send.at[0, 0, 0, 0], recv.at[t, part], (r, owner))
                later.add(came.wait_recv, k != owner)


class HeadsToOwners(Cargo):
    reach = "col"

    def __init__(self, slab):
        self.arrays = (slab,)
        self.outs = (jax.ShapeDtypeStruct((2, 2, 2, HALF, HD), LOW),)
        self.scratch = (pltpu.SemaphoreType.DMA((5,)), pltpu.SemaphoreType.DMA((2, 2, 2)))

    def start(self, place, ins, outs, scratch, later):
        (slab,), (tiles,), (send, recv) = ins, outs, scratch
        r, k, z, c = place.r, place.k, place.z, place.c
        for t in range(5):
            owner, i = tile_owner(z, t)
            which = z % 2 if t >= 3 else 0
            view, spot = slab.at[:, t * HD : (t + 1) * HD], tiles.at[i, c, which]
            here = k == owner
            copy = remote(view, spot, send.at[t], recv.at[i, c, which], (r, owner))
            pl.when(jnp.logical_not(here))(copy.start)
            later.add(copy.wait_send, jnp.logical_not(here))
            keep = pltpu.make_async_copy(view, spot, send.at[t])
            pl.when(here)(keep.start)
            later.add(keep.wait, here)
        for i in range(2):
            for which in range(2):
                chip = jnp.where(k < 6, (2 * k + i) // 3, 2 * i + which)
                for core in range(2):
                    wanted = k != 2 * chip + core
                    if which == 1:
                        wanted = wanted & (k >= 6)
                    came = remote(
                        slab.at[:, 0:HD],
                        tiles.at[i, core, which],
                        send.at[0],
                        recv.at[i, core, which],
                        (r, 2 * chip + core),
                    )
                    later.add(came.wait_recv, wanted)


class Exchange(Cargo):
    def __init__(self, chunks, every_row=False, same=False):
        self.arrays = (chunks,)
        self.same = same
        self.rows_too = every_row
        self.reach = "all" if every_row else "col"
        lead = (4,) if every_row else (8,) if same else ()
        self.outs = (jax.ShapeDtypeStruct((*lead, *chunks.shape), chunks.dtype),)
        self.scratch = (pltpu.SemaphoreType.DMA((4, 8)), pltpu.SemaphoreType.DMA((4, 8)))

    def start(self, place, ins, outs, sems, later):
        (src,), (dst,), (send, recv) = ins, outs, sems
        r, k = place.r, place.k
        for rr in range(4) if self.rows_too else (None,):
            to_row = r if rr is None else rr
            for kk in range(8):
                here = (k == kk) if rr is None else (k == kk) & (r == rr)
                mine = dst.at[k] if rr is None else dst.at[r, k]
                theirs = dst.at[kk] if rr is None else dst.at[rr, kk]
                at = 0 if rr is None else rr
                my_at = 0 if rr is None else r
                part = src if self.same else src.at[kk]
                copy = remote(part, mine, send.at[at, kk], recv.at[my_at, k], (to_row, kk))
                pl.when(jnp.logical_not(here))(copy.start)
                later.add(copy.wait_send, jnp.logical_not(here))
                came = remote(part, theirs, send.at[at, kk], recv.at[at, kk], (to_row, kk))
                later.add(came.wait_recv, jnp.logical_not(here))
                keep = pltpu.make_async_copy(part, mine, send.at[at, kk])
                pl.when(here)(keep.start)
                later.add(keep.wait, here)


def add_into(dst, views):
    rows = dst.shape[0]

    def step(i, carry):
        cut = pl.ds(pl.multiple_of(i * 16, 16), 16)
        total = views[0][cut, :].astype(F32)
        for view in views[1:]:
            total = total + view[cut, :].astype(F32)
        dst[cut, :] = total.astype(dst.dtype)
        return carry

    lax.fori_loop(0, rows // 16, step, 0)


def at_two(middle):
    def between(s):
        if s == 2:
            middle(1)

    return between


def pair_copy(place, part, from_p, sems, j):
    return remote(part.at[2 * j + 1 - place.c], from_p.at[j], sems[0].at[j], sems[1].at[j], place.at(place.z, 1 - place.c))


def reduce_line(place, part, out, from_p, from_r, from_l, held, sems, later, both, between, sent=False):
    send_p, recv_p, send, recv_r, recv_l = sems
    z, c = place.z, place.c
    right_at, left_at = place.at(jnp.minimum(z + 1, 3), c), place.at(jnp.maximum(z - 1, 0), c)

    def own(j):
        return part.at[2 * j + c] if both else part.at[j]

    def partner(j):
        return pair_copy(place, part, from_p, sems, j)

    def moving(j, buffer, sem, device):
        return remote(held.at[j], buffer.at[j], send.at[j], sem.at[j], device)

    if both:
        for j in (3, 0, 2, 1):
            copy = partner(j)
            if not sent:
                copy.start()
            later.add(copy.wait_send)

    def terms(j):
        if both:
            partner(j).wait_recv()
            return [own(j), from_p.at[j]]
        return [own(j)]

    for s in range(3):
        if s:
            between(s)
        for go_right in (True, False):
            if go_right:
                j, valid, first = 3 - s + z, z <= s, z == 0
                buffer, sem, device = from_r, recv_r, right_at
            else:
                j, valid, first = s - 3 + z, z >= 3 - s, z == 3
                buffer, sem, device = from_l, recv_l, left_at
            j = jnp.clip(j, 0, 3)
            copy = moving(j, buffer, sem, device)

            @pl.when(valid & first)
            def _(j=j, copy=copy):
                add_into(held.at[j], terms(j))
                copy.start()

            @pl.when(valid & jnp.logical_not(first))
            def _(j=j, copy=copy, buffer=buffer):
                views = terms(j)
                copy.wait_recv()
                add_into(held.at[j], [*views, buffer.at[j]])
                copy.start()

            later.add(copy.wait_send, valid)
    views = terms(z)
    last_r, last_l = moving(z, from_r, recv_r, right_at), moving(z, from_l, recv_l, left_at)

    @pl.when(z == 0)
    def _():
        last_l.wait_recv()
        add_into(out, [*views, from_l.at[z]])

    @pl.when(z == 3)
    def _():
        last_r.wait_recv()
        add_into(out, [*views, from_r.at[z]])

    @pl.when((z > 0) & (z < 3))
    def _():
        last_r.wait_recv()
        last_l.wait_recv()
        add_into(out, [*views, from_r.at[z], from_l.at[z]])


class Names:
    def __init__(self):
        self.next = 0

    def take(self):
        self.next += 1
        return self.next - 1


class Inner:
    def __init__(self, shape, dtype=LOW):
        self.shape, self.dtype = shape, dtype


def given_arrays(item):
    return [a for a in item.arrays if not isinstance(a, (From, Inner))]


def carry_kernel(body, reach, n_in, n_out, n_scratch, cargo, *refs):
    refs = list(refs)

    def pop(n):
        taken = refs[:n]
        del refs[:n]
        return taken

    ins = pop(n_in)
    given = [pop(len(given_arrays(item))) for item in cargo]
    outs = pop(n_out)
    made = {item: pop(len(item.outs)) for item in cargo}
    scratch = pop(n_scratch)
    held = {item: pop(len(item.scratch)) for item in cargo}
    taken = {
        item: [
            made[a.item][a.at] if isinstance(a, From) else a if isinstance(a, Inner) else mine.pop(0)
            for a in item.arrays
        ]
        for item, mine in zip(cargo, given)
    }
    place = Place()
    later = Later()
    owed = [Later() for _ in range(4)]
    greet(place, {reach, *(item.reach for item in cargo)})

    def start(phase, *inner):
        inner = list(inner)
        mine = [item for item in cargo if item.phase == phase]
        for before in sorted({a.item.phase for item in mine for a in item.arrays if isinstance(a, From)}):
            owed[before].run()
        for item in mine:
            taken[item] = [inner.pop(0) if isinstance(a, Inner) else a for a in taken[item]]
            item.start(place, taken[item], made[item], held[item], owed[phase])

    def middle(phase=0):
        for item in cargo:
            if item.phase == phase:
                item.middle(place, taken[item], made[item], held[item])

    start(0)
    body(place, ins, outs, scratch, later, middle, start)
    later.run()
    for waits in owed:
        waits.run()


def carry_call(names, body, reach, arrays, in_specs, outs, out_specs, scratch, cargo, name=None, vmem=40):
    given = [a for item in cargo for a in given_arrays(item)]
    call = pl.pallas_call(
        partial(carry_kernel, body, reach, len(arrays), len(outs), len(scratch), cargo),
        out_shape=[*outs, *(o for item in cargo for o in item.outs)],
        in_specs=[*in_specs, *(ANY for _ in given)],
        out_specs=[*out_specs, *(ANY for item in cargo for _ in item.outs)],
        scratch_shapes=[*scratch, *(s for item in cargo for s in item.scratch)],
        compiler_params=pltpu.CompilerParams(
            collective_id=names.take(), has_side_effects=True, vmem_limit_bytes=vmem * 2**20
        ),
        name=name,
    )
    results = list(call(*arrays, *given))
    main = results[: len(outs)]
    rest = results[len(outs) :]
    loads = []
    for item in cargo:
        loads.append(rest[: len(item.outs)])
        rest = rest[len(item.outs) :]
    return main, loads


class Gather:
    scratch = (
        pltpu.SemaphoreType.DMA((4,)),
        pltpu.SemaphoreType.DMA((4,)),
        pltpu.SemaphoreType.DMA((8,)),
        pltpu.SemaphoreType.DMA((8,)),
        pltpu.SemaphoreType.DMA((1,)),
    )

    def __init__(self, place, block, full, sems, both=True):
        self.place, self.block, self.full, self.both = place, block, full, both
        self.send_r, self.send_l, self.send_p, self.recv, self.keep = sems

    def spot(self, zz, c):
        return self.full.at[2 * zz + c] if self.both else self.full.at[zz]

    def copies(self, src, zz, t, way):
        z, c = self.place.z, self.place.c
        spot, sem = self.spot(zz, c), self.recv.at[2 * zz + c]
        right = remote(src, spot, self.send_r.at[t], sem, self.place.at(jnp.minimum(z + 1, 3), c))
        left = remote(src, spot, self.send_l.at[t], sem, self.place.at(jnp.maximum(z - 1, 0), c))
        partner = remote(src, spot, self.send_p.at[2 * t + way], sem, self.place.at(z, 1 - c))
        return right, left, partner

    def start(self, later):
        z, c = self.place.z, self.place.c
        right, left, partner = self.copies(self.block, z, 0, 0)
        pl.when(z < 3)(right.start)
        pl.when(z > 0)(left.start)
        later.add(right.wait_send, z < 3)
        later.add(left.wait_send, z > 0)
        if self.both:
            partner.start()
            later.add(partner.wait_send)
        keep = pltpu.make_async_copy(self.block, self.spot(z, c), self.keep.at[0])
        keep.start()
        keep.wait()
        for t in range(1, 4):
            for way in (0, 1):
                zz, valid, onward, may, partner = self.step(t, way)
                later.add(onward.wait_send, valid & may)
                if self.both:
                    later.add(partner.wait_send, valid)

    def step(self, t, way):
        z = self.place.z
        there = z + (2 * way - 1) * t
        zz = jnp.clip(there, 0, 3)
        right, left, partner = self.copies(self.spot(zz, self.place.c), zz, t, way)
        onward, may = (left, z > 0) if way else (right, z < 3)
        return zz, (there >= 0) & (there <= 3), onward, may, partner

    def pass_on(self, t):
        for way in (0, 1):
            _, valid, onward, may, partner = self.step(t, way)

            @pl.when(valid)
            def _(onward=onward, may=may, partner=partner):
                onward.wait_recv()
                pl.when(may)(onward.start)
                if self.both:
                    partner.start()

    def chunk(self, p):
        z, c = self.place.z, self.place.c
        edge = (z == 0) | (z == 3)
        t = jnp.where(edge, p, (p + 1) // 2)
        pl.when((p >= 1) & (edge | (p != 2)))(lambda: self.pass_on(t))
        second = jnp.where(z == 0, 1, z - 1)
        third = jnp.where(z == 0, 2, jnp.where(z == 3, 1, z + 1))
        fourth = jnp.where(z <= 1, 3, 0)
        j = jnp.where(p == 0, z, jnp.where(p == 1, second, jnp.where(p == 2, third, fourth)))
        if self.both:
            spot = self.spot(j, 1 - c)
            remote(spot, spot, self.send_p.at[0], self.recv.at[2 * j + 1 - c], self.place.at(z, 1 - c)).wait_recv()
        return j


def forward_feed(names, block, w_gate, w_up, w_down, cargo, name):
    tokens, width = block.shape
    inner = w_gate.shape[1]

    def body(place, ins, outs, scratch, later, middle, start):
        block_ref, gate_hbm, up_hbm, down_hbm = ins
        total, full_out, gate_out, up_out = outs
        n = len(Gather.scratch)
        gather_sems, scratch = scratch[:n], scratch[n:]
        full, part, gate_w, up_w, down_w, gates, ups, load_sem, keep_sem = scratch[:9]
        from_p, from_r, from_l, held, *sems = scratch[9:]
        gather = Gather(place, block_ref, full, gather_sems)
        loads = [
            pltpu.make_async_copy(src, dst, load_sem.at[i])
            for i, (src, dst) in enumerate(((gate_hbm, gate_w), (up_hbm, up_w), (down_hbm, down_w)))
        ]
        for load in loads:
            load.start()
        gather.start(later)
        for load in loads:
            load.wait()

        def keep(j):
            rows = pl.ds(pl.multiple_of(2 * tokens * j, 2 * tokens), 2 * tokens)
            return [
                pltpu.make_async_copy(full.at[pl.ds(2 * j, 2)], full_out.at[pl.ds(2 * j, 2)], keep_sem.at[0, j]),
                pltpu.make_async_copy(gates.at[rows, :], gate_out.at[rows, :], keep_sem.at[1, j]),
                pltpu.make_async_copy(ups.at[rows, :], up_out.at[rows, :], keep_sem.at[2, j]),
            ]

        def step(p, carry):
            j = gather.chunk(p)
            pl.when(p == 2)(middle)
            acts = full[pl.ds(2 * j, 2)].reshape(2 * tokens, width)
            rows = pl.ds(pl.multiple_of(2 * tokens * j, 2 * tokens), 2 * tokens)
            gate = jnp.dot(acts, gate_w[...], preferred_element_type=F32)
            up = jnp.dot(acts, up_w[...], preferred_element_type=F32)
            gates[rows, :] = gate.astype(LOW)
            ups[rows, :] = up.astype(LOW)
            hidden = (gate * jax.nn.sigmoid(gate) * up).astype(LOW)
            sums = jnp.dot(hidden, down_w[...], preferred_element_type=F32).astype(LOW)
            part[pl.ds(2 * j, 2)] = sums.reshape(2, tokens, width)
            pair_copy(place, part, from_p, sems, j).start()
            for copy in keep(j):
                copy.start()
            return carry

        lax.fori_loop(0, 4, step, 0)
        start(1)
        start(2)
        reduce_line(place, part, total, from_p, from_r, from_l, held, sems, later, True, at_two(middle), sent=True)
        for j in range(4):
            for copy in keep(j):
                copy.wait()

    (total, full, gate, up), loads = carry_call(
        names,
        body,
        "line",
        [block, w_gate, w_up, w_down],
        [ONCHIP, ANY, ANY, ANY],
        [
            jax.ShapeDtypeStruct((tokens, width), F32),
            jax.ShapeDtypeStruct((8, tokens, width), LOW),
            jax.ShapeDtypeStruct((8 * tokens, inner), LOW),
            jax.ShapeDtypeStruct((8 * tokens, inner), LOW),
        ],
        [ONCHIP, ANY, ANY, ANY],
        [
            *Gather.scratch,
            pltpu.VMEM((8, tokens, width), LOW),
            pltpu.VMEM((8, tokens, width), LOW),
            pltpu.VMEM(w_gate.shape, LOW),
            pltpu.VMEM(w_up.shape, LOW),
            pltpu.VMEM(w_down.shape, LOW),
            pltpu.VMEM((8 * tokens, inner), LOW),
            pltpu.VMEM((8 * tokens, inner), LOW),
            pltpu.SemaphoreType.DMA((3,)),
            pltpu.SemaphoreType.DMA((3, 4)),
            *[pltpu.VMEM((4, tokens, width), LOW)] * 4,
            *[pltpu.SemaphoreType.DMA((4,))] * 5,
        ],
        cargo,
        name=name,
        vmem=58,
    )
    return total, full.reshape(8 * tokens, width), gate, up, loads


REDUCE_SEMS = [pltpu.SemaphoreType.DMA((4,))] * 5


def reduce_scratch(tokens, width):
    return [*[pltpu.VMEM((4, tokens, width), LOW)] * 4, *REDUCE_SEMS]


def rows_of(first, count):
    return pl.ds(pl.multiple_of(first, count), count)


def copy_in(pairs, sem):
    copies = [pltpu.make_async_copy(src, dst, sem.at[i]) for i, (src, dst) in enumerate(pairs)]
    for copy in copies:
        copy.start()
    return copies


def open_call(names, shard, cargo):
    def body(place, ins, outs, scratch, later, middle, start):
        gather = Gather(place, ins[0], outs[0], scratch)
        gather.start(later)
        start(1)
        start(3)
        gather.pass_on(1)
        middle(1)
        gather.pass_on(2)
        start(2)
        gather.pass_on(3)
        middle(3)
        for zz in range(4):
            spot = gather.spot(zz, 1 - place.c)
            recv = gather.recv.at[2 * zz + 1 - place.c]
            later.add(remote(spot, spot, gather.send_p.at[0], recv, place.at(place.z, 1 - place.c)).wait_recv)

    (full,), loads = carry_call(
        names,
        body,
        "line",
        [shard],
        [ANY],
        [jax.ShapeDtypeStruct((8, *shard.shape), shard.dtype)],
        [ANY],
        list(Gather.scratch),
        cargo,
        name="open",
    )
    return full, loads


def close_call(names, cargo, name):
    def body(place, ins, outs, scratch, later, middle, start):
        middle(0)

    return carry_call(names, body, "col", [], [], [], [], [], cargo, name=name)[1]


def heads_of(ref, rows):
    return jnp.concatenate([ref[rows, h * HD : (h + 1) * HD] for h in range(3)], axis=0)


def block_probs(qkv, starts, b):
    reach = QB + SEQ_MAX
    first = jnp.maximum(b - SEQ_MAX // QB, 0) * QB
    rows, window = rows_of(b * QB, QB), pl.ds(pl.multiple_of(first, QB), reach)
    queries = heads_of(qkv, rows)
    keys, values = qkv[window, 3 * HD : 4 * HD], qkv[window, 4 * HD : 5 * HD]
    scores = (dot_t(queries, keys) * HD ** (-0.5)).reshape(3, QB, reach)
    key_at = first + lax.broadcasted_iota(jnp.int32, (QB, reach), 1)
    query_at = b * QB + lax.broadcasted_iota(jnp.int32, (QB, reach), 0)
    allowed = (key_at >= starts[rows, :]) & (key_at <= query_at)
    masked = jnp.where(allowed[None], scores, neg_fill)
    lifted = jnp.exp(masked - jnp.max(masked, axis=-1, keepdims=True))
    probs = lifted * (1.0 / jnp.sum(lifted, axis=-1, keepdims=True))
    return queries, keys, values, probs, rows, window


def roll_half(values):
    return pltpu.roll(values, HD // 2, 1)


def forward_heads(names, block, acts, w_qkv, bias, w_out, cosine, sine, starts, cargo, name):
    tokens, width = QB, D
    count = 8 * QB
    apart = acts is not None

    def body(place, ins, outs, scratch, later, middle, start):
        ins = list(ins)
        block_ref = ins.pop(0)
        acts_hbm = ins.pop(0) if apart else None
        qkv_hbm, bias_ref, out_hbm, cos_ref, sin_ref, starts_ref = ins
        total, full_out, qkv_out, mixed_out = outs
        scratch = list(scratch)
        gather_sems = [scratch.pop(0) for _ in Gather.scratch]
        full, acts_own, part, qkv_w, out_w, qkv, mixed, load_sem, keep_sem = scratch[:9]
        from_p, from_r, from_l, held, *sems = scratch[9:]
        pairs = [(qkv_hbm, qkv_w), (out_hbm, out_w)]
        if apart:
            pairs.append((acts_hbm, acts_own))
        loads = copy_in(pairs, load_sem)
        gather = Gather(place, block_ref, full, gather_sems)
        gather.start(later)
        for load in loads:
            load.wait()

        def keep(j):
            return pltpu.make_async_copy(full.at[pl.ds(2 * j, 2)], full_out.at[pl.ds(2 * j, 2)], keep_sem.at[j])

        def step(p, carry):
            j = gather.chunk(p)
            keep(j).start()
            pl.when(p == 2)(middle)
            rows = rows_of(j * 2 * QB, 2 * QB)
            chunk = acts_own[rows, :] if apart else full[pl.ds(2 * j, 2)].reshape(2 * tokens, width)
            raw = jnp.dot(chunk, qkv_w[...], preferred_element_type=F32) + bias_ref[...]
            cos, sin = cos_ref[rows, :], sin_ref[rows, :]
            for t in range(5):
                head = raw[:, t * HD : (t + 1) * HD]
                if t < 4:
                    head = head * cos + roll_half(head) * sin
                qkv[rows, t * HD : (t + 1) * HD] = head.astype(LOW)
            return carry

        lax.fori_loop(0, 4, step, 0)
        start(1)

        def attend(j, carry):
            _, _, values, probs, _, _ = block_probs(qkv, starts_ref, 2 * j + place.c)
            low = probs.astype(LOW).reshape(3 * QB, QB + SEQ_MAX)
            heads = jnp.dot(low, values, preferred_element_type=F32).astype(LOW)
            wide = jnp.concatenate([heads[h * QB : (h + 1) * QB] for h in range(3)], axis=1)
            mixed[rows_of(j * QB, QB), :] = wide
            part[j] = jnp.dot(wide, out_w[...], preferred_element_type=F32).astype(LOW)
            return carry

        lax.fori_loop(0, 4, attend, 0)
        saves = copy_in([(qkv, qkv_out), (mixed, mixed_out)], load_sem)
        reduce_line(place, part, total, from_p, from_r, from_l, held, sems, later, False, at_two(middle))
        for copy in saves:
            copy.wait()
        for j in range(4):
            keep(j).wait()

    (total, full, qkv, mixed), loads = carry_call(
        names,
        body,
        "line",
        [block, *([acts] if apart else []), w_qkv, bias, w_out, cosine, sine, starts],
        [ONCHIP, *([ANY] if apart else []), ANY, ONCHIP, ANY, ONCHIP, ONCHIP, ONCHIP],
        [
            jax.ShapeDtypeStruct((tokens, width), F32),
            jax.ShapeDtypeStruct((8, *block.shape), LOW),
            jax.ShapeDtypeStruct((count, 5 * HD), LOW),
            jax.ShapeDtypeStruct((count // 2, 3 * HD), LOW),
        ],
        [ONCHIP, ANY, ANY, ANY],
        [
            *Gather.scratch,
            pltpu.VMEM((8, *block.shape), LOW),
            pltpu.VMEM((count, width) if apart else (16, 128), LOW),
            pltpu.VMEM((4, tokens, width), LOW),
            pltpu.VMEM(w_qkv.shape, LOW),
            pltpu.VMEM(w_out.shape, LOW),
            pltpu.VMEM((count, 5 * HD), LOW),
            pltpu.VMEM((count // 2, 3 * HD), LOW),
            pltpu.SemaphoreType.DMA((3,)),
            pltpu.SemaphoreType.DMA((4,)),
            *reduce_scratch(tokens, width),
        ],
        cargo,
        name=name,
        vmem=50,
    )
    return total, full, qkv, mixed, loads


def backward_heads(names, block, acts, w_qkv, w_out, qkv, mixed, cosine, sine, starts, cargo, name):
    tokens, width = QB, D
    count = 8 * QB
    reach = QB + SEQ_MAX

    def body(place, ins, outs, scratch, later, middle, start):
        block_ref, acts_hbm, qkv_hbm, out_hbm, saved_hbm, mixed_hbm, cos_ref, sin_ref, starts_ref = ins
        total, slab_out, out_out = outs
        scratch = list(scratch)
        gather_sems = [scratch.pop(0) for _ in Gather.scratch]
        full, part, qkv_w, out_w, qkv, mixed, acts_own, d_raw, d_keys, d_values = scratch[:10]
        slab, d_out, slab_in, d_out_in, load_sem, swap_send, swap_recv = scratch[10:17]
        from_p, from_r, from_l, held, *sems = scratch[17:]
        pairs = [(qkv_hbm, qkv_w), (out_hbm, out_w), (saved_hbm, qkv), (mixed_hbm, mixed), (acts_hbm, acts_own)]
        loads = copy_in(pairs, load_sem)
        gather = Gather(place, block_ref, full, gather_sems, both=False)
        gather.start(later)
        d_keys[...] = jnp.zeros_like(d_keys)
        d_values[...] = jnp.zeros_like(d_values)
        for load in loads:
            load.wait()

        def step(p, carry):
            j = gather.chunk(p)
            pl.when(p == 2)(middle)
            b = 2 * j + place.c
            d_mixed = dot_t(full[j], out_w[...]).astype(LOW)
            d_heads = jnp.concatenate([d_mixed[:, h * HD : (h + 1) * HD] for h in range(3)], axis=0)
            queries, keys, values, probs, rows, window = block_probs(qkv, starts_ref, b)
            d_probs = dot_t(d_heads, values).reshape(3, QB, reach)
            inner = jnp.sum(probs * d_probs, axis=-1, keepdims=True)
            d_scores = (probs * (d_probs - inner)).astype(LOW).reshape(3 * QB, reach)
            d_queries = jnp.dot(d_scores, keys, preferred_element_type=F32) * HD ** (-0.5)
            d_keys[window, :] += t_dot(d_scores, queries) * HD ** (-0.5)
            d_values[window, :] += t_dot(probs.astype(LOW).reshape(3 * QB, reach), d_heads)
            cos, sin = cos_ref[rows, :], sin_ref[rows, :]
            for h in range(3):
                head = d_queries[h * QB : (h + 1) * QB]
                head = head * cos + roll_half(head * sin)
                d_raw[rows, h * HD : (h + 1) * HD] = head.astype(LOW)
            other = rows_of((2 * j + 1 - place.c) * QB, QB)
            d_raw[other, 0 : 3 * HD] = jnp.zeros((QB, 3 * HD), LOW)
            return carry

        lax.fori_loop(0, 4, step, 0)
        start(1)

        def project(j, carry):
            rows = rows_of(j * 2 * QB, 2 * QB)
            head = d_keys[rows, :]
            head = head * cos_ref[rows, :] + roll_half(head * sin_ref[rows, :])
            d_raw[rows, 3 * HD : 4 * HD] = head.astype(LOW)
            d_raw[rows, 4 * HD : 5 * HD] = d_values[rows, :].astype(LOW)
            part[pl.ds(2 * j, 2)] = dot_t(d_raw[rows, :], qkv_w[...]).astype(LOW).reshape(2, tokens, width)
            pair_copy(place, part, from_p, sems, j).start()
            return carry

        lax.fori_loop(0, 4, project, 0)

        def swap():
            to = place.at(place.z, 1 - place.c)
            return [
                remote(slab.at[1 - place.c], slab_in, swap_send.at[0], swap_recv.at[0], to),
                remote(d_out.at[1 - place.c], d_out_in, swap_send.at[1], swap_recv.at[1], to),
            ]

        def between(s):
            if s == 2:
                middle(1)
                for copy in swap():
                    copy.start()
                return

            def weights(i, carry):
                cut = pl.ds(pl.multiple_of(i * (D // 4), 128), D // 4)
                grads = t_dot(acts_own[:, cut], d_raw[...]).astype(LOW)
                slab[0, i, 0 : D // 8, :] = grads[: D // 8]
                slab[1, i, 0 : D // 8, :] = grads[D // 8 :]
                return carry

            lax.fori_loop(0, 4, weights, 0)
            sums = jnp.sum(d_raw[...].astype(F32), axis=0, keepdims=True)
            first = lax.broadcasted_iota(jnp.int32, (16, 5 * HD), 0) == 0
            tail = jnp.where(first, sums, 0.0).astype(LOW)
            for half in range(2):
                for i in range(4):
                    slab[half, i, D // 8 :, :] = tail
            grads = t_dot(mixed[...], full[...].reshape(4 * QB, D)).astype(LOW)
            d_out[0] = grads[: D // 8]
            d_out[1] = grads[D // 8 :]

        reduce_line(place, part, total, from_p, from_r, from_l, held, sems, later, True, between, sent=True)
        for copy in swap():
            copy.wait()
        for i in range(4):
            add_into(slab_out.at[i], [slab.at[place.c, i], slab_in.at[i]])
        add_into(out_out, [d_out.at[place.c], d_out_in])

    (total, slab, d_out), loads = carry_call(
        names,
        body,
        "line",
        [block, acts, w_qkv, w_out, qkv, mixed, cosine, sine, starts],
        [ONCHIP, ANY, ANY, ANY, ANY, ANY, ONCHIP, ONCHIP, ONCHIP],
        [
            jax.ShapeDtypeStruct((tokens, width), F32),
            jax.ShapeDtypeStruct((4, HALF, 5 * HD), LOW),
            jax.ShapeDtypeStruct((D // 8, D), LOW),
        ],
        [ONCHIP, ONCHIP, ONCHIP],
        [
            *Gather.scratch,
            pltpu.VMEM((4, tokens, width), LOW),
            pltpu.VMEM((8, tokens, width), LOW),
            pltpu.VMEM(w_qkv.shape, LOW),
            pltpu.VMEM(w_out.shape, LOW),
            pltpu.VMEM((count, 5 * HD), LOW),
            pltpu.VMEM((count // 2, 3 * HD), LOW),
            pltpu.VMEM((count, width), LOW),
            pltpu.VMEM((count, 5 * HD), LOW),
            pltpu.VMEM((count, HD), F32),
            pltpu.VMEM((count, HD), F32),
            pltpu.VMEM((2, 4, HALF, 5 * HD), LOW),
            pltpu.VMEM((2, D // 8, D), LOW),
            pltpu.VMEM((4, HALF, 5 * HD), LOW),
            pltpu.VMEM((D // 8, D), LOW),
            pltpu.SemaphoreType.DMA((5,)),
            pltpu.SemaphoreType.DMA((2,)),
            pltpu.SemaphoreType.DMA((2,)),
            *reduce_scratch(tokens, width),
        ],
        cargo,
        name=name,
        vmem=60,
    )
    return total, slab.reshape(4 * HALF, 5 * HD), d_out, loads


def backward_feed(names, block, grads_all, acts, w_gate, w_up, w_down, gate, up, cargo, name):
    tokens, width = QB, D
    inner = w_gate.shape[1]
    apart = grads_all is not None

    def body(place, ins, outs, scratch, later, middle, start):
        head_ref, acts_hbm, gate_hbm, up_hbm, down_hbm, gates_hbm, ups_hbm = ins
        total, gate_out, up_out, down_out = outs
        scratch = list(scratch)
        gather_sems = [scratch.pop(0) for _ in Gather.scratch]
        full, part, acts_own, gate_w, up_w, down_w, gates, ups, hiddens, load_sem, keep_sem = scratch[:11]
        from_p, from_r, from_l, held, *sems = scratch[11:]
        pairs = [(down_hbm, down_w), (gates_hbm, gates), (ups_hbm, ups), (gate_hbm, gate_w), (up_hbm, up_w)]
        pairs.append((acts_hbm, acts_own))
        if apart:
            pairs.append((head_ref, full))
        loads = copy_in(pairs, load_sem)
        gather = None
        if not apart:
            gather = Gather(place, head_ref, full, gather_sems)
            gather.start(later)
        for load in loads:
            load.wait()

        def step(p, carry):
            j = p if apart else gather.chunk(p)
            pl.when(p == 2)(middle)
            rows = rows_of(j * 2 * tokens, 2 * tokens)
            grads = full[pl.ds(2 * j, 2)].reshape(2 * tokens, width)
            d_hidden = dot_t(grads, down_w[...])
            gate, up = gates[rows, :].astype(F32), ups[rows, :].astype(F32)
            squash = jax.nn.sigmoid(gate)
            lit = gate * squash
            hiddens[rows, :] = (lit * up).astype(LOW)
            d_gate = (d_hidden * up * squash * (1.0 + gate * (1.0 - squash))).astype(LOW)
            d_up = (d_hidden * lit).astype(LOW)
            gates[rows, :] = d_gate
            ups[rows, :] = d_up
            sums = dot_t(d_gate, gate_w[...]) + dot_t(d_up, up_w[...])
            part[pl.ds(2 * j, 2)] = sums.astype(LOW).reshape(2, tokens, width)
            pair_copy(place, part, from_p, sems, j).start()
            return carry

        lax.fori_loop(0, 4, step, 0)

        def between(s):
            if s == 1:
                grads = full[...].reshape(8 * tokens, width)

                def down(i, carry):
                    cut = pl.ds(pl.multiple_of(i * 384, 128), 384)
                    down_w[:, cut] = t_dot(hiddens[...], full[:, :, cut].reshape(8 * tokens, 384)).astype(LOW)
                    return carry

                lax.fori_loop(0, width // 384, down, 0)
                start(1, down_w)
                return

            def rest(i, carry):
                cut = pl.ds(pl.multiple_of(i * 384, 128), 384)
                acts_cut = acts_own[:, cut]
                rows = pl.ds(pl.multiple_of(i * 384, 128), 384)
                gate_w[rows, :] = t_dot(acts_cut, gates[...]).astype(LOW)
                up_w[rows, :] = t_dot(acts_cut, ups[...]).astype(LOW)
                return carry

            lax.fori_loop(0, width // 384, rest, 0)
            middle(1)

        reduce_line(place, part, total, from_p, from_r, from_l, held, sems, later, True, between, sent=True)
        for copy in copy_in([(gate_w, gate_out), (up_w, up_out), (down_w, down_out)], keep_sem):
            copy.wait()

    head = grads_all.reshape(8, tokens, width) if apart else block
    (total, d_gate, d_up, d_down), loads = carry_call(
        names,
        body,
        "line",
        [head, acts, w_gate, w_up, w_down, gate, up],
        [ANY if apart else ONCHIP, ANY, ANY, ANY, ANY, ANY, ANY],
        [
            jax.ShapeDtypeStruct((tokens, width), F32),
            jax.ShapeDtypeStruct(w_gate.shape, LOW),
            jax.ShapeDtypeStruct(w_up.shape, LOW),
            jax.ShapeDtypeStruct(w_down.shape, LOW),
        ],
        [ONCHIP, ANY, ANY, ANY],
        [
            *Gather.scratch,
            pltpu.VMEM((8, tokens, width), LOW),
            pltpu.VMEM((8, tokens, width), LOW),
            pltpu.VMEM((8 * tokens, width), LOW),
            pltpu.VMEM(w_gate.shape, LOW),
            pltpu.VMEM(w_up.shape, LOW),
            pltpu.VMEM(w_down.shape, LOW),
            pltpu.VMEM((8 * tokens, inner), LOW),
            pltpu.VMEM((8 * tokens, inner), LOW),
            pltpu.VMEM((8 * tokens, inner), LOW),
            pltpu.SemaphoreType.DMA((7,)),
            pltpu.SemaphoreType.DMA((3,)),
            *reduce_scratch(tokens, width),
        ],
        cargo,
        name=name,
        vmem=61,
    )
    return total, d_gate, d_up, d_down, loads


eps_norm = 1e-06
rope_base = 1000000.0
neg_fill = -1e30


def row_starts(sizes, count):
    ends = jnp.cumsum(sizes)
    firsts = ends - sizes
    places = jnp.arange(count, dtype=jnp.int32)
    inside = (places[None, :] >= firsts[:, None]) & (places[None, :] < ends[:, None])
    return jnp.sum(jnp.where(inside, firsts[:, None], 0), axis=0)


def rope_tables(positions):
    half = HD // 2
    freq = rope_base ** (-(jnp.arange(half, dtype=jnp.float32) * (2.0 / HD)))
    angle = freq[:, None] * positions.astype(jnp.float32)[None, :]
    cosine = jnp.concatenate([jnp.cos(angle), jnp.cos(angle)], axis=0)
    sine = jnp.concatenate([jnp.sin(angle), jnp.sin(angle)], axis=0)
    return (cosine, sine)


def rotate(values, cosine, sine):
    half = HD // 2
    turned = jnp.concatenate([-values[:, half:], values[:, :half]], axis=1)
    return values * cosine + turned * sine


def rotate_back(grads, cosine, sine):
    half = HD // 2
    lifted = grads * sine
    turned = jnp.concatenate([lifted[:, half:], -lifted[:, :half]], axis=1)
    return grads * cosine + turned


def contract_first(left, right):
    return lax.dot_general(
        left, right, (((0,), (0,)), ((), ())), preferred_element_type=jnp.float32
    )


def contract_last(left, right):
    return lax.dot_general(
        left, right, (((1,), (1,)), ((), ())), preferred_element_type=jnp.float32
    )


def feature_total(values):
    return lax.psum(jnp.sum(values, axis=0), "col")


def spread(values):
    return lax.all_gather(values, "col", axis=0, tiled=True)


def summed_rows(make_term, rows):
    return lax.psum_scatter(
        make_term(jnp.int32(0), lax.axis_size("col") * rows), "col", scatter_dimension=0, tiled=True
    )


def to_blocks(values):
    return lax.all_to_all(values, "col", split_axis=1, concat_axis=0, tiled=True)


def to_tokens(values):
    return lax.all_to_all(values, "col", split_axis=0, concat_axis=1, tiled=True)


def by_columns(weight, acts, start, count):
    return contract_first(weight, acts)


def by_rows(weight, grads, start, count):
    return jnp.dot(weight, grads, preferred_element_type=jnp.float32)


def by_rows_pair(first_weight, first_grads, second_weight, second_grads, start, count):
    return by_rows(first_weight, first_grads, start, count) + by_rows(
        second_weight, second_grads, start, count
    )


def norm_forward(residual, gain):
    totals = feature_total(residual * residual)
    scale = lax.rsqrt(totals / D + eps_norm)
    return (scale, (residual * scale * gain[:, None]).astype(jnp.bfloat16))


def norm_backward(d_normed, residual, scale, gain):
    weighted = d_normed * gain[:, None]
    inner = feature_total(weighted * residual)
    d_residual = weighted * scale - residual * (scale * scale * scale) * inner / D
    d_gain = jnp.sum(d_normed * residual * scale, axis=1)
    return (d_residual, d_gain)


def attend_scores(queries, keys, mask):
    scores = jnp.einsum(
        "kghq,khj->kgqj", queries, keys, preferred_element_type=jnp.float32
    ) * HD ** (-0.5)
    return jnp.where(mask[None, None], scores, neg_fill)


def per_device(
    hidden_states,
    out_grad,
    lengths,
    norm_gains,
    qkv_weight,
    qkv_bias,
    out_weight,
    gate_weight,
    up_weight,
    down_weight,
):
    feat_rows, tok_row = hidden_states.shape
    col_at = lax.axis_index("col")
    starts = row_starts(lengths[0], tok_row)
    positions = jnp.arange(tok_row, dtype=jnp.int32) - starts
    cosine, sine = rope_tables(positions)
    first = col_at * QB
    block_starts = lax.dynamic_slice_in_dim(starts, first, QB)
    cos_block = lax.dynamic_slice_in_dim(cosine, first, QB, 1)
    sin_block = lax.dynamic_slice_in_dim(sine, first, QB, 1)
    reach = QB + SEQ_MAX
    window = jnp.maximum(first - SEQ_MAX, 0)
    key_places = window + jnp.arange(reach, dtype=jnp.int32)
    query_places = first + jnp.arange(QB, dtype=jnp.int32)
    mask = (key_places[None, :] >= block_starts[:, None]) & (
        key_places[None, :] <= query_places[:, None]
    )
    group = HEADS // KV_HEADS
    rotary = HEADS + KV_HEADS
    query_rows = HEADS * HD
    kv_rows = KV_HEADS * HD
    gains = norm_gains.astype(jnp.float32)
    residual = hidden_states.astype(jnp.float32)
    saved = []
    for layer in range(LAYERS):
        w_qkv, b_qkv, w_out, w_gate, w_up, w_down = (
            lax.all_gather(qkv_weight[layer], "row", axis=0, tiled=True),
            lax.all_gather(qkv_bias[layer], "row", axis=1, tiled=True),
            lax.all_gather(out_weight[layer], "row", axis=1, tiled=True),
            lax.all_gather(gate_weight[layer], "row", axis=0, tiled=True),
            lax.all_gather(up_weight[layer], "row", axis=0, tiled=True),
            lax.all_gather(down_weight[layer], "row", axis=1, tiled=True),
        )
        scale_one, normed_one = norm_forward(residual, gains[layer, 0])
        full_one = spread(normed_one)
        raw = contract_first(w_qkv, full_one) + b_qkv.reshape(-1).astype(jnp.float32)[:, None]
        local_heads = raw.shape[0] // HD
        shaped = raw.reshape(local_heads, HD, tok_row)
        head_ids = col_at * local_heads + jnp.arange(local_heads)
        turned = jnp.where((head_ids < rotary)[:, None, None], rotate(shaped, cosine, sine), shaped)
        blocked = to_blocks(turned.reshape(raw.shape).astype(jnp.bfloat16))
        kv_full = lax.all_gather(blocked[query_rows:], "col", axis=1, tiled=True)
        kv_window = lax.dynamic_slice_in_dim(kv_full, window, reach, 1)
        queries = blocked[:query_rows].reshape(KV_HEADS, group, HD, QB)
        keys = kv_window[:kv_rows].reshape(KV_HEADS, HD, reach)
        values = kv_window[kv_rows:].reshape(KV_HEADS, HD, reach)
        masked = attend_scores(queries, keys, mask)
        row_top = jnp.max(masked, axis=-1, keepdims=True)
        lifted = jnp.exp(masked - row_top)
        row_mass = jnp.sum(lifted, axis=-1, keepdims=True)
        probs = lifted / row_mass
        log_mass = row_top + jnp.log(row_mass)
        mixed = (
            jnp.einsum(
                "kgqj,khj->kghq",
                probs.astype(jnp.bfloat16),
                values,
                preferred_element_type=jnp.float32,
            )
            .reshape(query_rows, QB)
            .astype(jnp.bfloat16)
        )
        carried = to_tokens(mixed)
        attention = summed_rows(partial(by_columns, w_out, carried), feat_rows)
        residual_mid = residual + attention
        scale_two, normed_two = norm_forward(residual_mid, gains[layer, 1])
        full_two = spread(normed_two)
        gate = contract_first(w_gate, full_two)
        up = contract_first(w_up, full_two)
        hidden = (gate * jax.nn.sigmoid(gate) * up).astype(jnp.bfloat16)
        feed = summed_rows(partial(by_columns, w_down, hidden), feat_rows)
        saved.append(
            (
                residual,
                scale_one,
                full_one,
                blocked,
                kv_window,
                log_mass,
                mixed,
                carried,
                residual_mid,
                scale_two,
                full_two,
                gate,
                up,
                hidden,
                (w_qkv, w_out, w_gate, w_up, w_down),
                local_heads,
            )
        )
        residual = residual_mid + feed
    out_states = residual.astype(jnp.bfloat16)
    grad = out_grad.astype(jnp.float32)
    layer_grads = [None] * LAYERS
    gain_terms = [None] * LAYERS
    for layer in reversed(range(LAYERS)):
        (
            residual_in,
            scale_one,
            full_one,
            blocked,
            kv_window,
            log_mass,
            mixed,
            carried,
            residual_mid,
            scale_two,
            full_two,
            gate,
            up,
            hidden,
            weights_full,
            local_heads,
        ) = saved[layer]
        w_qkv, w_out, w_gate, w_up, w_down = weights_full
        grad_full = spread(grad.astype(jnp.bfloat16))
        d_down = contract_last(hidden, grad_full)
        d_hidden = jnp.dot(w_down, grad_full, preferred_element_type=jnp.float32)
        squash = jax.nn.sigmoid(gate)
        d_gate = (d_hidden * up * squash * (1.0 + gate * (1.0 - squash))).astype(jnp.bfloat16)
        d_up = (d_hidden * gate * squash).astype(jnp.bfloat16)
        d_gate_w = contract_last(full_two, d_gate)
        d_up_w = contract_last(full_two, d_up)
        d_normed_two = summed_rows(partial(by_rows_pair, w_gate, d_gate, w_up, d_up), feat_rows)
        d_residual, d_gain_two = norm_backward(
            d_normed_two, residual_mid, scale_two, gains[layer, 1]
        )
        grad = grad + d_residual
        grad_full = spread(grad.astype(jnp.bfloat16))
        d_out_w = contract_last(carried, grad_full)
        d_mixed = to_blocks(
            jnp.dot(w_out, grad_full, preferred_element_type=jnp.float32).astype(jnp.bfloat16)
        )
        queries = blocked[:query_rows].reshape(KV_HEADS, group, HD, QB)
        keys = kv_window[:kv_rows].reshape(KV_HEADS, HD, reach)
        values = kv_window[kv_rows:].reshape(KV_HEADS, HD, reach)
        masked = attend_scores(queries, keys, mask)
        probs = jnp.exp(masked - log_mass)
        low_probs = probs.astype(jnp.bfloat16)
        d_heads_mix = d_mixed.reshape(KV_HEADS, group, HD, QB)
        d_probs = jnp.einsum(
            "kghq,khj->kgqj", d_heads_mix, values, preferred_element_type=jnp.float32
        )
        inner = jnp.sum(probs * d_probs, axis=-1, keepdims=True)
        d_scores = (probs * (d_probs - inner)).astype(jnp.bfloat16)
        d_queries = (
            jnp.einsum("kgqj,khj->kghq", d_scores, keys, preferred_element_type=jnp.float32)
            * HD ** (-0.5)
        ).reshape(query_rows, QB)
        d_keys = (
            jnp.einsum("kgqj,kghq->khj", d_scores, queries, preferred_element_type=jnp.float32)
            * HD ** (-0.5)
        ).reshape(kv_rows, reach)
        d_values = jnp.einsum(
            "kgqj,kghq->khj", low_probs, d_heads_mix, preferred_element_type=jnp.float32
        ).reshape(kv_rows, reach)
        d_window = jnp.concatenate([d_keys, d_values], axis=0)
        d_placed = lax.dynamic_update_slice_in_dim(
            jnp.zeros((2 * kv_rows, tok_row), jnp.float32), d_window, window, 1
        )
        d_kv = lax.psum_scatter(d_placed, "col", scatter_dimension=1, tiled=True)
        d_heads = jnp.concatenate([d_queries, d_kv], axis=0).reshape(HEADS + 2 * KV_HEADS, HD, QB)
        d_turned = jnp.concatenate(
            [rotate_back(d_heads[:rotary], cos_block, sin_block), d_heads[rotary:]], axis=0
        )
        d_raw = to_tokens(d_turned.reshape((HEADS + 2 * KV_HEADS) * HD, QB).astype(jnp.bfloat16))
        d_bias = jnp.sum(d_raw, axis=1, dtype=jnp.float32).reshape(local_heads, HD)
        d_qkv_w = contract_last(full_one, d_raw)
        d_normed_one = summed_rows(partial(by_rows, w_qkv, d_raw), feat_rows)
        d_residual, d_gain_one = norm_backward(
            d_normed_one, residual_in, scale_one, gains[layer, 0]
        )
        grad = grad + d_residual
        layer_grads[layer] = (
            lax.psum_scatter(d_qkv_w, "row", scatter_dimension=0, tiled=True),
            lax.psum_scatter(d_bias, "row", scatter_dimension=1, tiled=True),
            lax.psum_scatter(d_out_w, "row", scatter_dimension=1, tiled=True),
            lax.psum_scatter(d_gate_w, "row", scatter_dimension=0, tiled=True),
            lax.psum_scatter(d_up_w, "row", scatter_dimension=0, tiled=True),
            lax.psum_scatter(d_down, "row", scatter_dimension=1, tiled=True),
        )
        gain_terms[layer] = jnp.stack([d_gain_one, d_gain_two])
    gain_grads = lax.psum(jnp.stack(gain_terms), "row")
    stacked = [jnp.stack([entry[member] for entry in layer_grads]) for member in range(6)]
    return (
        out_states,
        grad,
        gain_grads,
        stacked[0],
        stacked[1],
        stacked[2],
        stacked[3],
        stacked[4],
        stacked[5],
    )


def dot(a, b):
    return jnp.dot(a, b, preferred_element_type=F32)


def dot_t(a, b):
    return lax.dot_general(a, b, (((1,), (1,)), ((), ())), preferred_element_type=F32)


def t_dot(a, b):
    return lax.dot_general(a, b, (((0,), (0,)), ((), ())), preferred_element_type=F32)


def norm_on(residual, gain):
    scale = lax.rsqrt(jnp.mean(residual * residual, axis=1, keepdims=True) + eps_norm)
    return scale, (residual * scale * gain[None, :]).astype(LOW)


def norm_back(d_normed, residual, scale, gain):
    weighted = d_normed * gain[None, :]
    inner = jnp.sum(weighted * residual, axis=1, keepdims=True)
    d_residual = weighted * scale - residual * (scale * scale * scale) * inner / D
    d_gain = jnp.sum(d_normed * residual * scale, axis=0)
    return d_residual, d_gain


def per_device_line(
    hidden_states,
    out_grad,
    lengths,
    norm_gains,
    qkv_weight,
    qkv_bias,
    out_weight,
    gate_weight,
    up_weight,
    down_weight,
):
    names = Names()
    tok_row = hidden_states.shape[1]
    row_at = lax.axis_index("row")
    col_at = lax.axis_index("col")
    core = col_at % 2

    biases = jnp.zeros((LAYERS, 2, 16, HD), LOW)
    biases = lax.dynamic_update_slice(biases, qkv_bias[:, :, None], (0, 0, 0, row_at * (HD // 4)))
    gain_rows = jnp.pad(norm_gains.reshape(2 * LAYERS, D // 8), ((0, 16 - 2 * LAYERS), (0, 0)))

    def slab_of(mine, theirs, out_mine, out_theirs):
        first, second = jnp.where(core == 0, mine, theirs), jnp.where(core == 0, theirs, mine)
        both = jnp.stack([first.reshape(4, HALF, 5 * HD), second.reshape(4, HALF, 5 * HD)], axis=1)
        w_qkv = both[:, :, : D // 8].reshape(D, 5 * HD)
        bias = jnp.sum(both[:, 0, D // 8].astype(F32), axis=0, keepdims=True)
        w_out = jnp.concatenate(
            [jnp.where(core == 0, out_mine, out_theirs), jnp.where(core == 0, out_theirs, out_mine)], axis=0
        )
        return w_qkv, bias, w_out

    def rows_load(layer):
        return (
            GatherRows(gate_weight, 0, layer),
            GatherRows(up_weight, 0, layer),
            GatherRows(down_weight, 1, layer),
        )

    sent = rows_load(0)
    to_chips = [HeadsToChips(qkv_weight, biases, layer) for layer in range(LAYERS)]
    slab_rows, out_rows = GatherRows(From(to_chips[0]), 0, phase=1), GatherRows(out_weight, 1, 0, phase=1)
    swap = Swap(From(slab_rows), From(out_rows), phase=2)
    sent[0].phase = 3
    states, loads = open_call(
        names, hidden_states, [*to_chips, Exchange(gain_rows, same=True), slab_rows, out_rows, swap, sent[0]]
    )
    (_,), (slab_next,), (gains,), (mine,), (out_mine,), (theirs, out_theirs), (w_gate,) = loads
    load = (mine, theirs, out_mine, out_theirs)
    gains = gains[:, : 2 * LAYERS].transpose(1, 0, 2).reshape(LAYERS, 2, D).astype(F32)
    starts = row_starts(lengths[0], tok_row)
    cosine, sine = rope_tables(jnp.arange(tok_row, dtype=jnp.int32) - starts)
    cosine, sine = cosine.T, sine.T * jnp.where(jnp.arange(HD) < HD // 2, -1.0, 1.0)[None]
    starts = starts[:, None]

    def own_block(transposed):
        return lax.dynamic_slice_in_dim(transposed, col_at * QB, QB, 1).astype(F32).T

    wide = states.reshape(D, tok_row)
    residual = own_block(wide)
    wide = wide.astype(F32)
    scale_all = lax.rsqrt(jnp.mean(wide * wide, axis=0, keepdims=True) + eps_norm)
    full_one = (wide * scale_all * gains[0, 0][:, None]).astype(LOW).T
    scale_one, _ = norm_on(residual, gains[0, 0])

    saved = []
    for layer in range(LAYERS):
        w_qkv, bias, w_out = slab_of(*load)
        sent[1].phase, sent[2].phase = 0, 1
        if layer == 0:
            attention, grads_wide, qkv, mixed, loads = forward_heads(
                names, out_grad, full_one, w_qkv, bias, w_out, cosine, sine, starts, sent[1:], name="heads_0"
            )
            (w_up,), (w_down,) = loads
            grads_wide = grads_wide.reshape(D, tok_row)
        else:
            scale_one, normed_one = norm_on(residual, gains[layer, 0])
            attention, full_one, qkv, mixed, loads = forward_heads(
                names, normed_one, None, w_qkv, bias, w_out, cosine, sine, starts, sent[1:], name="heads_1"
            )
            (w_up,), (w_down,) = loads
            full_one = full_one.reshape(tok_row, D)
        residual_mid = residual + attention
        scale_two, normed_two = norm_on(residual_mid, gains[layer, 1])
        cargo = []
        if layer == 0:
            sent = rows_load(1)
            sent[0].phase = 1
            slab_rows, out_rows = GatherRows(slab_next, 0), GatherRows(out_weight, 1, 1)
            cargo = [slab_rows, out_rows, sent[0], Swap(From(slab_rows), From(out_rows), phase=2)]
        feed, full_two, gate, up, loads = forward_feed(
            names, normed_two, w_gate, w_up, w_down, cargo, name=f"feed_{layer}"
        )
        saved.append(
            (
                residual,
                scale_one,
                full_one,
                qkv,
                mixed,
                residual_mid,
                scale_two,
                full_two,
                gate,
                up,
                (w_qkv, w_out, w_gate, w_up, w_down),
            )
        )
        residual = residual_mid + feed
        if layer == 0:
            (mine,), (out_mine,), (w_gate,), (theirs, out_theirs) = loads
            load = (mine, theirs, out_mine, out_theirs)
    states = residual.astype(LOW)

    def own_part(full, dim):
        size = full.shape[dim] // 4
        return lax.dynamic_slice_in_dim(full, row_at * size, size, dim)

    def settle(full, dim, slots):
        return jnp.sum(slots.astype(F32), axis=0) + own_part(full, dim).astype(F32)

    def settle_heads(tiles):
        total = tiles[:, :, 0].astype(F32) + jnp.where(col_at >= 6, tiles[:, :, 1].astype(F32), 0.0)
        weight = total[:, :, : D // 8].transpose(1, 2, 0, 3).reshape(D // 4, 2 * HD)
        bias = lax.dynamic_slice_in_dim(total[:, 0, D // 8], row_at * (HD // 4), HD // 4, 1)
        return weight, bias

    grads = {}
    gain_terms = [None] * LAYERS
    grad = own_block(grads_wide)
    inner = w_gate.shape[1]
    for layer in reversed(range(LAYERS)):
        (
            residual_in,
            scale_one,
            full_one,
            qkv,
            mixed,
            residual_mid,
            scale_two,
            full_two,
            gate,
            up,
            (w_qkv, w_out, w_gate, w_up, w_down),
        ) = saved[layer]
        last = layer == LAYERS - 1
        cargo = [] if last else [ScatterRows(slab, 0), ScatterRows(d_out_w, 1)]
        cargo.append(ScatterRows(Inner((inner, D)), 1, phase=1))
        d_normed_two, d_gate_w, d_up_w, d_down, loads = backward_feed(
            names,
            None if last else grad.astype(LOW),
            grads_wide.T if last else None,
            full_two,
            w_gate,
            w_up,
            w_down,
            gate,
            up,
            cargo,
            name=f"back_feed_{layer}",
        )
        grads["down", layer] = settle(d_down, 1, loads[-1][0])
        cargo = [ScatterRows(d_gate_w, 0), ScatterRows(d_up_w, 0, phase=1)]
        if not last:
            grads["out", layer + 1] = settle(d_out_w, 1, loads[1][0])
            cargo.append(HeadsToOwners(settle(slab, 0, loads[0][0]).astype(LOW)))
        d_residual, d_gain_two = norm_back(d_normed_two, residual_mid, scale_two, gains[layer, 1])
        grad = grad + d_residual
        d_normed_one, slab, d_out_w, loads = backward_heads(
            names,
            grad.astype(LOW),
            full_one,
            w_qkv,
            w_out,
            qkv,
            mixed,
            cosine,
            sine,
            starts,
            cargo,
            name=f"back_heads_{layer}",
        )
        grads["gate", layer] = settle(d_gate_w, 0, loads[0][0])
        grads["up", layer] = settle(d_up_w, 0, loads[1][0])
        if not last:
            grads["qkv", layer + 1] = settle_heads(loads[2][0])
        d_residual, d_gain_one = norm_back(d_normed_one, residual_in, scale_one, gains[layer, 0])
        grad = grad + d_residual
        gain_terms[layer] = jnp.stack([d_gain_one, d_gain_two])
    leaving = jnp.concatenate([states.T, grad.astype(LOW).T], axis=1).reshape(8, D // 8, 2 * QB)
    gain_parts = jnp.pad(jnp.stack(gain_terms).reshape(2 * LAYERS, 8, D // 8), ((0, 8 - 2 * LAYERS), (0, 0), (0, 0)))
    (left,), (gain_all,), (slots,), (out_slots,) = close_call(
        names,
        [
            Exchange(leaving),
            Exchange(gain_parts.transpose(1, 0, 2), every_row=True),
            ScatterRows(slab, 0),
            ScatterRows(d_out_w, 1),
        ],
        "close",
    )
    ((tiles,),) = close_call(names, [HeadsToOwners(settle(slab, 0, slots).astype(LOW))], "close_heads")
    grads["qkv", 0] = settle_heads(tiles)
    grads["out", 0] = settle(d_out_w, 1, out_slots)
    left = left.transpose(1, 0, 2)
    out_states = left[:, :, :QB].reshape(D // 8, tok_row)
    input_grad = left[:, :, QB:].reshape(D // 8, tok_row).astype(F32)
    gain_grads = jnp.sum(gain_all, axis=(0, 1))[: 2 * LAYERS].reshape(LAYERS, 2, D // 8)

    def both_layers(kind):
        return jnp.stack([grads[kind, layer] for layer in range(LAYERS)])

    heads = [jnp.stack([grads["qkv", layer][i] for layer in range(LAYERS)]) for i in range(2)]
    return (
        out_states,
        input_grad,
        gain_grads,
        heads[0],
        heads[1],
        both_layers("out"),
        both_layers("gate"),
        both_layers("up"),
        both_layers("down"),
    )


def solution(mesh):
    placed = (
        P("col", "row"),
        P("col", "row"),
        P("row", None),
        P(None, None, "col"),
        P(None, "row", "col"),
        P(None, "col", "row"),
        P(None, "col", "row"),
        P(None, "row", "col"),
        P(None, "row", "col"),
        P(None, "col", "row"),
    )
    on_lines = mesh.shape["row"] == 4 and mesh.shape["col"] == 8
    return jax.shard_map(
        per_device_line if on_lines else per_device,
        mesh=mesh,
        in_specs=placed,
        out_specs=(
            P("col", "row"),
            P("col", "row"),
            P(None, None, "col"),
            P(None, "row", "col"),
            P(None, "col", "row"),
            P(None, "col", "row"),
            P(None, "row", "col"),
            P(None, "row", "col"),
            P(None, "col", "row"),
        ),
        check_vma=False,
    )
```

```python
from functools import partial

import jax
import jax.numpy as jnp
from jax import lax
from jax.experimental import pallas as pl
from jax.experimental.pallas import tpu as pltpu
from jax.sharding import PartitionSpec as P

D = 1536
HEADS = 12
KV_HEADS = 2
HD = 128
LAYERS = 2
SEQ_MAX = 512
QB = 128
MESH = pl.DeviceIdType.MESH
LOW = jnp.bfloat16
F32 = jnp.float32
ANY = pl.BlockSpec(memory_space=pl.ANY)
ONCHIP = pl.BlockSpec(memory_space=pltpu.VMEM)
VMEM = 62 * 2**20
HALF = 208


class Place:
    def __init__(self):
        self.r = lax.axis_index("row")
        self.k = lax.axis_index("col")
        self.z = self.k // 2
        self.c = self.k % 2

    def at(self, z, c):
        return (self.r, 2 * z + c)

    def rows(self):
        x, y = self.r % 2, self.r // 2
        return (2 * y + (1 - x), 2 * (1 - y) + x, 2 * (1 - y) + (1 - x))


def remote(src, dst, send, recv, device):
    return pltpu.make_async_remote_copy(
        src_ref=src, dst_ref=dst, send_sem=send, recv_sem=recv, device_id=device, device_id_type=MESH
    )


class Later:
    def __init__(self):
        self.todo = []

    def add(self, wait, cond=None):
        self.todo.append((wait, cond))

    def run(self):
        todo, self.todo = self.todo, []
        for wait, cond in todo:
            if cond is None:
                wait()
            else:
                pl.when(cond)(wait)


def greet(place, reach):
    barrier = pltpu.get_barrier_semaphore()

    def hail(device):
        pl.semaphore_signal(barrier, inc=1, device_id=device, device_id_type=MESH)

    if "all" in reach:
        for rr in range(4):
            for kk in range(8):
                pl.when((place.r != rr) | (place.k != kk))(partial(hail, (rr, kk)))
        pl.semaphore_wait(barrier, 31)
        return
    count = 0
    if "rows" in reach:
        for row in place.rows():
            hail((row, place.k))
        count += 3
    if "col" in reach:
        for kk in range(8):
            pl.when(place.k != kk)(partial(hail, (place.r, kk)))
        pl.semaphore_wait(barrier, count + 7)
        return
    hail(place.at(place.z, 1 - place.c))
    count += 1
    if "line" not in reach:
        pl.semaphore_wait(barrier, count)
        return
    pl.when(place.z < 3)(partial(hail, place.at(jnp.minimum(place.z + 1, 3), place.c)))
    pl.when(place.z > 0)(partial(hail, place.at(jnp.maximum(place.z - 1, 0), place.c)))
    edge = (place.z == 0) | (place.z == 3)
    pl.when(edge)(lambda: pl.semaphore_wait(barrier, count + 1))
    pl.when(jnp.logical_not(edge))(lambda: pl.semaphore_wait(barrier, count + 2))


class From:
    def __init__(self, item, at=0):
        self.item, self.at = item, at
        self.shape, self.dtype = item.outs[at].shape, item.outs[at].dtype


class Cargo:
    arrays = ()
    outs = ()
    scratch = ()
    reach = "rows"
    phase = 0
    slow = False

    def middle(self, place, ins, outs, scratch):
        pass


def part_of(ref, dim, row, size):
    cut = pl.ds(pl.multiple_of(row * size, 128 if dim else 16), size)
    return ref.at[:, cut] if dim else ref.at[cut, :]


class GatherRows(Cargo):
    def __init__(self, block, dim, layer=None, phase=0):
        self.dim, self.layer, self.phase = dim, layer, phase
        self.arrays = (block,)
        if layer is not None:
            block = jax.ShapeDtypeStruct(block.shape[1:], block.dtype)
        full = list(block.shape)
        full[dim] *= 4
        self.size = block.shape[dim]
        self.half = block.shape[0] // 32 * 16
        self.rest = block.shape[0] - self.half
        self.outs = (jax.ShapeDtypeStruct(tuple(full), block.dtype),)
        self.scratch = (
            pltpu.SemaphoreType.DMA((6,)),
            pltpu.SemaphoreType.DMA((6,)),
            pltpu.SemaphoreType.DMA((2,)),
            pltpu.VMEM(block.shape, block.dtype),
        )

    def halves(self, ref):
        return ref.at[0 : self.half, :], ref.at[self.half :, :]

    def spots(self, full, row):
        if self.dim:
            cut = pl.ds(pl.multiple_of(row * self.size, 128), self.size)
            return full.at[0 : self.half, cut], full.at[self.half :, cut]
        first = pl.multiple_of(row * self.size, 16)
        return full.at[pl.ds(first, self.half), :], full.at[pl.ds(first + self.half, self.rest), :]

    def source(self, ins):
        return ins[0] if self.layer is None else ins[0].at[self.layer]

    def copies(self, place, ins, outs, scratch):
        src, (dst,), (send, recv, *_) = self.source(ins), outs, scratch
        x, y, d = place.rows()
        block, mine = self.halves(src), self.spots(dst, place.r)
        from_x, from_y = self.spots(dst, x), self.spots(dst, y)
        out = [
            remote(block[0], mine[0], send.at[0], recv.at[0], (x, place.k)),
            remote(block[1], mine[1], send.at[1], recv.at[3], (y, place.k)),
            remote(block[1], mine[1], send.at[2], recv.at[1], (x, place.k)),
            remote(block[0], mine[0], send.at[3], recv.at[2], (y, place.k)),
        ]
        onward = [
            remote(from_x[0], from_x[0], send.at[4], recv.at[4], (y, place.k)),
            remote(from_y[1], from_y[1], send.at[5], recv.at[5], (x, place.k)),
        ]
        return out, onward

    def keep(self, place, ins, outs, scratch):
        *_, sem, buffer = scratch
        return (
            pltpu.make_async_copy(self.source(ins), buffer, sem.at[0]),
            pltpu.make_async_copy(buffer, part_of(outs[0], self.dim, place.r, self.size), sem.at[1]),
        )

    def arrived(self, place, scratch, view, sem, row):
        return remote(view, view, scratch[0].at[0], scratch[1].at[sem], (row, place.k))

    def start(self, place, ins, outs, scratch, later):
        (dst,) = outs
        out, onward = self.copies(place, ins, outs, scratch)
        for copy in out:
            copy.start()
        load, store = self.keep(place, ins, outs, scratch)
        load.start()
        later.add(store.wait)
        x, y, d = place.rows()
        from_x, from_y, from_d = self.spots(dst, x), self.spots(dst, y), self.spots(dst, d)
        for view, sem, row in ((from_x[1], 1, x), (from_y[0], 2, y), (from_d[0], 4, y), (from_d[1], 5, x)):
            later.add(self.arrived(place, scratch, view, sem, row).wait_recv)
        for copy in (*out, *onward):
            later.add(copy.wait_send)

    def middle(self, place, ins, outs, scratch):
        (dst,) = outs
        x, y, d = place.rows()
        _, onward = self.copies(place, ins, outs, scratch)
        load, store = self.keep(place, ins, outs, scratch)
        load.wait()
        store.start()
        self.arrived(place, scratch, self.spots(dst, x)[0], 0, x).wait_recv()
        onward[0].start()
        self.arrived(place, scratch, self.spots(dst, y)[1], 3, y).wait_recv()
        onward[1].start()


class ScatterRows(Cargo):
    def __init__(self, grad, dim, phase=0):
        self.dim, self.phase = dim, phase
        self.arrays = (grad,)
        part = list(grad.shape)
        part[dim] //= 4
        self.size = part[dim]
        self.half = part[0] // 32 * 16
        self.rest = part[0] - self.half
        self.outs = (jax.ShapeDtypeStruct((2, *part), grad.dtype),)
        upper, lower = pltpu.VMEM((self.half, part[1]), grad.dtype), pltpu.VMEM((self.rest, part[1]), grad.dtype)
        self.scratch = (
            *(upper, lower, lower, upper, lower, upper),
            pltpu.SemaphoreType.DMA((6,)),
            pltpu.SemaphoreType.DMA((6,)),
            pltpu.SemaphoreType.DMA((2,)),
        )

    def spots(self, full, row):
        if self.dim:
            cut = pl.ds(pl.multiple_of(row * self.size, 128), self.size)
            return full.at[0 : self.half, cut], full.at[self.half :, cut]
        first = pl.multiple_of(row * self.size, 16)
        return full.at[pl.ds(first, self.half), :], full.at[pl.ds(first + self.half, self.rest), :]

    def copies(self, place, ins, outs, scratch):
        (src,), (dst,) = ins, outs
        via_x, via_y, own_x, own_y, sum_x, sum_y, send, recv, keep = scratch
        x, y, d = place.rows()
        for_x, for_y, for_d = self.spots(src, x), self.spots(src, y), self.spots(src, d)
        slot_x = dst.at[0, 0 : self.half, :], dst.at[0, self.half :, :]
        slot_y = dst.at[1, 0 : self.half, :], dst.at[1, self.half :, :]
        first = [
            remote(for_d[0], via_x, send.at[0], recv.at[0], (x, place.k)),
            remote(for_d[1], via_y, send.at[1], recv.at[1], (y, place.k)),
            remote(for_x[0], slot_x[0], send.at[2], recv.at[2], (x, place.k)),
            remote(for_y[1], slot_y[1], send.at[3], recv.at[3], (y, place.k)),
        ]
        held = [
            pltpu.make_async_copy(for_x[1], own_x, keep.at[0]),
            pltpu.make_async_copy(for_y[0], own_y, keep.at[1]),
        ]
        last = [
            remote(sum_x, slot_x[1], send.at[4], recv.at[4], (x, place.k)),
            remote(sum_y, slot_y[0], send.at[5], recv.at[5], (y, place.k)),
        ]
        return first, held, last

    def start(self, place, ins, outs, scratch, later):
        first, held, last = self.copies(place, ins, outs, scratch)
        for copy in (*first, *held):
            copy.start()
        for copy in (*first, *last):
            later.add(copy.wait_send)
        for copy in (*first[2:], *last):
            later.add(copy.wait_recv)

    def middle(self, place, ins, outs, scratch):
        via_x, via_y, own_x, own_y, sum_x, sum_y, *_ = scratch
        first, held, last = self.copies(place, ins, outs, scratch)
        held[0].wait()
        first[1].wait_recv()
        add_into(sum_x, [own_x, via_y])
        last[0].start()
        held[1].wait()
        first[0].wait_recv()
        add_into(sum_y, [own_y, via_x])
        last[1].start()


class Swap(Cargo):
    reach = "line"

    def __init__(self, *arrays, phase=0):
        self.arrays, self.phase = arrays, phase
        self.outs = tuple(jax.ShapeDtypeStruct(a.shape, a.dtype) for a in arrays)
        self.scratch = (pltpu.SemaphoreType.DMA((len(arrays),)), pltpu.SemaphoreType.DMA((len(arrays),)))

    def start(self, place, ins, outs, scratch, later):
        send, recv = scratch
        for i, (src, dst) in enumerate(zip(ins, outs)):
            copy = remote(src, dst, send.at[i], recv.at[i], place.at(place.z, 1 - place.c))
            copy.start()
            later.add(copy.wait)


def tile_owner(z, t):
    if t < 3:
        head = 3 * z + t
        return head // 2, head % 2
    return 3 + t, z // 2


class HeadsToChips(Cargo):
    reach = "col"

    def __init__(self, weight, biases, layer):
        self.layer = layer
        self.arrays = (weight, biases)
        self.outs = (jax.ShapeDtypeStruct((HALF, 5 * HD), LOW),)
        self.scratch = (
            pltpu.SemaphoreType.DMA((2, 2, 2, 2)),
            pltpu.SemaphoreType.DMA((5, 2)),
            pltpu.VMEM(weight.shape[1:], weight.dtype),
            pltpu.VMEM(biases.shape[1:], biases.dtype),
            pltpu.SemaphoreType.DMA((2,)),
        )

    def start(self, place, ins, outs, scratch, later):
        (slab,), (send, recv, weight, biases, load_sem) = outs, scratch
        for load in copy_in([(ins[0].at[self.layer], weight), (ins[1].at[self.layer], biases)], load_sem):
            load.wait()
        r, k, z, c = place.r, place.k, place.z, place.c
        query = k < 6
        rows = D // 8
        for second in range(2):
            for i in range(2):
                head = 2 * k + i
                chip = jnp.where(query, head // 3, 2 * i + second)
                t = jnp.where(query, head % 3, k - 3)
                cut = pl.ds(pl.multiple_of(t * HD, HD), HD)
                spots = slab.at[0:rows, cut], slab.at[rows:HALF, cut]
                for core in range(2):
                    here = k == 2 * chip + core
                    away = jnp.logical_not(here)
                    if second == 1:
                        here, away = here & (k >= 6), away & (k >= 6)
                    views = (
                        weight.at[core * rows : (core + 1) * rows, i * HD : (i + 1) * HD],
                        biases.at[i],
                    )
                    for part in range(2):
                        sem = send.at[i, second, core, part]
                        copy = remote(views[part], spots[part], sem, recv.at[t, part], (r, 2 * chip + core))
                        pl.when(away)(copy.start)
                        later.add(copy.wait_send, away)
                        keep = pltpu.make_async_copy(views[part], spots[part], sem)
                        pl.when(here)(keep.start)
                        later.add(keep.wait, here)
        for t in range(5):
            owner, _ = tile_owner(z, t)
            cut = slice(t * HD, (t + 1) * HD)
            for part, spot in enumerate((slab.at[0:rows, cut], slab.at[rows:HALF, cut])):
                came = remote(spot, spot, send.at[0, 0, 0, 0], recv.at[t, part], (r, owner))
                later.add(came.wait_recv, k != owner)


class HeadsToOwners(Cargo):
    reach = "col"

    def __init__(self, slab):
        self.arrays = (slab,)
        self.outs = (jax.ShapeDtypeStruct((2, 2, 2, HALF, HD), LOW),)
        self.scratch = (pltpu.SemaphoreType.DMA((5,)), pltpu.SemaphoreType.DMA((2, 2, 2)))

    def start(self, place, ins, outs, scratch, later):
        (slab,), (tiles,), (send, recv) = ins, outs, scratch
        r, k, z, c = place.r, place.k, place.z, place.c
        for t in range(5):
            owner, i = tile_owner(z, t)
            which = z % 2 if t >= 3 else 0
            view, spot = slab.at[:, t * HD : (t + 1) * HD], tiles.at[i, c, which]
            here = k == owner
            copy = remote(view, spot, send.at[t], recv.at[i, c, which], (r, owner))
            pl.when(jnp.logical_not(here))(copy.start)
            later.add(copy.wait_send, jnp.logical_not(here))
            keep = pltpu.make_async_copy(view, spot, send.at[t])
            pl.when(here)(keep.start)
            later.add(keep.wait, here)
        for i in range(2):
            for which in range(2):
                chip = jnp.where(k < 6, (2 * k + i) // 3, 2 * i + which)
                for core in range(2):
                    wanted = k != 2 * chip + core
                    if which == 1:
                        wanted = wanted & (k >= 6)
                    came = remote(
                        slab.at[:, 0:HD],
                        tiles.at[i, core, which],
                        send.at[0],
                        recv.at[i, core, which],
                        (r, 2 * chip + core),
                    )
                    later.add(came.wait_recv, wanted)


class Exchange(Cargo):
    def __init__(self, chunks, every_row=False, same=False):
        self.arrays = (chunks,)
        self.same = same
        self.rows_too = every_row
        self.reach = "all" if every_row else "col"
        lead = (4,) if every_row else (8,) if same else ()
        self.outs = (jax.ShapeDtypeStruct((*lead, *chunks.shape), chunks.dtype),)
        self.scratch = (pltpu.SemaphoreType.DMA((4, 8)), pltpu.SemaphoreType.DMA((4, 8)))

    def start(self, place, ins, outs, sems, later):
        (src,), (dst,), (send, recv) = ins, outs, sems
        r, k = place.r, place.k
        for rr in range(4) if self.rows_too else (None,):
            to_row = r if rr is None else rr
            for kk in range(8):
                here = (k == kk) if rr is None else (k == kk) & (r == rr)
                mine = dst.at[k] if rr is None else dst.at[r, k]
                theirs = dst.at[kk] if rr is None else dst.at[rr, kk]
                at = 0 if rr is None else rr
                my_at = 0 if rr is None else r
                part = src if self.same else src.at[kk]
                copy = remote(part, mine, send.at[at, kk], recv.at[my_at, k], (to_row, kk))
                pl.when(jnp.logical_not(here))(copy.start)
                later.add(copy.wait_send, jnp.logical_not(here))
                came = remote(part, theirs, send.at[at, kk], recv.at[at, kk], (to_row, kk))
                later.add(came.wait_recv, jnp.logical_not(here))
                keep = pltpu.make_async_copy(part, mine, send.at[at, kk])
                pl.when(here)(keep.start)
                later.add(keep.wait, here)


def add_into(dst, views):
    rows = dst.shape[0]

    def step(i, carry):
        cut = pl.ds(pl.multiple_of(i * 16, 16), 16)
        total = views[0][cut, :].astype(F32)
        for view in views[1:]:
            total = total + view[cut, :].astype(F32)
        dst[cut, :] = total.astype(dst.dtype)
        return carry

    lax.fori_loop(0, rows // 16, step, 0)


SUB = 4


class Reduce:
    @staticmethod
    def scratch(tokens, width):
        return [
            pltpu.VMEM((4, tokens, width), LOW),
            pltpu.VMEM((2, 4, tokens, width), LOW),
            pltpu.VMEM((4, tokens, width), LOW),
            pltpu.SemaphoreType.DMA((4,)),
            pltpu.SemaphoreType.DMA((4,)),
            pltpu.SemaphoreType.DMA((4, SUB)),
            pltpu.SemaphoreType.DMA((2, 4, SUB)),
        ]

    def __init__(self, place, part, out, scratch, both=True, far=False):
        self.place, self.part, self.out, self.both, self.far = place, part, out, both, far
        self.from_p, self.moved, self.held, self.send_p, self.recv_p, self.send, self.recv = scratch
        z, c = place.z, place.c
        self.edge = (z == 0) | (z == 3)
        self.mid = jnp.logical_not(self.edge)
        self.right, self.left = place.at(jnp.minimum(z + 1, 3), c), place.at(jnp.maximum(z - 1, 0), c)
        self.size = part.shape[1] // SUB

    def pair(self, j):
        place = self.place
        other = self.part.at[2 * j + 1 - place.c]
        return remote(other, self.from_p.at[j], self.send_p.at[j], self.recv_p.at[j], place.at(place.z, 1 - place.c))

    def piece(self, j, sub, way):
        rows = pl.ds(sub * self.size, self.size)
        column = jnp.where(way == 0, self.right[1], self.left[1])
        return remote(
            self.held.at[j, rows, :],
            self.moved.at[way, j, rows, :],
            self.send.at[j, sub],
            self.recv.at[way, j, sub],
            (self.place.r, column),
        )

    def terms(self, j):
        if self.both:
            return [self.part.at[2 * j + self.place.c], self.from_p.at[j]]
        return [self.part.at[j]]

    def made(self, j):
        z = self.place.z
        if self.both:
            self.pair(j).start()

        @pl.when(self.edge & (j != z))
        def _():
            if self.both:
                self.pair(j).wait_recv()
            add_into(self.held.at[j], self.terms(j))
            for sub in range(SUB):
                self.piece(j, sub, jnp.where(z == 0, 0, 1)).start()

    def finish(self, later, between):
        z = self.place.z
        way = jnp.where(z == 1, 0, 1)
        near, far, back = jnp.where(z == 1, 2, 1), jnp.where(z == 1, 3, 0), jnp.where(z == 1, 0, 3)
        first, second = (far, near) if self.far else (near, far)

        def step(j, sub, way):
            copy = self.piece(j, sub, way)
            copy.wait_recv()
            rows = pl.ds(sub * self.size, self.size)
            views = [view.at[rows, :] for view in (*self.terms(j), self.moved.at[way, j])]
            add_into(self.held.at[j].at[rows, :], views)
            copy.start()

        for i in range(2 * SUB):
            sub = i % SUB

            @pl.when(self.mid)
            def _(i=i, sub=sub):
                if self.both and sub == 0:
                    self.pair(first if i == 0 else second).wait_recv()
                if i < SUB:
                    step(first, sub, way)
                    return
                step(second, sub, way)
                if self.both and sub == 0:
                    self.pair(back).wait_recv()
                step(back, sub, 1 - way)

            between(i)
        if self.both:
            self.pair(z).wait_recv()

        def came(way):
            for sub in range(SUB):
                self.piece(z, sub, way).wait_recv()

        views = self.terms(z)

        @pl.when(self.edge)
        def _():
            way = jnp.where(z == 0, 1, 0)
            came(way)
            add_into(self.out, [*views, self.moved.at[way, z]])

        @pl.when(self.mid)
        def _():
            came(0)
            came(1)
            add_into(self.out, [*views, self.moved.at[0, z], self.moved.at[1, z]])

        for j in range(4):
            if self.both:
                later.add(self.pair(j).wait_send)
            for sub in range(SUB):
                later.add(self.piece(j, sub, 0).wait_send, z != j)


def far_first(place, p):
    z = place.z
    edge = jnp.where(z == 0, 3 - p, p)
    mid = jnp.where(p == 0, jnp.where(z == 1, 3, 0), jnp.where(p == 1, jnp.where(z == 1, 2, 1), jnp.where(p == 2, jnp.where(z == 1, 0, 3), z)))
    return jnp.where((z == 0) | (z == 3), edge, mid)


class Names:
    def __init__(self):
        self.next = 0

    def take(self):
        self.next += 1
        return self.next - 1


class Inner:
    def __init__(self, shape, dtype=LOW):
        self.shape, self.dtype = shape, dtype


def given_arrays(item):
    return [a for a in item.arrays if not isinstance(a, (From, Inner))]


def carry_kernel(body, reach, n_in, n_out, n_scratch, cargo, *refs):
    refs = list(refs)

    def pop(n):
        taken = refs[:n]
        del refs[:n]
        return taken

    ins = pop(n_in)
    given = [pop(len(given_arrays(item))) for item in cargo]
    outs = pop(n_out)
    made = {item: pop(len(item.outs)) for item in cargo}
    scratch = pop(n_scratch)
    held = {item: pop(len(item.scratch)) for item in cargo}
    taken = {
        item: [
            made[a.item][a.at] if isinstance(a, From) else a if isinstance(a, Inner) else mine.pop(0)
            for a in item.arrays
        ]
        for item, mine in zip(cargo, given)
    }
    place = Place()
    later = Later()
    owed = [Later() for _ in range(4)]
    greet(place, {reach, *(item.reach for item in cargo)})

    def start(phase, *inner):
        inner = list(inner)
        mine = [item for item in cargo if item.phase == phase]
        for before in sorted({a.item.phase for item in mine for a in item.arrays if isinstance(a, From)}):
            owed[before].run()
        for item in mine:
            taken[item] = [inner.pop(0) if isinstance(a, Inner) else a for a in taken[item]]
            item.start(place, taken[item], made[item], held[item], owed[phase])

    def middle(phase=0):
        for item in cargo:
            if item.phase == phase:
                item.middle(place, taken[item], made[item], held[item])

    body(place, ins, outs, scratch, later, middle, start)
    later.run()
    for waits in owed:
        waits.run()


def carry_call(names, body, reach, arrays, in_specs, outs, out_specs, scratch, cargo, name=None):
    given = [a for item in cargo for a in given_arrays(item)]
    call = pl.pallas_call(
        partial(carry_kernel, body, reach, len(arrays), len(outs), len(scratch), cargo),
        out_shape=[*outs, *(o for item in cargo for o in item.outs)],
        in_specs=[*in_specs, *(ANY for _ in given)],
        out_specs=[*out_specs, *(ANY for item in cargo for _ in item.outs)],
        scratch_shapes=[*scratch, *(s for item in cargo for s in item.scratch)],
        compiler_params=pltpu.CompilerParams(
            collective_id=names.take(), has_side_effects=True, vmem_limit_bytes=VMEM
        ),
        name=name,
    )
    results = list(call(*arrays, *given))
    main = results[: len(outs)]
    rest = results[len(outs) :]
    loads = []
    for item in cargo:
        loads.append(rest[: len(item.outs)])
        rest = rest[len(item.outs) :]
    return main, loads


class Gather:
    scratch = (
        pltpu.SemaphoreType.DMA((4,)),
        pltpu.SemaphoreType.DMA((4,)),
        pltpu.SemaphoreType.DMA((8,)),
        pltpu.SemaphoreType.DMA((8,)),
        pltpu.SemaphoreType.DMA((1,)),
    )

    def __init__(self, place, block, full, sems, both=True):
        self.place, self.block, self.full, self.both = place, block, full, both
        self.send_r, self.send_l, self.send_p, self.recv, self.keep = sems

    def spot(self, zz, c):
        return self.full.at[2 * zz + c] if self.both else self.full.at[zz]

    def copies(self, src, zz, t, way):
        z, c = self.place.z, self.place.c
        spot, sem = self.spot(zz, c), self.recv.at[2 * zz + c]
        right = remote(src, spot, self.send_r.at[t], sem, self.place.at(jnp.minimum(z + 1, 3), c))
        left = remote(src, spot, self.send_l.at[t], sem, self.place.at(jnp.maximum(z - 1, 0), c))
        partner = remote(src, spot, self.send_p.at[2 * t + way], sem, self.place.at(z, 1 - c))
        return right, left, partner

    def start(self, later):
        z, c = self.place.z, self.place.c
        right, left, partner = self.copies(self.block, z, 0, 0)
        pl.when(z < 3)(right.start)
        pl.when(z > 0)(left.start)
        later.add(right.wait_send, z < 3)
        later.add(left.wait_send, z > 0)
        if self.both:
            partner.start()
            later.add(partner.wait_send)
        keep = pltpu.make_async_copy(self.block, self.spot(z, c), self.keep.at[0])
        keep.start()
        keep.wait()
        for t in range(1, 4):
            for way in (0, 1):
                zz, valid, onward, may, partner = self.step(t, way)
                later.add(onward.wait_send, valid & may)
                if self.both:
                    later.add(partner.wait_send, valid)

    def step(self, t, way):
        z = self.place.z
        there = z + (2 * way - 1) * t
        zz = jnp.clip(there, 0, 3)
        right, left, partner = self.copies(self.spot(zz, self.place.c), zz, t, way)
        onward, may = (left, z > 0) if way else (right, z < 3)
        return zz, (there >= 0) & (there <= 3), onward, may, partner

    def pass_on(self, t):
        for way in (0, 1):
            _, valid, onward, may, partner = self.step(t, way)

            @pl.when(valid)
            def _(onward=onward, may=may, partner=partner):
                onward.wait_recv()
                pl.when(may)(onward.start)
                if self.both:
                    partner.start()

    def chunk(self, p):
        z, c = self.place.z, self.place.c
        edge = (z == 0) | (z == 3)
        t = jnp.where(edge, p, (p + 1) // 2)
        pl.when((p >= 1) & (edge | (p != 2)))(lambda: self.pass_on(t))
        second = jnp.where(z == 0, 1, z - 1)
        third = jnp.where(z == 0, 2, jnp.where(z == 3, 1, z + 1))
        fourth = jnp.where(z <= 1, 3, 0)
        j = jnp.where(p == 0, z, jnp.where(p == 1, second, jnp.where(p == 2, third, fourth)))
        if self.both:
            spot = self.spot(j, 1 - c)
            remote(spot, spot, self.send_p.at[0], self.recv.at[2 * j + 1 - c], self.place.at(z, 1 - c)).wait_recv()
        return j


def forward_feed(names, block, w_gate, w_up, w_down, cargo, name):
    tokens, width = block.shape
    inner = w_gate.shape[0]

    def body(place, ins, outs, scratch, later, middle, start):
        block_ref, gate_hbm, up_hbm, down_hbm = ins
        total, full_out, gate_out, up_out = outs
        n = len(Gather.scratch)
        gather_sems, scratch = scratch[:n], scratch[n:]
        full, part, gate_w, up_w, down_w, gates, ups, load_sem, keep_sem = scratch[:9]
        reduce = Reduce(place, part, total, scratch[9:])
        gather = Gather(place, block_ref, full, gather_sems)
        loads = [
            pltpu.make_async_copy(src, dst, load_sem.at[i])
            for i, (src, dst) in enumerate(((gate_hbm, gate_w), (up_hbm, up_w), (down_hbm, down_w)))
        ]
        for load in loads:
            load.start()
        gather.start(later)
        start(0)
        start(3)
        for load in loads:
            load.wait()

        def keep(j):
            rows = pl.ds(pl.multiple_of(2 * tokens * j, 2 * tokens), 2 * tokens)
            return [
                pltpu.make_async_copy(full.at[pl.ds(2 * j, 2)], full_out.at[pl.ds(2 * j, 2)], keep_sem.at[0, j]),
                pltpu.make_async_copy(gates.at[rows, :], gate_out.at[rows, :], keep_sem.at[1, j]),
                pltpu.make_async_copy(ups.at[rows, :], up_out.at[rows, :], keep_sem.at[2, j]),
            ]

        def step(p, carry):
            j = gather.chunk(p)
            pl.when(p == 2)(middle)
            acts = full[pl.ds(2 * j, 2)].reshape(2 * tokens, width)
            rows = pl.ds(pl.multiple_of(2 * tokens * j, 2 * tokens), 2 * tokens)
            gate = dot_t(acts, gate_w[...])
            up = dot_t(acts, up_w[...])
            gates[rows, :] = gate.astype(LOW)
            ups[rows, :] = up.astype(LOW)
            hidden = (gate * jax.nn.sigmoid(gate) * up).astype(LOW)
            sums = jnp.dot(hidden, down_w[...], preferred_element_type=F32).astype(LOW)
            part[pl.ds(2 * j, 2)] = sums.reshape(2, tokens, width)
            reduce.made(j)
            for copy in keep(j):
                copy.start()
            return carry

        lax.fori_loop(0, 4, step, 0)
        start(1)
        start(2)
        reduce.finish(later, lambda i: middle(3) if i == 0 else None)
        for j in range(4):
            for copy in keep(j):
                copy.wait()

    (total, full, gate, up), loads = carry_call(
        names,
        body,
        "line",
        [block, w_gate, w_up, w_down],
        [ONCHIP, ANY, ANY, ANY],
        [
            jax.ShapeDtypeStruct((tokens, width), F32),
            jax.ShapeDtypeStruct((8, tokens, width), LOW),
            jax.ShapeDtypeStruct((8 * tokens, inner), LOW),
            jax.ShapeDtypeStruct((8 * tokens, inner), LOW),
        ],
        [ONCHIP, ANY, ANY, ANY],
        [
            *Gather.scratch,
            pltpu.VMEM((8, tokens, width), LOW),
            pltpu.VMEM((8, tokens, width), LOW),
            pltpu.VMEM(w_gate.shape, LOW),
            pltpu.VMEM(w_up.shape, LOW),
            pltpu.VMEM(w_down.shape, LOW),
            pltpu.VMEM((8 * tokens, inner), LOW),
            pltpu.VMEM((8 * tokens, inner), LOW),
            pltpu.SemaphoreType.DMA((3,)),
            pltpu.SemaphoreType.DMA((3, 4)),
            *Reduce.scratch(tokens, width),
        ],
        cargo,
        name=name,
    )
    return total, full.reshape(8 * tokens, width), gate, up, loads


def rows_of(first, count):
    return pl.ds(pl.multiple_of(first, count), count)


def copy_in(pairs, sem):
    copies = [pltpu.make_async_copy(src, dst, sem.at[i]) for i, (src, dst) in enumerate(pairs)]
    for copy in copies:
        copy.start()
    return copies


def open_call(names, shard, cargo):
    def body(place, ins, outs, scratch, later, middle, start):
        gather = Gather(place, ins[0], outs[0], scratch)
        gather.start(later)
        start(0)
        start(3)
        start(1)
        gather.pass_on(1)
        middle(1)
        gather.pass_on(2)
        middle(3)
        start(2)
        gather.pass_on(3)
        for zz in range(4):
            spot = gather.spot(zz, 1 - place.c)
            recv = gather.recv.at[2 * zz + 1 - place.c]
            later.add(remote(spot, spot, gather.send_p.at[0], recv, place.at(place.z, 1 - place.c)).wait_recv)

    (full,), loads = carry_call(
        names,
        body,
        "line",
        [shard],
        [ANY],
        [jax.ShapeDtypeStruct((8, *shard.shape), shard.dtype)],
        [ANY],
        list(Gather.scratch),
        cargo,
        name="open",
    )
    return full, loads


def close_call(names, cargo, name):
    def body(place, ins, outs, scratch, later, middle, start):
        start(0)
        middle(0)

    return carry_call(names, body, "col", [], [], [], [], [], cargo, name=name)[1]


def heads_of(ref, rows):
    return jnp.concatenate([ref[rows, h * HD : (h + 1) * HD] for h in range(3)], axis=0)


def block_probs(qkv, starts, b):
    reach = QB + SEQ_MAX
    first = jnp.maximum(b - SEQ_MAX // QB, 0) * QB
    rows, window = rows_of(b * QB, QB), pl.ds(pl.multiple_of(first, QB), reach)
    queries = heads_of(qkv, rows)
    keys, values = qkv[window, 3 * HD : 4 * HD], qkv[window, 4 * HD : 5 * HD]
    scores = (dot_t(queries, keys) * HD ** (-0.5)).reshape(3, QB, reach)
    key_at = first + lax.broadcasted_iota(jnp.int32, (QB, reach), 1)
    query_at = b * QB + lax.broadcasted_iota(jnp.int32, (QB, reach), 0)
    allowed = (key_at >= starts[rows, :]) & (key_at <= query_at)
    masked = jnp.where(allowed[None], scores, neg_fill)
    lifted = jnp.exp(masked - jnp.max(masked, axis=-1, keepdims=True))
    probs = lifted * (1.0 / jnp.sum(lifted, axis=-1, keepdims=True))
    return queries, keys, values, probs, rows, window


def roll_half(values):
    return pltpu.roll(values, HD // 2, 1)


def forward_heads(names, block, wide, gain, w_qkv, bias, w_out, cosine, sine, starts, cargo, name):
    tokens, width = QB, D
    count = 8 * QB
    apart = wide is not None

    def body(place, ins, outs, scratch, later, middle, start):
        ins = list(ins)
        block_ref = ins.pop(0)
        if apart:
            wide_hbm, gain_ref = ins.pop(0), ins.pop(0)
        qkv_hbm, bias_ref, out_hbm, cos_ref, sin_ref, starts_ref = ins
        total, full_out, qkv_out, mixed_out = outs[:4]
        scratch = list(scratch)
        gather_sems = [scratch.pop(0) for _ in Gather.scratch]
        full, acts, flat, part, qkv_w, out_w, qkv, mixed, load_sem, keep_sem = scratch[:10]
        reduce = Reduce(place, part, total, scratch[10:], both=False, far=True)
        pairs = [(qkv_hbm, qkv_w), (out_hbm, out_w)]
        if apart:
            pairs.append((wide_hbm, acts))
        loads = copy_in(pairs, load_sem)
        gather = Gather(place, block_ref, full, gather_sems)
        gather.start(later)
        start(0)
        start(3)
        for load in loads:
            load.wait()

        def keep(j):
            if apart:
                rows = rows_of(j * 2 * QB, 2 * QB)
                return pltpu.make_async_copy(flat.at[rows, :], full_out.at[rows, :], keep_sem.at[j])
            return pltpu.make_async_copy(full.at[pl.ds(2 * j, 2)], full_out.at[pl.ds(2 * j, 2)], keep_sem.at[j])

        def step(p, carry):
            j = gather.chunk(p)
            pl.when(p == 2)(middle)
            rows = rows_of(j * 2 * QB, 2 * QB)
            if apart:
                chunk = acts[:, rows].astype(F32)
                scale = lax.rsqrt(jnp.mean(chunk * chunk, axis=0, keepdims=True) + eps_norm)
                chunk = (chunk * scale * gain_ref[...]).astype(LOW)
                acts[:, rows] = chunk
                raw = t_dot(chunk, qkv_w[...]) + bias_ref[...]
            else:
                keep(j).start()
                raw = jnp.dot(full[pl.ds(2 * j, 2)].reshape(2 * tokens, width), qkv_w[...], preferred_element_type=F32)
                raw = raw + bias_ref[...]
            cos, sin = cos_ref[rows, :], sin_ref[rows, :]
            for t in range(5):
                head = raw[:, t * HD : (t + 1) * HD]
                if t < 4:
                    head = head * cos + roll_half(head) * sin
                qkv[rows, t * HD : (t + 1) * HD] = head.astype(LOW)
            return carry

        lax.fori_loop(0, 4, step, 0)
        start(1)

        def attend(p, carry):
            j = far_first(place, p)
            _, _, values, probs, _, _ = block_probs(qkv, starts_ref, 2 * j + place.c)
            low = probs.astype(LOW).reshape(3 * QB, QB + SEQ_MAX)
            heads = jnp.dot(low, values, preferred_element_type=F32).astype(LOW)
            both = jnp.concatenate([heads[h * QB : (h + 1) * QB] for h in range(3)], axis=1)
            mixed[rows_of(j * QB, QB), :] = both
            part[j] = jnp.dot(both, out_w[...], preferred_element_type=F32).astype(LOW)
            reduce.made(j)
            return carry

        lax.fori_loop(0, 4, attend, 0)
        saves = copy_in([(qkv, qkv_out), (mixed, mixed_out)], load_sem)
        if apart:
            saves.append(pltpu.make_async_copy(acts, outs[4], load_sem.at[2]))
            saves[-1].start()

        def between(i):
            if i == 0:
                middle(3)
            if not apart or i % 2:
                return
            j = i // 2

            def turn(t, carry):
                rows = rows_of(t * 2 * QB, 2 * QB)
                piece = full[2 * j : 2 * j + 2, :, rows].reshape(D // 4, 2 * QB)
                flat[rows, j * (D // 4) : (j + 1) * (D // 4)] = piece.T
                return carry

            lax.fori_loop(0, 4, turn, 0)

        reduce.finish(later, between)
        if apart:
            for j in range(4):
                keep(j).start()
        for copy in saves:
            copy.wait()
        for j in range(4):
            keep(j).wait()

    gathered = (count, width) if apart else (8, tokens, width)
    results, loads = carry_call(
        names,
        body,
        "line",
        [block, *([wide, gain] if apart else []), w_qkv, bias, w_out, cosine, sine, starts],
        [ONCHIP, *([ANY, ONCHIP] if apart else []), ANY, ONCHIP, ANY, ONCHIP, ONCHIP, ONCHIP],
        [
            jax.ShapeDtypeStruct((tokens, width), F32),
            jax.ShapeDtypeStruct(gathered, LOW),
            jax.ShapeDtypeStruct((count, 5 * HD), LOW),
            jax.ShapeDtypeStruct((count // 2, 3 * HD), LOW),
            *([jax.ShapeDtypeStruct((width, count), LOW)] if apart else []),
        ],
        [ONCHIP, ANY, ANY, ANY, *([ANY] if apart else [])],
        [
            *Gather.scratch,
            pltpu.VMEM((8, *block.shape), LOW),
            pltpu.VMEM((width, count) if apart else (16, 128), LOW),
            pltpu.VMEM((count, width) if apart else (16, 128), LOW),
            pltpu.VMEM((4, tokens, width), LOW),
            pltpu.VMEM(w_qkv.shape, LOW),
            pltpu.VMEM(w_out.shape, LOW),
            pltpu.VMEM((count, 5 * HD), LOW),
            pltpu.VMEM((count // 2, 3 * HD), LOW),
            pltpu.SemaphoreType.DMA((3,)),
            pltpu.SemaphoreType.DMA((4,)),
            *Reduce.scratch(tokens, width),
        ],
        cargo,
        name=name,
    )
    total, full, qkv, mixed = results[:4]
    return total, full.reshape(count, width), qkv, mixed, results[4] if apart else None, loads


def backward_heads(names, block, acts, turned, w_qkv, w_out, qkv, mixed, cosine, sine, starts, cargo, name):
    tokens, width = QB, D
    count = 8 * QB
    reach = QB + SEQ_MAX

    def body(place, ins, outs, scratch, later, middle, start):
        block_ref, acts_hbm, qkv_hbm, out_hbm, saved_hbm, mixed_hbm, cos_ref, sin_ref, starts_ref = ins
        total, slab_out, out_out = outs
        scratch = list(scratch)
        gather_sems = [scratch.pop(0) for _ in Gather.scratch]
        full, part, qkv_w, out_w, qkv, mixed, acts_own, d_raw, d_keys, d_values = scratch[:10]
        slab, d_out, slab_in, d_out_in, load_sem, swap_send, swap_recv = scratch[10:17]
        reduce = Reduce(place, part, total, scratch[17:], far=True)
        pairs = [(qkv_hbm, qkv_w), (out_hbm, out_w), (saved_hbm, qkv), (mixed_hbm, mixed), (acts_hbm, acts_own)]
        loads = copy_in(pairs, load_sem)
        gather = Gather(place, block_ref, full, gather_sems, both=False)
        gather.start(later)
        start(0)
        start(3)
        d_keys[...] = jnp.zeros_like(d_keys)
        d_values[...] = jnp.zeros_like(d_values)
        for load in loads:
            load.wait()

        def step(p, carry):
            j = gather.chunk(p)
            pl.when(p == 2)(middle)
            b = 2 * j + place.c
            d_mixed = dot_t(full[j], out_w[...]).astype(LOW)
            d_heads = jnp.concatenate([d_mixed[:, h * HD : (h + 1) * HD] for h in range(3)], axis=0)
            queries, keys, values, probs, rows, window = block_probs(qkv, starts_ref, b)
            d_probs = dot_t(d_heads, values).reshape(3, QB, reach)
            inner = jnp.sum(probs * d_probs, axis=-1, keepdims=True)
            d_scores = (probs * (d_probs - inner)).astype(LOW).reshape(3 * QB, reach)
            d_queries = jnp.dot(d_scores, keys, preferred_element_type=F32) * HD ** (-0.5)
            d_keys[window, :] += t_dot(d_scores, queries) * HD ** (-0.5)
            d_values[window, :] += t_dot(probs.astype(LOW).reshape(3 * QB, reach), d_heads)
            cos, sin = cos_ref[rows, :], sin_ref[rows, :]
            for h in range(3):
                head = d_queries[h * QB : (h + 1) * QB]
                head = head * cos + roll_half(head * sin)
                d_raw[rows, h * HD : (h + 1) * HD] = head.astype(LOW)
            other = rows_of((2 * j + 1 - place.c) * QB, QB)
            d_raw[other, 0 : 3 * HD] = jnp.zeros((QB, 3 * HD), LOW)
            return carry

        lax.fori_loop(0, 4, step, 0)
        start(1)

        def project(p, carry):
            j = far_first(place, p)
            rows = rows_of(j * 2 * QB, 2 * QB)
            head = d_keys[rows, :]
            head = head * cos_ref[rows, :] + roll_half(head * sin_ref[rows, :])
            d_raw[rows, 3 * HD : 4 * HD] = head.astype(LOW)
            d_raw[rows, 4 * HD : 5 * HD] = d_values[rows, :].astype(LOW)
            part[pl.ds(2 * j, 2)] = dot_t(d_raw[rows, :], qkv_w[...]).astype(LOW).reshape(2, tokens, width)
            reduce.made(j)
            return carry

        lax.fori_loop(0, 4, project, 0)

        def swap():
            to = place.at(place.z, 1 - place.c)
            return [
                remote(slab.at[1 - place.c], slab_in, swap_send.at[0], swap_recv.at[0], to),
                remote(d_out.at[1 - place.c], d_out_in, swap_send.at[1], swap_recv.at[1], to),
            ]

        def between(i):
            if i < 4:
                cut = slice(i * (D // 4), (i + 1) * (D // 4))
                if turned:
                    grads = jnp.dot(acts_own[cut, :], d_raw[...], preferred_element_type=F32).astype(LOW)
                else:
                    grads = t_dot(acts_own[:, cut], d_raw[...]).astype(LOW)
                slab[0, i, 0 : D // 8, :] = grads[: D // 8]
                slab[1, i, 0 : D // 8, :] = grads[D // 8 :]
            elif i == 4:
                sums = jnp.sum(d_raw[...].astype(F32), axis=0, keepdims=True)
                first = lax.broadcasted_iota(jnp.int32, (16, 5 * HD), 0) == 0
                tail = jnp.where(first, sums, 0.0).astype(LOW)
                for half in range(2):
                    for part_at in range(4):
                        slab[half, part_at, D // 8 :, :] = tail
                grads = t_dot(mixed[...], full[...].reshape(4 * QB, D)).astype(LOW)
                d_out[0] = grads[: D // 8]
                d_out[1] = grads[D // 8 :]
                for copy in swap():
                    copy.start()
            if i == 0:
                middle(3)

        reduce.finish(later, between)
        for copy in swap():
            copy.wait()
        for i in range(4):
            add_into(slab_out.at[i], [slab.at[place.c, i], slab_in.at[i]])
        add_into(out_out, [d_out.at[place.c], d_out_in])

    (total, slab, d_out), loads = carry_call(
        names,
        body,
        "line",
        [block, acts, w_qkv, w_out, qkv, mixed, cosine, sine, starts],
        [ONCHIP, ANY, ANY, ANY, ANY, ANY, ONCHIP, ONCHIP, ONCHIP],
        [
            jax.ShapeDtypeStruct((tokens, width), F32),
            jax.ShapeDtypeStruct((4, HALF, 5 * HD), LOW),
            jax.ShapeDtypeStruct((D // 8, D), LOW),
        ],
        [ONCHIP, ONCHIP, ONCHIP],
        [
            *Gather.scratch,
            pltpu.VMEM((4, tokens, width), LOW),
            pltpu.VMEM((8, tokens, width), LOW),
            pltpu.VMEM(w_qkv.shape, LOW),
            pltpu.VMEM(w_out.shape, LOW),
            pltpu.VMEM((count, 5 * HD), LOW),
            pltpu.VMEM((count // 2, 3 * HD), LOW),
            pltpu.VMEM(acts.shape, LOW),
            pltpu.VMEM((count, 5 * HD), LOW),
            pltpu.VMEM((count, HD), F32),
            pltpu.VMEM((count, HD), F32),
            pltpu.VMEM((2, 4, HALF, 5 * HD), LOW),
            pltpu.VMEM((2, D // 8, D), LOW),
            pltpu.VMEM((4, HALF, 5 * HD), LOW),
            pltpu.VMEM((D // 8, D), LOW),
            pltpu.SemaphoreType.DMA((5,)),
            pltpu.SemaphoreType.DMA((2,)),
            pltpu.SemaphoreType.DMA((2,)),
            *Reduce.scratch(tokens, width),
        ],
        cargo,
        name=name,
    )
    return total, slab.reshape(4 * HALF, 5 * HD), d_out, loads


def settle_rows(row, fulls, slots):
    kinds, layers = len(fulls), len(fulls[0])
    count, size = slots[0][0].shape[1:]
    tile = count // 5

    def kernel(row_ref, *refs):
        ins, outs = refs[: 2 * kinds * layers], refs[2 * kinds * layers :]
        for kind in range(kinds):
            for layer in range(layers):
                full, slot = ins[2 * (kind * layers + layer)], ins[2 * (kind * layers + layer) + 1]
                outs[kind][layer] = full[...].astype(F32) + slot[0].astype(F32) + slot[1].astype(F32)

    pairs = [pair for kind in range(kinds) for pair in zip(fulls[kind], slots[kind])]
    return pl.pallas_call(
        kernel,
        out_shape=[jax.ShapeDtypeStruct((layers, count, size), F32)] * kinds,
        grid_spec=pltpu.PrefetchScalarGridSpec(
            num_scalar_prefetch=1,
            grid=(count // tile,),
            in_specs=[
                pl.BlockSpec((tile, size), lambda i, row: (i, row[0])),
                pl.BlockSpec((2, tile, size), lambda i, row: (0, i, 0)),
            ]
            * (kinds * layers),
            out_specs=[pl.BlockSpec((layers, tile, size), lambda i, row: (0, i, 0))] * kinds,
        ),
        compiler_params=pltpu.CompilerParams(vmem_limit_bytes=VMEM),
        name="settle",
    )(row.reshape(1), *[array for pair in pairs for array in pair])


def backward_feed(names, block, grads_all, acts, w_gate, w_up, w_down, gate, up, cargo, name):
    tokens, width = QB, D
    inner = w_gate.shape[0]
    apart = grads_all is not None

    def body(place, ins, outs, scratch, later, middle, start):
        head_ref, acts_hbm, gate_hbm, up_hbm, down_hbm, gates_hbm, ups_hbm = ins
        total, gate_out, up_out, down_out = outs
        scratch = list(scratch)
        gather_sems = [scratch.pop(0) for _ in Gather.scratch]
        full, part, acts_own, gate_w, up_w, down_w, gates, ups, hiddens, load_sem, keep_sem = scratch[:11]
        reduce = Reduce(place, part, total, scratch[11:], far=apart)
        pairs = [(down_hbm, down_w), (gates_hbm, gates), (ups_hbm, ups), (gate_hbm, gate_w), (up_hbm, up_w)]
        pairs.append((acts_hbm, acts_own))
        if apart:
            pairs.append((head_ref, full))
        loads = copy_in(pairs, load_sem)
        gather = None
        if not apart:
            gather = Gather(place, head_ref, full, gather_sems)
            gather.start(later)
        start(0)
        start(3)
        for load in loads:
            load.wait()

        def step(p, carry):
            j = far_first(place, p) if apart else gather.chunk(p)
            pl.when(p == 2)(middle)
            rows = rows_of(j * 2 * tokens, 2 * tokens)
            grads = full[pl.ds(2 * j, 2)].reshape(2 * tokens, width)
            d_hidden = dot_t(grads, down_w[...])
            gate, up = gates[rows, :].astype(F32), ups[rows, :].astype(F32)
            squash = jax.nn.sigmoid(gate)
            lit = gate * squash
            hiddens[rows, :] = (lit * up).astype(LOW)
            d_gate = (d_hidden * up * squash * (1.0 + gate * (1.0 - squash))).astype(LOW)
            d_up = (d_hidden * lit).astype(LOW)
            gates[rows, :] = d_gate
            ups[rows, :] = d_up
            sums = dot(d_gate, gate_w[...]) + dot(d_up, up_w[...])
            part[pl.ds(2 * j, 2)] = sums.astype(LOW).reshape(2, tokens, width)
            reduce.made(j)
            return carry

        lax.fori_loop(0, 4, step, 0)

        def weights(dst, left, right, low, high):
            def tile(i, carry):
                cut = pl.ds(pl.multiple_of(i * 256, 256), 256)
                dst[cut, :] = t_dot(left[:, cut], right()).astype(LOW)
                return carry

            whole = inner // 256
            lax.fori_loop(low, min(high, whole), tile, 0)
            if high > whole and inner % 256:
                dst[whole * 256 :, :] = t_dot(left[:, whole * 256 :], right()).astype(LOW)

        def grads_flat():
            return full[...].reshape(8 * tokens, width)

        def acts_flat():
            return acts_own[...]

        work = [
            (down_w, hiddens, grads_flat, 0, 3),
            (down_w, hiddens, grads_flat, 3, 5),
            (gate_w, gates, acts_flat, 0, 3),
            (gate_w, gates, acts_flat, 3, 5),
            (up_w, ups, acts_flat, 0, 3),
            (up_w, ups, acts_flat, 3, 5),
        ]

        def between(i):
            if i < len(work):
                weights(*work[i])
            if i == 1:
                start(1, down_w)
            if i == 5:
                middle(1)

        reduce.finish(later, between)
        for copy in copy_in([(gate_w, gate_out), (up_w, up_out), (down_w, down_out)], keep_sem):
            copy.wait()

    head = grads_all.reshape(8, tokens, width) if apart else block
    (total, d_gate, d_up, d_down), loads = carry_call(
        names,
        body,
        "line",
        [head, acts, w_gate, w_up, w_down, gate, up],
        [ANY if apart else ONCHIP, ANY, ANY, ANY, ANY, ANY, ANY],
        [
            jax.ShapeDtypeStruct((tokens, width), F32),
            jax.ShapeDtypeStruct(w_gate.shape, LOW),
            jax.ShapeDtypeStruct(w_up.shape, LOW),
            jax.ShapeDtypeStruct(w_down.shape, LOW),
        ],
        [ONCHIP, ANY, ANY, ANY],
        [
            *Gather.scratch,
            pltpu.VMEM((8, tokens, width), LOW),
            pltpu.VMEM((8, tokens, width), LOW),
            pltpu.VMEM((8 * tokens, width), LOW),
            pltpu.VMEM(w_gate.shape, LOW),
            pltpu.VMEM(w_up.shape, LOW),
            pltpu.VMEM(w_down.shape, LOW),
            pltpu.VMEM((8 * tokens, inner), LOW),
            pltpu.VMEM((8 * tokens, inner), LOW),
            pltpu.VMEM((8 * tokens, inner), LOW),
            pltpu.SemaphoreType.DMA((7,)),
            pltpu.SemaphoreType.DMA((3,)),
            *Reduce.scratch(tokens, width),
        ],
        cargo,
        name=name,
    )
    return total, d_gate, d_up, d_down, loads


eps_norm = 1e-06
rope_base = 1000000.0
neg_fill = -1e30


def row_starts(sizes, count):
    ends = jnp.cumsum(sizes)
    firsts = ends - sizes
    places = jnp.arange(count, dtype=jnp.int32)
    inside = (places[None, :] >= firsts[:, None]) & (places[None, :] < ends[:, None])
    return jnp.sum(jnp.where(inside, firsts[:, None], 0), axis=0)


def rope_tables(positions):
    half = HD // 2
    freq = rope_base ** (-(jnp.arange(half, dtype=jnp.float32) * (2.0 / HD)))
    angle = freq[:, None] * positions.astype(jnp.float32)[None, :]
    cosine = jnp.concatenate([jnp.cos(angle), jnp.cos(angle)], axis=0)
    sine = jnp.concatenate([jnp.sin(angle), jnp.sin(angle)], axis=0)
    return (cosine, sine)


def rotate(values, cosine, sine):
    half = HD // 2
    turned = jnp.concatenate([-values[:, half:], values[:, :half]], axis=1)
    return values * cosine + turned * sine


def rotate_back(grads, cosine, sine):
    half = HD // 2
    lifted = grads * sine
    turned = jnp.concatenate([lifted[:, half:], -lifted[:, :half]], axis=1)
    return grads * cosine + turned


def contract_first(left, right):
    return lax.dot_general(
        left, right, (((0,), (0,)), ((), ())), preferred_element_type=jnp.float32
    )


def contract_last(left, right):
    return lax.dot_general(
        left, right, (((1,), (1,)), ((), ())), preferred_element_type=jnp.float32
    )


def feature_total(values):
    return lax.psum(jnp.sum(values, axis=0), "col")


def spread(values):
    return lax.all_gather(values, "col", axis=0, tiled=True)


def summed_rows(make_term, rows):
    return lax.psum_scatter(
        make_term(jnp.int32(0), lax.axis_size("col") * rows), "col", scatter_dimension=0, tiled=True
    )


def to_blocks(values):
    return lax.all_to_all(values, "col", split_axis=1, concat_axis=0, tiled=True)


def to_tokens(values):
    return lax.all_to_all(values, "col", split_axis=0, concat_axis=1, tiled=True)


def by_columns(weight, acts, start, count):
    return contract_first(weight, acts)


def by_rows(weight, grads, start, count):
    return jnp.dot(weight, grads, preferred_element_type=jnp.float32)


def by_rows_pair(first_weight, first_grads, second_weight, second_grads, start, count):
    return by_rows(first_weight, first_grads, start, count) + by_rows(
        second_weight, second_grads, start, count
    )


def norm_forward(residual, gain):
    totals = feature_total(residual * residual)
    scale = lax.rsqrt(totals / D + eps_norm)
    return (scale, (residual * scale * gain[:, None]).astype(jnp.bfloat16))


def norm_backward(d_normed, residual, scale, gain):
    weighted = d_normed * gain[:, None]
    inner = feature_total(weighted * residual)
    d_residual = weighted * scale - residual * (scale * scale * scale) * inner / D
    d_gain = jnp.sum(d_normed * residual * scale, axis=1)
    return (d_residual, d_gain)


def attend_scores(queries, keys, mask):
    scores = jnp.einsum(
        "kghq,khj->kgqj", queries, keys, preferred_element_type=jnp.float32
    ) * HD ** (-0.5)
    return jnp.where(mask[None, None], scores, neg_fill)


def per_device(
    hidden_states,
    out_grad,
    lengths,
    norm_gains,
    qkv_weight,
    qkv_bias,
    out_weight,
    gate_weight,
    up_weight,
    down_weight,
):
    feat_rows, tok_row = hidden_states.shape
    col_at = lax.axis_index("col")
    starts = row_starts(lengths[0], tok_row)
    positions = jnp.arange(tok_row, dtype=jnp.int32) - starts
    cosine, sine = rope_tables(positions)
    first = col_at * QB
    block_starts = lax.dynamic_slice_in_dim(starts, first, QB)
    cos_block = lax.dynamic_slice_in_dim(cosine, first, QB, 1)
    sin_block = lax.dynamic_slice_in_dim(sine, first, QB, 1)
    reach = QB + SEQ_MAX
    window = jnp.maximum(first - SEQ_MAX, 0)
    key_places = window + jnp.arange(reach, dtype=jnp.int32)
    query_places = first + jnp.arange(QB, dtype=jnp.int32)
    mask = (key_places[None, :] >= block_starts[:, None]) & (
        key_places[None, :] <= query_places[:, None]
    )
    group = HEADS // KV_HEADS
    rotary = HEADS + KV_HEADS
    query_rows = HEADS * HD
    kv_rows = KV_HEADS * HD
    gains = norm_gains.astype(jnp.float32)
    residual = hidden_states.astype(jnp.float32)
    saved = []
    for layer in range(LAYERS):
        w_qkv, b_qkv, w_out, w_gate, w_up, w_down = (
            lax.all_gather(qkv_weight[layer], "row", axis=0, tiled=True),
            lax.all_gather(qkv_bias[layer], "row", axis=1, tiled=True),
            lax.all_gather(out_weight[layer], "row", axis=1, tiled=True),
            lax.all_gather(gate_weight[layer], "row", axis=0, tiled=True),
            lax.all_gather(up_weight[layer], "row", axis=0, tiled=True),
            lax.all_gather(down_weight[layer], "row", axis=1, tiled=True),
        )
        scale_one, normed_one = norm_forward(residual, gains[layer, 0])
        full_one = spread(normed_one)
        raw = contract_first(w_qkv, full_one) + b_qkv.reshape(-1).astype(jnp.float32)[:, None]
        local_heads = raw.shape[0] // HD
        shaped = raw.reshape(local_heads, HD, tok_row)
        head_ids = col_at * local_heads + jnp.arange(local_heads)
        turned = jnp.where((head_ids < rotary)[:, None, None], rotate(shaped, cosine, sine), shaped)
        blocked = to_blocks(turned.reshape(raw.shape).astype(jnp.bfloat16))
        kv_full = lax.all_gather(blocked[query_rows:], "col", axis=1, tiled=True)
        kv_window = lax.dynamic_slice_in_dim(kv_full, window, reach, 1)
        queries = blocked[:query_rows].reshape(KV_HEADS, group, HD, QB)
        keys = kv_window[:kv_rows].reshape(KV_HEADS, HD, reach)
        values = kv_window[kv_rows:].reshape(KV_HEADS, HD, reach)
        masked = attend_scores(queries, keys, mask)
        row_top = jnp.max(masked, axis=-1, keepdims=True)
        lifted = jnp.exp(masked - row_top)
        row_mass = jnp.sum(lifted, axis=-1, keepdims=True)
        probs = lifted / row_mass
        log_mass = row_top + jnp.log(row_mass)
        mixed = (
            jnp.einsum(
                "kgqj,khj->kghq",
                probs.astype(jnp.bfloat16),
                values,
                preferred_element_type=jnp.float32,
            )
            .reshape(query_rows, QB)
            .astype(jnp.bfloat16)
        )
        carried = to_tokens(mixed)
        attention = summed_rows(partial(by_columns, w_out, carried), feat_rows)
        residual_mid = residual + attention
        scale_two, normed_two = norm_forward(residual_mid, gains[layer, 1])
        full_two = spread(normed_two)
        gate = contract_first(w_gate, full_two)
        up = contract_first(w_up, full_two)
        hidden = (gate * jax.nn.sigmoid(gate) * up).astype(jnp.bfloat16)
        feed = summed_rows(partial(by_columns, w_down, hidden), feat_rows)
        saved.append(
            (
                residual,
                scale_one,
                full_one,
                blocked,
                kv_window,
                log_mass,
                mixed,
                carried,
                residual_mid,
                scale_two,
                full_two,
                gate,
                up,
                hidden,
                (w_qkv, w_out, w_gate, w_up, w_down),
                local_heads,
            )
        )
        residual = residual_mid + feed
    out_states = residual.astype(jnp.bfloat16)
    grad = out_grad.astype(jnp.float32)
    layer_grads = [None] * LAYERS
    gain_terms = [None] * LAYERS
    for layer in reversed(range(LAYERS)):
        (
            residual_in,
            scale_one,
            full_one,
            blocked,
            kv_window,
            log_mass,
            mixed,
            carried,
            residual_mid,
            scale_two,
            full_two,
            gate,
            up,
            hidden,
            weights_full,
            local_heads,
        ) = saved[layer]
        w_qkv, w_out, w_gate, w_up, w_down = weights_full
        grad_full = spread(grad.astype(jnp.bfloat16))
        d_down = contract_last(hidden, grad_full)
        d_hidden = jnp.dot(w_down, grad_full, preferred_element_type=jnp.float32)
        squash = jax.nn.sigmoid(gate)
        d_gate = (d_hidden * up * squash * (1.0 + gate * (1.0 - squash))).astype(jnp.bfloat16)
        d_up = (d_hidden * gate * squash).astype(jnp.bfloat16)
        d_gate_w = contract_last(full_two, d_gate)
        d_up_w = contract_last(full_two, d_up)
        d_normed_two = summed_rows(partial(by_rows_pair, w_gate, d_gate, w_up, d_up), feat_rows)
        d_residual, d_gain_two = norm_backward(
            d_normed_two, residual_mid, scale_two, gains[layer, 1]
        )
        grad = grad + d_residual
        grad_full = spread(grad.astype(jnp.bfloat16))
        d_out_w = contract_last(carried, grad_full)
        d_mixed = to_blocks(
            jnp.dot(w_out, grad_full, preferred_element_type=jnp.float32).astype(jnp.bfloat16)
        )
        queries = blocked[:query_rows].reshape(KV_HEADS, group, HD, QB)
        keys = kv_window[:kv_rows].reshape(KV_HEADS, HD, reach)
        values = kv_window[kv_rows:].reshape(KV_HEADS, HD, reach)
        masked = attend_scores(queries, keys, mask)
        probs = jnp.exp(masked - log_mass)
        low_probs = probs.astype(jnp.bfloat16)
        d_heads_mix = d_mixed.reshape(KV_HEADS, group, HD, QB)
        d_probs = jnp.einsum(
            "kghq,khj->kgqj", d_heads_mix, values, preferred_element_type=jnp.float32
        )
        inner = jnp.sum(probs * d_probs, axis=-1, keepdims=True)
        d_scores = (probs * (d_probs - inner)).astype(jnp.bfloat16)
        d_queries = (
            jnp.einsum("kgqj,khj->kghq", d_scores, keys, preferred_element_type=jnp.float32)
            * HD ** (-0.5)
        ).reshape(query_rows, QB)
        d_keys = (
            jnp.einsum("kgqj,kghq->khj", d_scores, queries, preferred_element_type=jnp.float32)
            * HD ** (-0.5)
        ).reshape(kv_rows, reach)
        d_values = jnp.einsum(
            "kgqj,kghq->khj", low_probs, d_heads_mix, preferred_element_type=jnp.float32
        ).reshape(kv_rows, reach)
        d_window = jnp.concatenate([d_keys, d_values], axis=0)
        d_placed = lax.dynamic_update_slice_in_dim(
            jnp.zeros((2 * kv_rows, tok_row), jnp.float32), d_window, window, 1
        )
        d_kv = lax.psum_scatter(d_placed, "col", scatter_dimension=1, tiled=True)
        d_heads = jnp.concatenate([d_queries, d_kv], axis=0).reshape(HEADS + 2 * KV_HEADS, HD, QB)
        d_turned = jnp.concatenate(
            [rotate_back(d_heads[:rotary], cos_block, sin_block), d_heads[rotary:]], axis=0
        )
        d_raw = to_tokens(d_turned.reshape((HEADS + 2 * KV_HEADS) * HD, QB).astype(jnp.bfloat16))
        d_bias = jnp.sum(d_raw, axis=1, dtype=jnp.float32).reshape(local_heads, HD)
        d_qkv_w = contract_last(full_one, d_raw)
        d_normed_one = summed_rows(partial(by_rows, w_qkv, d_raw), feat_rows)
        d_residual, d_gain_one = norm_backward(
            d_normed_one, residual_in, scale_one, gains[layer, 0]
        )
        grad = grad + d_residual
        layer_grads[layer] = (
            lax.psum_scatter(d_qkv_w, "row", scatter_dimension=0, tiled=True),
            lax.psum_scatter(d_bias, "row", scatter_dimension=1, tiled=True),
            lax.psum_scatter(d_out_w, "row", scatter_dimension=1, tiled=True),
            lax.psum_scatter(d_gate_w, "row", scatter_dimension=0, tiled=True),
            lax.psum_scatter(d_up_w, "row", scatter_dimension=0, tiled=True),
            lax.psum_scatter(d_down, "row", scatter_dimension=1, tiled=True),
        )
        gain_terms[layer] = jnp.stack([d_gain_one, d_gain_two])
    gain_grads = lax.psum(jnp.stack(gain_terms), "row")
    stacked = [jnp.stack([entry[member] for entry in layer_grads]) for member in range(6)]
    return (
        out_states,
        grad,
        gain_grads,
        stacked[0],
        stacked[1],
        stacked[2],
        stacked[3],
        stacked[4],
        stacked[5],
    )


def dot(a, b):
    return jnp.dot(a, b, preferred_element_type=F32)


def dot_t(a, b):
    return lax.dot_general(a, b, (((1,), (1,)), ((), ())), preferred_element_type=F32)


def t_dot(a, b):
    return lax.dot_general(a, b, (((0,), (0,)), ((), ())), preferred_element_type=F32)


def norm_on(residual, gain):
    scale = lax.rsqrt(jnp.mean(residual * residual, axis=1, keepdims=True) + eps_norm)
    return scale, (residual * scale * gain[None, :]).astype(LOW)


def norm_back(d_normed, residual, scale, gain):
    weighted = d_normed * gain[None, :]
    inner = jnp.sum(weighted * residual, axis=1, keepdims=True)
    d_residual = weighted * scale - residual * (scale * scale * scale) * inner / D
    d_gain = jnp.sum(d_normed * residual * scale, axis=0)
    return d_residual, d_gain


def per_device_line(
    hidden_states,
    out_grad,
    lengths,
    norm_gains,
    qkv_weight,
    qkv_bias,
    out_weight,
    gate_weight,
    up_weight,
    down_weight,
):
    names = Names()
    tok_row = hidden_states.shape[1]
    row_at = lax.axis_index("row")
    col_at = lax.axis_index("col")
    core = col_at % 2

    biases = jnp.zeros((LAYERS, 2, 16, HD), LOW)
    biases = lax.dynamic_update_slice(biases, qkv_bias[:, :, None], (0, 0, 0, row_at * (HD // 4)))
    gain_rows = jnp.pad(norm_gains.reshape(2 * LAYERS, D // 8), ((0, 16 - 2 * LAYERS), (0, 0)))

    def slab_of(mine, theirs, out_mine, out_theirs):
        first, second = jnp.where(core == 0, mine, theirs), jnp.where(core == 0, theirs, mine)
        both = jnp.stack([first.reshape(4, HALF, 5 * HD), second.reshape(4, HALF, 5 * HD)], axis=1)
        w_qkv = both[:, :, : D // 8].reshape(D, 5 * HD)
        bias = jnp.sum(both[:, 0, D // 8].astype(F32), axis=0, keepdims=True)
        w_out = jnp.concatenate(
            [jnp.where(core == 0, out_mine, out_theirs), jnp.where(core == 0, out_theirs, out_mine)], axis=0
        )
        return w_qkv, bias, w_out

    def rows_load(layer):
        return (
            GatherRows(gate_weight.swapaxes(1, 2), 1, layer),
            GatherRows(up_weight.swapaxes(1, 2), 1, layer),
            GatherRows(down_weight, 1, layer),
        )

    sent = rows_load(0)
    to_chips = [HeadsToChips(qkv_weight, biases, layer) for layer in range(LAYERS)]
    slab_rows, out_rows = GatherRows(From(to_chips[0]), 0, phase=1), GatherRows(out_weight, 1, 0, phase=1)
    swap = Swap(From(slab_rows), From(out_rows), phase=2)
    sent[0].phase = 3
    states, loads = open_call(
        names, hidden_states, [*to_chips, Exchange(gain_rows, same=True), slab_rows, out_rows, swap, sent[0]]
    )
    (_,), (slab_next,), (gains,), (mine,), (out_mine,), (theirs, out_theirs), (w_gate,) = loads
    load = (mine, theirs, out_mine, out_theirs)
    gains = gains[:, : 2 * LAYERS].transpose(1, 0, 2).reshape(LAYERS, 2, D).astype(F32)
    starts = row_starts(lengths[0], tok_row)
    cosine, sine = rope_tables(jnp.arange(tok_row, dtype=jnp.int32) - starts)
    cosine, sine = cosine.T, sine.T * jnp.where(jnp.arange(HD) < HD // 2, -1.0, 1.0)[None]
    starts = starts[:, None]

    wide = states.reshape(D, tok_row)
    residual = lax.dynamic_slice_in_dim(wide, col_at * QB, QB, 1).astype(F32).T

    def own_rows(full):
        return lax.dynamic_slice_in_dim(full, col_at * QB, QB, 0).astype(F32)

    saved = []
    for layer in range(LAYERS):
        w_qkv, bias, w_out = slab_of(*load)
        sent[1].phase, sent[2].phase = 0, 3
        scale_one, normed_one = norm_on(residual, gains[layer, 0])
        fixed = (w_qkv, bias, w_out, cosine, sine, starts, sent[1:])
        if layer == 0:
            attention, grads_all, qkv, mixed, full_one, loads = forward_heads(
                names, out_grad, wide, gains[0, 0][:, None], *fixed, name="heads_0"
            )
        else:
            attention, full_one, qkv, mixed, _, loads = forward_heads(names, normed_one, None, None, *fixed, name="heads_1")
        (w_up,), (w_down,) = loads
        residual_mid = residual + attention
        scale_two, normed_two = norm_on(residual_mid, gains[layer, 1])
        cargo = []
        if layer == 0:
            sent = rows_load(1)
            sent[0].phase = 3
            slab_rows, out_rows = GatherRows(slab_next, 0), GatherRows(out_weight, 1, 1)
            cargo = [slab_rows, out_rows, sent[0], Swap(From(slab_rows), From(out_rows), phase=2)]
        feed, full_two, gate, up, loads = forward_feed(
            names, normed_two, w_gate, w_up, w_down, cargo, name=f"feed_{layer}"
        )
        saved.append(
            (
                residual,
                scale_one,
                full_one,
                qkv,
                mixed,
                residual_mid,
                scale_two,
                full_two,
                gate,
                up,
                (w_qkv, w_out, w_gate, w_up, w_down),
            )
        )
        residual = residual_mid + feed
        if layer == 0:
            (mine,), (out_mine,), (w_gate,), (theirs, out_theirs) = loads
            load = (mine, theirs, out_mine, out_theirs)
    states = residual.astype(LOW)

    def own_part(full, dim):
        size = full.shape[dim] // 4
        return lax.dynamic_slice_in_dim(full, row_at * size, size, dim)

    def settle(full, dim, slots):
        return jnp.sum(slots.astype(F32), axis=0) + own_part(full, dim).astype(F32)

    def settle_heads(tiles):
        total = tiles[:, :, 0].astype(F32) + jnp.where(col_at >= 6, tiles[:, :, 1].astype(F32), 0.0)
        weight = total[:, :, : D // 8].transpose(1, 2, 0, 3).reshape(D // 4, 2 * HD)
        bias = lax.dynamic_slice_in_dim(total[:, 0, D // 8], row_at * (HD // 4), HD // 4, 1)
        return weight, bias

    grads = {}
    gain_terms = [None] * LAYERS
    grad = own_rows(grads_all)
    inner = w_gate.shape[0]
    for layer in reversed(range(LAYERS)):
        (
            residual_in,
            scale_one,
            full_one,
            qkv,
            mixed,
            residual_mid,
            scale_two,
            full_two,
            gate,
            up,
            (w_qkv, w_out, w_gate, w_up, w_down),
        ) = saved[layer]
        last = layer == LAYERS - 1
        cargo = [] if last else [ScatterRows(slab, 0), ScatterRows(d_out_w, 1)]
        cargo.append(ScatterRows(Inner((inner, D)), 1, phase=1))
        d_normed_two, d_gate_w, d_up_w, d_down, loads = backward_feed(
            names,
            None if last else grad.astype(LOW),
            grads_all if last else None,
            full_two,
            w_gate,
            w_up,
            w_down,
            gate,
            up,
            cargo,
            name=f"back_feed_{layer}",
        )
        grads["down", layer] = d_down, loads[-1][0]
        cargo = [ScatterRows(d_gate_w, 1), ScatterRows(d_up_w, 1, phase=3)]
        if not last:
            grads["out", layer + 1] = settle(d_out_w, 1, loads[1][0])
            cargo.append(HeadsToOwners(settle(slab, 0, loads[0][0]).astype(LOW)))
        d_residual, d_gain_two = norm_back(d_normed_two, residual_mid, scale_two, gains[layer, 1])
        grad = grad + d_residual
        d_normed_one, slab, d_out_w, loads = backward_heads(
            names,
            grad.astype(LOW),
            full_one,
            layer == 0,
            w_qkv,
            w_out,
            qkv,
            mixed,
            cosine,
            sine,
            starts,
            cargo,
            name=f"back_heads_{layer}",
        )
        grads["gate", layer] = d_gate_w, loads[0][0]
        grads["up", layer] = d_up_w, loads[1][0]
        if not last:
            grads["qkv", layer + 1] = settle_heads(loads[2][0])
        d_residual, d_gain_one = norm_back(d_normed_one, residual_in, scale_one, gains[layer, 0])
        grad = grad + d_residual
        gain_terms[layer] = jnp.stack([d_gain_one, d_gain_two])
    leaving = jnp.concatenate([states.T, grad.astype(LOW).T], axis=1).reshape(8, D // 8, 2 * QB)
    gain_parts = jnp.pad(jnp.stack(gain_terms).reshape(2 * LAYERS, 8, D // 8), ((0, 8 - 2 * LAYERS), (0, 0), (0, 0)))
    (left,), (gain_all,), (slots,), (out_slots,) = close_call(
        names,
        [
            Exchange(leaving),
            Exchange(gain_parts.transpose(1, 0, 2), every_row=True),
            ScatterRows(slab, 0),
            ScatterRows(d_out_w, 1),
        ],
        "close",
    )
    ((tiles,),) = close_call(names, [HeadsToOwners(settle(slab, 0, slots).astype(LOW))], "close_heads")
    grads["qkv", 0] = settle_heads(tiles)
    grads["out", 0] = settle(d_out_w, 1, out_slots)
    left = left.transpose(1, 0, 2)
    out_states = left[:, :, :QB].reshape(D // 8, tok_row)
    input_grad = left[:, :, QB:].reshape(D // 8, tok_row).astype(F32)
    gain_grads = jnp.sum(gain_all, axis=(0, 1))[: 2 * LAYERS].reshape(LAYERS, 2, D // 8)

    def both_layers(kind):
        return jnp.stack([grads[kind, layer] for layer in range(LAYERS)])

    kinds = ("gate", "up", "down")
    d_gate, d_up, d_down = settle_rows(
        row_at,
        [[grads[kind, layer][0] for layer in range(LAYERS)] for kind in kinds],
        [[grads[kind, layer][1] for layer in range(LAYERS)] for kind in kinds],
    )
    heads = [jnp.stack([grads["qkv", layer][i] for layer in range(LAYERS)]) for i in range(2)]
    return (
        out_states,
        input_grad,
        gain_grads,
        heads[0],
        heads[1],
        both_layers("out"),
        d_gate.swapaxes(1, 2),
        d_up.swapaxes(1, 2),
        d_down,
    )


def solution(mesh):
    placed = (
        P("col", "row"),
        P("col", "row"),
        P("row", None),
        P(None, None, "col"),
        P(None, "row", "col"),
        P(None, "col", "row"),
        P(None, "col", "row"),
        P(None, "row", "col"),
        P(None, "row", "col"),
        P(None, "col", "row"),
    )
    on_lines = mesh.shape["row"] == 4 and mesh.shape["col"] == 8
    return jax.shard_map(
        per_device_line if on_lines else per_device,
        mesh=mesh,
        in_specs=placed,
        out_specs=(
            P("col", "row"),
            P("col", "row"),
            P(None, None, "col"),
            P(None, "row", "col"),
            P(None, "col", "row"),
            P(None, "col", "row"),
            P(None, "row", "col"),
            P(None, "row", "col"),
            P(None, "col", "row"),
        ),
        check_vma=False,
    )
```

```python
from functools import partial

import jax
import jax.numpy as jnp
from jax import lax
from jax.experimental import pallas as pl
from jax.experimental.pallas import tpu as pltpu
from jax.sharding import PartitionSpec as P

D = 1536
HEADS = 12
KV_HEADS = 2
HD = 128
LAYERS = 2
SEQ_MAX = 512
QB = 128
MESH = pl.DeviceIdType.MESH
LOW = jnp.bfloat16
F32 = jnp.float32
ANY = pl.BlockSpec(memory_space=pl.ANY)
ONCHIP = pl.BlockSpec(memory_space=pltpu.VMEM)
VMEM = 62 * 2**20
HALF = 208


class Place:
    def __init__(self):
        self.r = lax.axis_index("row")
        self.k = lax.axis_index("col")
        self.z = self.k // 2
        self.c = self.k % 2

    def at(self, z, c):
        return (self.r, 2 * z + c)

    def rows(self):
        x, y = self.r % 2, self.r // 2
        return (2 * y + (1 - x), 2 * (1 - y) + x, 2 * (1 - y) + (1 - x))


def remote(src, dst, send, recv, device):
    return pltpu.make_async_remote_copy(
        src_ref=src, dst_ref=dst, send_sem=send, recv_sem=recv, device_id=device, device_id_type=MESH
    )


class Later:
    def __init__(self):
        self.todo = []

    def add(self, wait, cond=None):
        self.todo.append((wait, cond))

    def run(self):
        todo, self.todo = self.todo, []
        for wait, cond in todo:
            if cond is None:
                wait()
            else:
                pl.when(cond)(wait)


def greet(place, reach):
    barrier = pltpu.get_barrier_semaphore()

    def hail(device):
        pl.semaphore_signal(barrier, inc=1, device_id=device, device_id_type=MESH)

    if "all" in reach:
        for rr in range(4):
            for kk in range(8):
                pl.when((place.r != rr) | (place.k != kk))(partial(hail, (rr, kk)))
        pl.semaphore_wait(barrier, 31)
        return
    count = 0
    if "rows" in reach:
        for row in place.rows():
            hail((row, place.k))
        count += 3
    if "col" in reach:
        for kk in range(8):
            pl.when(place.k != kk)(partial(hail, (place.r, kk)))
        pl.semaphore_wait(barrier, count + 7)
        return
    hail(place.at(place.z, 1 - place.c))
    count += 1
    if "line" not in reach:
        pl.semaphore_wait(barrier, count)
        return
    pl.when(place.z < 3)(partial(hail, place.at(jnp.minimum(place.z + 1, 3), place.c)))
    pl.when(place.z > 0)(partial(hail, place.at(jnp.maximum(place.z - 1, 0), place.c)))
    edge = (place.z == 0) | (place.z == 3)
    pl.when(edge)(lambda: pl.semaphore_wait(barrier, count + 1))
    pl.when(jnp.logical_not(edge))(lambda: pl.semaphore_wait(barrier, count + 2))


class From:
    def __init__(self, item, at=0):
        self.item, self.at = item, at
        self.shape, self.dtype = item.outs[at].shape, item.outs[at].dtype


class Cargo:
    arrays = ()
    outs = ()
    scratch = ()
    reach = "rows"
    phase = 0
    slow = False

    def middle(self, place, ins, outs, scratch):
        pass


def part_of(ref, dim, row, size):
    cut = pl.ds(pl.multiple_of(row * size, 128 if dim else 16), size)
    return ref.at[:, cut] if dim else ref.at[cut, :]


class GatherRows(Cargo):
    def __init__(self, block, dim, layer=None, phase=0):
        self.dim, self.layer, self.phase = dim, layer, phase
        self.arrays = (block,)
        if layer is not None:
            block = jax.ShapeDtypeStruct(block.shape[1:], block.dtype)
        full = list(block.shape)
        full[dim] *= 4
        self.size = block.shape[dim]
        self.half = block.shape[0] // 32 * 16
        self.rest = block.shape[0] - self.half
        self.outs = (jax.ShapeDtypeStruct(tuple(full), block.dtype),)
        self.scratch = (
            pltpu.SemaphoreType.DMA((6,)),
            pltpu.SemaphoreType.DMA((6,)),
            pltpu.SemaphoreType.DMA((2,)),
            pltpu.VMEM(block.shape, block.dtype),
        )

    def halves(self, ref):
        return ref.at[0 : self.half, :], ref.at[self.half :, :]

    def spots(self, full, row):
        if self.dim:
            cut = pl.ds(pl.multiple_of(row * self.size, 128), self.size)
            return full.at[0 : self.half, cut], full.at[self.half :, cut]
        first = pl.multiple_of(row * self.size, 16)
        return full.at[pl.ds(first, self.half), :], full.at[pl.ds(first + self.half, self.rest), :]

    split = False

    def source(self, ins):
        return ins[0] if self.layer is None else ins[0].at[self.layer]

    def copies(self, place, ins, outs, scratch):
        src, (dst,), (send, recv, *_) = self.source(ins), outs, scratch
        x, y, d = place.rows()
        block, mine = self.halves(src), self.spots(dst, place.r)
        from_x, from_y = self.spots(dst, x), self.spots(dst, y)
        out = [
            remote(block[0], mine[0], send.at[0], recv.at[0], (x, place.k)),
            remote(block[1], mine[1], send.at[1], recv.at[3], (y, place.k)),
            remote(block[1], mine[1], send.at[2], recv.at[1], (x, place.k)),
            remote(block[0], mine[0], send.at[3], recv.at[2], (y, place.k)),
        ]
        onward = [
            remote(from_x[0], from_x[0], send.at[4], recv.at[4], (y, place.k)),
            remote(from_y[1], from_y[1], send.at[5], recv.at[5], (x, place.k)),
        ]
        return out, onward

    def keep(self, place, ins, outs, scratch):
        *_, sem, buffer = scratch
        return (
            pltpu.make_async_copy(self.source(ins), buffer, sem.at[0]),
            pltpu.make_async_copy(buffer, part_of(outs[0], self.dim, place.r, self.size), sem.at[1]),
        )

    def arrived(self, place, scratch, view, sem, row):
        return remote(view, view, scratch[0].at[0], scratch[1].at[sem], (row, place.k))

    def start(self, place, ins, outs, scratch, later):
        (dst,) = outs
        out, onward = self.copies(place, ins, outs, scratch)
        for copy in out[:2] if self.split else out:
            copy.start()
        load, store = self.keep(place, ins, outs, scratch)
        load.start()
        later.add(store.wait)
        x, y, d = place.rows()
        from_x, from_y, from_d = self.spots(dst, x), self.spots(dst, y), self.spots(dst, d)
        for view, sem, row in ((from_x[1], 1, x), (from_y[0], 2, y), (from_d[0], 4, y), (from_d[1], 5, x)):
            later.add(self.arrived(place, scratch, view, sem, row).wait_recv)
        for copy in (*out, *onward):
            later.add(copy.wait_send)

    def send_rest(self, place, ins, outs, scratch):
        for copy in self.copies(place, ins, outs, scratch)[0][2:]:
            copy.start()

    def middle(self, place, ins, outs, scratch):
        (dst,) = outs
        x, y, d = place.rows()
        _, onward = self.copies(place, ins, outs, scratch)
        load, store = self.keep(place, ins, outs, scratch)
        load.wait()
        store.start()
        self.arrived(place, scratch, self.spots(dst, x)[0], 0, x).wait_recv()
        onward[0].start()
        self.arrived(place, scratch, self.spots(dst, y)[1], 3, y).wait_recv()
        onward[1].start()


class ScatterRows(Cargo):
    def __init__(self, grad, dim, phase=0):
        self.dim, self.phase = dim, phase
        self.arrays = (grad,)
        part = list(grad.shape)
        part[dim] //= 4
        self.size = part[dim]
        self.half = part[0] // 32 * 16
        self.rest = part[0] - self.half
        self.outs = (jax.ShapeDtypeStruct((2, *part), grad.dtype),)
        upper, lower = pltpu.VMEM((self.half, part[1]), grad.dtype), pltpu.VMEM((self.rest, part[1]), grad.dtype)
        self.scratch = (
            *(upper, lower, lower, upper, lower, upper),
            pltpu.SemaphoreType.DMA((6,)),
            pltpu.SemaphoreType.DMA((6,)),
            pltpu.SemaphoreType.DMA((2,)),
        )

    def spots(self, full, row):
        if self.dim:
            cut = pl.ds(pl.multiple_of(row * self.size, 128), self.size)
            return full.at[0 : self.half, cut], full.at[self.half :, cut]
        first = pl.multiple_of(row * self.size, 16)
        return full.at[pl.ds(first, self.half), :], full.at[pl.ds(first + self.half, self.rest), :]

    def copies(self, place, ins, outs, scratch):
        (src,), (dst,) = ins, outs
        via_x, via_y, own_x, own_y, sum_x, sum_y, send, recv, keep = scratch
        x, y, d = place.rows()
        for_x, for_y, for_d = self.spots(src, x), self.spots(src, y), self.spots(src, d)
        slot_x = dst.at[0, 0 : self.half, :], dst.at[0, self.half :, :]
        slot_y = dst.at[1, 0 : self.half, :], dst.at[1, self.half :, :]
        first = [
            remote(for_d[0], via_x, send.at[0], recv.at[0], (x, place.k)),
            remote(for_d[1], via_y, send.at[1], recv.at[1], (y, place.k)),
            remote(for_x[0], slot_x[0], send.at[2], recv.at[2], (x, place.k)),
            remote(for_y[1], slot_y[1], send.at[3], recv.at[3], (y, place.k)),
        ]
        held = [
            pltpu.make_async_copy(for_x[1], own_x, keep.at[0]),
            pltpu.make_async_copy(for_y[0], own_y, keep.at[1]),
        ]
        last = [
            remote(sum_x, slot_x[1], send.at[4], recv.at[4], (x, place.k)),
            remote(sum_y, slot_y[0], send.at[5], recv.at[5], (y, place.k)),
        ]
        return first, held, last

    def start(self, place, ins, outs, scratch, later):
        first, held, last = self.copies(place, ins, outs, scratch)
        for copy in (*first, *held):
            copy.start()
        for copy in (*first, *last):
            later.add(copy.wait_send)
        for copy in (*first[2:], *last):
            later.add(copy.wait_recv)

    def middle(self, place, ins, outs, scratch):
        via_x, via_y, own_x, own_y, sum_x, sum_y, *_ = scratch
        first, held, last = self.copies(place, ins, outs, scratch)
        held[0].wait()
        first[1].wait_recv()
        add_into(sum_x, [own_x, via_y])
        last[0].start()
        held[1].wait()
        first[0].wait_recv()
        add_into(sum_y, [own_y, via_x])
        last[1].start()


class Swap(Cargo):
    reach = "line"

    def __init__(self, *arrays, phase=0):
        self.arrays, self.phase = arrays, phase
        self.outs = tuple(jax.ShapeDtypeStruct(a.shape, a.dtype) for a in arrays)
        self.scratch = (pltpu.SemaphoreType.DMA((len(arrays),)), pltpu.SemaphoreType.DMA((len(arrays),)))

    def start(self, place, ins, outs, scratch, later):
        send, recv = scratch
        for i, (src, dst) in enumerate(zip(ins, outs)):
            copy = remote(src, dst, send.at[i], recv.at[i], place.at(place.z, 1 - place.c))
            copy.start()
            later.add(copy.wait)


def tile_owner(z, t):
    if t < 3:
        head = 3 * z + t
        return head // 2, head % 2
    return 3 + t, z // 2


class HeadsToChips(Cargo):
    reach = "col"

    def __init__(self, weight, biases, layer):
        self.layer = layer
        self.arrays = (weight, biases)
        self.outs = (jax.ShapeDtypeStruct((HALF, 5 * HD), LOW),)
        self.scratch = (
            pltpu.SemaphoreType.DMA((2, 2, 2, 2)),
            pltpu.SemaphoreType.DMA((5, 2)),
            pltpu.VMEM(weight.shape[1:], weight.dtype),
            pltpu.VMEM(biases.shape[1:], biases.dtype),
            pltpu.SemaphoreType.DMA((2,)),
        )

    def start(self, place, ins, outs, scratch, later):
        (slab,), (send, recv, weight, biases, load_sem) = outs, scratch
        for load in copy_in([(ins[0].at[self.layer], weight), (ins[1].at[self.layer], biases)], load_sem):
            load.wait()
        r, k, z, c = place.r, place.k, place.z, place.c
        query = k < 6
        rows = D // 8
        for second in range(2):
            for i in range(2):
                head = 2 * k + i
                chip = jnp.where(query, head // 3, 2 * i + second)
                t = jnp.where(query, head % 3, k - 3)
                cut = pl.ds(pl.multiple_of(t * HD, HD), HD)
                spots = slab.at[0:rows, cut], slab.at[rows:HALF, cut]
                for core in range(2):
                    here = k == 2 * chip + core
                    away = jnp.logical_not(here)
                    if second == 1:
                        here, away = here & (k >= 6), away & (k >= 6)
                    views = (
                        weight.at[core * rows : (core + 1) * rows, i * HD : (i + 1) * HD],
                        biases.at[i],
                    )
                    for part in range(2):
                        sem = send.at[i, second, core, part]
                        copy = remote(views[part], spots[part], sem, recv.at[t, part], (r, 2 * chip + core))
                        pl.when(away)(copy.start)
                        later.add(copy.wait_send, away)
                        keep = pltpu.make_async_copy(views[part], spots[part], sem)
                        pl.when(here)(keep.start)
                        later.add(keep.wait, here)
        for t in range(5):
            owner, _ = tile_owner(z, t)
            cut = slice(t * HD, (t + 1) * HD)
            for part, spot in enumerate((slab.at[0:rows, cut], slab.at[rows:HALF, cut])):
                came = remote(spot, spot, send.at[0, 0, 0, 0], recv.at[t, part], (r, owner))
                later.add(came.wait_recv, k != owner)


class HeadsToOwners(Cargo):
    reach = "col"

    def __init__(self, slab):
        self.arrays = (slab,)
        self.outs = (jax.ShapeDtypeStruct((2, 2, 2, HALF, HD), LOW),)
        self.scratch = (pltpu.SemaphoreType.DMA((5,)), pltpu.SemaphoreType.DMA((2, 2, 2)))

    def start(self, place, ins, outs, scratch, later):
        (slab,), (tiles,), (send, recv) = ins, outs, scratch
        r, k, z, c = place.r, place.k, place.z, place.c
        for t in range(5):
            owner, i = tile_owner(z, t)
            which = z % 2 if t >= 3 else 0
            view, spot = slab.at[:, t * HD : (t + 1) * HD], tiles.at[i, c, which]
            here = k == owner
            copy = remote(view, spot, send.at[t], recv.at[i, c, which], (r, owner))
            pl.when(jnp.logical_not(here))(copy.start)
            later.add(copy.wait_send, jnp.logical_not(here))
            keep = pltpu.make_async_copy(view, spot, send.at[t])
            pl.when(here)(keep.start)
            later.add(keep.wait, here)
        for i in range(2):
            for which in range(2):
                chip = jnp.where(k < 6, (2 * k + i) // 3, 2 * i + which)
                for core in range(2):
                    wanted = k != 2 * chip + core
                    if which == 1:
                        wanted = wanted & (k >= 6)
                    came = remote(
                        slab.at[:, 0:HD],
                        tiles.at[i, core, which],
                        send.at[0],
                        recv.at[i, core, which],
                        (r, 2 * chip + core),
                    )
                    later.add(came.wait_recv, wanted)


class Exchange(Cargo):
    def __init__(self, chunks, every_row=False, same=False):
        self.arrays = (chunks,)
        self.same = same
        self.rows_too = every_row
        self.reach = "all" if every_row else "col"
        lead = (4,) if every_row else (8,) if same else ()
        self.outs = (jax.ShapeDtypeStruct((*lead, *chunks.shape), chunks.dtype),)
        self.scratch = (pltpu.SemaphoreType.DMA((4, 8)), pltpu.SemaphoreType.DMA((4, 8)))

    def start(self, place, ins, outs, sems, later):
        (src,), (dst,), (send, recv) = ins, outs, sems
        r, k = place.r, place.k
        for rr in range(4) if self.rows_too else (None,):
            to_row = r if rr is None else rr
            for kk in range(8):
                here = (k == kk) if rr is None else (k == kk) & (r == rr)
                mine = dst.at[k] if rr is None else dst.at[r, k]
                theirs = dst.at[kk] if rr is None else dst.at[rr, kk]
                at = 0 if rr is None else rr
                my_at = 0 if rr is None else r
                part = src if self.same else src.at[kk]
                copy = remote(part, mine, send.at[at, kk], recv.at[my_at, k], (to_row, kk))
                pl.when(jnp.logical_not(here))(copy.start)
                later.add(copy.wait_send, jnp.logical_not(here))
                came = remote(part, theirs, send.at[at, kk], recv.at[at, kk], (to_row, kk))
                later.add(came.wait_recv, jnp.logical_not(here))
                keep = pltpu.make_async_copy(part, mine, send.at[at, kk])
                pl.when(here)(keep.start)
                later.add(keep.wait, here)


def add_into(dst, views):
    rows = dst.shape[0]

    def step(i, carry):
        cut = pl.ds(pl.multiple_of(i * 16, 16), 16)
        total = views[0][cut, :].astype(F32)
        for view in views[1:]:
            total = total + view[cut, :].astype(F32)
        dst[cut, :] = total.astype(dst.dtype)
        return carry

    lax.fori_loop(0, rows // 16, step, 0)


SUB = 4
LAG = 2


class Reduce:
    @staticmethod
    def scratch(tokens, width):
        return [
            pltpu.VMEM((4, tokens, width), LOW),
            pltpu.VMEM((2, 4, tokens, width), LOW),
            pltpu.VMEM((4, tokens, width), LOW),
            pltpu.SemaphoreType.DMA((4,)),
            pltpu.SemaphoreType.DMA((4,)),
            pltpu.SemaphoreType.DMA((4, SUB)),
            pltpu.SemaphoreType.DMA((2, 4, SUB)),
        ]

    def __init__(self, place, part, out, scratch, both=True, far=False):
        self.place, self.part, self.out, self.both, self.far = place, part, out, both, far
        self.from_p, self.moved, self.held, self.send_p, self.recv_p, self.send, self.recv = scratch
        z, c = place.z, place.c
        self.edge = (z == 0) | (z == 3)
        self.mid = jnp.logical_not(self.edge)
        self.right, self.left = place.at(jnp.minimum(z + 1, 3), c), place.at(jnp.maximum(z - 1, 0), c)
        self.size = part.shape[1] // SUB

    def pair(self, j):
        place = self.place
        other = self.part.at[2 * j + 1 - place.c]
        return remote(other, self.from_p.at[j], self.send_p.at[j], self.recv_p.at[j], place.at(place.z, 1 - place.c))

    def piece(self, j, sub, way):
        rows = pl.ds(sub * self.size, self.size)
        column = jnp.where(way == 0, self.right[1], self.left[1])
        return remote(
            self.held.at[j, rows, :],
            self.moved.at[way, j, rows, :],
            self.send.at[j, sub],
            self.recv.at[way, j, sub],
            (self.place.r, column),
        )

    def terms(self, j):
        if self.both:
            return [self.part.at[2 * j + self.place.c], self.from_p.at[j]]
        return [self.part.at[j]]

    def made(self, j):
        z = self.place.z
        if self.both:
            self.pair(j).start()

        @pl.when(self.edge & (j != z))
        def _():
            if self.both:
                self.pair(j).wait_recv()
            add_into(self.held.at[j], self.terms(j))
            for sub in range(SUB):
                self.piece(j, sub, jnp.where(z == 0, 0, 1)).start()

    def finish(self, later, between):
        z = self.place.z
        way = jnp.where(z == 1, 0, 1)
        near, far, back = jnp.where(z == 1, 2, 1), jnp.where(z == 1, 3, 0), jnp.where(z == 1, 0, 3)
        first, second = (far, near) if self.far else (near, far)

        def step(j, sub, way):
            copy = self.piece(j, sub, way)
            copy.wait_recv()
            rows = pl.ds(sub * self.size, self.size)
            views = [view.at[rows, :] for view in (*self.terms(j), self.moved.at[way, j])]
            add_into(self.held.at[j].at[rows, :], views)
            copy.start()

        def pair_here(j):
            if self.both:
                self.pair(j).wait_recv()

        def firsts(sub):
            if sub == 0:
                pair_here(first)
            step(first, sub, way)

        def seconds(sub):
            if sub == 0:
                pair_here(second)
            step(second, sub, way)

        def backs(sub):
            if sub == 0:
                pair_here(back)
            step(back, sub, 1 - way)

        for sub in range(SUB):
            pl.when(self.mid)(partial(firsts, sub))
            between(sub)
        for sub in range(SUB):
            pl.when(self.mid)(partial(seconds, sub))
            if sub >= LAG:
                pl.when(self.mid)(partial(backs, sub - LAG))
            between(SUB + sub)
        for sub in range(SUB - LAG, SUB):
            pl.when(self.mid)(partial(backs, sub))
        if self.both:
            self.pair(z).wait_recv()

        def came(way):
            for sub in range(SUB):
                self.piece(z, sub, way).wait_recv()

        views = self.terms(z)

        @pl.when(self.edge)
        def _():
            way = jnp.where(z == 0, 1, 0)
            came(way)
            add_into(self.out, [*views, self.moved.at[way, z]])

        @pl.when(self.mid)
        def _():
            came(0)
            came(1)
            add_into(self.out, [*views, self.moved.at[0, z], self.moved.at[1, z]])

        for j in range(4):
            if self.both:
                later.add(self.pair(j).wait_send)
            for sub in range(SUB):
                later.add(self.piece(j, sub, 0).wait_send, z != j)


def far_first(place, p):
    z = place.z
    edge = jnp.where(z == 0, 3 - p, p)
    mid = jnp.where(p == 0, jnp.where(z == 1, 3, 0), jnp.where(p == 1, jnp.where(z == 1, 2, 1), jnp.where(p == 2, jnp.where(z == 1, 0, 3), z)))
    return jnp.where((z == 0) | (z == 3), edge, mid)


class Names:
    def __init__(self):
        self.next = 0

    def take(self):
        self.next += 1
        return self.next - 1


class Inner:
    def __init__(self, shape, dtype=LOW):
        self.shape, self.dtype = shape, dtype


def given_arrays(item):
    return [a for a in item.arrays if not isinstance(a, (From, Inner))]


def carry_kernel(body, reach, n_in, n_out, n_scratch, cargo, *refs):
    refs = list(refs)

    def pop(n):
        taken = refs[:n]
        del refs[:n]
        return taken

    ins = pop(n_in)
    given = [pop(len(given_arrays(item))) for item in cargo]
    outs = pop(n_out)
    made = {item: pop(len(item.outs)) for item in cargo}
    scratch = pop(n_scratch)
    held = {item: pop(len(item.scratch)) for item in cargo}
    taken = {
        item: [
            made[a.item][a.at] if isinstance(a, From) else a if isinstance(a, Inner) else mine.pop(0)
            for a in item.arrays
        ]
        for item, mine in zip(cargo, given)
    }
    place = Place()
    later = Later()
    owed = [Later() for _ in range(4)]
    greet(place, {reach, *(item.reach for item in cargo)})

    def start(phase, *inner):
        inner = list(inner)
        mine = [item for item in cargo if item.phase == phase]
        for before in sorted({a.item.phase for item in mine for a in item.arrays if isinstance(a, From)}):
            owed[before].run()
        for item in mine:
            taken[item] = [inner.pop(0) if isinstance(a, Inner) else a for a in taken[item]]
            item.start(place, taken[item], made[item], held[item], owed[phase])

    def middle(phase=0, rest=False):
        for item in cargo:
            if item.phase == phase:
                (item.send_rest if rest else item.middle)(place, taken[item], made[item], held[item])

    body(place, ins, outs, scratch, later, middle, start)
    later.run()
    for waits in owed:
        waits.run()


def carry_call(names, body, reach, arrays, in_specs, outs, out_specs, scratch, cargo, name=None):
    given = [a for item in cargo for a in given_arrays(item)]
    call = pl.pallas_call(
        partial(carry_kernel, body, reach, len(arrays), len(outs), len(scratch), cargo),
        out_shape=[*outs, *(o for item in cargo for o in item.outs)],
        in_specs=[*in_specs, *(ANY for _ in given)],
        out_specs=[*out_specs, *(ANY for item in cargo for _ in item.outs)],
        scratch_shapes=[*scratch, *(s for item in cargo for s in item.scratch)],
        compiler_params=pltpu.CompilerParams(
            collective_id=names.take(), has_side_effects=True, vmem_limit_bytes=VMEM
        ),
        name=name,
    )
    results = list(call(*arrays, *given))
    main = results[: len(outs)]
    rest = results[len(outs) :]
    loads = []
    for item in cargo:
        loads.append(rest[: len(item.outs)])
        rest = rest[len(item.outs) :]
    return main, loads


class Gather:
    scratch = (
        pltpu.SemaphoreType.DMA((4, 2)),
        pltpu.SemaphoreType.DMA((4, 2)),
        pltpu.SemaphoreType.DMA((8, 2)),
        pltpu.SemaphoreType.DMA((8, 2)),
        pltpu.SemaphoreType.DMA((1,)),
    )

    def __init__(self, place, block, full, sems, both=True):
        self.place, self.block, self.full, self.both = place, block, full, both
        self.send_r, self.send_l, self.send_p, self.recv, self.keep = sems
        self.size = block.shape[0] // 2

    def spot(self, zz, c):
        return self.full.at[2 * zz + c] if self.both else self.full.at[zz]

    def copies(self, src, zz, t, way, half):
        z, c = self.place.z, self.place.c
        rows = pl.ds(half * self.size, self.size)
        src, spot, sem = src.at[rows, :], self.spot(zz, c).at[rows, :], self.recv.at[2 * zz + c, half]
        right = remote(src, spot, self.send_r.at[t, half], sem, self.place.at(jnp.minimum(z + 1, 3), c))
        left = remote(src, spot, self.send_l.at[t, half], sem, self.place.at(jnp.maximum(z - 1, 0), c))
        partner = remote(src, spot, self.send_p.at[2 * t + way, half], sem, self.place.at(z, 1 - c))
        return right, left, partner

    def start(self, later):
        z, c = self.place.z, self.place.c
        for half in range(2):
            right, left, partner = self.copies(self.block, z, 0, 0, half)
            pl.when(z < 3)(right.start)
            pl.when(z > 0)(left.start)
            later.add(right.wait_send, z < 3)
            later.add(left.wait_send, z > 0)
            if self.both:
                partner.start()
                later.add(partner.wait_send)
        keep = pltpu.make_async_copy(self.block, self.spot(z, c), self.keep.at[0])
        keep.start()
        keep.wait()
        for t in range(1, 4):
            for way in (0, 1):
                for half in range(2):
                    valid, onward, may, partner = self.step(t, way, half)
                    later.add(onward.wait_send, valid & may)
                    if self.both:
                        later.add(partner.wait_send, valid)

    def step(self, t, way, half):
        z = self.place.z
        there = z + (2 * way - 1) * t
        zz = jnp.clip(there, 0, 3)
        right, left, partner = self.copies(self.spot(zz, self.place.c), zz, t, way, half)
        onward, may = (left, z > 0) if way else (right, z < 3)
        return (there >= 0) & (there <= 3), onward, may, partner

    def pass_on(self, t):
        for half in range(2):
            for way in (0, 1):
                valid, onward, may, partner = self.step(t, way, half)

                @pl.when(valid)
                def _(onward=onward, may=may, partner=partner):
                    onward.wait_recv()
                    pl.when(may)(onward.start)
                    if self.both:
                        partner.start()

    def from_partner(self, zz):
        c = self.place.c
        for half in range(2):
            spot = self.spot(zz, 1 - c).at[pl.ds(half * self.size, self.size), :]
            recv = self.recv.at[2 * zz + 1 - c, half]
            yield remote(spot, spot, self.send_p.at[0, half], recv, self.place.at(self.place.z, 1 - c)).wait_recv

    def order(self, p):
        z = self.place.z
        second = jnp.where(z == 0, 1, z - 1)
        third = jnp.where(z == 0, 2, jnp.where(z == 3, 1, z + 1))
        fourth = jnp.where(z <= 1, 3, 0)
        return jnp.where(p == 0, z, jnp.where(p == 1, second, jnp.where(p == 2, third, fourth)))

    def chunk(self, p):
        z = self.place.z
        edge = (z == 0) | (z == 3)
        t = jnp.where(edge, p, (p + 1) // 2)
        pl.when((p >= 1) & (edge | (p != 2)))(lambda: self.pass_on(t))
        j = self.order(p)
        if self.both:
            for wait in self.from_partner(j):
                wait()
        return j


def forward_feed(names, block, residual, gain, w_gate, w_up, w_down, cargo, name):
    tokens, width = block.shape
    inner = w_gate.shape[0]
    normed = gain is not None

    def body(place, ins, outs, scratch, later, middle, start):
        block_ref, residual_ref, gain_ref, gate_hbm, up_hbm, down_hbm = ins
        states_out, normed_out, full_out, gate_out, up_out = outs
        n = len(Gather.scratch)
        gather_sems, scratch = scratch[:n], scratch[n:]
        full, part, gate_w, up_w, down_w, gates, ups, load_sem, keep_sem, total = scratch[:10]
        reduce = Reduce(place, part, total, scratch[10:])
        gather = Gather(place, block_ref, full, gather_sems)
        loads = [
            pltpu.make_async_copy(src, dst, load_sem.at[i])
            for i, (src, dst) in enumerate(((gate_hbm, gate_w), (up_hbm, up_w), (down_hbm, down_w)))
        ]
        for load in loads:
            load.start()
        gather.start(later)
        start(0)
        start(3)
        for load in loads:
            load.wait()

        def keep(j):
            rows = pl.ds(pl.multiple_of(2 * tokens * j, 2 * tokens), 2 * tokens)
            return [
                pltpu.make_async_copy(full.at[pl.ds(2 * j, 2)], full_out.at[pl.ds(2 * j, 2)], keep_sem.at[0, j]),
                pltpu.make_async_copy(gates.at[rows, :], gate_out.at[rows, :], keep_sem.at[1, j]),
                pltpu.make_async_copy(ups.at[rows, :], up_out.at[rows, :], keep_sem.at[2, j]),
            ]

        def step(p, carry):
            j = gather.chunk(p)
            pl.when(p == 2)(middle)
            acts = full[pl.ds(2 * j, 2)].reshape(2 * tokens, width)
            rows = pl.ds(pl.multiple_of(2 * tokens * j, 2 * tokens), 2 * tokens)
            gate = dot_t(acts, gate_w[...])
            up = dot_t(acts, up_w[...])
            gates[rows, :] = gate.astype(LOW)
            ups[rows, :] = up.astype(LOW)
            hidden = (gate * jax.nn.sigmoid(gate) * up).astype(LOW)
            sums = jnp.dot(hidden, down_w[...], preferred_element_type=F32).astype(LOW)
            part[pl.ds(2 * j, 2)] = sums.reshape(2, tokens, width)
            reduce.made(j)
            for copy in keep(j):
                copy.start()
            return carry

        lax.fori_loop(0, 4, step, 0)
        start(1)
        start(2)
        reduce.finish(later, lambda i: middle(3) if i == 0 else None)
        after_forward(total, residual_ref, gain_ref if normed else None, states_out, normed_out)
        for j in range(4):
            for copy in keep(j):
                copy.wait()

    (states, low, full, gate, up), loads = carry_call(
        names,
        body,
        "line",
        [block, residual, gain if normed else jnp.ones((1, width), F32), w_gate, w_up, w_down],
        [ONCHIP, ONCHIP, ONCHIP, ANY, ANY, ANY],
        [
            jax.ShapeDtypeStruct((tokens, width), F32),
            jax.ShapeDtypeStruct((tokens, width), LOW),
            jax.ShapeDtypeStruct((8, tokens, width), LOW),
            jax.ShapeDtypeStruct((8 * tokens, inner), LOW),
            jax.ShapeDtypeStruct((8 * tokens, inner), LOW),
        ],
        [ONCHIP, ONCHIP, ANY, ANY, ANY],
        [
            *Gather.scratch,
            pltpu.VMEM((8, tokens, width), LOW),
            pltpu.VMEM((8, tokens, width), LOW),
            pltpu.VMEM(w_gate.shape, LOW),
            pltpu.VMEM(w_up.shape, LOW),
            pltpu.VMEM(w_down.shape, LOW),
            pltpu.VMEM((8 * tokens, inner), LOW),
            pltpu.VMEM((8 * tokens, inner), LOW),
            pltpu.SemaphoreType.DMA((3,)),
            pltpu.SemaphoreType.DMA((3, 4)),
            pltpu.VMEM((tokens, width), F32),
            *Reduce.scratch(tokens, width),
        ],
        cargo,
        name=name,
    )
    return states, low, full.reshape(8 * tokens, width), gate, up, loads


def rows_of(first, count):
    return pl.ds(pl.multiple_of(first, count), count)


def copy_in(pairs, sem):
    copies = [pltpu.make_async_copy(src, dst, sem.at[i]) for i, (src, dst) in enumerate(pairs)]
    for copy in copies:
        copy.start()
    return copies


def open_call(names, shard, cargo):
    def body(place, ins, outs, scratch, later, middle, start):
        gather = Gather(place, ins[0], outs[0], scratch)
        gather.start(later)
        start(0)
        start(3)
        start(1)
        middle(3, rest=True)
        gather.pass_on(1)
        middle(1)
        gather.pass_on(2)
        middle(3)
        start(2)
        gather.pass_on(3)
        for zz in range(4):
            for wait in gather.from_partner(zz):
                later.add(wait)

    (full,), loads = carry_call(
        names,
        body,
        "line",
        [shard],
        [ANY],
        [jax.ShapeDtypeStruct((8, *shard.shape), shard.dtype)],
        [ANY],
        list(Gather.scratch),
        cargo,
        name="open",
    )
    return full, loads


def close_call(names, cargo, name):
    def body(place, ins, outs, scratch, later, middle, start):
        start(0)
        middle(0)

    return carry_call(names, body, "col", [], [], [], [], [], cargo, name=name)[1]


def after_forward(sums, residual, gain, states, normed):
    def step(i, carry):
        rows = rows_of(i * 16, 16)
        now = residual[rows, :] + sums[rows, :]
        states[rows, :] = now
        if gain is not None:
            now = now * lax.rsqrt(jnp.mean(now * now, axis=1, keepdims=True) + eps_norm) * gain[...]
        normed[rows, :] = now.astype(LOW)
        return carry

    lax.fori_loop(0, sums.shape[0] // 16, step, 0)


def after_backward(sums, grad, residual, gain, grad_out, low_out, gain_out):
    def step(i, total):
        rows = rows_of(i * 16, 16)
        d_normed, now = sums[rows, :], residual[rows, :]
        scale = lax.rsqrt(jnp.mean(now * now, axis=1, keepdims=True) + eps_norm)
        weighted = d_normed * gain[...]
        inner = jnp.sum(weighted * now, axis=1, keepdims=True)
        out = grad[rows, :] + (weighted * scale - now * (scale * scale * scale) * inner / D)
        grad_out[rows, :] = out
        low_out[rows, :] = out.astype(LOW)
        return total + jnp.sum(d_normed * now * scale, axis=0, keepdims=True)

    gain_out[...] = lax.fori_loop(0, sums.shape[0] // 16, step, jnp.zeros((1, D), F32))


class Slab:
    scratch = (
        pltpu.VMEM((D, 5 * HD), LOW),
        pltpu.VMEM((3 * HD, D), LOW),
        pltpu.VMEM((4, 16, 5 * HD), LOW),
        pltpu.SemaphoreType.DMA((2, 5)),
        pltpu.SemaphoreType.DMA((4,)),
    )

    def __init__(self, place, refs, scratch):
        self.place = place
        self.mine, self.theirs, self.out_mine, self.out_theirs = refs
        self.qkv, self.out, self.tails, self.sems, self.tail_sems = scratch

    def copies(self, half, mine):
        source, out = (self.mine, self.out_mine) if mine else (self.theirs, self.out_theirs)
        sem = self.sems.at[half]
        rows = D // 8
        for row in range(4):
            spot = self.qkv.at[(2 * row + half) * rows : (2 * row + half + 1) * rows, :]
            yield pltpu.make_async_copy(source.at[row * HALF : row * HALF + rows, :], spot, sem.at[row])
        yield pltpu.make_async_copy(out, self.out.at[half * rows : (half + 1) * rows, :], sem.at[4])
        if half == 0:
            for row in range(4):
                tail = source.at[row * HALF + rows : (row + 1) * HALF, :]
                yield pltpu.make_async_copy(tail, self.tails.at[row], self.tail_sems.at[row])

    def start(self):
        for half in range(2):
            for mine in (True, False):

                @pl.when((self.place.c == half) == mine)
                def _(half=half, mine=mine):
                    for copy in self.copies(half, mine):
                        copy.start()

    def wait(self):
        for half in range(2):
            for copy in self.copies(half, True):
                copy.wait()

    def bias(self):
        return jnp.sum(self.tails[:, 0, :].astype(F32), axis=0, keepdims=True)


def heads_of(ref, rows):
    return jnp.concatenate([ref[rows, h * HD : (h + 1) * HD] for h in range(3)], axis=0)


def block_probs(qkv, starts, b):
    reach = QB + SEQ_MAX
    first = jnp.maximum(b - SEQ_MAX // QB, 0) * QB
    rows, window = rows_of(b * QB, QB), pl.ds(pl.multiple_of(first, QB), reach)
    queries = heads_of(qkv, rows)
    keys, values = qkv[window, 3 * HD : 4 * HD], qkv[window, 4 * HD : 5 * HD]
    scores = (dot_t(queries, keys) * HD ** (-0.5)).reshape(3, QB, reach)
    key_at = first + lax.broadcasted_iota(jnp.int32, (QB, reach), 1)
    query_at = b * QB + lax.broadcasted_iota(jnp.int32, (QB, reach), 0)
    allowed = (key_at >= starts[rows, :]) & (key_at <= query_at)
    masked = jnp.where(allowed[None], scores, neg_fill)
    lifted = jnp.exp(masked - jnp.max(masked, axis=-1, keepdims=True))
    probs = lifted * (1.0 / jnp.sum(lifted, axis=-1, keepdims=True))
    return queries, keys, values, probs, rows, window


def roll_half(values):
    return pltpu.roll(values, HD // 2, 1)


def forward_heads(names, block, wide, gain, residual, gain_two, slab, cosine, sine, starts, cargo, name):
    tokens, width = QB, D
    count = 8 * QB
    apart = wide is not None

    def body(place, ins, outs, scratch, later, middle, start):
        ins = list(ins)
        block_ref = ins.pop(0)
        if apart:
            wide_hbm, gain_ref = ins.pop(0), ins.pop(0)
        residual_ref, two_ref, cos_ref, sin_ref, starts_ref, *slab_refs = ins
        states_out, normed_out, full_out, qkv_out, mixed_out = outs[:5]
        scratch = list(scratch)
        gather_sems = [scratch.pop(0) for _ in Gather.scratch]
        weights = Slab(place, slab_refs, [scratch.pop(0) for _ in Slab.scratch])
        full, acts, flat, part, qkv, mixed, load_sem, keep_sem, total = scratch[:9]
        reduce = Reduce(place, part, total, scratch[9:], both=False, far=True)
        weights.start()
        loads = copy_in([(wide_hbm, acts)] if apart else [], load_sem)
        gather = Gather(place, block_ref, full, gather_sems)
        gather.start(later)
        start(0)
        start(3)
        for load in loads:
            load.wait()
        weights.wait()
        bias = weights.bias()

        def keep(j):
            if apart:
                rows = rows_of(j * 2 * QB, 2 * QB)
                return pltpu.make_async_copy(flat.at[rows, :], full_out.at[rows, :], keep_sem.at[j])
            return pltpu.make_async_copy(full.at[pl.ds(2 * j, 2)], full_out.at[pl.ds(2 * j, 2)], keep_sem.at[j])

        def step(p, carry):
            if apart:
                j = gather.order(p)
            else:
                j = gather.chunk(p)
                pl.when(p == 2)(middle)
            rows = rows_of(j * 2 * QB, 2 * QB)
            if apart:
                chunk = acts[:, rows].astype(F32)
                scale = lax.rsqrt(jnp.mean(chunk * chunk, axis=0, keepdims=True) + eps_norm)
                chunk = (chunk * scale * gain_ref[...]).astype(LOW)
                acts[:, rows] = chunk
                raw = t_dot(chunk, weights.qkv[...]) + bias
            else:
                keep(j).start()
                raw = jnp.dot(full[pl.ds(2 * j, 2)].reshape(2 * tokens, width), weights.qkv[...], preferred_element_type=F32)
                raw = raw + bias
            cos, sin = cos_ref[rows, :], sin_ref[rows, :]
            for t in range(5):
                head = raw[:, t * HD : (t + 1) * HD]
                if t < 4:
                    head = head * cos + roll_half(head) * sin
                qkv[rows, t * HD : (t + 1) * HD] = head.astype(LOW)
            return carry

        lax.fori_loop(0, 4, step, 0)
        start(1)

        def attend(p, carry):
            j = far_first(place, p)
            _, _, values, probs, _, _ = block_probs(qkv, starts_ref, 2 * j + place.c)
            low = probs.astype(LOW).reshape(3 * QB, QB + SEQ_MAX)
            heads = jnp.dot(low, values, preferred_element_type=F32).astype(LOW)
            both = jnp.concatenate([heads[h * QB : (h + 1) * QB] for h in range(3)], axis=1)
            mixed[rows_of(j * QB, QB), :] = both
            part[j] = jnp.dot(both, weights.out[...], preferred_element_type=F32).astype(LOW)
            reduce.made(j)
            return carry

        lax.fori_loop(0, 4, attend, 0)
        saves = copy_in([(qkv, qkv_out), (mixed, mixed_out)], load_sem)
        if apart:
            saves.append(pltpu.make_async_copy(acts, outs[5], load_sem.at[2]))
            saves[-1].start()

        def between(i):
            if not apart:
                if i == 0:
                    middle(3)
                return
            if i in (0, SUB, 2 * SUB - 1):
                gather.pass_on(1 + (i + 1) // SUB)
            if i == SUB:
                middle(0)
            if i == 2 * SUB - 1:
                middle(3)

        reduce.finish(later, between)
        after_forward(total, residual_ref, two_ref, states_out, normed_out)
        if apart:
            for zz in range(4):
                for wait in gather.from_partner(zz):
                    wait()

            def turn(t, carry):
                rows = rows_of(t * 2 * QB, 2 * QB)
                for j in range(4):
                    piece = full[2 * j : 2 * j + 2, :, rows].reshape(D // 4, 2 * QB)
                    flat[rows, j * (D // 4) : (j + 1) * (D // 4)] = piece.T
                keep(t).start()
                return carry

            lax.fori_loop(0, 4, turn, 0)
        for copy in saves:
            copy.wait()
        for j in range(4):
            keep(j).wait()

    gathered = (count, width) if apart else (8, tokens, width)
    results, loads = carry_call(
        names,
        body,
        "line",
        [block, *([wide, gain] if apart else []), residual, gain_two, cosine, sine, starts, *slab],
        [ONCHIP, *([ANY, ONCHIP] if apart else []), *[ONCHIP] * 5, *[ANY] * 4],
        [
            jax.ShapeDtypeStruct((tokens, width), F32),
            jax.ShapeDtypeStruct((tokens, width), LOW),
            jax.ShapeDtypeStruct(gathered, LOW),
            jax.ShapeDtypeStruct((count, 5 * HD), LOW),
            jax.ShapeDtypeStruct((count // 2, 3 * HD), LOW),
            *([jax.ShapeDtypeStruct((width, count), LOW)] if apart else []),
        ],
        [ONCHIP, ONCHIP, ANY, ANY, ANY, *([ANY] if apart else [])],
        [
            *Gather.scratch,
            *Slab.scratch,
            pltpu.VMEM((8, *block.shape), LOW),
            pltpu.VMEM((width, count) if apart else (16, 128), LOW),
            pltpu.VMEM((count, width) if apart else (16, 128), LOW),
            pltpu.VMEM((4, tokens, width), LOW),
            pltpu.VMEM((count, 5 * HD), LOW),
            pltpu.VMEM((count // 2, 3 * HD), LOW),
            pltpu.SemaphoreType.DMA((3,)),
            pltpu.SemaphoreType.DMA((4,)),
            pltpu.VMEM((tokens, width), F32),
            *Reduce.scratch(tokens, width),
        ],
        cargo,
        name=name,
    )
    states, low, full, qkv, mixed = results[:5]
    return states, low, full.reshape(count, width), qkv, mixed, results[5] if apart else None, loads


def backward_heads(names, block, grad, residual, gain, acts, turned, slab, qkv, mixed, cosine, sine, starts, cargo, name):
    tokens, width = QB, D
    count = 8 * QB
    reach = QB + SEQ_MAX

    def body(place, ins, outs, scratch, later, middle, start):
        block_ref, grad_ref, residual_ref, gain_ref, acts_hbm, saved_hbm, mixed_hbm = ins[:7]
        cos_ref, sin_ref, starts_ref, *slab_refs = ins[7:]
        grad_out, low_out, gain_out, slab_out, out_out = outs
        scratch = list(scratch)
        gather_sems = [scratch.pop(0) for _ in Gather.scratch]
        weights = Slab(place, slab_refs, [scratch.pop(0) for _ in Slab.scratch])
        full, part, qkv, mixed, acts_own, d_raw, d_keys, d_values = scratch[:8]
        slab, d_out, slab_in, d_out_in, load_sem, swap_send, swap_recv, total = scratch[8:16]
        reduce = Reduce(place, part, total, scratch[16:], far=True)
        weights.start()
        loads = copy_in([(saved_hbm, qkv), (mixed_hbm, mixed), (acts_hbm, acts_own)], load_sem)
        gather = Gather(place, block_ref, full, gather_sems, both=False)
        gather.start(later)
        start(0)
        start(3)
        d_keys[...] = jnp.zeros_like(d_keys)
        d_values[...] = jnp.zeros_like(d_values)
        for load in loads:
            load.wait()
        weights.wait()

        def step(p, carry):
            j = gather.chunk(p)
            pl.when(p == 2)(middle)
            b = 2 * j + place.c
            d_mixed = dot_t(full[j], weights.out[...]).astype(LOW)
            d_heads = jnp.concatenate([d_mixed[:, h * HD : (h + 1) * HD] for h in range(3)], axis=0)
            queries, keys, values, probs, rows, window = block_probs(qkv, starts_ref, b)
            d_probs = dot_t(d_heads, values).reshape(3, QB, reach)
            inner = jnp.sum(probs * d_probs, axis=-1, keepdims=True)
            d_scores = (probs * (d_probs - inner)).astype(LOW).reshape(3 * QB, reach)
            d_queries = jnp.dot(d_scores, keys, preferred_element_type=F32) * HD ** (-0.5)
            d_keys[window, :] += t_dot(d_scores, queries) * HD ** (-0.5)
            d_values[window, :] += t_dot(probs.astype(LOW).reshape(3 * QB, reach), d_heads)
            cos, sin = cos_ref[rows, :], sin_ref[rows, :]
            for h in range(3):
                head = d_queries[h * QB : (h + 1) * QB]
                head = head * cos + roll_half(head * sin)
                d_raw[rows, h * HD : (h + 1) * HD] = head.astype(LOW)
            other = rows_of((2 * j + 1 - place.c) * QB, QB)
            d_raw[other, 0 : 3 * HD] = jnp.zeros((QB, 3 * HD), LOW)
            return carry

        lax.fori_loop(0, 4, step, 0)
        start(1)

        def project(p, carry):
            j = far_first(place, p)
            rows = rows_of(j * 2 * QB, 2 * QB)
            head = d_keys[rows, :]
            head = head * cos_ref[rows, :] + roll_half(head * sin_ref[rows, :])
            d_raw[rows, 3 * HD : 4 * HD] = head.astype(LOW)
            d_raw[rows, 4 * HD : 5 * HD] = d_values[rows, :].astype(LOW)
            part[pl.ds(2 * j, 2)] = dot_t(d_raw[rows, :], weights.qkv[...]).astype(LOW).reshape(2, tokens, width)
            reduce.made(j)
            return carry

        lax.fori_loop(0, 4, project, 0)

        def swap():
            to = place.at(place.z, 1 - place.c)
            return [
                remote(slab.at[1 - place.c], slab_in, swap_send.at[0], swap_recv.at[0], to),
                remote(d_out.at[1 - place.c], d_out_in, swap_send.at[1], swap_recv.at[1], to),
            ]

        def between(i):
            if i < 4:
                cut = slice(i * (D // 4), (i + 1) * (D // 4))
                if turned:
                    grads = jnp.dot(acts_own[cut, :], d_raw[...], preferred_element_type=F32).astype(LOW)
                else:
                    grads = t_dot(acts_own[:, cut], d_raw[...]).astype(LOW)
                slab[0, i, 0 : D // 8, :] = grads[: D // 8]
                slab[1, i, 0 : D // 8, :] = grads[D // 8 :]
            elif i == 4:
                sums = jnp.sum(d_raw[...].astype(F32), axis=0, keepdims=True)
                first = lax.broadcasted_iota(jnp.int32, (16, 5 * HD), 0) == 0
                tail = jnp.where(first, sums, 0.0).astype(LOW)
                for half in range(2):
                    for part_at in range(4):
                        slab[half, part_at, D // 8 :, :] = tail
                grads = t_dot(mixed[...], full[...].reshape(4 * QB, D)).astype(LOW)
                d_out[0] = grads[: D // 8]
                d_out[1] = grads[D // 8 :]
                for copy in swap():
                    copy.start()
            if i == 0:
                middle(3)

        reduce.finish(later, between)
        after_backward(total, grad_ref, residual_ref, gain_ref, grad_out, low_out, gain_out)
        for copy in swap():
            copy.wait()
        for i in range(4):
            add_into(slab_out.at[i], [slab.at[place.c, i], slab_in.at[i]])
        add_into(out_out, [d_out.at[place.c], d_out_in])

    (grad, low, d_gain, d_slab, d_out), loads = carry_call(
        names,
        body,
        "line",
        [block, grad, residual, gain, acts, qkv, mixed, cosine, sine, starts, *slab],
        [*[ONCHIP] * 4, *[ANY] * 3, *[ONCHIP] * 3, *[ANY] * 4],
        [
            jax.ShapeDtypeStruct((tokens, width), F32),
            jax.ShapeDtypeStruct((tokens, width), LOW),
            jax.ShapeDtypeStruct((1, width), F32),
            jax.ShapeDtypeStruct((4, HALF, 5 * HD), LOW),
            jax.ShapeDtypeStruct((D // 8, D), LOW),
        ],
        [ONCHIP] * 5,
        [
            *Gather.scratch,
            *Slab.scratch,
            pltpu.VMEM((4, tokens, width), LOW),
            pltpu.VMEM((8, tokens, width), LOW),
            pltpu.VMEM((count, 5 * HD), LOW),
            pltpu.VMEM((count // 2, 3 * HD), LOW),
            pltpu.VMEM(acts.shape, LOW),
            pltpu.VMEM((count, 5 * HD), LOW),
            pltpu.VMEM((count, HD), F32),
            pltpu.VMEM((count, HD), F32),
            pltpu.VMEM((2, 4, HALF, 5 * HD), LOW),
            pltpu.VMEM((2, D // 8, D), LOW),
            pltpu.VMEM((4, HALF, 5 * HD), LOW),
            pltpu.VMEM((D // 8, D), LOW),
            pltpu.SemaphoreType.DMA((3,)),
            pltpu.SemaphoreType.DMA((2,)),
            pltpu.SemaphoreType.DMA((2,)),
            pltpu.VMEM((tokens, width), F32),
            *Reduce.scratch(tokens, width),
        ],
        cargo,
        name=name,
    )
    return grad, low, d_gain, d_slab.reshape(4 * HALF, 5 * HD), d_out, loads


def settle_rows(row, fulls, slots):
    kinds, layers = len(fulls), len(fulls[0])
    count, size = slots[0][0].shape[1:]
    tile = count // 5

    def kernel(row_ref, *refs):
        ins, outs = refs[: 2 * kinds * layers], refs[2 * kinds * layers :]
        for kind in range(kinds):
            for layer in range(layers):
                full, slot = ins[2 * (kind * layers + layer)], ins[2 * (kind * layers + layer) + 1]
                outs[kind][layer] = full[...].astype(F32) + slot[0].astype(F32) + slot[1].astype(F32)

    pairs = [pair for kind in range(kinds) for pair in zip(fulls[kind], slots[kind])]
    return pl.pallas_call(
        kernel,
        out_shape=[jax.ShapeDtypeStruct((layers, count, size), F32)] * kinds,
        grid_spec=pltpu.PrefetchScalarGridSpec(
            num_scalar_prefetch=1,
            grid=(count // tile,),
            in_specs=[
                pl.BlockSpec((tile, size), lambda i, row: (i, row[0])),
                pl.BlockSpec((2, tile, size), lambda i, row: (0, i, 0)),
            ]
            * (kinds * layers),
            out_specs=[pl.BlockSpec((layers, tile, size), lambda i, row: (0, i, 0))] * kinds,
        ),
        compiler_params=pltpu.CompilerParams(vmem_limit_bytes=VMEM),
        name="settle",
    )(row.reshape(1), *[array for pair in pairs for array in pair])


def backward_feed(names, block, grads_all, grad, residual, gain, acts, w_gate, w_up, w_down, gate, up, cargo, name):
    tokens, width = QB, D
    inner = w_gate.shape[0]
    apart = grads_all is not None

    def body(place, ins, outs, scratch, later, middle, start):
        head_ref, grad_ref, residual_ref, gain_ref, acts_hbm, gate_hbm, up_hbm, down_hbm, gates_hbm, ups_hbm = ins
        grad_out, low_out, gain_out, gate_out, up_out, down_out = outs
        scratch = list(scratch)
        gather_sems = [scratch.pop(0) for _ in Gather.scratch]
        full, part, acts_own, gate_w, up_w, down_w, gates, ups, hiddens, load_sem, keep_sem, total, d_down = scratch[:13]
        reduce = Reduce(place, part, total, scratch[13:], far=apart)
        if not apart:
            d_down = down_w
        def weights(dst, left, right, low, high):
            def tile(i, carry):
                cut = pl.ds(pl.multiple_of(i * 256, 256), 256)
                dst[cut, :] = t_dot(left[:, cut], right()).astype(LOW)
                return carry

            whole = inner // 256
            lax.fori_loop(low, min(high, whole), tile, 0)
            if high > whole and inner % 256:
                dst[whole * 256 :, :] = t_dot(left[:, whole * 256 :], right()).astype(LOW)

        def grads_flat():
            return full[...].reshape(8 * tokens, width)

        def acts_flat():
            return acts_own[...]

        pairs = [(gates_hbm, gates), (ups_hbm, ups)]
        if apart:
            pairs.append((head_ref, full))
        early = len(pairs)
        pairs += [(down_hbm, down_w), (gate_hbm, gate_w), (up_hbm, up_w), (acts_hbm, acts_own)]
        loads = copy_in(pairs, load_sem)
        gather = None
        if not apart:
            gather = Gather(place, head_ref, full, gather_sems)
            gather.start(later)
        start(0)
        start(3)
        for load in loads[:early]:
            load.wait()

        def lit(rows):
            gate, up = gates[rows, :].astype(F32), ups[rows, :].astype(F32)
            squash = jax.nn.sigmoid(gate)
            glow = gate * squash
            hiddens[rows, :] = (glow * up).astype(LOW)
            return gate, up, squash, glow

        if apart:

            def light(i, carry):
                lit(rows_of(i * tokens, tokens))
                return carry

            lax.fori_loop(0, 8, light, 0)
            weights(d_down, hiddens, grads_flat, 0, 5)
            start(1, d_down)
        for load in loads[early:]:
            load.wait()

        def step(p, carry):
            j = far_first(place, p) if apart else gather.chunk(p)
            pl.when(p == 2)(middle)
            rows = rows_of(j * 2 * tokens, 2 * tokens)
            grads = full[pl.ds(2 * j, 2)].reshape(2 * tokens, width)
            d_hidden = dot_t(grads, down_w[...])
            gate, up, squash, glow = lit(rows)
            d_gate = (d_hidden * up * squash * (1.0 + gate * (1.0 - squash))).astype(LOW)
            d_up = (d_hidden * glow).astype(LOW)
            gates[rows, :] = d_gate
            ups[rows, :] = d_up
            sums = dot(d_gate, gate_w[...]) + dot(d_up, up_w[...])
            part[pl.ds(2 * j, 2)] = sums.astype(LOW).reshape(2, tokens, width)
            reduce.made(j)
            return carry

        lax.fori_loop(0, 4, step, 0)

        work = [
            (gate_w, gates, acts_flat, 0, 3),
            (gate_w, gates, acts_flat, 3, 5),
            (up_w, ups, acts_flat, 0, 3),
            (up_w, ups, acts_flat, 3, 5),
        ]
        if not apart:
            weights(d_down, hiddens, grads_flat, 0, 5)
            start(1, d_down)

        def between(i):
            if apart and i == 0 or not apart and i == 5:
                middle(1)
            if i < len(work):
                weights(*work[i])

        reduce.finish(later, between)
        saves = copy_in([(gate_w, gate_out), (up_w, up_out), (d_down, down_out)], keep_sem)
        after_backward(total, grad_ref, residual_ref, gain_ref, grad_out, low_out, gain_out)
        for copy in saves:
            copy.wait()

    head = grads_all.reshape(8, tokens, width) if apart else block
    (grad, low, d_gain, d_gate, d_up, d_down), loads = carry_call(
        names,
        body,
        "line",
        [head, grad, residual, gain, acts, w_gate, w_up, w_down, gate, up],
        [ANY if apart else ONCHIP, ONCHIP, ONCHIP, ONCHIP, ANY, ANY, ANY, ANY, ANY, ANY],
        [
            jax.ShapeDtypeStruct((tokens, width), F32),
            jax.ShapeDtypeStruct((tokens, width), LOW),
            jax.ShapeDtypeStruct((1, width), F32),
            jax.ShapeDtypeStruct(w_gate.shape, LOW),
            jax.ShapeDtypeStruct(w_up.shape, LOW),
            jax.ShapeDtypeStruct(w_down.shape, LOW),
        ],
        [ONCHIP, ONCHIP, ONCHIP, ANY, ANY, ANY],
        [
            *Gather.scratch,
            pltpu.VMEM((8, tokens, width), LOW),
            pltpu.VMEM((8, tokens, width), LOW),
            pltpu.VMEM((8 * tokens, width), LOW),
            pltpu.VMEM(w_gate.shape, LOW),
            pltpu.VMEM(w_up.shape, LOW),
            pltpu.VMEM(w_down.shape, LOW),
            pltpu.VMEM((8 * tokens, inner), LOW),
            pltpu.VMEM((8 * tokens, inner), LOW),
            pltpu.VMEM((8 * tokens, inner), LOW),
            pltpu.SemaphoreType.DMA((7,)),
            pltpu.SemaphoreType.DMA((3,)),
            pltpu.VMEM((tokens, width), F32),
            pltpu.VMEM(w_down.shape if apart else (16, 128), LOW),
            *Reduce.scratch(tokens, width),
        ],
        cargo,
        name=name,
    )
    return grad, low, d_gain, d_gate, d_up, d_down, loads


eps_norm = 1e-06
rope_base = 1000000.0
neg_fill = -1e30


def row_starts(sizes, count):
    ends = jnp.cumsum(sizes)
    firsts = ends - sizes
    places = jnp.arange(count, dtype=jnp.int32)
    inside = (places[None, :] >= firsts[:, None]) & (places[None, :] < ends[:, None])
    return jnp.sum(jnp.where(inside, firsts[:, None], 0), axis=0)


def rope_tables(positions):
    half = HD // 2
    freq = rope_base ** (-(jnp.arange(half, dtype=jnp.float32) * (2.0 / HD)))
    angle = freq[:, None] * positions.astype(jnp.float32)[None, :]
    cosine = jnp.concatenate([jnp.cos(angle), jnp.cos(angle)], axis=0)
    sine = jnp.concatenate([jnp.sin(angle), jnp.sin(angle)], axis=0)
    return (cosine, sine)


def rotate(values, cosine, sine):
    half = HD // 2
    turned = jnp.concatenate([-values[:, half:], values[:, :half]], axis=1)
    return values * cosine + turned * sine


def rotate_back(grads, cosine, sine):
    half = HD // 2
    lifted = grads * sine
    turned = jnp.concatenate([lifted[:, half:], -lifted[:, :half]], axis=1)
    return grads * cosine + turned


def contract_first(left, right):
    return lax.dot_general(
        left, right, (((0,), (0,)), ((), ())), preferred_element_type=jnp.float32
    )


def contract_last(left, right):
    return lax.dot_general(
        left, right, (((1,), (1,)), ((), ())), preferred_element_type=jnp.float32
    )


def feature_total(values):
    return lax.psum(jnp.sum(values, axis=0), "col")


def spread(values):
    return lax.all_gather(values, "col", axis=0, tiled=True)


def summed_rows(make_term, rows):
    return lax.psum_scatter(
        make_term(jnp.int32(0), lax.axis_size("col") * rows), "col", scatter_dimension=0, tiled=True
    )


def to_blocks(values):
    return lax.all_to_all(values, "col", split_axis=1, concat_axis=0, tiled=True)


def to_tokens(values):
    return lax.all_to_all(values, "col", split_axis=0, concat_axis=1, tiled=True)


def by_columns(weight, acts, start, count):
    return contract_first(weight, acts)


def by_rows(weight, grads, start, count):
    return jnp.dot(weight, grads, preferred_element_type=jnp.float32)


def by_rows_pair(first_weight, first_grads, second_weight, second_grads, start, count):
    return by_rows(first_weight, first_grads, start, count) + by_rows(
        second_weight, second_grads, start, count
    )


def norm_forward(residual, gain):
    totals = feature_total(residual * residual)
    scale = lax.rsqrt(totals / D + eps_norm)
    return (scale, (residual * scale * gain[:, None]).astype(jnp.bfloat16))


def norm_backward(d_normed, residual, scale, gain):
    weighted = d_normed * gain[:, None]
    inner = feature_total(weighted * residual)
    d_residual = weighted * scale - residual * (scale * scale * scale) * inner / D
    d_gain = jnp.sum(d_normed * residual * scale, axis=1)
    return (d_residual, d_gain)


def attend_scores(queries, keys, mask):
    scores = jnp.einsum(
        "kghq,khj->kgqj", queries, keys, preferred_element_type=jnp.float32
    ) * HD ** (-0.5)
    return jnp.where(mask[None, None], scores, neg_fill)


def per_device(
    hidden_states,
    out_grad,
    lengths,
    norm_gains,
    qkv_weight,
    qkv_bias,
    out_weight,
    gate_weight,
    up_weight,
    down_weight,
):
    feat_rows, tok_row = hidden_states.shape
    col_at = lax.axis_index("col")
    starts = row_starts(lengths[0], tok_row)
    positions = jnp.arange(tok_row, dtype=jnp.int32) - starts
    cosine, sine = rope_tables(positions)
    first = col_at * QB
    block_starts = lax.dynamic_slice_in_dim(starts, first, QB)
    cos_block = lax.dynamic_slice_in_dim(cosine, first, QB, 1)
    sin_block = lax.dynamic_slice_in_dim(sine, first, QB, 1)
    reach = QB + SEQ_MAX
    window = jnp.maximum(first - SEQ_MAX, 0)
    key_places = window + jnp.arange(reach, dtype=jnp.int32)
    query_places = first + jnp.arange(QB, dtype=jnp.int32)
    mask = (key_places[None, :] >= block_starts[:, None]) & (
        key_places[None, :] <= query_places[:, None]
    )
    group = HEADS // KV_HEADS
    rotary = HEADS + KV_HEADS
    query_rows = HEADS * HD
    kv_rows = KV_HEADS * HD
    gains = norm_gains.astype(jnp.float32)
    residual = hidden_states.astype(jnp.float32)
    saved = []
    for layer in range(LAYERS):
        w_qkv, b_qkv, w_out, w_gate, w_up, w_down = (
            lax.all_gather(qkv_weight[layer], "row", axis=0, tiled=True),
            lax.all_gather(qkv_bias[layer], "row", axis=1, tiled=True),
            lax.all_gather(out_weight[layer], "row", axis=1, tiled=True),
            lax.all_gather(gate_weight[layer], "row", axis=0, tiled=True),
            lax.all_gather(up_weight[layer], "row", axis=0, tiled=True),
            lax.all_gather(down_weight[layer], "row", axis=1, tiled=True),
        )
        scale_one, normed_one = norm_forward(residual, gains[layer, 0])
        full_one = spread(normed_one)
        raw = contract_first(w_qkv, full_one) + b_qkv.reshape(-1).astype(jnp.float32)[:, None]
        local_heads = raw.shape[0] // HD
        shaped = raw.reshape(local_heads, HD, tok_row)
        head_ids = col_at * local_heads + jnp.arange(local_heads)
        turned = jnp.where((head_ids < rotary)[:, None, None], rotate(shaped, cosine, sine), shaped)
        blocked = to_blocks(turned.reshape(raw.shape).astype(jnp.bfloat16))
        kv_full = lax.all_gather(blocked[query_rows:], "col", axis=1, tiled=True)
        kv_window = lax.dynamic_slice_in_dim(kv_full, window, reach, 1)
        queries = blocked[:query_rows].reshape(KV_HEADS, group, HD, QB)
        keys = kv_window[:kv_rows].reshape(KV_HEADS, HD, reach)
        values = kv_window[kv_rows:].reshape(KV_HEADS, HD, reach)
        masked = attend_scores(queries, keys, mask)
        row_top = jnp.max(masked, axis=-1, keepdims=True)
        lifted = jnp.exp(masked - row_top)
        row_mass = jnp.sum(lifted, axis=-1, keepdims=True)
        probs = lifted / row_mass
        log_mass = row_top + jnp.log(row_mass)
        mixed = (
            jnp.einsum(
                "kgqj,khj->kghq",
                probs.astype(jnp.bfloat16),
                values,
                preferred_element_type=jnp.float32,
            )
            .reshape(query_rows, QB)
            .astype(jnp.bfloat16)
        )
        carried = to_tokens(mixed)
        attention = summed_rows(partial(by_columns, w_out, carried), feat_rows)
        residual_mid = residual + attention
        scale_two, normed_two = norm_forward(residual_mid, gains[layer, 1])
        full_two = spread(normed_two)
        gate = contract_first(w_gate, full_two)
        up = contract_first(w_up, full_two)
        hidden = (gate * jax.nn.sigmoid(gate) * up).astype(jnp.bfloat16)
        feed = summed_rows(partial(by_columns, w_down, hidden), feat_rows)
        saved.append(
            (
                residual,
                scale_one,
                full_one,
                blocked,
                kv_window,
                log_mass,
                mixed,
                carried,
                residual_mid,
                scale_two,
                full_two,
                gate,
                up,
                hidden,
                (w_qkv, w_out, w_gate, w_up, w_down),
                local_heads,
            )
        )
        residual = residual_mid + feed
    out_states = residual.astype(jnp.bfloat16)
    grad = out_grad.astype(jnp.float32)
    layer_grads = [None] * LAYERS
    gain_terms = [None] * LAYERS
    for layer in reversed(range(LAYERS)):
        (
            residual_in,
            scale_one,
            full_one,
            blocked,
            kv_window,
            log_mass,
            mixed,
            carried,
            residual_mid,
            scale_two,
            full_two,
            gate,
            up,
            hidden,
            weights_full,
            local_heads,
        ) = saved[layer]
        w_qkv, w_out, w_gate, w_up, w_down = weights_full
        grad_full = spread(grad.astype(jnp.bfloat16))
        d_down = contract_last(hidden, grad_full)
        d_hidden = jnp.dot(w_down, grad_full, preferred_element_type=jnp.float32)
        squash = jax.nn.sigmoid(gate)
        d_gate = (d_hidden * up * squash * (1.0 + gate * (1.0 - squash))).astype(jnp.bfloat16)
        d_up = (d_hidden * gate * squash).astype(jnp.bfloat16)
        d_gate_w = contract_last(full_two, d_gate)
        d_up_w = contract_last(full_two, d_up)
        d_normed_two = summed_rows(partial(by_rows_pair, w_gate, d_gate, w_up, d_up), feat_rows)
        d_residual, d_gain_two = norm_backward(
            d_normed_two, residual_mid, scale_two, gains[layer, 1]
        )
        grad = grad + d_residual
        grad_full = spread(grad.astype(jnp.bfloat16))
        d_out_w = contract_last(carried, grad_full)
        d_mixed = to_blocks(
            jnp.dot(w_out, grad_full, preferred_element_type=jnp.float32).astype(jnp.bfloat16)
        )
        queries = blocked[:query_rows].reshape(KV_HEADS, group, HD, QB)
        keys = kv_window[:kv_rows].reshape(KV_HEADS, HD, reach)
        values = kv_window[kv_rows:].reshape(KV_HEADS, HD, reach)
        masked = attend_scores(queries, keys, mask)
        probs = jnp.exp(masked - log_mass)
        low_probs = probs.astype(jnp.bfloat16)
        d_heads_mix = d_mixed.reshape(KV_HEADS, group, HD, QB)
        d_probs = jnp.einsum(
            "kghq,khj->kgqj", d_heads_mix, values, preferred_element_type=jnp.float32
        )
        inner = jnp.sum(probs * d_probs, axis=-1, keepdims=True)
        d_scores = (probs * (d_probs - inner)).astype(jnp.bfloat16)
        d_queries = (
            jnp.einsum("kgqj,khj->kghq", d_scores, keys, preferred_element_type=jnp.float32)
            * HD ** (-0.5)
        ).reshape(query_rows, QB)
        d_keys = (
            jnp.einsum("kgqj,kghq->khj", d_scores, queries, preferred_element_type=jnp.float32)
            * HD ** (-0.5)
        ).reshape(kv_rows, reach)
        d_values = jnp.einsum(
            "kgqj,kghq->khj", low_probs, d_heads_mix, preferred_element_type=jnp.float32
        ).reshape(kv_rows, reach)
        d_window = jnp.concatenate([d_keys, d_values], axis=0)
        d_placed = lax.dynamic_update_slice_in_dim(
            jnp.zeros((2 * kv_rows, tok_row), jnp.float32), d_window, window, 1
        )
        d_kv = lax.psum_scatter(d_placed, "col", scatter_dimension=1, tiled=True)
        d_heads = jnp.concatenate([d_queries, d_kv], axis=0).reshape(HEADS + 2 * KV_HEADS, HD, QB)
        d_turned = jnp.concatenate(
            [rotate_back(d_heads[:rotary], cos_block, sin_block), d_heads[rotary:]], axis=0
        )
        d_raw = to_tokens(d_turned.reshape((HEADS + 2 * KV_HEADS) * HD, QB).astype(jnp.bfloat16))
        d_bias = jnp.sum(d_raw, axis=1, dtype=jnp.float32).reshape(local_heads, HD)
        d_qkv_w = contract_last(full_one, d_raw)
        d_normed_one = summed_rows(partial(by_rows, w_qkv, d_raw), feat_rows)
        d_residual, d_gain_one = norm_backward(
            d_normed_one, residual_in, scale_one, gains[layer, 0]
        )
        grad = grad + d_residual
        layer_grads[layer] = (
            lax.psum_scatter(d_qkv_w, "row", scatter_dimension=0, tiled=True),
            lax.psum_scatter(d_bias, "row", scatter_dimension=1, tiled=True),
            lax.psum_scatter(d_out_w, "row", scatter_dimension=1, tiled=True),
            lax.psum_scatter(d_gate_w, "row", scatter_dimension=0, tiled=True),
            lax.psum_scatter(d_up_w, "row", scatter_dimension=0, tiled=True),
            lax.psum_scatter(d_down, "row", scatter_dimension=1, tiled=True),
        )
        gain_terms[layer] = jnp.stack([d_gain_one, d_gain_two])
    gain_grads = lax.psum(jnp.stack(gain_terms), "row")
    stacked = [jnp.stack([entry[member] for entry in layer_grads]) for member in range(6)]
    return (
        out_states,
        grad,
        gain_grads,
        stacked[0],
        stacked[1],
        stacked[2],
        stacked[3],
        stacked[4],
        stacked[5],
    )


def dot(a, b):
    return jnp.dot(a, b, preferred_element_type=F32)


def dot_t(a, b):
    return lax.dot_general(a, b, (((1,), (1,)), ((), ())), preferred_element_type=F32)


def t_dot(a, b):
    return lax.dot_general(a, b, (((0,), (0,)), ((), ())), preferred_element_type=F32)


def per_device_line(
    hidden_states,
    out_grad,
    lengths,
    norm_gains,
    qkv_weight,
    qkv_bias,
    out_weight,
    gate_weight,
    up_weight,
    down_weight,
):
    names = Names()
    tok_row = hidden_states.shape[1]
    row_at = lax.axis_index("row")
    col_at = lax.axis_index("col")
    core = col_at % 2

    biases = jnp.zeros((LAYERS, 2, 16, HD), LOW)
    biases = lax.dynamic_update_slice(biases, qkv_bias[:, :, None], (0, 0, 0, row_at * (HD // 4)))
    gain_rows = jnp.pad(norm_gains.reshape(2 * LAYERS, D // 8), ((0, 16 - 2 * LAYERS), (0, 0)))

    def rows_load(layer):
        return (
            GatherRows(gate_weight.swapaxes(1, 2), 1, layer),
            GatherRows(up_weight.swapaxes(1, 2), 1, layer),
            GatherRows(down_weight, 1, layer),
        )

    sent = rows_load(0)
    to_chips = [HeadsToChips(qkv_weight, biases, layer) for layer in range(LAYERS)]
    slab_rows, out_rows = GatherRows(From(to_chips[0]), 0, phase=1), GatherRows(out_weight, 1, 0, phase=1)
    swap = Swap(From(slab_rows), From(out_rows), phase=2)
    sent[0].phase, sent[0].split = 3, True
    states, loads = open_call(
        names, hidden_states, [*to_chips, Exchange(gain_rows, same=True), slab_rows, out_rows, swap, sent[0]]
    )
    (_,), (slab_next,), (gains,), (mine,), (out_mine,), (theirs, out_theirs), (w_gate,) = loads
    load = (mine, theirs, out_mine, out_theirs)
    gains = gains[:, : 2 * LAYERS].transpose(1, 0, 2).reshape(LAYERS, 2, D).astype(F32)
    starts = row_starts(lengths[0], tok_row)
    cosine, sine = rope_tables(jnp.arange(tok_row, dtype=jnp.int32) - starts)
    cosine, sine = cosine.T, sine.T * jnp.where(jnp.arange(HD) < HD // 2, -1.0, 1.0)[None]
    starts = starts[:, None]

    wide = states.reshape(D, tok_row)
    residual = lax.dynamic_slice_in_dim(wide, col_at * QB, QB, 1).astype(F32).T

    def own_rows(full):
        return lax.dynamic_slice_in_dim(full, col_at * QB, QB, 0).astype(F32)

    def gain_of(layer, which):
        return gains[layer, which][None]

    saved = []
    normed = None
    for layer in range(LAYERS):
        slab = load
        sent[1].phase, sent[2].phase = 0, 3
        fixed = (residual, gain_of(layer, 1), slab, cosine, sine, starts, sent[1:])
        if layer == 0:
            mid, normed, grads_all, qkv, mixed, full_one, loads = forward_heads(
                names, out_grad, wide, gains[0, 0][:, None], *fixed, name="heads_0"
            )
        else:
            mid, normed, full_one, qkv, mixed, _, loads = forward_heads(names, normed, None, None, *fixed, name="heads_1")
        (w_up,), (w_down,) = loads
        cargo = []
        if layer == 0:
            sent = rows_load(1)
            sent[0].phase = 3
            slab_rows, out_rows = GatherRows(slab_next, 0), GatherRows(out_weight, 1, 1)
            cargo = [slab_rows, out_rows, sent[0], Swap(From(slab_rows), From(out_rows), phase=2)]
        following = gain_of(layer + 1, 0) if layer + 1 < LAYERS else None
        states, normed, full_two, gate, up, loads = forward_feed(
            names, normed, mid, following, w_gate, w_up, w_down, cargo, name=f"feed_{layer}"
        )
        saved.append((residual, full_one, slab, qkv, mixed, mid, full_two, gate, up, (w_gate, w_up, w_down)))
        residual = states
        if layer == 0:
            (mine,), (out_mine,), (w_gate,), (theirs, out_theirs) = loads
            load = (mine, theirs, out_mine, out_theirs)
    states = normed

    def own_part(full, dim):
        size = full.shape[dim] // 4
        return lax.dynamic_slice_in_dim(full, row_at * size, size, dim)

    def settle(full, dim, slots):
        return jnp.sum(slots.astype(F32), axis=0) + own_part(full, dim).astype(F32)

    def settle_heads(tiles):
        total = tiles[:, :, 0].astype(F32) + jnp.where(col_at >= 6, tiles[:, :, 1].astype(F32), 0.0)
        weight = total[:, :, : D // 8].transpose(1, 2, 0, 3).reshape(D // 4, 2 * HD)
        bias = lax.dynamic_slice_in_dim(total[:, 0, D // 8], row_at * (HD // 4), HD // 4, 1)
        return weight, bias

    grads = {}
    gain_terms = [None] * LAYERS
    grad, low = own_rows(grads_all), None
    inner = w_gate.shape[0]
    owners = []
    for layer in reversed(range(LAYERS)):
        residual_in, full_one, slab, qkv, mixed, mid, full_two, gate, up, feed_weights = saved[layer]
        last = layer == LAYERS - 1
        cargo = [] if last else [ScatterRows(d_slab, 0), ScatterRows(d_out_w, 1)]
        cargo.append(ScatterRows(Inner((inner, D)), 1, phase=1))
        grad, low, d_gain_two, d_gate_w, d_up_w, d_down, loads = backward_feed(
            names,
            low,
            grads_all if last else None,
            grad,
            mid,
            gain_of(layer, 1),
            full_two,
            *feed_weights,
            gate,
            up,
            cargo,
            name=f"back_feed_{layer}",
        )
        grads["down", layer] = d_down, loads[-1][0]
        if not last:
            grads["out", layer + 1] = settle(d_out_w, 1, loads[1][0])
            owners.append(HeadsToOwners(settle(d_slab, 0, loads[0][0]).astype(LOW)))
        grad, low, d_gain_one, d_slab, d_out_w, loads = backward_heads(
            names,
            low,
            grad,
            residual_in,
            gain_of(layer, 0),
            full_one,
            layer == 0,
            slab,
            qkv,
            mixed,
            cosine,
            sine,
            starts,
            [ScatterRows(d_gate_w, 1), ScatterRows(d_up_w, 1, phase=3)],
            name=f"back_heads_{layer}",
        )
        grads["gate", layer] = d_gate_w, loads[0][0]
        grads["up", layer] = d_up_w, loads[1][0]
        gain_terms[layer] = jnp.concatenate([d_gain_one, d_gain_two], axis=0)
    leaving = jnp.concatenate([states, low], axis=0).T.reshape(8, D // 8, 2 * QB)
    gain_parts = jnp.pad(jnp.stack(gain_terms).reshape(2 * LAYERS, 8, D // 8), ((0, 8 - 2 * LAYERS), (0, 0), (0, 0)))
    (left,), (gain_all,), (slots,), (out_slots,), (tiles,) = close_call(
        names,
        [
            Exchange(leaving),
            Exchange(gain_parts.transpose(1, 0, 2), every_row=True),
            ScatterRows(d_slab, 0),
            ScatterRows(d_out_w, 1),
            *owners,
        ],
        "close",
    )
    grads["qkv", 1] = settle_heads(tiles)
    ((tiles,),) = close_call(names, [HeadsToOwners(settle(d_slab, 0, slots).astype(LOW))], "close_heads")
    grads["qkv", 0] = settle_heads(tiles)
    grads["out", 0] = settle(d_out_w, 1, out_slots)
    left = left.transpose(1, 0, 2)
    out_states = left[:, :, :QB].reshape(D // 8, tok_row)
    input_grad = left[:, :, QB:].reshape(D // 8, tok_row).astype(F32)
    gain_grads = jnp.sum(gain_all, axis=(0, 1))[: 2 * LAYERS].reshape(LAYERS, 2, D // 8)

    def both_layers(kind):
        return jnp.stack([grads[kind, layer] for layer in range(LAYERS)])

    kinds = ("gate", "up", "down")
    d_gate, d_up, d_down = settle_rows(
        row_at,
        [[grads[kind, layer][0] for layer in range(LAYERS)] for kind in kinds],
        [[grads[kind, layer][1] for layer in range(LAYERS)] for kind in kinds],
    )
    heads = [jnp.stack([grads["qkv", layer][i] for layer in range(LAYERS)]) for i in range(2)]
    return (
        out_states,
        input_grad,
        gain_grads,
        heads[0],
        heads[1],
        both_layers("out"),
        d_gate.swapaxes(1, 2),
        d_up.swapaxes(1, 2),
        d_down,
    )


def solution(mesh):
    placed = (
        P("col", "row"),
        P("col", "row"),
        P("row", None),
        P(None, None, "col"),
        P(None, "row", "col"),
        P(None, "col", "row"),
        P(None, "col", "row"),
        P(None, "row", "col"),
        P(None, "row", "col"),
        P(None, "col", "row"),
    )
    on_lines = mesh.shape["row"] == 4 and mesh.shape["col"] == 8
    return jax.shard_map(
        per_device_line if on_lines else per_device,
        mesh=mesh,
        in_specs=placed,
        out_specs=(
            P("col", "row"),
            P("col", "row"),
            P(None, None, "col"),
            P(None, "row", "col"),
            P(None, "col", "row"),
            P(None, "col", "row"),
            P(None, "row", "col"),
            P(None, "row", "col"),
            P(None, "col", "row"),
        ),
        check_vma=False,
    )
```

```python
from functools import partial

import jax
import jax.numpy as jnp
from jax import lax
from jax.experimental import pallas as pl
from jax.experimental.pallas import tpu as pltpu
from jax.sharding import PartitionSpec as P

D = 1536
HEADS = 12
KV_HEADS = 2
HD = 128
LAYERS = 2
SEQ_MAX = 512
QB = 128
MESH = pl.DeviceIdType.MESH
LOW = jnp.bfloat16
F32 = jnp.float32
ANY = pl.BlockSpec(memory_space=pl.ANY)
ONCHIP = pl.BlockSpec(memory_space=pltpu.VMEM)
VMEM = 62 * 2**20
HALF = 208


class Place:
    def __init__(self):
        self.r = lax.axis_index("row")
        self.k = lax.axis_index("col")
        self.z = self.k // 2
        self.c = self.k % 2

    def at(self, z, c):
        return (self.r, 2 * z + c)

    def rows(self):
        x, y = self.r % 2, self.r // 2
        return (2 * y + (1 - x), 2 * (1 - y) + x, 2 * (1 - y) + (1 - x))


def remote(src, dst, send, recv, device):
    return pltpu.make_async_remote_copy(
        src_ref=src, dst_ref=dst, send_sem=send, recv_sem=recv, device_id=device, device_id_type=MESH
    )


class Later:
    def __init__(self):
        self.todo = []

    def add(self, wait, cond=None):
        self.todo.append((wait, cond))

    def run(self):
        todo, self.todo = self.todo, []
        for wait, cond in todo:
            if cond is None:
                wait()
            else:
                pl.when(cond)(wait)


def greet(place, reach):
    barrier = pltpu.get_barrier_semaphore()

    def hail(device):
        pl.semaphore_signal(barrier, inc=1, device_id=device, device_id_type=MESH)

    if "all" in reach:
        for rr in range(4):
            for kk in range(8):
                pl.when((place.r != rr) | (place.k != kk))(partial(hail, (rr, kk)))
        pl.semaphore_wait(barrier, 31)
        return
    count = 0
    if "rows" in reach:
        for row in place.rows():
            hail((row, place.k))
        count += 3
    if "col" in reach:
        for kk in range(8):
            pl.when(place.k != kk)(partial(hail, (place.r, kk)))
        pl.semaphore_wait(barrier, count + 7)
        return
    hail(place.at(place.z, 1 - place.c))
    count += 1
    if "line" not in reach:
        pl.semaphore_wait(barrier, count)
        return
    pl.when(place.z < 3)(partial(hail, place.at(jnp.minimum(place.z + 1, 3), place.c)))
    pl.when(place.z > 0)(partial(hail, place.at(jnp.maximum(place.z - 1, 0), place.c)))
    edge = (place.z == 0) | (place.z == 3)
    pl.when(edge)(lambda: pl.semaphore_wait(barrier, count + 1))
    pl.when(jnp.logical_not(edge))(lambda: pl.semaphore_wait(barrier, count + 2))


class From:
    def __init__(self, item, at=0):
        self.item, self.at = item, at
        self.shape, self.dtype = item.outs[at].shape, item.outs[at].dtype


class Cargo:
    arrays = ()
    outs = ()
    scratch = ()
    reach = "rows"
    phase = 0
    slow = False

    def middle(self, place, ins, outs, scratch):
        pass


def part_of(ref, dim, row, size):
    cut = pl.ds(pl.multiple_of(row * size, 128 if dim else 16), size)
    return ref.at[:, cut] if dim else ref.at[cut, :]


class GatherRows(Cargo):
    def __init__(self, block, dim, layer=None, phase=0):
        self.dim, self.layer, self.phase = dim, layer, phase
        self.arrays = (block,)
        if layer is not None:
            block = jax.ShapeDtypeStruct(block.shape[1:], block.dtype)
        full = list(block.shape)
        full[dim] *= 4
        self.size = block.shape[dim]
        self.half = block.shape[0] // 32 * 16
        self.rest = block.shape[0] - self.half
        self.outs = (jax.ShapeDtypeStruct(tuple(full), block.dtype),)
        self.scratch = (
            pltpu.SemaphoreType.DMA((6,)),
            pltpu.SemaphoreType.DMA((6,)),
            pltpu.SemaphoreType.DMA((2,)),
            pltpu.VMEM(block.shape, block.dtype),
        )

    def halves(self, ref):
        return ref.at[0 : self.half, :], ref.at[self.half :, :]

    def spots(self, full, row):
        if self.dim:
            cut = pl.ds(pl.multiple_of(row * self.size, 128), self.size)
            return full.at[0 : self.half, cut], full.at[self.half :, cut]
        first = pl.multiple_of(row * self.size, 16)
        return full.at[pl.ds(first, self.half), :], full.at[pl.ds(first + self.half, self.rest), :]

    def source(self, ins):
        return ins[0] if self.layer is None else ins[0].at[self.layer]

    def copies(self, place, ins, outs, scratch):
        src, (dst,), (send, recv, *_) = self.source(ins), outs, scratch
        x, y, d = place.rows()
        block, mine = self.halves(src), self.spots(dst, place.r)
        from_x, from_y = self.spots(dst, x), self.spots(dst, y)
        out = [
            remote(block[0], mine[0], send.at[0], recv.at[0], (x, place.k)),
            remote(block[1], mine[1], send.at[1], recv.at[3], (y, place.k)),
            remote(block[1], mine[1], send.at[2], recv.at[1], (x, place.k)),
            remote(block[0], mine[0], send.at[3], recv.at[2], (y, place.k)),
        ]
        onward = [
            remote(from_x[0], from_x[0], send.at[4], recv.at[4], (y, place.k)),
            remote(from_y[1], from_y[1], send.at[5], recv.at[5], (x, place.k)),
        ]
        return out, onward

    def keep(self, place, ins, outs, scratch):
        *_, sem, buffer = scratch
        return (
            pltpu.make_async_copy(self.source(ins), buffer, sem.at[0]),
            pltpu.make_async_copy(buffer, part_of(outs[0], self.dim, place.r, self.size), sem.at[1]),
        )

    def arrived(self, place, scratch, view, sem, row):
        return remote(view, view, scratch[0].at[0], scratch[1].at[sem], (row, place.k))

    def start(self, place, ins, outs, scratch, later):
        (dst,) = outs
        out, onward = self.copies(place, ins, outs, scratch)
        for copy in out:
            copy.start()
        load, store = self.keep(place, ins, outs, scratch)
        load.start()
        later.add(store.wait)
        x, y, d = place.rows()
        from_x, from_y, from_d = self.spots(dst, x), self.spots(dst, y), self.spots(dst, d)
        for view, sem, row in ((from_x[1], 1, x), (from_y[0], 2, y), (from_d[0], 4, y), (from_d[1], 5, x)):
            later.add(self.arrived(place, scratch, view, sem, row).wait_recv)
        for copy in (*out, *onward):
            later.add(copy.wait_send)

    def middle(self, place, ins, outs, scratch):
        (dst,) = outs
        x, y, d = place.rows()
        _, onward = self.copies(place, ins, outs, scratch)
        load, store = self.keep(place, ins, outs, scratch)
        load.wait()
        store.start()
        self.arrived(place, scratch, self.spots(dst, x)[0], 0, x).wait_recv()
        onward[0].start()
        self.arrived(place, scratch, self.spots(dst, y)[1], 3, y).wait_recv()
        onward[1].start()


class ScatterRows(Cargo):
    def __init__(self, grad, dim, phase=0):
        self.dim, self.phase = dim, phase
        self.arrays = (grad,)
        part = list(grad.shape)
        part[dim] //= 4
        self.size = part[dim]
        self.half = part[0] // 32 * 16
        self.rest = part[0] - self.half
        self.outs = (jax.ShapeDtypeStruct((2, *part), grad.dtype),)
        upper, lower = pltpu.VMEM((self.half, part[1]), grad.dtype), pltpu.VMEM((self.rest, part[1]), grad.dtype)
        self.scratch = (
            *(upper, lower, lower, upper, lower, upper),
            pltpu.SemaphoreType.DMA((6,)),
            pltpu.SemaphoreType.DMA((6,)),
            pltpu.SemaphoreType.DMA((2,)),
        )

    def spots(self, full, row):
        if self.dim:
            cut = pl.ds(pl.multiple_of(row * self.size, 128), self.size)
            return full.at[0 : self.half, cut], full.at[self.half :, cut]
        first = pl.multiple_of(row * self.size, 16)
        return full.at[pl.ds(first, self.half), :], full.at[pl.ds(first + self.half, self.rest), :]

    def copies(self, place, ins, outs, scratch):
        (src,), (dst,) = ins, outs
        via_x, via_y, own_x, own_y, sum_x, sum_y, send, recv, keep = scratch
        x, y, d = place.rows()
        for_x, for_y, for_d = self.spots(src, x), self.spots(src, y), self.spots(src, d)
        slot_x = dst.at[0, 0 : self.half, :], dst.at[0, self.half :, :]
        slot_y = dst.at[1, 0 : self.half, :], dst.at[1, self.half :, :]
        first = [
            remote(for_d[0], via_x, send.at[0], recv.at[0], (x, place.k)),
            remote(for_d[1], via_y, send.at[1], recv.at[1], (y, place.k)),
            remote(for_x[0], slot_x[0], send.at[2], recv.at[2], (x, place.k)),
            remote(for_y[1], slot_y[1], send.at[3], recv.at[3], (y, place.k)),
        ]
        held = [
            pltpu.make_async_copy(for_x[1], own_x, keep.at[0]),
            pltpu.make_async_copy(for_y[0], own_y, keep.at[1]),
        ]
        last = [
            remote(sum_x, slot_x[1], send.at[4], recv.at[4], (x, place.k)),
            remote(sum_y, slot_y[0], send.at[5], recv.at[5], (y, place.k)),
        ]
        return first, held, last

    tell = None

    def start(self, place, ins, outs, scratch, later):
        if self.tell is not None:
            self.tell[0] = lambda: outs[0]
        first, held, last = self.copies(place, ins, outs, scratch)
        for copy in (*first, *held):
            copy.start()
        for copy in (*first, *last):
            later.add(copy.wait_send)
        for copy in (*first[2:], *last):
            later.add(copy.wait_recv)

    def middle(self, place, ins, outs, scratch):
        via_x, via_y, own_x, own_y, sum_x, sum_y, *_ = scratch
        first, held, last = self.copies(place, ins, outs, scratch)
        held[0].wait()
        first[1].wait_recv()
        add_into(sum_x, [own_x, via_y])
        last[0].start()
        held[1].wait()
        first[0].wait_recv()
        add_into(sum_y, [own_y, via_x])
        last[1].start()


class Swap(Cargo):
    reach = "line"

    def __init__(self, *arrays, phase=0):
        self.arrays, self.phase = arrays, phase
        self.outs = tuple(jax.ShapeDtypeStruct(a.shape, a.dtype) for a in arrays)
        self.scratch = (pltpu.SemaphoreType.DMA((len(arrays),)), pltpu.SemaphoreType.DMA((len(arrays),)))

    def start(self, place, ins, outs, scratch, later):
        send, recv = scratch
        for i, (src, dst) in enumerate(zip(ins, outs)):
            copy = remote(src, dst, send.at[i], recv.at[i], place.at(place.z, 1 - place.c))
            copy.start()
            later.add(copy.wait)


def tile_owner(z, t):
    if t < 3:
        head = 3 * z + t
        return head // 2, head % 2
    return 3 + t, z // 2


class HeadsToChips(Cargo):
    reach = "col"

    def __init__(self, weight, biases, layer):
        self.layer = layer
        self.phase = 0 if layer == 0 else 3
        self.arrays = (weight, biases)
        self.outs = (jax.ShapeDtypeStruct((HALF, 5 * HD), LOW),)
        self.scratch = (
            pltpu.SemaphoreType.DMA((2, 2, 2, 2)),
            pltpu.SemaphoreType.DMA((5, 2)),
            pltpu.VMEM(weight.shape[1:], weight.dtype),
            pltpu.VMEM(biases.shape[1:], biases.dtype),
            pltpu.SemaphoreType.DMA((2,)),
        )

    def start(self, place, ins, outs, scratch, later):
        (slab,), (send, recv, weight, biases, load_sem) = outs, scratch
        for load in copy_in([(ins[0].at[self.layer], weight), (ins[1].at[self.layer], biases)], load_sem):
            load.wait()
        r, k, z, c = place.r, place.k, place.z, place.c
        query = k < 6
        rows = D // 8
        for second in range(2):
            for i in range(2):
                head = 2 * k + i
                chip = jnp.where(query, head // 3, 2 * i + second)
                t = jnp.where(query, head % 3, k - 3)
                cut = pl.ds(pl.multiple_of(t * HD, HD), HD)
                spots = slab.at[0:rows, cut], slab.at[rows:HALF, cut]
                for core in range(2):
                    here = k == 2 * chip + core
                    away = jnp.logical_not(here)
                    if second == 1:
                        here, away = here & (k >= 6), away & (k >= 6)
                    views = (
                        weight.at[core * rows : (core + 1) * rows, i * HD : (i + 1) * HD],
                        biases.at[i],
                    )
                    for part in range(2):
                        sem = send.at[i, second, core, part]
                        copy = remote(views[part], spots[part], sem, recv.at[t, part], (r, 2 * chip + core))
                        pl.when(away)(copy.start)
                        later.add(copy.wait_send, away)
                        keep = pltpu.make_async_copy(views[part], spots[part], sem)
                        pl.when(here)(keep.start)
                        later.add(keep.wait, here)
        for t in range(5):
            owner, _ = tile_owner(z, t)
            cut = slice(t * HD, (t + 1) * HD)
            for part, spot in enumerate((slab.at[0:rows, cut], slab.at[rows:HALF, cut])):
                came = remote(spot, spot, send.at[0, 0, 0, 0], recv.at[t, part], (r, owner))
                later.add(came.wait_recv, k != owner)


class HeadsToOwners(Cargo):
    reach = "col"

    def __init__(self, slab):
        self.arrays = (slab,)
        self.outs = (jax.ShapeDtypeStruct((2, 2, 2, HALF, HD), LOW),)
        self.scratch = (pltpu.SemaphoreType.DMA((5,)), pltpu.SemaphoreType.DMA((2, 2, 2)))

    def start(self, place, ins, outs, scratch, later):
        (slab,), (tiles,), (send, recv) = ins, outs, scratch
        r, k, z, c = place.r, place.k, place.z, place.c
        for t in range(5):
            owner, i = tile_owner(z, t)
            which = z % 2 if t >= 3 else 0
            view, spot = slab.at[:, t * HD : (t + 1) * HD], tiles.at[i, c, which]
            here = k == owner
            copy = remote(view, spot, send.at[t], recv.at[i, c, which], (r, owner))
            pl.when(jnp.logical_not(here))(copy.start)
            later.add(copy.wait_send, jnp.logical_not(here))
            keep = pltpu.make_async_copy(view, spot, send.at[t])
            pl.when(here)(keep.start)
            later.add(keep.wait, here)
        for i in range(2):
            for which in range(2):
                chip = jnp.where(k < 6, (2 * k + i) // 3, 2 * i + which)
                for core in range(2):
                    wanted = k != 2 * chip + core
                    if which == 1:
                        wanted = wanted & (k >= 6)
                    came = remote(
                        slab.at[:, 0:HD],
                        tiles.at[i, core, which],
                        send.at[0],
                        recv.at[i, core, which],
                        (r, 2 * chip + core),
                    )
                    later.add(came.wait_recv, wanted)


class Exchange(Cargo):
    def __init__(self, chunks, every_row=False, same=False):
        self.arrays = (chunks,)
        self.same = same
        self.phase = 3
        self.rows_too = every_row
        self.reach = "all" if every_row else "col"
        lead = (4,) if every_row else (8,) if same else ()
        self.outs = (jax.ShapeDtypeStruct((*lead, *chunks.shape), chunks.dtype),)
        self.scratch = (pltpu.SemaphoreType.DMA((4, 8)), pltpu.SemaphoreType.DMA((4, 8)))

    def start(self, place, ins, outs, sems, later):
        (src,), (dst,), (send, recv) = ins, outs, sems
        r, k = place.r, place.k
        for rr in range(4) if self.rows_too else (None,):
            to_row = r if rr is None else rr
            for kk in range(8):
                here = (k == kk) if rr is None else (k == kk) & (r == rr)
                mine = dst.at[k] if rr is None else dst.at[r, k]
                theirs = dst.at[kk] if rr is None else dst.at[rr, kk]
                at = 0 if rr is None else rr
                my_at = 0 if rr is None else r
                part = src if self.same else src.at[kk]
                copy = remote(part, mine, send.at[at, kk], recv.at[my_at, k], (to_row, kk))
                pl.when(jnp.logical_not(here))(copy.start)
                later.add(copy.wait_send, jnp.logical_not(here))
                came = remote(part, theirs, send.at[at, kk], recv.at[at, kk], (to_row, kk))
                later.add(came.wait_recv, jnp.logical_not(here))
                keep = pltpu.make_async_copy(part, mine, send.at[at, kk])
                pl.when(here)(keep.start)
                later.add(keep.wait, here)


def add_into(dst, views):
    rows = dst.shape[0]

    def step(i, carry):
        cut = pl.ds(pl.multiple_of(i * 16, 16), 16)
        total = views[0][cut, :].astype(F32)
        for view in views[1:]:
            total = total + view[cut, :].astype(F32)
        dst[cut, :] = total.astype(dst.dtype)
        return carry

    lax.fori_loop(0, rows // 16, step, 0)


SUB = 4
LAG = 2


class Reduce:
    @staticmethod
    def scratch(tokens, width):
        return [
            pltpu.VMEM((4, tokens, width), LOW),
            pltpu.VMEM((2, 4, tokens, width), LOW),
            pltpu.VMEM((4, tokens, width), LOW),
            pltpu.SemaphoreType.DMA((4,)),
            pltpu.SemaphoreType.DMA((4,)),
            pltpu.SemaphoreType.DMA((4, SUB)),
            pltpu.SemaphoreType.DMA((2, 4, SUB)),
        ]

    def __init__(self, place, part, out, scratch, both=True, far=False):
        self.place, self.part, self.out, self.both, self.far = place, part, out, both, far
        self.from_p, self.moved, self.held, self.send_p, self.recv_p, self.send, self.recv = scratch
        z, c = place.z, place.c
        self.edge = (z == 0) | (z == 3)
        self.mid = jnp.logical_not(self.edge)
        self.right, self.left = place.at(jnp.minimum(z + 1, 3), c), place.at(jnp.maximum(z - 1, 0), c)
        self.size = part.shape[1] // SUB

    def pair(self, j):
        place = self.place
        other = self.part.at[2 * j + 1 - place.c]
        return remote(other, self.from_p.at[j], self.send_p.at[j], self.recv_p.at[j], place.at(place.z, 1 - place.c))

    def piece(self, j, sub, way):
        rows = rows_of(sub * self.size, self.size)
        column = jnp.where(way == 0, self.right[1], self.left[1])
        return remote(
            self.held.at[j, rows, :],
            self.moved.at[way, j, rows, :],
            self.send.at[j, sub],
            self.recv.at[way, j, sub],
            (self.place.r, column),
        )

    def terms(self, j):
        if self.both:
            return [self.part.at[2 * j + self.place.c], self.from_p.at[j]]
        return [self.part.at[j]]

    def made(self, j):
        z = self.place.z
        if self.both:
            self.pair(j).start()

        @pl.when(self.edge & (j != z))
        def _():
            if self.both:
                self.pair(j).wait_recv()
            add_into(self.held.at[j], self.terms(j))
            for sub in range(SUB):
                self.piece(j, sub, jnp.where(z == 0, 0, 1)).start()

    def finish(self, later, early=None, late=None):
        z = self.place.z
        way = jnp.where(z == 1, 0, 1)
        near, far, back = jnp.where(z == 1, 2, 1), jnp.where(z == 1, 3, 0), jnp.where(z == 1, 0, 3)
        first, second = (far, near) if self.far else (near, far)

        def step(j, sub, way):
            if self.both:
                pl.when(sub == 0)(lambda: self.pair(j).wait_recv())
            copy = self.piece(j, sub, way)
            copy.wait_recv()
            rows = rows_of(sub * self.size, self.size)
            views = [view.at[rows, :] for view in (*self.terms(j), self.moved.at[way, j])]
            add_into(self.held.at[j].at[rows, :], views)
            copy.start()

        def one(sub, carry):
            pl.when(self.mid)(lambda: step(first, sub, way))
            if early is not None:
                early(sub)
            return carry

        def two(sub, carry):
            pl.when(self.mid)(lambda: step(second, sub, way))
            pl.when(self.mid & (sub >= LAG))(lambda: step(back, sub - LAG, 1 - way))
            if late is not None:
                late(sub)
            return carry

        def three(sub, carry):
            pl.when(self.mid)(lambda: step(back, sub, 1 - way))
            return carry

        lax.fori_loop(0, SUB, one, 0)
        lax.fori_loop(0, SUB, two, 0)
        lax.fori_loop(SUB - LAG, SUB, three, 0)
        if self.both:
            self.pair(z).wait_recv()

        def came(way):
            for sub in range(SUB):
                self.piece(z, sub, way).wait_recv()

        views = self.terms(z)

        @pl.when(self.edge)
        def _():
            way = jnp.where(z == 0, 1, 0)
            came(way)
            add_into(self.out, [*views, self.moved.at[way, z]])

        @pl.when(self.mid)
        def _():
            came(0)
            came(1)
            add_into(self.out, [*views, self.moved.at[0, z], self.moved.at[1, z]])

        for j in range(4):
            if self.both:
                later.add(self.pair(j).wait_send)
            for sub in range(SUB):
                later.add(self.piece(j, sub, 0).wait_send, z != j)


def far_first(place, p):
    z = place.z
    edge = jnp.where(z == 0, 3 - p, p)
    mid = jnp.where(p == 0, jnp.where(z == 1, 3, 0), jnp.where(p == 1, jnp.where(z == 1, 2, 1), jnp.where(p == 2, jnp.where(z == 1, 0, 3), z)))
    return jnp.where((z == 0) | (z == 3), edge, mid)


class Names:
    def __init__(self):
        self.next = 0

    def take(self):
        self.next += 1
        return self.next - 1


class Inner:
    def __init__(self, shape, dtype=LOW):
        self.shape, self.dtype = shape, dtype


def given_arrays(item):
    return [a for a in item.arrays if not isinstance(a, (From, Inner))]


def carry_kernel(body, reach, n_in, n_out, n_scratch, cargo, *refs):
    refs = list(refs)

    def pop(n):
        taken = refs[:n]
        del refs[:n]
        return taken

    ins = pop(n_in)
    given = [pop(len(given_arrays(item))) for item in cargo]
    outs = pop(n_out)
    made = {item: pop(len(item.outs)) for item in cargo}
    scratch = pop(n_scratch)
    held = {item: pop(len(item.scratch)) for item in cargo}
    taken = {
        item: [
            made[a.item][a.at] if isinstance(a, From) else a if isinstance(a, Inner) else mine.pop(0)
            for a in item.arrays
        ]
        for item, mine in zip(cargo, given)
    }
    place = Place()
    later = Later()
    owed = [Later() for _ in range(4)]
    greet(place, {reach, *(item.reach for item in cargo)})

    def start(phase, *inner):
        inner = list(inner)
        mine = [item for item in cargo if item.phase == phase]
        for before in sorted({a.item.phase for item in mine for a in item.arrays if isinstance(a, From)}):
            owed[before].run()
        for item in mine:
            taken[item] = [inner.pop(0) if isinstance(a, Inner) else a for a in taken[item]]
            item.start(place, taken[item], made[item], held[item], owed[phase])

    start.wait = lambda phase: owed[phase].run()

    def middle(phase=0):
        for item in cargo:
            if item.phase == phase:
                item.middle(place, taken[item], made[item], held[item])

    body(place, ins, outs, scratch, later, middle, start)
    later.run()
    for waits in owed:
        waits.run()


def carry_call(names, body, reach, arrays, in_specs, outs, out_specs, scratch, cargo, name=None):
    given = [a for item in cargo for a in given_arrays(item)]
    call = pl.pallas_call(
        partial(carry_kernel, body, reach, len(arrays), len(outs), len(scratch), cargo),
        out_shape=[*outs, *(o for item in cargo for o in item.outs)],
        in_specs=[*in_specs, *(ANY for _ in given)],
        out_specs=[*out_specs, *(ANY for item in cargo for _ in item.outs)],
        scratch_shapes=[*scratch, *(s for item in cargo for s in item.scratch)],
        compiler_params=pltpu.CompilerParams(
            collective_id=names.take(), has_side_effects=True, vmem_limit_bytes=VMEM
        ),
        name=name,
    )
    results = list(call(*arrays, *given))
    main = results[: len(outs)]
    rest = results[len(outs) :]
    loads = []
    for item in cargo:
        loads.append(rest[: len(item.outs)])
        rest = rest[len(item.outs) :]
    return main, loads


class Gather:
    scratch = (
        pltpu.SemaphoreType.DMA((4, 2)),
        pltpu.SemaphoreType.DMA((4, 2)),
        pltpu.SemaphoreType.DMA((8, 2)),
        pltpu.SemaphoreType.DMA((8, 2)),
        pltpu.SemaphoreType.DMA((1,)),
    )

    def __init__(self, place, block, full, sems, both=True):
        self.place, self.block, self.full, self.both = place, block, full, both
        self.send_r, self.send_l, self.send_p, self.recv, self.keep = sems
        self.size = block.shape[0] // 2

    def spot(self, zz, c):
        return self.full.at[2 * zz + c] if self.both else self.full.at[zz]

    def copies(self, src, zz, t, way, half):
        z, c = self.place.z, self.place.c
        rows = pl.ds(half * self.size, self.size)
        src, spot, sem = src.at[rows, :], self.spot(zz, c).at[rows, :], self.recv.at[2 * zz + c, half]
        right = remote(src, spot, self.send_r.at[t, half], sem, self.place.at(jnp.minimum(z + 1, 3), c))
        left = remote(src, spot, self.send_l.at[t, half], sem, self.place.at(jnp.maximum(z - 1, 0), c))
        partner = remote(src, spot, self.send_p.at[2 * t + way, half], sem, self.place.at(z, 1 - c))
        return right, left, partner

    def start(self, later):
        z, c = self.place.z, self.place.c
        for half in range(2):
            right, left, partner = self.copies(self.block, z, 0, 0, half)
            pl.when(z < 3)(right.start)
            pl.when(z > 0)(left.start)
            later.add(right.wait_send, z < 3)
            later.add(left.wait_send, z > 0)
            if self.both:
                partner.start()
                later.add(partner.wait_send)
        keep = pltpu.make_async_copy(self.block, self.spot(z, c), self.keep.at[0])
        keep.start()
        keep.wait()
        for t in range(1, 4):
            for way in (0, 1):
                for half in range(2):
                    valid, onward, may, partner = self.step(t, way, half)
                    later.add(onward.wait_send, valid & may)
                    if self.both:
                        later.add(partner.wait_send, valid)

    def step(self, t, way, half):
        z = self.place.z
        there = z + (2 * way - 1) * t
        zz = jnp.clip(there, 0, 3)
        right, left, partner = self.copies(self.spot(zz, self.place.c), zz, t, way, half)
        onward, may = (left, z > 0) if way else (right, z < 3)
        return (there >= 0) & (there <= 3), onward, may, partner

    def pass_on(self, t):
        for half in range(2):
            for way in (0, 1):
                valid, onward, may, partner = self.step(t, way, half)

                @pl.when(valid)
                def _(onward=onward, may=may, partner=partner):
                    onward.wait_recv()
                    pl.when(may)(onward.start)
                    if self.both:
                        partner.start()

    def from_partner(self, zz):
        c = self.place.c
        for half in range(2):
            spot = self.spot(zz, 1 - c).at[pl.ds(half * self.size, self.size), :]
            recv = self.recv.at[2 * zz + 1 - c, half]
            yield remote(spot, spot, self.send_p.at[0, half], recv, self.place.at(self.place.z, 1 - c)).wait_recv

    def order(self, p):
        z = self.place.z
        second = jnp.where(z == 0, 1, z - 1)
        third = jnp.where(z == 0, 2, jnp.where(z == 3, 1, z + 1))
        fourth = jnp.where(z <= 1, 3, 0)
        return jnp.where(p == 0, z, jnp.where(p == 1, second, jnp.where(p == 2, third, fourth)))

    def chunk(self, p):
        z = self.place.z
        edge = (z == 0) | (z == 3)
        t = jnp.where(edge, p, (p + 1) // 2)
        pl.when((p >= 1) & (edge | (p != 2)))(lambda: self.pass_on(t))
        j = self.order(p)
        if self.both:
            for wait in self.from_partner(j):
                wait()
        return j


def tiles(count, work, size=256):
    def tile(i, carry):
        work(rows_of(i * size, size))
        return carry

    lax.fori_loop(0, count // size, tile, 0)
    if count % size:
        work(pl.ds(count // size * size, count % size))


def forward_feed(names, block, residual, gain, w_gate, w_up, w_down, cargo, name):
    tokens, width = block.shape
    inner = w_gate.shape[0]
    normed = gain is not None

    def body(place, ins, outs, scratch, later, middle, start):
        block_ref, residual_ref, gain_ref, gate_hbm, up_hbm, down_hbm = ins
        states_out, normed_out, full_out, gate_out, up_out = outs
        n = len(Gather.scratch)
        gather_sems, scratch = scratch[:n], scratch[n:]
        full, part, gate_w, up_w, down_w, gates, ups, load_sem, keep_sem, total, hidden = scratch[:11]
        reduce = Reduce(place, part, total, scratch[11:])
        gather = Gather(place, block_ref, full, gather_sems)
        loads = [
            pltpu.make_async_copy(src, dst, load_sem.at[i])
            for i, (src, dst) in enumerate(((gate_hbm, gate_w), (up_hbm, up_w), (down_hbm, down_w)))
        ]
        for load in loads:
            load.start()
        gather.start(later)
        start(0)
        start(3)
        for load in loads:
            load.wait()

        def keep(j):
            rows = pl.ds(pl.multiple_of(2 * tokens * j, 2 * tokens), 2 * tokens)
            return [
                pltpu.make_async_copy(full.at[pl.ds(2 * j, 2)], full_out.at[pl.ds(2 * j, 2)], keep_sem.at[0, j]),
                pltpu.make_async_copy(gates.at[rows, :], gate_out.at[rows, :], keep_sem.at[1, j]),
                pltpu.make_async_copy(ups.at[rows, :], up_out.at[rows, :], keep_sem.at[2, j]),
            ]

        def step(p, carry):
            j = gather.chunk(p)
            pl.when(p == 2)(middle)
            acts = full[pl.ds(2 * j, 2)].reshape(2 * tokens, width)
            rows = pl.ds(pl.multiple_of(2 * tokens * j, 2 * tokens), 2 * tokens)

            def columns(cut):
                gate = dot_t(acts, gate_w[cut, :])
                up = dot_t(acts, up_w[cut, :])
                gates[rows, cut] = gate.astype(LOW)
                ups[rows, cut] = up.astype(LOW)
                hidden[:, cut] = (gate * jax.nn.sigmoid(gate) * up).astype(LOW)

            tiles(inner, columns, 512)

            def outputs(cut):
                sums = dot(hidden[...], down_w[:, cut]).astype(LOW)
                part[pl.ds(2 * j, 2), :, cut] = sums.reshape(2, tokens, cut.size)

            tiles(width, outputs, 768)
            reduce.made(j)
            for copy in keep(j):
                copy.start()
            return carry

        lax.fori_loop(0, 4, step, 0)
        start(1)
        start(2)
        reduce.finish(later, early=lambda i: pl.when(i == 0)(lambda: middle(3)))
        after_forward(total, residual_ref, gain_ref if normed else None, states_out, normed_out)
        for j in range(4):
            for copy in keep(j):
                copy.wait()

    (states, low, full, gate, up), loads = carry_call(
        names,
        body,
        "line",
        [block, residual, gain if normed else jnp.ones((1, width), F32), w_gate, w_up, w_down],
        [ONCHIP, ONCHIP, ONCHIP, ANY, ANY, ANY],
        [
            jax.ShapeDtypeStruct((tokens, width), F32),
            jax.ShapeDtypeStruct((tokens, width), LOW),
            jax.ShapeDtypeStruct((8, tokens, width), LOW),
            jax.ShapeDtypeStruct((8 * tokens, inner), LOW),
            jax.ShapeDtypeStruct((8 * tokens, inner), LOW),
        ],
        [ONCHIP, ONCHIP, ANY, ANY, ANY],
        [
            *Gather.scratch,
            pltpu.VMEM((8, tokens, width), LOW),
            pltpu.VMEM((8, tokens, width), LOW),
            pltpu.VMEM(w_gate.shape, LOW),
            pltpu.VMEM(w_up.shape, LOW),
            pltpu.VMEM(w_down.shape, LOW),
            pltpu.VMEM((8 * tokens, inner), LOW),
            pltpu.VMEM((8 * tokens, inner), LOW),
            pltpu.SemaphoreType.DMA((3,)),
            pltpu.SemaphoreType.DMA((3, 4)),
            pltpu.VMEM((tokens, width), F32),
            pltpu.VMEM((2 * tokens, inner), LOW),
            *Reduce.scratch(tokens, width),
        ],
        cargo,
        name=name,
    )
    return states, low, full.reshape(8 * tokens, width), gate, up, loads


def rows_of(first, count):
    return pl.ds(pl.multiple_of(first, count), count)


def copy_in(pairs, sem):
    copies = [pltpu.make_async_copy(src, dst, sem.at[i]) for i, (src, dst) in enumerate(pairs)]
    for copy in copies:
        copy.start()
    return copies


def open_call(names, shard, cargo):
    def body(place, ins, outs, scratch, later, middle, start):
        gather = Gather(place, ins[0], outs[0], scratch)
        start(0)
        gather.start(later)
        start(3)
        start(1)
        gather.pass_on(1)
        middle(1)
        gather.pass_on(2)
        middle(3)
        start(2)
        gather.pass_on(3)
        for zz in range(4):
            for wait in gather.from_partner(zz):
                later.add(wait)

    (full,), loads = carry_call(
        names,
        body,
        "line",
        [shard],
        [ANY],
        [jax.ShapeDtypeStruct((8, *shard.shape), shard.dtype)],
        [ANY],
        list(Gather.scratch),
        cargo,
        name="open",
    )
    return full, loads


def close_call(names, slab, cargo):
    def body(place, ins, outs, scratch, later, middle, start):
        slab_ref = ins[0]
        own, came, total, sem = scratch
        start(0)
        start(3)
        middle(0)
        middle(3)
        load = pltpu.make_async_copy(slab_ref.at[rows_of(place.r * HALF, HALF), :], own, sem.at[0])
        load.start()
        start.wait(0)
        fetch = pltpu.make_async_copy(cargo_refs[0](), came, sem.at[1])
        fetch.start()
        load.wait()
        fetch.wait()
        add_into(total, [own, came.at[0], came.at[1]])
        start(1, total)

    cargo_refs = [None]
    rows, owners = ScatterRows(slab, 0), HeadsToOwners(Inner((HALF, 5 * HD)))
    owners.phase = 1
    rows.tell = cargo_refs
    _, loads = carry_call(
        names,
        body,
        "col",
        [slab],
        [ANY],
        [],
        [],
        [
            pltpu.VMEM((HALF, 5 * HD), LOW),
            pltpu.VMEM((2, HALF, 5 * HD), LOW),
            pltpu.VMEM((HALF, 5 * HD), LOW),
            pltpu.SemaphoreType.DMA((2,)),
        ],
        [rows, owners, *cargo],
        name="close",
    )
    return loads[1][0], loads[2:]


def after_forward(sums, residual, gain, states, normed):
    def step(i, carry):
        rows = rows_of(i * 16, 16)
        now = residual[rows, :] + sums[rows, :]
        states[rows, :] = now
        if gain is not None:
            now = now * lax.rsqrt(jnp.mean(now * now, axis=1, keepdims=True) + eps_norm) * gain[...]
        normed[rows, :] = now.astype(LOW)
        return carry

    lax.fori_loop(0, sums.shape[0] // 16, step, 0)


def after_backward(sums, grad, residual, gain, grad_out, low_out, gain_out):
    def step(i, total):
        rows = rows_of(i * 16, 16)
        d_normed, now = sums[rows, :], residual[rows, :]
        scale = lax.rsqrt(jnp.mean(now * now, axis=1, keepdims=True) + eps_norm)
        weighted = d_normed * gain[...]
        inner = jnp.sum(weighted * now, axis=1, keepdims=True)
        out = grad[rows, :] + (weighted * scale - now * (scale * scale * scale) * inner / D)
        grad_out[rows, :] = out
        low_out[rows, :] = out.astype(LOW)
        return total + jnp.sum(d_normed * now * scale, axis=0, keepdims=True)

    gain_out[...] = lax.fori_loop(0, sums.shape[0] // 16, step, jnp.zeros((1, D), F32))


class Slab:
    scratch = (
        pltpu.VMEM((D, 5 * HD), LOW),
        pltpu.VMEM((3 * HD, D), LOW),
        pltpu.VMEM((4, 16, 5 * HD), LOW),
        pltpu.SemaphoreType.DMA((2, 5)),
        pltpu.SemaphoreType.DMA((4,)),
    )

    def __init__(self, place, refs, scratch):
        self.place = place
        self.mine, self.theirs, self.out_mine, self.out_theirs = refs
        self.qkv, self.out, self.tails, self.sems, self.tail_sems = scratch

    def copies(self, half, mine):
        source, out = (self.mine, self.out_mine) if mine else (self.theirs, self.out_theirs)
        sem = self.sems.at[half]
        rows = D // 8
        for row in range(4):
            spot = self.qkv.at[(2 * row + half) * rows : (2 * row + half + 1) * rows, :]
            yield pltpu.make_async_copy(source.at[row * HALF : row * HALF + rows, :], spot, sem.at[row])
        yield pltpu.make_async_copy(out, self.out.at[half * rows : (half + 1) * rows, :], sem.at[4])
        if half == 0:
            for row in range(4):
                tail = source.at[row * HALF + rows : (row + 1) * HALF, :]
                yield pltpu.make_async_copy(tail, self.tails.at[row], self.tail_sems.at[row])

    def start(self):
        for half in range(2):
            for mine in (True, False):

                @pl.when((self.place.c == half) == mine)
                def _(half=half, mine=mine):
                    for copy in self.copies(half, mine):
                        copy.start()

    def wait(self):
        for half in range(2):
            for copy in self.copies(half, True):
                copy.wait()

    def bias(self):
        return jnp.sum(self.tails[:, 0, :].astype(F32), axis=0, keepdims=True)


def heads_of(ref, rows):
    return jnp.concatenate([ref[rows, h * HD : (h + 1) * HD] for h in range(3)], axis=0)


def block_window(b):
    first = jnp.maximum(b - SEQ_MAX // QB, 0) * QB
    return rows_of(b * QB, QB), pl.ds(pl.multiple_of(first, QB), QB + SEQ_MAX), first


def block_probs(queries, keys, starts, b):
    reach = QB + SEQ_MAX
    rows, _, first = block_window(b)
    scores = (dot_t(queries, keys) * HD ** (-0.5)).reshape(-1, QB, reach)
    key_at = first + lax.broadcasted_iota(jnp.int32, (QB, reach), 1)
    query_at = b * QB + lax.broadcasted_iota(jnp.int32, (QB, reach), 0)
    allowed = (key_at >= starts[rows, :]) & (key_at <= query_at)
    masked = jnp.where(allowed[None], scores, neg_fill)
    lifted = jnp.exp(masked - jnp.max(masked, axis=-1, keepdims=True))
    probs = lifted * (1.0 / jnp.sum(lifted, axis=-1, keepdims=True))
    return probs.reshape(-1, reach)


def roll_half(values):
    return pltpu.roll(values, HD // 2, 1)


def forward_heads(names, block, wide, gain, residual, gain_two, slab, cosine, sine, starts, cargo, name):
    tokens, width = QB, D
    count = 8 * QB
    apart = wide is not None

    def body(place, ins, outs, scratch, later, middle, start):
        ins = list(ins)
        block_ref = ins.pop(0)
        if apart:
            wide_hbm, gain_ref = ins.pop(0), ins.pop(0)
        residual_ref, two_ref, cos_ref, sin_ref, starts_ref, *slab_refs = ins
        states_out, normed_out, full_out, qkv_out, mixed_out = outs[:5]
        scratch = list(scratch)
        gather_sems = [scratch.pop(0) for _ in Gather.scratch]
        weights = Slab(place, slab_refs, [scratch.pop(0) for _ in Slab.scratch])
        full, acts, flat, part, qkv, mixed, load_sem, keep_sem, total = scratch[:9]
        reduce = Reduce(place, part, total, scratch[9:], both=False, far=True)
        weights.start()
        loads = copy_in([(wide_hbm, acts)] if apart else [], load_sem)
        gather = Gather(place, block_ref, full, gather_sems)
        gather.start(later)
        start(0)
        start(3)
        for load in loads:
            load.wait()
        weights.wait()
        bias = weights.bias()

        def keep(j):
            if apart:
                rows = rows_of(j * 2 * QB, 2 * QB)
                return pltpu.make_async_copy(flat.at[rows, :], full_out.at[rows, :], keep_sem.at[j])
            return pltpu.make_async_copy(full.at[pl.ds(2 * j, 2)], full_out.at[pl.ds(2 * j, 2)], keep_sem.at[j])

        def step(p, carry):
            if apart:
                j = gather.order(p)
            else:
                j = gather.chunk(p)
                pl.when(p == 2)(middle)
            rows = rows_of(j * 2 * QB, 2 * QB)
            if apart:
                chunk = acts[:, rows].astype(F32)
                scale = lax.rsqrt(jnp.mean(chunk * chunk, axis=0, keepdims=True) + eps_norm)
                chunk = (chunk * scale * gain_ref[...]).astype(LOW)
                acts[:, rows] = chunk
                raw = t_dot(chunk, weights.qkv[...]) + bias
            else:
                keep(j).start()
                raw = jnp.dot(full[pl.ds(2 * j, 2)].reshape(2 * tokens, width), weights.qkv[...], preferred_element_type=F32)
                raw = raw + bias
            cos, sin = cos_ref[rows, :], sin_ref[rows, :]
            for t in range(5):
                head = raw[:, t * HD : (t + 1) * HD]
                if t < 4:
                    head = head * cos + roll_half(head) * sin
                qkv[rows, t * HD : (t + 1) * HD] = head.astype(LOW)
            return carry

        lax.fori_loop(0, 4, step, 0)
        start(1)

        def attend(p, carry):
            j = far_first(place, p)
            b = 2 * j + place.c
            rows, window, _ = block_window(b)
            probs = block_probs(heads_of(qkv, rows), qkv[window, 3 * HD : 4 * HD], starts_ref, b)
            heads = dot(probs.astype(LOW), qkv[window, 4 * HD : 5 * HD]).astype(LOW)
            both = jnp.concatenate([heads[h * QB : (h + 1) * QB] for h in range(3)], axis=1)
            mixed[rows_of(j * QB, QB), :] = both
            part[j] = jnp.dot(both, weights.out[...], preferred_element_type=F32).astype(LOW)
            reduce.made(j)
            return carry

        lax.fori_loop(0, 4, attend, 0)
        saves = copy_in([(qkv, qkv_out), (mixed, mixed_out)], load_sem)
        if apart:
            saves.append(pltpu.make_async_copy(acts, outs[5], load_sem.at[2]))
            saves[-1].start()

        def early(i):
            if apart:
                pl.when(i == 0)(lambda: gather.pass_on(1))
            else:
                pl.when(i == 0)(lambda: middle(3))

        def late(i):
            if apart:

                @pl.when(i == 0)
                def _():
                    gather.pass_on(2)
                    middle(0)

                @pl.when(i == SUB - 1)
                def _():
                    gather.pass_on(3)
                    middle(3)

        reduce.finish(later, early, late)
        after_forward(total, residual_ref, two_ref, states_out, normed_out)
        if apart:
            for zz in range(4):
                for wait in gather.from_partner(zz):
                    wait()

            def turn(t, carry):
                rows = rows_of(t * 2 * QB, 2 * QB)
                for j in range(4):
                    piece = full[2 * j : 2 * j + 2, :, rows].reshape(D // 4, 2 * QB)
                    flat[rows, j * (D // 4) : (j + 1) * (D // 4)] = piece.T
                keep(t).start()
                return carry

            lax.fori_loop(0, 4, turn, 0)
        for copy in saves:
            copy.wait()
        for j in range(4):
            keep(j).wait()

    gathered = (count, width) if apart else (8, tokens, width)
    results, loads = carry_call(
        names,
        body,
        "line",
        [block, *([wide, gain] if apart else []), residual, gain_two, cosine, sine, starts, *slab],
        [ONCHIP, *([ANY, ONCHIP] if apart else []), *[ONCHIP] * 5, *[ANY] * 4],
        [
            jax.ShapeDtypeStruct((tokens, width), F32),
            jax.ShapeDtypeStruct((tokens, width), LOW),
            jax.ShapeDtypeStruct(gathered, LOW),
            jax.ShapeDtypeStruct((count, 5 * HD), LOW),
            jax.ShapeDtypeStruct((count // 2, 3 * HD), LOW),
            *([jax.ShapeDtypeStruct((width, count), LOW)] if apart else []),
        ],
        [ONCHIP, ONCHIP, ANY, ANY, ANY, *([ANY] if apart else [])],
        [
            *Gather.scratch,
            *Slab.scratch,
            pltpu.VMEM((8, *block.shape), LOW),
            pltpu.VMEM((width, count) if apart else (16, 128), LOW),
            pltpu.VMEM((count, width) if apart else (16, 128), LOW),
            pltpu.VMEM((4, tokens, width), LOW),
            pltpu.VMEM((count, 5 * HD), LOW),
            pltpu.VMEM((count // 2, 3 * HD), LOW),
            pltpu.SemaphoreType.DMA((3,)),
            pltpu.SemaphoreType.DMA((4,)),
            pltpu.VMEM((tokens, width), F32),
            *Reduce.scratch(tokens, width),
        ],
        cargo,
        name=name,
    )
    states, low, full, qkv, mixed = results[:5]
    return states, low, full.reshape(count, width), qkv, mixed, results[5] if apart else None, loads


def backward_heads(names, block, grad, residual, gain, acts, turned, slab, qkv, mixed, cosine, sine, starts, cargo, name):
    tokens, width = QB, D
    count = 8 * QB
    reach = QB + SEQ_MAX

    def body(place, ins, outs, scratch, later, middle, start):
        block_ref, grad_ref, residual_ref, gain_ref, acts_hbm, saved_hbm, mixed_hbm = ins[:7]
        cos_ref, sin_ref, starts_ref, *slab_refs = ins[7:]
        grad_out, low_out, gain_out, slab_out, out_out = outs
        scratch = list(scratch)
        gather_sems = [scratch.pop(0) for _ in Gather.scratch]
        weights = Slab(place, slab_refs, [scratch.pop(0) for _ in Slab.scratch])
        full, part, qkv, mixed, acts_own, d_raw, d_keys, d_values = scratch[:8]
        slab, d_out, slab_in, d_out_in, load_sem, swap_send, swap_recv, total, d_mixed = scratch[8:17]
        reduce = Reduce(place, part, total, scratch[17:], far=True)
        weights.start()
        loads = copy_in([(saved_hbm, qkv), (mixed_hbm, mixed), (acts_hbm, acts_own)], load_sem)
        gather = Gather(place, block_ref, full, gather_sems, both=False)
        gather.start(later)
        start(0)
        start(3)
        d_keys[...] = jnp.zeros_like(d_keys)
        d_values[...] = jnp.zeros_like(d_values)
        for load in loads:
            load.wait()
        weights.wait()

        def step(p, carry):
            j = gather.chunk(p)
            pl.when(p == 2)(middle)
            b = 2 * j + place.c
            d_mixed[...] = dot_t(full[j], weights.out[...]).astype(LOW)
            rows, window, _ = block_window(b)

            def head(h, carry):
                cut = rows_of(h * HD, HD)
                queries, d_head = qkv[rows, cut], d_mixed[:, cut]
                keys, values = qkv[window, 3 * HD : 4 * HD], qkv[window, 4 * HD : 5 * HD]
                probs = block_probs(queries, keys, starts_ref, b)
                d_probs = dot_t(d_head, values)
                inner = jnp.sum(probs * d_probs, axis=-1, keepdims=True)
                d_scores = (probs * (d_probs - inner)).astype(LOW)
                d_queries = dot(d_scores, keys) * HD ** (-0.5)
                d_keys[window, :] += t_dot(d_scores, queries) * HD ** (-0.5)
                d_values[window, :] += t_dot(probs.astype(LOW), d_head)
                turned_back = d_queries * cos_ref[rows, :] + roll_half(d_queries * sin_ref[rows, :])
                d_raw[rows, cut] = turned_back.astype(LOW)
                return carry

            lax.fori_loop(0, 3, head, 0)
            other = rows_of((2 * j + 1 - place.c) * QB, QB)
            d_raw[other, 0 : 3 * HD] = jnp.zeros((QB, 3 * HD), LOW)
            return carry

        lax.fori_loop(0, 4, step, 0)
        start(1)

        def project(p, carry):
            j = far_first(place, p)
            rows = rows_of(j * 2 * QB, 2 * QB)
            head = d_keys[rows, :]
            head = head * cos_ref[rows, :] + roll_half(head * sin_ref[rows, :])
            d_raw[rows, 3 * HD : 4 * HD] = head.astype(LOW)
            d_raw[rows, 4 * HD : 5 * HD] = d_values[rows, :].astype(LOW)
            part[pl.ds(2 * j, 2)] = dot_t(d_raw[rows, :], weights.qkv[...]).astype(LOW).reshape(2, tokens, width)
            reduce.made(j)
            return carry

        lax.fori_loop(0, 4, project, 0)

        def swap():
            to = place.at(place.z, 1 - place.c)
            return [
                remote(slab.at[1 - place.c], slab_in, swap_send.at[0], swap_recv.at[0], to),
                remote(d_out.at[1 - place.c], d_out_in, swap_send.at[1], swap_recv.at[1], to),
            ]

        def early(i):
            cut = rows_of(i * (D // 4), D // 4)
            if turned:
                grads = dot(acts_own[cut, :], d_raw[...]).astype(LOW)
            else:
                grads = t_dot(acts_own[:, cut], d_raw[...]).astype(LOW)
            slab[0, i, 0 : D // 8, :] = grads[: D // 8]
            slab[1, i, 0 : D // 8, :] = grads[D // 8 :]
            pl.when(i == 0)(lambda: middle(3))

        def late(i):
            @pl.when(i == 0)
            def _():
                sums = jnp.sum(d_raw[...].astype(F32), axis=0, keepdims=True)
                first = lax.broadcasted_iota(jnp.int32, (16, 5 * HD), 0) == 0
                tail = jnp.where(first, sums, 0.0).astype(LOW)
                for half in range(2):
                    for part_at in range(4):
                        slab[half, part_at, D // 8 :, :] = tail
                grads = t_dot(mixed[...], full[...].reshape(4 * QB, D)).astype(LOW)
                d_out[0] = grads[: D // 8]
                d_out[1] = grads[D // 8 :]
                for copy in swap():
                    copy.start()

        reduce.finish(later, early, late)
        after_backward(total, grad_ref, residual_ref, gain_ref, grad_out, low_out, gain_out)
        for copy in swap():
            copy.wait()
        for i in range(4):
            add_into(slab_out.at[i], [slab.at[place.c, i], slab_in.at[i]])
        add_into(out_out, [d_out.at[place.c], d_out_in])

    (grad, low, d_gain, d_slab, d_out), loads = carry_call(
        names,
        body,
        "line",
        [block, grad, residual, gain, acts, qkv, mixed, cosine, sine, starts, *slab],
        [*[ONCHIP] * 4, *[ANY] * 3, *[ONCHIP] * 3, *[ANY] * 4],
        [
            jax.ShapeDtypeStruct((tokens, width), F32),
            jax.ShapeDtypeStruct((tokens, width), LOW),
            jax.ShapeDtypeStruct((1, width), F32),
            jax.ShapeDtypeStruct((4, HALF, 5 * HD), LOW),
            jax.ShapeDtypeStruct((D // 8, D), LOW),
        ],
        [ONCHIP] * 5,
        [
            *Gather.scratch,
            *Slab.scratch,
            pltpu.VMEM((4, tokens, width), LOW),
            pltpu.VMEM((8, tokens, width), LOW),
            pltpu.VMEM((count, 5 * HD), LOW),
            pltpu.VMEM((count // 2, 3 * HD), LOW),
            pltpu.VMEM(acts.shape, LOW),
            pltpu.VMEM((count, 5 * HD), LOW),
            pltpu.VMEM((count, HD), F32),
            pltpu.VMEM((count, HD), F32),
            pltpu.VMEM((2, 4, HALF, 5 * HD), LOW),
            pltpu.VMEM((2, D // 8, D), LOW),
            pltpu.VMEM((4, HALF, 5 * HD), LOW),
            pltpu.VMEM((D // 8, D), LOW),
            pltpu.SemaphoreType.DMA((3,)),
            pltpu.SemaphoreType.DMA((2,)),
            pltpu.SemaphoreType.DMA((2,)),
            pltpu.VMEM((tokens, width), F32),
            pltpu.VMEM((QB, 3 * HD), LOW),
            *Reduce.scratch(tokens, width),
        ],
        cargo,
        name=name,
    )
    return grad, low, d_gain, d_slab.reshape(4 * HALF, 5 * HD), d_out, loads


def settle_rows(row, fulls, slots):
    kinds, layers = len(fulls), len(fulls[0])
    count, size = slots[0][0].shape[1:]
    tile = count // 5

    def kernel(row_ref, *refs):
        ins, outs = refs[: 2 * kinds * layers], refs[2 * kinds * layers :]
        for kind in range(kinds):
            for layer in range(layers):
                full, slot = ins[2 * (kind * layers + layer)], ins[2 * (kind * layers + layer) + 1]
                outs[kind][layer] = full[...].astype(F32) + slot[0].astype(F32) + slot[1].astype(F32)

    pairs = [pair for kind in range(kinds) for pair in zip(fulls[kind], slots[kind])]
    return pl.pallas_call(
        kernel,
        out_shape=[jax.ShapeDtypeStruct((layers, count, size), F32)] * kinds,
        grid_spec=pltpu.PrefetchScalarGridSpec(
            num_scalar_prefetch=1,
            grid=(count // tile,),
            in_specs=[
                pl.BlockSpec((tile, size), lambda i, row: (i, row[0])),
                pl.BlockSpec((2, tile, size), lambda i, row: (0, i, 0)),
            ]
            * (kinds * layers),
            out_specs=[pl.BlockSpec((layers, tile, size), lambda i, row: (0, i, 0))] * kinds,
        ),
        compiler_params=pltpu.CompilerParams(vmem_limit_bytes=VMEM),
        name="settle",
    )(row.reshape(1), *[array for pair in pairs for array in pair])


def backward_feed(names, block, grads_all, grad, residual, gain, acts, w_gate, w_up, w_down, gate, up, cargo, name):
    tokens, width = QB, D
    inner = w_gate.shape[0]
    apart = grads_all is not None

    def body(place, ins, outs, scratch, later, middle, start):
        head_ref, grad_ref, residual_ref, gain_ref, acts_hbm, gate_hbm, up_hbm, down_hbm, gates_hbm, ups_hbm = ins
        grad_out, low_out, gain_out, gate_out, up_out, down_out = outs
        scratch = list(scratch)
        gather_sems = [scratch.pop(0) for _ in Gather.scratch]
        full, part, acts_own, pair_w, down_w, pair, hiddens, load_sem, keep_sem, total, d_down = scratch[:11]
        gate_w, up_w, gates, ups = pair_w.at[0], pair_w.at[1], pair.at[0], pair.at[1]
        reduce = Reduce(place, part, total, scratch[11:], far=apart)
        if not apart:
            d_down = down_w
        def weights(dst, left, right, cut):
            dst[cut, :] = t_dot(left[:, cut], right()).astype(LOW)

        def grads_flat():
            return full[...].reshape(8 * tokens, width)

        def acts_flat():
            return acts_own[...]

        pairs = [(gates_hbm, gates), (ups_hbm, ups)]
        if apart:
            pairs.append((head_ref, full))
        early = len(pairs)
        pairs += [(down_hbm, down_w), (gate_hbm, gate_w), (up_hbm, up_w), (acts_hbm, acts_own)]
        loads = copy_in(pairs, load_sem)
        gather = None
        if not apart:
            gather = Gather(place, head_ref, full, gather_sems)
            gather.start(later)
        start(0)
        start(3)
        for load in loads[:early]:
            load.wait()

        def lit(rows, cut):
            gate, up = gates[rows, cut].astype(F32), ups[rows, cut].astype(F32)
            squash = jax.nn.sigmoid(gate)
            glow = gate * squash
            hiddens[rows, cut] = (glow * up).astype(LOW)
            return gate, up, squash, glow

        if apart:

            def light(i, carry):
                lit(rows_of(i * tokens, tokens), slice(None))
                return carry

            lax.fori_loop(0, 8, light, 0)
            tiles(inner, partial(weights, d_down, hiddens, grads_flat))
            start(1, d_down)
        for load in loads[early:]:
            load.wait()

        def step(p, carry):
            j = far_first(place, p) if apart else gather.chunk(p)
            pl.when(p == 2)(middle)
            rows = rows_of(j * 2 * tokens, 2 * tokens)
            grads = full[pl.ds(2 * j, 2)].reshape(2 * tokens, width)

            def columns(cut):
                d_hidden = dot_t(grads, down_w[cut, :])
                gate, up, squash, glow = lit(rows, cut)
                gates[rows, cut] = (d_hidden * up * squash * (1.0 + gate * (1.0 - squash))).astype(LOW)
                ups[rows, cut] = (d_hidden * glow).astype(LOW)

            tiles(inner, columns)

            def outputs(cut):
                sums = dot(gates[rows, :], gate_w[:, cut]) + dot(ups[rows, :], up_w[:, cut])
                part[pl.ds(2 * j, 2), :, cut] = sums.astype(LOW).reshape(2, tokens, cut.size)

            tiles(width, outputs, 512)
            reduce.made(j)
            return carry

        lax.fori_loop(0, 4, step, 0)

        if not apart:
            tiles(inner, partial(weights, d_down, hiddens, grads_flat))
            start(1, d_down)

        def both_rows(cut):
            def kind(k, carry):
                weights(pair_w.at[k], pair.at[k], acts_flat, cut)
                return carry

            lax.fori_loop(0, 2, kind, 0)

        def early(i):
            if apart:
                pl.when(i == 0)(lambda: middle(1))
            both_rows(rows_of(i * 256, 256))

        def late(i):
            @pl.when(i == 0)
            def _():
                if inner > 256 * SUB:
                    both_rows(pl.ds(256 * SUB, inner - 256 * SUB))
                if not apart:
                    middle(1)

        reduce.finish(later, early, late)
        saves = copy_in([(gate_w, gate_out), (up_w, up_out), (d_down, down_out)], keep_sem)
        after_backward(total, grad_ref, residual_ref, gain_ref, grad_out, low_out, gain_out)
        for copy in saves:
            copy.wait()

    head = grads_all.reshape(8, tokens, width) if apart else block
    (grad, low, d_gain, d_gate, d_up, d_down), loads = carry_call(
        names,
        body,
        "line",
        [head, grad, residual, gain, acts, w_gate, w_up, w_down, gate, up],
        [ANY if apart else ONCHIP, ONCHIP, ONCHIP, ONCHIP, ANY, ANY, ANY, ANY, ANY, ANY],
        [
            jax.ShapeDtypeStruct((tokens, width), F32),
            jax.ShapeDtypeStruct((tokens, width), LOW),
            jax.ShapeDtypeStruct((1, width), F32),
            jax.ShapeDtypeStruct(w_gate.shape, LOW),
            jax.ShapeDtypeStruct(w_up.shape, LOW),
            jax.ShapeDtypeStruct(w_down.shape, LOW),
        ],
        [ONCHIP, ONCHIP, ONCHIP, ANY, ANY, ANY],
        [
            *Gather.scratch,
            pltpu.VMEM((8, tokens, width), LOW),
            pltpu.VMEM((8, tokens, width), LOW),
            pltpu.VMEM((8 * tokens, width), LOW),
            pltpu.VMEM((2, *w_gate.shape), LOW),
            pltpu.VMEM(w_down.shape, LOW),
            pltpu.VMEM((2, 8 * tokens, inner), LOW),
            pltpu.VMEM((8 * tokens, inner), LOW),
            pltpu.SemaphoreType.DMA((7,)),
            pltpu.SemaphoreType.DMA((3,)),
            pltpu.VMEM((tokens, width), F32),
            pltpu.VMEM(w_down.shape if apart else (16, 128), LOW),
            *Reduce.scratch(tokens, width),
        ],
        cargo,
        name=name,
    )
    return grad, low, d_gain, d_gate, d_up, d_down, loads


eps_norm = 1e-06
rope_base = 1000000.0
neg_fill = -1e30


def row_starts(sizes, count):
    ends = jnp.cumsum(sizes)
    firsts = ends - sizes
    places = jnp.arange(count, dtype=jnp.int32)
    inside = (places[None, :] >= firsts[:, None]) & (places[None, :] < ends[:, None])
    return jnp.sum(jnp.where(inside, firsts[:, None], 0), axis=0)


def rope_tables(positions):
    half = HD // 2
    freq = rope_base ** (-(jnp.arange(half, dtype=jnp.float32) * (2.0 / HD)))
    angle = freq[:, None] * positions.astype(jnp.float32)[None, :]
    cosine = jnp.concatenate([jnp.cos(angle), jnp.cos(angle)], axis=0)
    sine = jnp.concatenate([jnp.sin(angle), jnp.sin(angle)], axis=0)
    return (cosine, sine)


def rotate(values, cosine, sine):
    half = HD // 2
    turned = jnp.concatenate([-values[:, half:], values[:, :half]], axis=1)
    return values * cosine + turned * sine


def rotate_back(grads, cosine, sine):
    half = HD // 2
    lifted = grads * sine
    turned = jnp.concatenate([lifted[:, half:], -lifted[:, :half]], axis=1)
    return grads * cosine + turned


def contract_first(left, right):
    return lax.dot_general(
        left, right, (((0,), (0,)), ((), ())), preferred_element_type=jnp.float32
    )


def contract_last(left, right):
    return lax.dot_general(
        left, right, (((1,), (1,)), ((), ())), preferred_element_type=jnp.float32
    )


def feature_total(values):
    return lax.psum(jnp.sum(values, axis=0), "col")


def spread(values):
    return lax.all_gather(values, "col", axis=0, tiled=True)


def summed_rows(make_term, rows):
    return lax.psum_scatter(
        make_term(jnp.int32(0), lax.axis_size("col") * rows), "col", scatter_dimension=0, tiled=True
    )


def to_blocks(values):
    return lax.all_to_all(values, "col", split_axis=1, concat_axis=0, tiled=True)


def to_tokens(values):
    return lax.all_to_all(values, "col", split_axis=0, concat_axis=1, tiled=True)


def by_columns(weight, acts, start, count):
    return contract_first(weight, acts)


def by_rows(weight, grads, start, count):
    return jnp.dot(weight, grads, preferred_element_type=jnp.float32)


def by_rows_pair(first_weight, first_grads, second_weight, second_grads, start, count):
    return by_rows(first_weight, first_grads, start, count) + by_rows(
        second_weight, second_grads, start, count
    )


def norm_forward(residual, gain):
    totals = feature_total(residual * residual)
    scale = lax.rsqrt(totals / D + eps_norm)
    return (scale, (residual * scale * gain[:, None]).astype(jnp.bfloat16))


def norm_backward(d_normed, residual, scale, gain):
    weighted = d_normed * gain[:, None]
    inner = feature_total(weighted * residual)
    d_residual = weighted * scale - residual * (scale * scale * scale) * inner / D
    d_gain = jnp.sum(d_normed * residual * scale, axis=1)
    return (d_residual, d_gain)


def attend_scores(queries, keys, mask):
    scores = jnp.einsum(
        "kghq,khj->kgqj", queries, keys, preferred_element_type=jnp.float32
    ) * HD ** (-0.5)
    return jnp.where(mask[None, None], scores, neg_fill)


def per_device(
    hidden_states,
    out_grad,
    lengths,
    norm_gains,
    qkv_weight,
    qkv_bias,
    out_weight,
    gate_weight,
    up_weight,
    down_weight,
):
    feat_rows, tok_row = hidden_states.shape
    col_at = lax.axis_index("col")
    starts = row_starts(lengths[0], tok_row)
    positions = jnp.arange(tok_row, dtype=jnp.int32) - starts
    cosine, sine = rope_tables(positions)
    first = col_at * QB
    block_starts = lax.dynamic_slice_in_dim(starts, first, QB)
    cos_block = lax.dynamic_slice_in_dim(cosine, first, QB, 1)
    sin_block = lax.dynamic_slice_in_dim(sine, first, QB, 1)
    reach = QB + SEQ_MAX
    window = jnp.maximum(first - SEQ_MAX, 0)
    key_places = window + jnp.arange(reach, dtype=jnp.int32)
    query_places = first + jnp.arange(QB, dtype=jnp.int32)
    mask = (key_places[None, :] >= block_starts[:, None]) & (
        key_places[None, :] <= query_places[:, None]
    )
    group = HEADS // KV_HEADS
    rotary = HEADS + KV_HEADS
    query_rows = HEADS * HD
    kv_rows = KV_HEADS * HD
    gains = norm_gains.astype(jnp.float32)
    residual = hidden_states.astype(jnp.float32)
    saved = []
    for layer in range(LAYERS):
        w_qkv, b_qkv, w_out, w_gate, w_up, w_down = (
            lax.all_gather(qkv_weight[layer], "row", axis=0, tiled=True),
            lax.all_gather(qkv_bias[layer], "row", axis=1, tiled=True),
            lax.all_gather(out_weight[layer], "row", axis=1, tiled=True),
            lax.all_gather(gate_weight[layer], "row", axis=0, tiled=True),
            lax.all_gather(up_weight[layer], "row", axis=0, tiled=True),
            lax.all_gather(down_weight[layer], "row", axis=1, tiled=True),
        )
        scale_one, normed_one = norm_forward(residual, gains[layer, 0])
        full_one = spread(normed_one)
        raw = contract_first(w_qkv, full_one) + b_qkv.reshape(-1).astype(jnp.float32)[:, None]
        local_heads = raw.shape[0] // HD
        shaped = raw.reshape(local_heads, HD, tok_row)
        head_ids = col_at * local_heads + jnp.arange(local_heads)
        turned = jnp.where((head_ids < rotary)[:, None, None], rotate(shaped, cosine, sine), shaped)
        blocked = to_blocks(turned.reshape(raw.shape).astype(jnp.bfloat16))
        kv_full = lax.all_gather(blocked[query_rows:], "col", axis=1, tiled=True)
        kv_window = lax.dynamic_slice_in_dim(kv_full, window, reach, 1)
        queries = blocked[:query_rows].reshape(KV_HEADS, group, HD, QB)
        keys = kv_window[:kv_rows].reshape(KV_HEADS, HD, reach)
        values = kv_window[kv_rows:].reshape(KV_HEADS, HD, reach)
        masked = attend_scores(queries, keys, mask)
        row_top = jnp.max(masked, axis=-1, keepdims=True)
        lifted = jnp.exp(masked - row_top)
        row_mass = jnp.sum(lifted, axis=-1, keepdims=True)
        probs = lifted / row_mass
        log_mass = row_top + jnp.log(row_mass)
        mixed = (
            jnp.einsum(
                "kgqj,khj->kghq",
                probs.astype(jnp.bfloat16),
                values,
                preferred_element_type=jnp.float32,
            )
            .reshape(query_rows, QB)
            .astype(jnp.bfloat16)
        )
        carried = to_tokens(mixed)
        attention = summed_rows(partial(by_columns, w_out, carried), feat_rows)
        residual_mid = residual + attention
        scale_two, normed_two = norm_forward(residual_mid, gains[layer, 1])
        full_two = spread(normed_two)
        gate = contract_first(w_gate, full_two)
        up = contract_first(w_up, full_two)
        hidden = (gate * jax.nn.sigmoid(gate) * up).astype(jnp.bfloat16)
        feed = summed_rows(partial(by_columns, w_down, hidden), feat_rows)
        saved.append(
            (
                residual,
                scale_one,
                full_one,
                blocked,
                kv_window,
                log_mass,
                mixed,
                carried,
                residual_mid,
                scale_two,
                full_two,
                gate,
                up,
                hidden,
                (w_qkv, w_out, w_gate, w_up, w_down),
                local_heads,
            )
        )
        residual = residual_mid + feed
    out_states = residual.astype(jnp.bfloat16)
    grad = out_grad.astype(jnp.float32)
    layer_grads = [None] * LAYERS
    gain_terms = [None] * LAYERS
    for layer in reversed(range(LAYERS)):
        (
            residual_in,
            scale_one,
            full_one,
            blocked,
            kv_window,
            log_mass,
            mixed,
            carried,
            residual_mid,
            scale_two,
            full_two,
            gate,
            up,
            hidden,
            weights_full,
            local_heads,
        ) = saved[layer]
        w_qkv, w_out, w_gate, w_up, w_down = weights_full
        grad_full = spread(grad.astype(jnp.bfloat16))
        d_down = contract_last(hidden, grad_full)
        d_hidden = jnp.dot(w_down, grad_full, preferred_element_type=jnp.float32)
        squash = jax.nn.sigmoid(gate)
        d_gate = (d_hidden * up * squash * (1.0 + gate * (1.0 - squash))).astype(jnp.bfloat16)
        d_up = (d_hidden * gate * squash).astype(jnp.bfloat16)
        d_gate_w = contract_last(full_two, d_gate)
        d_up_w = contract_last(full_two, d_up)
        d_normed_two = summed_rows(partial(by_rows_pair, w_gate, d_gate, w_up, d_up), feat_rows)
        d_residual, d_gain_two = norm_backward(
            d_normed_two, residual_mid, scale_two, gains[layer, 1]
        )
        grad = grad + d_residual
        grad_full = spread(grad.astype(jnp.bfloat16))
        d_out_w = contract_last(carried, grad_full)
        d_mixed = to_blocks(
            jnp.dot(w_out, grad_full, preferred_element_type=jnp.float32).astype(jnp.bfloat16)
        )
        queries = blocked[:query_rows].reshape(KV_HEADS, group, HD, QB)
        keys = kv_window[:kv_rows].reshape(KV_HEADS, HD, reach)
        values = kv_window[kv_rows:].reshape(KV_HEADS, HD, reach)
        masked = attend_scores(queries, keys, mask)
        probs = jnp.exp(masked - log_mass)
        low_probs = probs.astype(jnp.bfloat16)
        d_heads_mix = d_mixed.reshape(KV_HEADS, group, HD, QB)
        d_probs = jnp.einsum(
            "kghq,khj->kgqj", d_heads_mix, values, preferred_element_type=jnp.float32
        )
        inner = jnp.sum(probs * d_probs, axis=-1, keepdims=True)
        d_scores = (probs * (d_probs - inner)).astype(jnp.bfloat16)
        d_queries = (
            jnp.einsum("kgqj,khj->kghq", d_scores, keys, preferred_element_type=jnp.float32)
            * HD ** (-0.5)
        ).reshape(query_rows, QB)
        d_keys = (
            jnp.einsum("kgqj,kghq->khj", d_scores, queries, preferred_element_type=jnp.float32)
            * HD ** (-0.5)
        ).reshape(kv_rows, reach)
        d_values = jnp.einsum(
            "kgqj,kghq->khj", low_probs, d_heads_mix, preferred_element_type=jnp.float32
        ).reshape(kv_rows, reach)
        d_window = jnp.concatenate([d_keys, d_values], axis=0)
        d_placed = lax.dynamic_update_slice_in_dim(
            jnp.zeros((2 * kv_rows, tok_row), jnp.float32), d_window, window, 1
        )
        d_kv = lax.psum_scatter(d_placed, "col", scatter_dimension=1, tiled=True)
        d_heads = jnp.concatenate([d_queries, d_kv], axis=0).reshape(HEADS + 2 * KV_HEADS, HD, QB)
        d_turned = jnp.concatenate(
            [rotate_back(d_heads[:rotary], cos_block, sin_block), d_heads[rotary:]], axis=0
        )
        d_raw = to_tokens(d_turned.reshape((HEADS + 2 * KV_HEADS) * HD, QB).astype(jnp.bfloat16))
        d_bias = jnp.sum(d_raw, axis=1, dtype=jnp.float32).reshape(local_heads, HD)
        d_qkv_w = contract_last(full_one, d_raw)
        d_normed_one = summed_rows(partial(by_rows, w_qkv, d_raw), feat_rows)
        d_residual, d_gain_one = norm_backward(
            d_normed_one, residual_in, scale_one, gains[layer, 0]
        )
        grad = grad + d_residual
        layer_grads[layer] = (
            lax.psum_scatter(d_qkv_w, "row", scatter_dimension=0, tiled=True),
            lax.psum_scatter(d_bias, "row", scatter_dimension=1, tiled=True),
            lax.psum_scatter(d_out_w, "row", scatter_dimension=1, tiled=True),
            lax.psum_scatter(d_gate_w, "row", scatter_dimension=0, tiled=True),
            lax.psum_scatter(d_up_w, "row", scatter_dimension=0, tiled=True),
            lax.psum_scatter(d_down, "row", scatter_dimension=1, tiled=True),
        )
        gain_terms[layer] = jnp.stack([d_gain_one, d_gain_two])
    gain_grads = lax.psum(jnp.stack(gain_terms), "row")
    stacked = [jnp.stack([entry[member] for entry in layer_grads]) for member in range(6)]
    return (
        out_states,
        grad,
        gain_grads,
        stacked[0],
        stacked[1],
        stacked[2],
        stacked[3],
        stacked[4],
        stacked[5],
    )


def dot(a, b):
    return jnp.dot(a, b, preferred_element_type=F32)


def dot_t(a, b):
    return lax.dot_general(a, b, (((1,), (1,)), ((), ())), preferred_element_type=F32)


def t_dot(a, b):
    return lax.dot_general(a, b, (((0,), (0,)), ((), ())), preferred_element_type=F32)


def line_tables(sizes, count):
    fine = 32
    freq = rope_base ** (-(jnp.arange(HD // 2, dtype=F32) * (2.0 / HD)))
    firsts = jnp.cumsum(sizes) - sizes
    places = jnp.arange(count, dtype=jnp.int32)[:, None]
    inside = (places >= firsts[None]) & (places < (firsts + sizes)[None])
    starts = jnp.sum(jnp.where(inside, firsts[None], 0), axis=1, keepdims=True)
    points = jnp.concatenate([jnp.arange(count // fine) * fine, jnp.arange(fine), -firsts])
    angles = points.astype(F32)[:, None] * freq[None]
    cosines, sines = jnp.cos(angles), jnp.sin(angles)

    def add(one, two):
        return one[0] * two[0] - one[1] * two[1], one[1] * two[0] + one[0] * two[1]

    def pick(low, high):
        return cosines[low:high], sines[low:high]

    coarse = count // fine
    upper = [part[:, None] for part in pick(0, coarse)]
    lower = [part[None] for part in pick(coarse, coarse + fine)]
    at = [part.reshape(count, HD // 2) for part in add(upper, lower)]
    shift = [jnp.sum(jnp.where(inside[:, :, None], part[None], 0.0), axis=1) for part in pick(coarse + fine, None)]
    cosine, sine = add(at, shift)
    return starts, jnp.concatenate([cosine, cosine], axis=1), jnp.concatenate([-sine, sine], axis=1)


def per_device_line(
    hidden_states,
    out_grad,
    lengths,
    norm_gains,
    qkv_weight,
    qkv_bias,
    out_weight,
    gate_weight,
    up_weight,
    down_weight,
):
    names = Names()
    tok_row = hidden_states.shape[1]
    row_at = lax.axis_index("row")
    col_at = lax.axis_index("col")
    core = col_at % 2

    biases = jnp.zeros((LAYERS, 2, 16, HD), LOW)
    biases = lax.dynamic_update_slice(biases, qkv_bias[:, :, None], (0, 0, 0, row_at * (HD // 4)))
    gain_rows = jnp.pad(norm_gains.reshape(2 * LAYERS, D // 8), ((0, 16 - 2 * LAYERS), (0, 0)))

    def rows_load(layer):
        return (
            GatherRows(gate_weight.swapaxes(1, 2), 1, layer),
            GatherRows(up_weight.swapaxes(1, 2), 1, layer),
            GatherRows(down_weight, 1, layer),
        )

    sent = rows_load(0)
    to_chips = [HeadsToChips(qkv_weight, biases, layer) for layer in range(LAYERS)]
    slab_rows, out_rows = GatherRows(From(to_chips[0]), 0, phase=1), GatherRows(out_weight, 1, 0, phase=1)
    swap = Swap(From(slab_rows), From(out_rows), phase=2)
    sent[0].phase = 3
    states, loads = open_call(
        names, hidden_states, [*to_chips, Exchange(gain_rows, same=True), slab_rows, out_rows, swap, sent[0]]
    )
    (_,), (slab_next,), (gains,), (mine,), (out_mine,), (theirs, out_theirs), (w_gate,) = loads
    load = (mine, theirs, out_mine, out_theirs)
    gains = gains[:, : 2 * LAYERS].transpose(1, 0, 2).reshape(LAYERS, 2, D).astype(F32)
    starts, cosine, sine = line_tables(lengths[0], tok_row)

    wide = states.reshape(D, tok_row)
    residual = lax.dynamic_slice_in_dim(wide, col_at * QB, QB, 1).astype(F32).T

    def own_rows(full):
        return lax.dynamic_slice_in_dim(full, col_at * QB, QB, 0).astype(F32)

    def gain_of(layer, which):
        return gains[layer, which][None]

    saved = []
    normed = None
    for layer in range(LAYERS):
        slab = load
        sent[1].phase, sent[2].phase = 0, 3
        fixed = (residual, gain_of(layer, 1), slab, cosine, sine, starts, sent[1:])
        if layer == 0:
            mid, normed, grads_all, qkv, mixed, full_one, loads = forward_heads(
                names, out_grad, wide, gains[0, 0][:, None], *fixed, name="heads_0"
            )
        else:
            mid, normed, full_one, qkv, mixed, _, loads = forward_heads(names, normed, None, None, *fixed, name="heads_1")
        (w_up,), (w_down,) = loads
        cargo = []
        if layer == 0:
            sent = rows_load(1)
            sent[0].phase = 3
            slab_rows, out_rows = GatherRows(slab_next, 0), GatherRows(out_weight, 1, 1)
            cargo = [slab_rows, out_rows, sent[0], Swap(From(slab_rows), From(out_rows), phase=2)]
        following = gain_of(layer + 1, 0) if layer + 1 < LAYERS else None
        states, normed, full_two, gate, up, loads = forward_feed(
            names, normed, mid, following, w_gate, w_up, w_down, cargo, name=f"feed_{layer}"
        )
        saved.append((residual, full_one, slab, qkv, mixed, mid, full_two, gate, up, (w_gate, w_up, w_down)))
        residual = states
        if layer == 0:
            (mine,), (out_mine,), (w_gate,), (theirs, out_theirs) = loads
            load = (mine, theirs, out_mine, out_theirs)
    states = normed

    def own_part(full, dim):
        size = full.shape[dim] // 4
        return lax.dynamic_slice_in_dim(full, row_at * size, size, dim)

    def settle(full, dim, slots):
        return jnp.sum(slots.astype(F32), axis=0) + own_part(full, dim).astype(F32)

    def settle_heads(tiles):
        total = tiles[:, :, 0].astype(F32) + jnp.where(col_at >= 6, tiles[:, :, 1].astype(F32), 0.0)
        weight = total[:, :, : D // 8].transpose(1, 2, 0, 3).reshape(D // 4, 2 * HD)
        bias = lax.dynamic_slice_in_dim(total[:, 0, D // 8], row_at * (HD // 4), HD // 4, 1)
        return weight, bias

    grads = {}
    gain_terms = [None] * LAYERS
    grad, low = own_rows(grads_all), None
    inner = w_gate.shape[0]
    owners = []
    for layer in reversed(range(LAYERS)):
        residual_in, full_one, slab, qkv, mixed, mid, full_two, gate, up, feed_weights = saved[layer]
        last = layer == LAYERS - 1
        if last:
            cargo = [Exchange(states.T.reshape(8, D // 8, QB))]
        else:
            cargo = [ScatterRows(d_slab, 0), ScatterRows(d_out_w, 1)]
        cargo.append(ScatterRows(Inner((inner, D)), 1, phase=1))
        grad, low, d_gain_two, d_gate_w, d_up_w, d_down, loads = backward_feed(
            names,
            low,
            grads_all if last else None,
            grad,
            mid,
            gain_of(layer, 1),
            full_two,
            *feed_weights,
            gate,
            up,
            cargo,
            name=f"back_feed_{layer}",
        )
        grads["down", layer] = d_down, loads[-1][0]
        if last:
            out_states = loads[0][0]
        else:
            grads["out", layer + 1] = settle(d_out_w, 1, loads[1][0])
            owners.append(HeadsToOwners(settle(d_slab, 0, loads[0][0]).astype(LOW)))
        grad, low, d_gain_one, d_slab, d_out_w, loads = backward_heads(
            names,
            low,
            grad,
            residual_in,
            gain_of(layer, 0),
            full_one,
            layer == 0,
            slab,
            qkv,
            mixed,
            cosine,
            sine,
            starts,
            [ScatterRows(d_gate_w, 1), ScatterRows(d_up_w, 1, phase=3)],
            name=f"back_heads_{layer}",
        )
        grads["gate", layer] = d_gate_w, loads[0][0]
        grads["up", layer] = d_up_w, loads[1][0]
        gain_terms[layer] = jnp.concatenate([d_gain_one, d_gain_two], axis=0)
    gain_parts = jnp.pad(jnp.stack(gain_terms).reshape(2 * LAYERS, 8, D // 8), ((0, 8 - 2 * LAYERS), (0, 0), (0, 0)))
    for owner in owners:
        owner.phase = 3
    tiles, ((left,), (gain_all,), (out_slots,), (tiles_next,)) = close_call(
        names,
        d_slab,
        [
            Exchange(low.T.reshape(8, D // 8, QB)),
            Exchange(gain_parts.transpose(1, 0, 2), every_row=True),
            ScatterRows(d_out_w, 1, phase=3),
            *owners,
        ],
    )
    grads["qkv", 1] = settle_heads(tiles_next)
    grads["qkv", 0] = settle_heads(tiles)
    grads["out", 0] = settle(d_out_w, 1, out_slots)
    out_states = out_states.transpose(1, 0, 2).reshape(D // 8, tok_row)
    input_grad = left.transpose(1, 0, 2).reshape(D // 8, tok_row).astype(F32)
    gain_grads = jnp.sum(gain_all, axis=(0, 1))[: 2 * LAYERS].reshape(LAYERS, 2, D // 8)

    def both_layers(kind):
        return jnp.stack([grads[kind, layer] for layer in range(LAYERS)])

    kinds = ("gate", "up", "down")
    d_gate, d_up, d_down = settle_rows(
        row_at,
        [[grads[kind, layer][0] for layer in range(LAYERS)] for kind in kinds],
        [[grads[kind, layer][1] for layer in range(LAYERS)] for kind in kinds],
    )
    heads = [jnp.stack([grads["qkv", layer][i] for layer in range(LAYERS)]) for i in range(2)]
    return (
        out_states,
        input_grad,
        gain_grads,
        heads[0],
        heads[1],
        both_layers("out"),
        d_gate.swapaxes(1, 2),
        d_up.swapaxes(1, 2),
        d_down,
    )


def solution(mesh):
    placed = (
        P("col", "row"),
        P("col", "row"),
        P("row", None),
        P(None, None, "col"),
        P(None, "row", "col"),
        P(None, "col", "row"),
        P(None, "col", "row"),
        P(None, "row", "col"),
        P(None, "row", "col"),
        P(None, "col", "row"),
    )
    on_lines = mesh.shape["row"] == 4 and mesh.shape["col"] == 8
    return jax.shard_map(
        per_device_line if on_lines else per_device,
        mesh=mesh,
        in_specs=placed,
        out_specs=(
            P("col", "row"),
            P("col", "row"),
            P(None, None, "col"),
            P(None, "row", "col"),
            P(None, "col", "row"),
            P(None, "col", "row"),
            P(None, "row", "col"),
            P(None, "row", "col"),
            P(None, "col", "row"),
        ),
        check_vma=False,
    )
```

```python
from functools import partial

import jax
import jax.numpy as jnp
from jax import lax
from jax.experimental import pallas as pl
from jax.experimental.pallas import tpu as pltpu
from jax.sharding import PartitionSpec as P

D = 1536
HEADS = 12
KV_HEADS = 2
HD = 128
LAYERS = 2
SEQ_MAX = 512
QB = 128
MESH = pl.DeviceIdType.MESH
LOW = jnp.bfloat16
F32 = jnp.float32
ANY = pl.BlockSpec(memory_space=pl.ANY)
ONCHIP = pl.BlockSpec(memory_space=pltpu.VMEM)
VMEM = 62 * 2**20
HALF = 208


class Place:
    def __init__(self):
        self.r = lax.axis_index("row")
        self.k = lax.axis_index("col")
        self.z = self.k // 2
        self.c = self.k % 2

    def at(self, z, c):
        return (self.r, 2 * z + c)

    def rows(self):
        x, y = self.r % 2, self.r // 2
        return (2 * y + (1 - x), 2 * (1 - y) + x, 2 * (1 - y) + (1 - x))


def remote(src, dst, send, recv, device):
    return pltpu.make_async_remote_copy(
        src_ref=src, dst_ref=dst, send_sem=send, recv_sem=recv, device_id=device, device_id_type=MESH
    )


class Later:
    def __init__(self):
        self.todo = []

    def add(self, wait, cond=None):
        self.todo.append((wait, cond))

    def run(self):
        todo, self.todo = self.todo, []
        for wait, cond in todo:
            if cond is None:
                wait()
            else:
                pl.when(cond)(wait)


def greet(place, reach):
    barrier = pltpu.get_barrier_semaphore()

    def hail(device):
        pl.semaphore_signal(barrier, inc=1, device_id=device, device_id_type=MESH)

    if "all" in reach:
        for rr in range(4):
            for kk in range(8):
                pl.when((place.r != rr) | (place.k != kk))(partial(hail, (rr, kk)))
        pl.semaphore_wait(barrier, 31)
        return
    count = 0
    if "rows" in reach:
        for row in place.rows():
            hail((row, place.k))
        count += 3
    if "col" in reach:
        for kk in range(8):
            pl.when(place.k != kk)(partial(hail, (place.r, kk)))
        pl.semaphore_wait(barrier, count + 7)
        return
    hail(place.at(place.z, 1 - place.c))
    count += 1
    if "line" not in reach:
        pl.semaphore_wait(barrier, count)
        return
    pl.when(place.z < 3)(partial(hail, place.at(jnp.minimum(place.z + 1, 3), place.c)))
    pl.when(place.z > 0)(partial(hail, place.at(jnp.maximum(place.z - 1, 0), place.c)))
    edge = (place.z == 0) | (place.z == 3)
    pl.when(edge)(lambda: pl.semaphore_wait(barrier, count + 1))
    pl.when(jnp.logical_not(edge))(lambda: pl.semaphore_wait(barrier, count + 2))


class From:
    def __init__(self, item, at=0):
        self.item, self.at = item, at
        self.shape, self.dtype = item.outs[at].shape, item.outs[at].dtype


class Cargo:
    arrays = ()
    outs = ()
    scratch = ()
    reach = "rows"
    phase = 0
    slow = False

    def middle(self, place, ins, outs, scratch):
        pass


def part_of(ref, dim, row, size):
    cut = pl.ds(pl.multiple_of(row * size, 128 if dim else 16), size)
    return ref.at[:, cut] if dim else ref.at[cut, :]


class GatherRows(Cargo):
    def __init__(self, block, dim, layer=None, phase=0):
        self.dim, self.layer, self.phase = dim, layer, phase
        self.arrays = (block,)
        if layer is not None:
            block = jax.ShapeDtypeStruct(block.shape[1:], block.dtype)
        full = list(block.shape)
        full[dim] *= 4
        self.size = block.shape[dim]
        self.half = block.shape[0] // 32 * 16
        self.rest = block.shape[0] - self.half
        self.outs = (jax.ShapeDtypeStruct(tuple(full), block.dtype),)
        self.scratch = (
            pltpu.SemaphoreType.DMA((6,)),
            pltpu.SemaphoreType.DMA((6,)),
            pltpu.SemaphoreType.DMA((2,)),
            pltpu.VMEM(block.shape, block.dtype),
        )

    def halves(self, ref):
        return ref.at[0 : self.half, :], ref.at[self.half :, :]

    def spots(self, full, row):
        if self.dim:
            cut = pl.ds(pl.multiple_of(row * self.size, 128), self.size)
            return full.at[0 : self.half, cut], full.at[self.half :, cut]
        first = pl.multiple_of(row * self.size, 16)
        return full.at[pl.ds(first, self.half), :], full.at[pl.ds(first + self.half, self.rest), :]

    def source(self, ins):
        return ins[0] if self.layer is None else ins[0].at[self.layer]

    def copies(self, place, ins, outs, scratch):
        src, (dst,), (send, recv, *_) = self.source(ins), outs, scratch
        x, y, d = place.rows()
        block, mine = self.halves(src), self.spots(dst, place.r)
        from_x, from_y = self.spots(dst, x), self.spots(dst, y)
        out = [
            remote(block[0], mine[0], send.at[0], recv.at[0], (x, place.k)),
            remote(block[1], mine[1], send.at[1], recv.at[3], (y, place.k)),
            remote(block[1], mine[1], send.at[2], recv.at[1], (x, place.k)),
            remote(block[0], mine[0], send.at[3], recv.at[2], (y, place.k)),
        ]
        onward = [
            remote(from_x[0], from_x[0], send.at[4], recv.at[4], (y, place.k)),
            remote(from_y[1], from_y[1], send.at[5], recv.at[5], (x, place.k)),
        ]
        return out, onward

    def keep(self, place, ins, outs, scratch):
        *_, sem, buffer = scratch
        return (
            pltpu.make_async_copy(self.source(ins), buffer, sem.at[0]),
            pltpu.make_async_copy(buffer, part_of(outs[0], self.dim, place.r, self.size), sem.at[1]),
        )

    def arrived(self, place, scratch, view, sem, row):
        return remote(view, view, scratch[0].at[0], scratch[1].at[sem], (row, place.k))

    def start(self, place, ins, outs, scratch, later):
        (dst,) = outs
        out, onward = self.copies(place, ins, outs, scratch)
        for copy in out:
            copy.start()
        load, store = self.keep(place, ins, outs, scratch)
        load.start()
        later.add(store.wait)
        x, y, d = place.rows()
        from_x, from_y, from_d = self.spots(dst, x), self.spots(dst, y), self.spots(dst, d)
        for view, sem, row in ((from_x[1], 1, x), (from_y[0], 2, y), (from_d[0], 4, y), (from_d[1], 5, x)):
            later.add(self.arrived(place, scratch, view, sem, row).wait_recv)
        for copy in (*out, *onward):
            later.add(copy.wait_send)

    def middle(self, place, ins, outs, scratch):
        (dst,) = outs
        x, y, d = place.rows()
        _, onward = self.copies(place, ins, outs, scratch)
        load, store = self.keep(place, ins, outs, scratch)
        load.wait()
        store.start()
        self.arrived(place, scratch, self.spots(dst, x)[0], 0, x).wait_recv()
        onward[0].start()
        self.arrived(place, scratch, self.spots(dst, y)[1], 3, y).wait_recv()
        onward[1].start()


class ScatterRows(Cargo):
    def __init__(self, grad, dim, phase=0):
        self.dim, self.phase = dim, phase
        self.arrays = (grad,)
        part = list(grad.shape)
        part[dim] //= 4
        self.size = part[dim]
        self.half = part[0] // 32 * 16
        self.rest = part[0] - self.half
        self.outs = (jax.ShapeDtypeStruct((2, *part), grad.dtype),)
        upper, lower = pltpu.VMEM((self.half, part[1]), grad.dtype), pltpu.VMEM((self.rest, part[1]), grad.dtype)
        self.scratch = (
            *(upper, lower, lower, upper, lower, upper),
            pltpu.SemaphoreType.DMA((6,)),
            pltpu.SemaphoreType.DMA((6,)),
            pltpu.SemaphoreType.DMA((2,)),
        )

    def spots(self, full, row):
        if self.dim:
            cut = pl.ds(pl.multiple_of(row * self.size, 128), self.size)
            return full.at[0 : self.half, cut], full.at[self.half :, cut]
        first = pl.multiple_of(row * self.size, 16)
        return full.at[pl.ds(first, self.half), :], full.at[pl.ds(first + self.half, self.rest), :]

    def copies(self, place, ins, outs, scratch):
        (src,), (dst,) = ins, outs
        via_x, via_y, own_x, own_y, sum_x, sum_y, send, recv, keep = scratch
        x, y, d = place.rows()
        for_x, for_y, for_d = self.spots(src, x), self.spots(src, y), self.spots(src, d)
        slot_x = dst.at[0, 0 : self.half, :], dst.at[0, self.half :, :]
        slot_y = dst.at[1, 0 : self.half, :], dst.at[1, self.half :, :]
        first = [
            remote(for_d[0], via_x, send.at[0], recv.at[0], (x, place.k)),
            remote(for_d[1], via_y, send.at[1], recv.at[1], (y, place.k)),
            remote(for_x[0], slot_x[0], send.at[2], recv.at[2], (x, place.k)),
            remote(for_y[1], slot_y[1], send.at[3], recv.at[3], (y, place.k)),
        ]
        held = [
            pltpu.make_async_copy(for_x[1], own_x, keep.at[0]),
            pltpu.make_async_copy(for_y[0], own_y, keep.at[1]),
        ]
        last = [
            remote(sum_x, slot_x[1], send.at[4], recv.at[4], (x, place.k)),
            remote(sum_y, slot_y[0], send.at[5], recv.at[5], (y, place.k)),
        ]
        return first, held, last

    tell = None

    def start(self, place, ins, outs, scratch, later):
        if self.tell is not None:
            self.tell[0] = lambda: outs[0]
        first, held, last = self.copies(place, ins, outs, scratch)
        for copy in (*first, *held):
            copy.start()
        for copy in (*first, *last):
            later.add(copy.wait_send)
        for copy in (*first[2:], *last):
            later.add(copy.wait_recv)

    def middle(self, place, ins, outs, scratch):
        via_x, via_y, own_x, own_y, sum_x, sum_y, *_ = scratch
        first, held, last = self.copies(place, ins, outs, scratch)
        held[0].wait()
        first[1].wait_recv()
        add_into(sum_x, [own_x, via_y])
        last[0].start()
        held[1].wait()
        first[0].wait_recv()
        add_into(sum_y, [own_y, via_x])
        last[1].start()


class Swap(Cargo):
    reach = "line"

    def __init__(self, *arrays, phase=0):
        self.arrays, self.phase = arrays, phase
        self.outs = tuple(jax.ShapeDtypeStruct(a.shape, a.dtype) for a in arrays)
        self.scratch = (pltpu.SemaphoreType.DMA((len(arrays),)), pltpu.SemaphoreType.DMA((len(arrays),)))

    def start(self, place, ins, outs, scratch, later):
        send, recv = scratch
        for i, (src, dst) in enumerate(zip(ins, outs)):
            copy = remote(src, dst, send.at[i], recv.at[i], place.at(place.z, 1 - place.c))
            copy.start()
            later.add(copy.wait)


def tile_owner(z, t):
    if t < 3:
        head = 3 * z + t
        return head // 2, head % 2
    return 3 + t, z // 2


class HeadsToChips(Cargo):
    reach = "col"

    def __init__(self, weight, biases, layer):
        self.layer = layer
        self.phase = 0 if layer == 0 else 3
        self.arrays = (weight, biases)
        self.outs = (jax.ShapeDtypeStruct((HALF, 5 * HD), LOW),)
        self.scratch = (
            pltpu.SemaphoreType.DMA((2, 2, 2, 2)),
            pltpu.SemaphoreType.DMA((5, 2)),
            pltpu.VMEM(weight.shape[1:], weight.dtype),
            pltpu.VMEM(biases.shape[1:], biases.dtype),
            pltpu.SemaphoreType.DMA((2,)),
        )

    def start(self, place, ins, outs, scratch, later):
        (slab,), (send, recv, weight, biases, load_sem) = outs, scratch
        for load in copy_in([(ins[0].at[self.layer], weight), (ins[1].at[self.layer], biases)], load_sem):
            load.wait()
        r, k, z, c = place.r, place.k, place.z, place.c
        query = k < 6
        rows = D // 8
        for second in range(2):
            for i in range(2):
                head = 2 * k + i
                chip = jnp.where(query, head // 3, 2 * i + second)
                t = jnp.where(query, head % 3, k - 3)
                cut = pl.ds(pl.multiple_of(t * HD, HD), HD)
                spots = slab.at[0:rows, cut], slab.at[rows:HALF, cut]
                for core in range(2):
                    here = k == 2 * chip + core
                    away = jnp.logical_not(here)
                    if second == 1:
                        here, away = here & (k >= 6), away & (k >= 6)
                    views = (
                        weight.at[core * rows : (core + 1) * rows, i * HD : (i + 1) * HD],
                        biases.at[i],
                    )
                    for part in range(2):
                        sem = send.at[i, second, core, part]
                        copy = remote(views[part], spots[part], sem, recv.at[t, part], (r, 2 * chip + core))
                        pl.when(away)(copy.start)
                        later.add(copy.wait_send, away)
                        keep = pltpu.make_async_copy(views[part], spots[part], sem)
                        pl.when(here)(keep.start)
                        later.add(keep.wait, here)
        for t in range(5):
            owner, _ = tile_owner(z, t)
            cut = slice(t * HD, (t + 1) * HD)
            for part, spot in enumerate((slab.at[0:rows, cut], slab.at[rows:HALF, cut])):
                came = remote(spot, spot, send.at[0, 0, 0, 0], recv.at[t, part], (r, owner))
                later.add(came.wait_recv, k != owner)


class HeadsToOwners(Cargo):
    reach = "col"

    def __init__(self, slab):
        self.arrays = (slab,)
        self.outs = (jax.ShapeDtypeStruct((2, 2, 2, HALF, HD), LOW),)
        self.scratch = (pltpu.SemaphoreType.DMA((5,)), pltpu.SemaphoreType.DMA((2, 2, 2)))

    def start(self, place, ins, outs, scratch, later):
        (slab,), (tiles,), (send, recv) = ins, outs, scratch
        r, k, z, c = place.r, place.k, place.z, place.c
        for t in range(5):
            owner, i = tile_owner(z, t)
            which = z % 2 if t >= 3 else 0
            view, spot = slab.at[:, t * HD : (t + 1) * HD], tiles.at[i, c, which]
            here = k == owner
            copy = remote(view, spot, send.at[t], recv.at[i, c, which], (r, owner))
            pl.when(jnp.logical_not(here))(copy.start)
            later.add(copy.wait_send, jnp.logical_not(here))
            keep = pltpu.make_async_copy(view, spot, send.at[t])
            pl.when(here)(keep.start)
            later.add(keep.wait, here)
        for i in range(2):
            for which in range(2):
                chip = jnp.where(k < 6, (2 * k + i) // 3, 2 * i + which)
                for core in range(2):
                    wanted = k != 2 * chip + core
                    if which == 1:
                        wanted = wanted & (k >= 6)
                    came = remote(
                        slab.at[:, 0:HD],
                        tiles.at[i, core, which],
                        send.at[0],
                        recv.at[i, core, which],
                        (r, 2 * chip + core),
                    )
                    later.add(came.wait_recv, wanted)


class Exchange(Cargo):
    def __init__(self, chunks, every_row=False, same=False):
        self.arrays = (chunks,)
        self.same = same
        self.phase = 3
        self.rows_too = every_row
        self.reach = "all" if every_row else "col"
        lead = (4,) if every_row else (8,) if same else ()
        self.outs = (jax.ShapeDtypeStruct((*lead, *chunks.shape), chunks.dtype),)
        self.scratch = (pltpu.SemaphoreType.DMA((4, 8)), pltpu.SemaphoreType.DMA((4, 8)))

    def start(self, place, ins, outs, sems, later):
        (src,), (dst,), (send, recv) = ins, outs, sems
        r, k = place.r, place.k
        for rr in range(4) if self.rows_too else (None,):
            to_row = r if rr is None else rr
            for kk in range(8):
                here = (k == kk) if rr is None else (k == kk) & (r == rr)
                mine = dst.at[k] if rr is None else dst.at[r, k]
                theirs = dst.at[kk] if rr is None else dst.at[rr, kk]
                at = 0 if rr is None else rr
                my_at = 0 if rr is None else r
                part = src if self.same else src.at[kk]
                copy = remote(part, mine, send.at[at, kk], recv.at[my_at, k], (to_row, kk))
                pl.when(jnp.logical_not(here))(copy.start)
                later.add(copy.wait_send, jnp.logical_not(here))
                came = remote(part, theirs, send.at[at, kk], recv.at[at, kk], (to_row, kk))
                later.add(came.wait_recv, jnp.logical_not(here))
                keep = pltpu.make_async_copy(part, mine, send.at[at, kk])
                pl.when(here)(keep.start)
                later.add(keep.wait, here)


def add_into(dst, views):
    rows = dst.shape[0]

    def step(i, carry):
        cut = pl.ds(pl.multiple_of(i * 16, 16), 16)
        total = views[0][cut, :].astype(F32)
        for view in views[1:]:
            total = total + view[cut, :].astype(F32)
        dst[cut, :] = total.astype(dst.dtype)
        return carry

    lax.fori_loop(0, rows // 16, step, 0)


SUB = 4
LAG = 2


class Reduce:
    @staticmethod
    def scratch(tokens, width):
        return [
            pltpu.VMEM((4, tokens, width), LOW),
            pltpu.VMEM((2, 4, tokens, width), LOW),
            pltpu.VMEM((4, tokens, width), LOW),
            pltpu.SemaphoreType.DMA((4,)),
            pltpu.SemaphoreType.DMA((4,)),
            pltpu.SemaphoreType.DMA((4, SUB)),
            pltpu.SemaphoreType.DMA((2, 4, SUB)),
        ]

    def __init__(self, place, part, out, scratch, both=True, far=False):
        self.place, self.part, self.out, self.both, self.far = place, part, out, both, far
        self.from_p, self.moved, self.held, self.send_p, self.recv_p, self.send, self.recv = scratch
        z, c = place.z, place.c
        self.edge = (z == 0) | (z == 3)
        self.mid = jnp.logical_not(self.edge)
        self.right, self.left = place.at(jnp.minimum(z + 1, 3), c), place.at(jnp.maximum(z - 1, 0), c)
        self.size = part.shape[1] // SUB

    def pair(self, j):
        place = self.place
        other = self.part.at[2 * j + 1 - place.c]
        return remote(other, self.from_p.at[j], self.send_p.at[j], self.recv_p.at[j], place.at(place.z, 1 - place.c))

    def piece(self, j, sub, way):
        rows = rows_of(sub * self.size, self.size)
        column = jnp.where(way == 0, self.right[1], self.left[1])
        return remote(
            self.held.at[j, rows, :],
            self.moved.at[way, j, rows, :],
            self.send.at[j, sub],
            self.recv.at[way, j, sub],
            (self.place.r, column),
        )

    def terms(self, j):
        if self.both:
            return [self.part.at[2 * j + self.place.c], self.from_p.at[j]]
        return [self.part.at[j]]

    def made(self, j):
        z = self.place.z
        if self.both:
            self.pair(j).start()

        @pl.when(self.edge & (j != z))
        def _():
            if self.both:
                self.pair(j).wait_recv()
            add_into(self.held.at[j], self.terms(j))
            for sub in range(SUB):
                self.piece(j, sub, jnp.where(z == 0, 0, 1)).start()

    def finish(self, later, early=None, late=None):
        z = self.place.z
        way = jnp.where(z == 1, 0, 1)
        near, far, back = jnp.where(z == 1, 2, 1), jnp.where(z == 1, 3, 0), jnp.where(z == 1, 0, 3)
        first, second = (far, near) if self.far else (near, far)

        def step(j, sub, way):
            if self.both:
                pl.when(sub == 0)(lambda: self.pair(j).wait_recv())
            copy = self.piece(j, sub, way)
            copy.wait_recv()
            rows = rows_of(sub * self.size, self.size)
            views = [view.at[rows, :] for view in (*self.terms(j), self.moved.at[way, j])]
            add_into(self.held.at[j].at[rows, :], views)
            copy.start()

        def one(sub, carry):
            pl.when(self.mid)(lambda: step(first, sub, way))
            if early is not None:
                early(sub)
            return carry

        def two(sub, carry):
            pl.when(self.mid)(lambda: step(second, sub, way))
            pl.when(self.mid & (sub >= LAG))(lambda: step(back, sub - LAG, 1 - way))
            if late is not None:
                late(sub)
            return carry

        def three(sub, carry):
            pl.when(self.mid)(lambda: step(back, sub, 1 - way))
            return carry

        lax.fori_loop(0, SUB, one, 0)
        lax.fori_loop(0, SUB, two, 0)
        lax.fori_loop(SUB - LAG, SUB, three, 0)
        if self.both:
            self.pair(z).wait_recv()

        def came(way):
            for sub in range(SUB):
                self.piece(z, sub, way).wait_recv()

        views = self.terms(z)

        @pl.when(self.edge)
        def _():
            way = jnp.where(z == 0, 1, 0)
            came(way)
            add_into(self.out, [*views, self.moved.at[way, z]])

        @pl.when(self.mid)
        def _():
            came(0)
            came(1)
            add_into(self.out, [*views, self.moved.at[0, z], self.moved.at[1, z]])

        for j in range(4):
            if self.both:
                later.add(self.pair(j).wait_send)
            for sub in range(SUB):
                later.add(self.piece(j, sub, 0).wait_send, z != j)


def far_first(place, p):
    z = place.z
    edge = jnp.where(z == 0, 3 - p, p)
    mid = jnp.where(p == 0, jnp.where(z == 1, 3, 0), jnp.where(p == 1, jnp.where(z == 1, 2, 1), jnp.where(p == 2, jnp.where(z == 1, 0, 3), z)))
    return jnp.where((z == 0) | (z == 3), edge, mid)


class Names:
    def __init__(self):
        self.next = 0

    def take(self):
        self.next += 1
        return self.next - 1


class Inner:
    def __init__(self, shape, dtype=LOW):
        self.shape, self.dtype = shape, dtype


def given_arrays(item):
    return [a for a in item.arrays if not isinstance(a, (From, Inner))]


def carry_kernel(body, reach, n_in, n_out, n_scratch, cargo, *refs):
    refs = list(refs)

    def pop(n):
        taken = refs[:n]
        del refs[:n]
        return taken

    ins = pop(n_in)
    given = [pop(len(given_arrays(item))) for item in cargo]
    outs = pop(n_out)
    made = {item: pop(len(item.outs)) for item in cargo}
    scratch = pop(n_scratch)
    held = {item: pop(len(item.scratch)) for item in cargo}
    taken = {
        item: [
            made[a.item][a.at] if isinstance(a, From) else a if isinstance(a, Inner) else mine.pop(0)
            for a in item.arrays
        ]
        for item, mine in zip(cargo, given)
    }
    place = Place()
    later = Later()
    owed = [Later() for _ in range(4)]
    greet(place, {reach, *(item.reach for item in cargo)})

    def start(phase, *inner):
        inner = list(inner)
        mine = [item for item in cargo if item.phase == phase]
        for before in sorted({a.item.phase for item in mine for a in item.arrays if isinstance(a, From)}):
            owed[before].run()
        for item in mine:
            taken[item] = [inner.pop(0) if isinstance(a, Inner) else a for a in taken[item]]
            item.start(place, taken[item], made[item], held[item], owed[phase])

    start.wait = lambda phase: owed[phase].run()

    def middle(phase=0):
        for item in cargo:
            if item.phase == phase:
                item.middle(place, taken[item], made[item], held[item])

    body(place, ins, outs, scratch, later, middle, start)
    later.run()
    for waits in owed:
        waits.run()


def carry_call(names, body, reach, arrays, in_specs, outs, out_specs, scratch, cargo, name=None):
    given = [a for item in cargo for a in given_arrays(item)]
    call = pl.pallas_call(
        partial(carry_kernel, body, reach, len(arrays), len(outs), len(scratch), cargo),
        out_shape=[*outs, *(o for item in cargo for o in item.outs)],
        in_specs=[*in_specs, *(ANY for _ in given)],
        out_specs=[*out_specs, *(ANY for item in cargo for _ in item.outs)],
        scratch_shapes=[*scratch, *(s for item in cargo for s in item.scratch)],
        compiler_params=pltpu.CompilerParams(
            collective_id=names.take(), has_side_effects=True, vmem_limit_bytes=VMEM
        ),
        name=name,
    )
    results = list(call(*arrays, *given))
    main = results[: len(outs)]
    rest = results[len(outs) :]
    loads = []
    for item in cargo:
        loads.append(rest[: len(item.outs)])
        rest = rest[len(item.outs) :]
    return main, loads


class Gather:
    scratch = (
        pltpu.SemaphoreType.DMA((4, 2)),
        pltpu.SemaphoreType.DMA((4, 2)),
        pltpu.SemaphoreType.DMA((8, 2)),
        pltpu.SemaphoreType.DMA((8, 2)),
        pltpu.SemaphoreType.DMA((1,)),
    )

    def __init__(self, place, block, full, sems, both=True):
        self.place, self.block, self.full, self.both = place, block, full, both
        self.send_r, self.send_l, self.send_p, self.recv, self.keep = sems
        self.size = block.shape[0] // 2

    def spot(self, zz, c):
        return self.full.at[2 * zz + c] if self.both else self.full.at[zz]

    def copies(self, src, zz, t, way, half):
        z, c = self.place.z, self.place.c
        rows = pl.ds(half * self.size, self.size)
        src, spot, sem = src.at[rows, :], self.spot(zz, c).at[rows, :], self.recv.at[2 * zz + c, half]
        right = remote(src, spot, self.send_r.at[t, half], sem, self.place.at(jnp.minimum(z + 1, 3), c))
        left = remote(src, spot, self.send_l.at[t, half], sem, self.place.at(jnp.maximum(z - 1, 0), c))
        partner = remote(src, spot, self.send_p.at[2 * t + way, half], sem, self.place.at(z, 1 - c))
        return right, left, partner

    def start(self, later):
        z, c = self.place.z, self.place.c
        for half in range(2):
            right, left, partner = self.copies(self.block, z, 0, 0, half)
            pl.when(z < 3)(right.start)
            pl.when(z > 0)(left.start)
            later.add(right.wait_send, z < 3)
            later.add(left.wait_send, z > 0)
            if self.both:
                partner.start()
                later.add(partner.wait_send)
        keep = pltpu.make_async_copy(self.block, self.spot(z, c), self.keep.at[0])
        keep.start()
        keep.wait()
        for t in range(1, 4):
            for way in (0, 1):
                for half in range(2):
                    valid, onward, may, partner = self.step(t, way, half)
                    later.add(onward.wait_send, valid & may)
                    if self.both:
                        later.add(partner.wait_send, valid)

    def step(self, t, way, half):
        z = self.place.z
        there = z + (2 * way - 1) * t
        zz = jnp.clip(there, 0, 3)
        right, left, partner = self.copies(self.spot(zz, self.place.c), zz, t, way, half)
        onward, may = (left, z > 0) if way else (right, z < 3)
        return (there >= 0) & (there <= 3), onward, may, partner

    def pass_on(self, t):
        for half in range(2):
            for way in (0, 1):
                valid, onward, may, partner = self.step(t, way, half)

                @pl.when(valid)
                def _(onward=onward, may=may, partner=partner):
                    onward.wait_recv()
                    pl.when(may)(onward.start)
                    if self.both:
                        partner.start()

    def from_partner(self, zz):
        c = self.place.c
        for half in range(2):
            spot = self.spot(zz, 1 - c).at[pl.ds(half * self.size, self.size), :]
            recv = self.recv.at[2 * zz + 1 - c, half]
            yield remote(spot, spot, self.send_p.at[0, half], recv, self.place.at(self.place.z, 1 - c)).wait_recv

    def order(self, p):
        z = self.place.z
        second = jnp.where(z == 0, 1, z - 1)
        third = jnp.where(z == 0, 2, jnp.where(z == 3, 1, z + 1))
        fourth = jnp.where(z <= 1, 3, 0)
        return jnp.where(p == 0, z, jnp.where(p == 1, second, jnp.where(p == 2, third, fourth)))

    def chunk(self, p):
        z = self.place.z
        edge = (z == 0) | (z == 3)
        t = jnp.where(edge, p, (p + 1) // 2)
        pl.when((p >= 1) & (edge | (p != 2)))(lambda: self.pass_on(t))
        j = self.order(p)
        if self.both:
            for wait in self.from_partner(j):
                wait()
        return j


def tiles(count, work, size=256):
    def tile(i, carry):
        work(rows_of(i * size, size))
        return carry

    lax.fori_loop(0, count // size, tile, 0)
    if count % size:
        work(pl.ds(count // size * size, count % size))


def forward_feed(names, block, residual, gain, w_gate, w_up, w_down, cargo, name):
    tokens, width = block.shape
    inner = w_gate.shape[0]
    normed = gain is not None

    def body(place, ins, outs, scratch, later, middle, start):
        block_ref, residual_ref, gain_ref, gate_hbm, up_hbm, down_hbm = ins
        states_out, normed_out, full_out, gate_out, up_out = outs
        n = len(Gather.scratch)
        gather_sems, scratch = scratch[:n], scratch[n:]
        full, part, gate_w, up_w, down_w, gates, ups, load_sem, keep_sem, total, hidden = scratch[:11]
        reduce = Reduce(place, part, total, scratch[11:])
        gather = Gather(place, block_ref, full, gather_sems)
        loads = [
            pltpu.make_async_copy(src, dst, load_sem.at[i])
            for i, (src, dst) in enumerate(((gate_hbm, gate_w), (up_hbm, up_w), (down_hbm, down_w)))
        ]
        for load in loads:
            load.start()
        gather.start(later)
        start(0)
        start(3)
        for load in loads:
            load.wait()

        def keep(j):
            rows = pl.ds(pl.multiple_of(2 * tokens * j, 2 * tokens), 2 * tokens)
            return [
                pltpu.make_async_copy(full.at[pl.ds(2 * j, 2)], full_out.at[pl.ds(2 * j, 2)], keep_sem.at[0, j]),
                pltpu.make_async_copy(gates.at[rows, :], gate_out.at[rows, :], keep_sem.at[1, j]),
                pltpu.make_async_copy(ups.at[rows, :], up_out.at[rows, :], keep_sem.at[2, j]),
            ]

        def step(p, carry):
            j = gather.chunk(p)
            pl.when(p == 2)(middle)
            acts = full[pl.ds(2 * j, 2)].reshape(2 * tokens, width)
            rows = pl.ds(pl.multiple_of(2 * tokens * j, 2 * tokens), 2 * tokens)

            def columns(cut):
                gate = dot_t(acts, gate_w[cut, :])
                up = dot_t(acts, up_w[cut, :])
                gates[rows, cut] = gate.astype(LOW)
                ups[rows, cut] = up.astype(LOW)
                hidden[:, cut] = (gate * jax.nn.sigmoid(gate) * up).astype(LOW)

            tiles(inner, columns)

            def outputs(cut):
                sums = dot(hidden[...], down_w[:, cut]).astype(LOW)
                part[pl.ds(2 * j, 2), :, cut] = sums.reshape(2, tokens, cut.size)

            tiles(width, outputs, 512)
            reduce.made(j)
            for copy in keep(j):
                copy.start()
            return carry

        lax.fori_loop(0, 4, step, 0)
        start(1)
        start(2)
        reduce.finish(later, early=lambda i: pl.when(i == 0)(lambda: middle(3)))
        after_forward(total, residual_ref, gain_ref if normed else None, states_out, normed_out)
        for j in range(4):
            for copy in keep(j):
                copy.wait()

    (states, low, full, gate, up), loads = carry_call(
        names,
        body,
        "line",
        [block, residual, gain if normed else jnp.ones((1, width), F32), w_gate, w_up, w_down],
        [ONCHIP, ONCHIP, ONCHIP, ANY, ANY, ANY],
        [
            jax.ShapeDtypeStruct((tokens, width), F32),
            jax.ShapeDtypeStruct((tokens, width), LOW),
            jax.ShapeDtypeStruct((8, tokens, width), LOW),
            jax.ShapeDtypeStruct((8 * tokens, inner), LOW),
            jax.ShapeDtypeStruct((8 * tokens, inner), LOW),
        ],
        [ONCHIP, ONCHIP, ANY, ANY, ANY],
        [
            *Gather.scratch,
            pltpu.VMEM((8, tokens, width), LOW),
            pltpu.VMEM((8, tokens, width), LOW),
            pltpu.VMEM(w_gate.shape, LOW),
            pltpu.VMEM(w_up.shape, LOW),
            pltpu.VMEM(w_down.shape, LOW),
            pltpu.VMEM((8 * tokens, inner), LOW),
            pltpu.VMEM((8 * tokens, inner), LOW),
            pltpu.SemaphoreType.DMA((3,)),
            pltpu.SemaphoreType.DMA((3, 4)),
            pltpu.VMEM((tokens, width), F32),
            pltpu.VMEM((2 * tokens, inner), LOW),
            *Reduce.scratch(tokens, width),
        ],
        cargo,
        name=name,
    )
    return states, low, full.reshape(8 * tokens, width), gate, up, loads


def rows_of(first, count):
    return pl.ds(pl.multiple_of(first, count), count)


def copy_in(pairs, sem):
    copies = [pltpu.make_async_copy(src, dst, sem.at[i]) for i, (src, dst) in enumerate(pairs)]
    for copy in copies:
        copy.start()
    return copies


def open_call(names, shard, cargo):
    def body(place, ins, outs, scratch, later, middle, start):
        gather = Gather(place, ins[0], outs[0], scratch)
        start(0)
        gather.start(later)
        start(3)
        start(1)
        gather.pass_on(1)
        middle(1)
        gather.pass_on(2)
        middle(3)
        start(2)
        gather.pass_on(3)
        for zz in range(4):
            for wait in gather.from_partner(zz):
                later.add(wait)

    (full,), loads = carry_call(
        names,
        body,
        "line",
        [shard],
        [ANY],
        [jax.ShapeDtypeStruct((8, *shard.shape), shard.dtype)],
        [ANY],
        list(Gather.scratch),
        cargo,
        name="open",
    )
    return full, loads


def close_call(names, slab, cargo):
    def body(place, ins, outs, scratch, later, middle, start):
        slab_ref = ins[0]
        own, came, total, sem = scratch
        start(0)
        start(3)
        middle(0)
        middle(3)
        load = pltpu.make_async_copy(slab_ref.at[rows_of(place.r * HALF, HALF), :], own, sem.at[0])
        load.start()
        start.wait(0)
        fetch = pltpu.make_async_copy(cargo_refs[0](), came, sem.at[1])
        fetch.start()
        load.wait()
        fetch.wait()
        add_into(total, [own, came.at[0], came.at[1]])
        start(1, total)

    cargo_refs = [None]
    rows, owners = ScatterRows(slab, 0), HeadsToOwners(Inner((HALF, 5 * HD)))
    owners.phase = 1
    rows.tell = cargo_refs
    _, loads = carry_call(
        names,
        body,
        "col",
        [slab],
        [ANY],
        [],
        [],
        [
            pltpu.VMEM((HALF, 5 * HD), LOW),
            pltpu.VMEM((2, HALF, 5 * HD), LOW),
            pltpu.VMEM((HALF, 5 * HD), LOW),
            pltpu.SemaphoreType.DMA((2,)),
        ],
        [rows, owners, *cargo],
        name="close",
    )
    return loads[1][0], loads[2:]


def after_forward(sums, residual, gain, states, normed):
    def step(i, carry):
        rows = rows_of(i * 16, 16)
        now = residual[rows, :] + sums[rows, :]
        states[rows, :] = now
        if gain is not None:
            now = now * lax.rsqrt(jnp.mean(now * now, axis=1, keepdims=True) + eps_norm) * gain[...]
        normed[rows, :] = now.astype(LOW)
        return carry

    lax.fori_loop(0, sums.shape[0] // 16, step, 0)


def after_backward(sums, grad, residual, gain, grad_out, low_out, gain_out):
    def step(i, total):
        rows = rows_of(i * 16, 16)
        d_normed, now = sums[rows, :], residual[rows, :]
        scale = lax.rsqrt(jnp.mean(now * now, axis=1, keepdims=True) + eps_norm)
        weighted = d_normed * gain[...]
        inner = jnp.sum(weighted * now, axis=1, keepdims=True)
        out = grad[rows, :] + (weighted * scale - now * (scale * scale * scale) * inner / D)
        grad_out[rows, :] = out
        low_out[rows, :] = out.astype(LOW)
        return total + jnp.sum(d_normed * now * scale, axis=0, keepdims=True)

    gain_out[...] = lax.fori_loop(0, sums.shape[0] // 16, step, jnp.zeros((1, D), F32))


class Slab:
    scratch = (
        pltpu.VMEM((D, 5 * HD), LOW),
        pltpu.VMEM((3 * HD, D), LOW),
        pltpu.VMEM((4, 16, 5 * HD), LOW),
        pltpu.SemaphoreType.DMA((2, 5)),
        pltpu.SemaphoreType.DMA((4,)),
    )

    def __init__(self, place, refs, scratch):
        self.place = place
        self.mine, self.theirs, self.out_mine, self.out_theirs = refs
        self.qkv, self.out, self.tails, self.sems, self.tail_sems = scratch

    def copies(self, half, mine):
        source, out = (self.mine, self.out_mine) if mine else (self.theirs, self.out_theirs)
        sem = self.sems.at[half]
        rows = D // 8
        for row in range(4):
            spot = self.qkv.at[(2 * row + half) * rows : (2 * row + half + 1) * rows, :]
            yield pltpu.make_async_copy(source.at[row * HALF : row * HALF + rows, :], spot, sem.at[row])
        yield pltpu.make_async_copy(out, self.out.at[half * rows : (half + 1) * rows, :], sem.at[4])
        if half == 0:
            for row in range(4):
                tail = source.at[row * HALF + rows : (row + 1) * HALF, :]
                yield pltpu.make_async_copy(tail, self.tails.at[row], self.tail_sems.at[row])

    def start(self):
        for half in range(2):
            for mine in (True, False):

                @pl.when((self.place.c == half) == mine)
                def _(half=half, mine=mine):
                    for copy in self.copies(half, mine):
                        copy.start()

    def wait(self):
        for half in range(2):
            for copy in self.copies(half, True):
                copy.wait()

    def bias(self):
        return jnp.sum(self.tails[:, 0, :].astype(F32), axis=0, keepdims=True)


def after_forward(sums, residual, gain, states, normed):
    def step(i, carry):
        rows = rows_of(i * 16, 16)
        now = residual[rows, :] + sums[rows, :]
        states[rows, :] = now
        if gain is not None:
            now = now * lax.rsqrt(jnp.mean(now * now, axis=1, keepdims=True) + eps_norm) * gain[...]
        normed[rows, :] = now.astype(LOW)
        return carry

    lax.fori_loop(0, sums.shape[0] // 16, step, 0)


def after_backward(sums, grad, residual, gain, grad_out, low_out, gain_out):
    def step(i, total):
        rows = rows_of(i * 16, 16)
        d_normed, now = sums[rows, :], residual[rows, :]
        scale = lax.rsqrt(jnp.mean(now * now, axis=1, keepdims=True) + eps_norm)
        weighted = d_normed * gain[...]
        inner = jnp.sum(weighted * now, axis=1, keepdims=True)
        out = grad[rows, :] + (weighted * scale - now * (scale * scale * scale) * inner / D)
        grad_out[rows, :] = out
        low_out[rows, :] = out.astype(LOW)
        return total + jnp.sum(d_normed * now * scale, axis=0, keepdims=True)

    gain_out[...] = lax.fori_loop(0, sums.shape[0] // 16, step, jnp.zeros((1, D), F32))


class Slab:
    scratch = (
        pltpu.VMEM((D, 5 * HD), LOW),
        pltpu.VMEM((3 * HD, D), LOW),
        pltpu.VMEM((4, 16, 5 * HD), LOW),
        pltpu.SemaphoreType.DMA((2, 5)),
        pltpu.SemaphoreType.DMA((4,)),
    )

    def __init__(self, place, refs, scratch):
        self.place = place
        self.mine, self.theirs, self.out_mine, self.out_theirs = refs
        self.qkv, self.out, self.tails, self.sems, self.tail_sems = scratch

    def copies(self, half, mine):
        source, out = (self.mine, self.out_mine) if mine else (self.theirs, self.out_theirs)
        sem = self.sems.at[half]
        rows = D // 8
        for row in range(4):
            spot = self.qkv.at[(2 * row + half) * rows : (2 * row + half + 1) * rows, :]
            yield pltpu.make_async_copy(source.at[row * HALF : row * HALF + rows, :], spot, sem.at[row])
        yield pltpu.make_async_copy(out, self.out.at[half * rows : (half + 1) * rows, :], sem.at[4])
        if half == 0:
            for row in range(4):
                tail = source.at[row * HALF + rows : (row + 1) * HALF, :]
                yield pltpu.make_async_copy(tail, self.tails.at[row], self.tail_sems.at[row])

    def start(self):
        for half in range(2):
            for mine in (True, False):

                @pl.when((self.place.c == half) == mine)
                def _(half=half, mine=mine):
                    for copy in self.copies(half, mine):
                        copy.start()

    def wait(self):
        for half in range(2):
            for copy in self.copies(half, True):
                copy.wait()

    def bias(self):
        return jnp.sum(self.tails[:, 0, :].astype(F32), axis=0, keepdims=True)


def heads_of(ref, rows):
    return jnp.concatenate([ref[rows, h * HD : (h + 1) * HD] for h in range(3)], axis=0)


def block_window(b):
    first = jnp.maximum(b - SEQ_MAX // QB, 0) * QB
    return rows_of(b * QB, QB), pl.ds(pl.multiple_of(first, QB), QB + SEQ_MAX), first


def block_probs(queries, keys, starts, b):
    reach = QB + SEQ_MAX
    rows, _, first = block_window(b)
    scores = (dot_t(queries, keys) * HD ** (-0.5)).reshape(-1, QB, reach)
    key_at = first + lax.broadcasted_iota(jnp.int32, (QB, reach), 1)
    query_at = b * QB + lax.broadcasted_iota(jnp.int32, (QB, reach), 0)
    allowed = (key_at >= starts[rows, :]) & (key_at <= query_at)
    masked = jnp.where(allowed[None], scores, neg_fill)
    lifted = jnp.exp(masked - jnp.max(masked, axis=-1, keepdims=True))
    probs = lifted * (1.0 / jnp.sum(lifted, axis=-1, keepdims=True))
    return probs.reshape(-1, reach)


def roll_half(values):
    return pltpu.roll(values, HD // 2, 1)


def forward_heads(names, block, wide, gain, residual, gain_two, slab, cosine, sine, starts, cargo, name):
    tokens, width = QB, D
    count = 8 * QB
    apart = wide is not None

    def body(place, ins, outs, scratch, later, middle, start):
        ins = list(ins)
        block_ref = ins.pop(0)
        if apart:
            wide_hbm, gain_ref = ins.pop(0), ins.pop(0)
        residual_ref, two_ref, cos_ref, sin_ref, starts_ref, *slab_refs = ins
        states_out, normed_out, full_out, qkv_out, mixed_out = outs[:5]
        scratch = list(scratch)
        gather_sems = [scratch.pop(0) for _ in Gather.scratch]
        weights = Slab(place, slab_refs, [scratch.pop(0) for _ in Slab.scratch])
        full, acts, flat, part, qkv, mixed, load_sem, keep_sem, total = scratch[:9]
        reduce = Reduce(place, part, total, scratch[9:], both=False, far=True)
        weights.start()
        loads = copy_in([(wide_hbm, acts)] if apart else [], load_sem)
        gather = Gather(place, block_ref, full, gather_sems)
        gather.start(later)
        start(0)
        start(3)
        for load in loads:
            load.wait()
        weights.wait()
        bias = weights.bias()

        def keep(j):
            if apart:
                rows = rows_of(j * 2 * QB, 2 * QB)
                return pltpu.make_async_copy(flat.at[rows, :], full_out.at[rows, :], keep_sem.at[j])
            return pltpu.make_async_copy(full.at[pl.ds(2 * j, 2)], full_out.at[pl.ds(2 * j, 2)], keep_sem.at[j])

        def step(p, carry):
            if apart:
                j = gather.order(p)
            else:
                j = gather.chunk(p)
                pl.when(p == 2)(middle)
            rows = rows_of(j * 2 * QB, 2 * QB)
            if apart:
                chunk = acts[:, rows].astype(F32)
                scale = lax.rsqrt(jnp.mean(chunk * chunk, axis=0, keepdims=True) + eps_norm)
                chunk = (chunk * scale * gain_ref[...]).astype(LOW)
                acts[:, rows] = chunk
                raw = t_dot(chunk, weights.qkv[...]) + bias
            else:
                keep(j).start()
                raw = jnp.dot(full[pl.ds(2 * j, 2)].reshape(2 * tokens, width), weights.qkv[...], preferred_element_type=F32)
                raw = raw + bias
            cos, sin = cos_ref[rows, :], sin_ref[rows, :]
            for t in range(5):
                head = raw[:, t * HD : (t + 1) * HD]
                if t < 4:
                    head = head * cos + roll_half(head) * sin
                qkv[rows, t * HD : (t + 1) * HD] = head.astype(LOW)
            return carry

        lax.fori_loop(0, 4, step, 0)
        start(1)

        def attend(p, carry):
            j = far_first(place, p)
            b = 2 * j + place.c
            rows, window, _ = block_window(b)
            mine = rows_of(j * QB, QB)

            def head(h, carry):
                cut = rows_of(h * HD, HD)
                probs = block_probs(qkv[rows, cut], qkv[window, 3 * HD : 4 * HD], starts_ref, b)
                mixed[mine, cut] = dot(probs.astype(LOW), qkv[window, 4 * HD : 5 * HD]).astype(LOW)
                return carry

            lax.fori_loop(0, 3, head, 0)
            part[j] = dot(mixed[mine, :], weights.out[...]).astype(LOW)
            reduce.made(j)
            return carry

        lax.fori_loop(0, 4, attend, 0)
        saves = copy_in([(qkv, qkv_out), (mixed, mixed_out)], load_sem)
        if apart:
            saves.append(pltpu.make_async_copy(acts, outs[5], load_sem.at[2]))
            saves[-1].start()

        def early(i):
            if apart:
                pl.when(i == 0)(lambda: gather.pass_on(1))
            else:
                pl.when(i == 0)(lambda: middle(3))

        def late(i):
            if apart:

                @pl.when(i == 0)
                def _():
                    gather.pass_on(2)
                    middle(0)

                @pl.when(i == SUB - 1)
                def _():
                    gather.pass_on(3)
                    middle(3)

        reduce.finish(later, early, late)
        after_forward(total, residual_ref, two_ref, states_out, normed_out)
        if apart:
            for zz in range(4):
                for wait in gather.from_partner(zz):
                    wait()

            def turn(t, carry):
                rows = rows_of(t * 2 * QB, 2 * QB)

                def piece(j, carry):
                    flat[rows, rows_of(j * (D // 4), D // 4)] = full[pl.ds(2 * j, 2), :, rows].reshape(D // 4, 2 * QB).T
                    return carry

                lax.fori_loop(0, 4, piece, 0)
                keep(t).start()
                return carry

            lax.fori_loop(0, 4, turn, 0)
        for copy in saves:
            copy.wait()
        for j in range(4):
            keep(j).wait()

    gathered = (count, width) if apart else (8, tokens, width)
    results, loads = carry_call(
        names,
        body,
        "line",
        [block, *([wide, gain] if apart else []), residual, gain_two, cosine, sine, starts, *slab],
        [ONCHIP, *([ANY, ONCHIP] if apart else []), *[ONCHIP] * 5, *[ANY] * 4],
        [
            jax.ShapeDtypeStruct((tokens, width), F32),
            jax.ShapeDtypeStruct((tokens, width), LOW),
            jax.ShapeDtypeStruct(gathered, LOW),
            jax.ShapeDtypeStruct((count, 5 * HD), LOW),
            jax.ShapeDtypeStruct((count // 2, 3 * HD), LOW),
            *([jax.ShapeDtypeStruct((width, count), LOW)] if apart else []),
        ],
        [ONCHIP, ONCHIP, ANY, ANY, ANY, *([ANY] if apart else [])],
        [
            *Gather.scratch,
            *Slab.scratch,
            pltpu.VMEM((8, *block.shape), LOW),
            pltpu.VMEM((width, count) if apart else (16, 128), LOW),
            pltpu.VMEM((count, width) if apart else (16, 128), LOW),
            pltpu.VMEM((4, tokens, width), LOW),
            pltpu.VMEM((count, 5 * HD), LOW),
            pltpu.VMEM((count // 2, 3 * HD), LOW),
            pltpu.SemaphoreType.DMA((3,)),
            pltpu.SemaphoreType.DMA((4,)),
            pltpu.VMEM((tokens, width), F32),
            *Reduce.scratch(tokens, width),
        ],
        cargo,
        name=name,
    )
    states, low, full, qkv, mixed = results[:5]
    return states, low, full.reshape(count, width), qkv, mixed, results[5] if apart else None, loads


def backward_heads(names, block, grad, residual, gain, acts, turned, slab, qkv, mixed, cosine, sine, starts, cargo, name):
    tokens, width = QB, D
    count = 8 * QB
    reach = QB + SEQ_MAX

    def body(place, ins, outs, scratch, later, middle, start):
        block_ref, grad_ref, residual_ref, gain_ref, acts_hbm, saved_hbm, mixed_hbm = ins[:7]
        cos_ref, sin_ref, starts_ref, *slab_refs = ins[7:]
        grad_out, low_out, gain_out, slab_out, out_out = outs
        scratch = list(scratch)
        gather_sems = [scratch.pop(0) for _ in Gather.scratch]
        weights = Slab(place, slab_refs, [scratch.pop(0) for _ in Slab.scratch])
        full, part, qkv, mixed, acts_own, d_raw, d_keys, d_values = scratch[:8]
        slab, d_out, slab_in, d_out_in, load_sem, swap_send, swap_recv, total, d_mixed = scratch[8:17]
        reduce = Reduce(place, part, total, scratch[17:], far=True)
        weights.start()
        loads = copy_in([(saved_hbm, qkv), (mixed_hbm, mixed), (acts_hbm, acts_own)], load_sem)
        gather = Gather(place, block_ref, full, gather_sems, both=False)
        gather.start(later)
        start(0)
        start(3)
        d_keys[...] = jnp.zeros_like(d_keys)
        d_values[...] = jnp.zeros_like(d_values)
        for load in loads:
            load.wait()
        weights.wait()

        def step(p, carry):
            j = gather.chunk(p)
            pl.when(p == 2)(middle)
            b = 2 * j + place.c
            d_mixed[...] = dot_t(full[j], weights.out[...]).astype(LOW)
            rows, window, _ = block_window(b)

            def head(h, carry):
                cut = rows_of(h * HD, HD)
                queries, d_head = qkv[rows, cut], d_mixed[:, cut]
                keys, values = qkv[window, 3 * HD : 4 * HD], qkv[window, 4 * HD : 5 * HD]
                probs = block_probs(queries, keys, starts_ref, b)
                d_probs = dot_t(d_head, values)
                inner = jnp.sum(probs * d_probs, axis=-1, keepdims=True)
                d_scores = (probs * (d_probs - inner)).astype(LOW)
                d_queries = dot(d_scores, keys) * HD ** (-0.5)
                d_keys[window, :] += t_dot(d_scores, queries) * HD ** (-0.5)
                d_values[window, :] += t_dot(probs.astype(LOW), d_head)
                turned_back = d_queries * cos_ref[rows, :] + roll_half(d_queries * sin_ref[rows, :])
                d_raw[rows, cut] = turned_back.astype(LOW)
                return carry

            lax.fori_loop(0, 3, head, 0)
            other = rows_of((2 * j + 1 - place.c) * QB, QB)
            d_raw[other, 0 : 3 * HD] = jnp.zeros((QB, 3 * HD), LOW)
            return carry

        lax.fori_loop(0, 4, step, 0)
        start(1)

        def project(p, carry):
            j = far_first(place, p)
            rows = rows_of(j * 2 * QB, 2 * QB)
            head = d_keys[rows, :]
            head = head * cos_ref[rows, :] + roll_half(head * sin_ref[rows, :])
            d_raw[rows, 3 * HD : 4 * HD] = head.astype(LOW)
            d_raw[rows, 4 * HD : 5 * HD] = d_values[rows, :].astype(LOW)
            part[pl.ds(2 * j, 2)] = dot_t(d_raw[rows, :], weights.qkv[...]).astype(LOW).reshape(2, tokens, width)
            reduce.made(j)
            return carry

        lax.fori_loop(0, 4, project, 0)

        def swap():
            to = place.at(place.z, 1 - place.c)
            return [
                remote(slab.at[1 - place.c], slab_in, swap_send.at[0], swap_recv.at[0], to),
                remote(d_out.at[1 - place.c], d_out_in, swap_send.at[1], swap_recv.at[1], to),
            ]

        def early(i):
            cut = rows_of(i * (D // 4), D // 4)
            if turned:
                grads = dot(acts_own[cut, :], d_raw[...]).astype(LOW)
            else:
                grads = t_dot(acts_own[:, cut], d_raw[...]).astype(LOW)
            slab[0, i, 0 : D // 8, :] = grads[: D // 8]
            slab[1, i, 0 : D // 8, :] = grads[D // 8 :]
            pl.when(i == 0)(lambda: middle(3))

        def late(i):
            @pl.when(i == 0)
            def _():
                sums = jnp.sum(d_raw[...].astype(F32), axis=0, keepdims=True)
                first = lax.broadcasted_iota(jnp.int32, (16, 5 * HD), 0) == 0
                tail = jnp.where(first, sums, 0.0).astype(LOW)
                for half in range(2):
                    for part_at in range(4):
                        slab[half, part_at, D // 8 :, :] = tail
                grads = t_dot(mixed[...], full[...].reshape(4 * QB, D)).astype(LOW)
                d_out[0] = grads[: D // 8]
                d_out[1] = grads[D // 8 :]
                for copy in swap():
                    copy.start()

        reduce.finish(later, early, late)
        after_backward(total, grad_ref, residual_ref, gain_ref, grad_out, low_out, gain_out)
        for copy in swap():
            copy.wait()
        for i in range(4):
            add_into(slab_out.at[i], [slab.at[place.c, i], slab_in.at[i]])
        add_into(out_out, [d_out.at[place.c], d_out_in])

    (grad, low, d_gain, d_slab, d_out), loads = carry_call(
        names,
        body,
        "line",
        [block, grad, residual, gain, acts, qkv, mixed, cosine, sine, starts, *slab],
        [*[ONCHIP] * 4, *[ANY] * 3, *[ONCHIP] * 3, *[ANY] * 4],
        [
            jax.ShapeDtypeStruct((tokens, width), F32),
            jax.ShapeDtypeStruct((tokens, width), LOW),
            jax.ShapeDtypeStruct((1, width), F32),
            jax.ShapeDtypeStruct((4, HALF, 5 * HD), LOW),
            jax.ShapeDtypeStruct((D // 8, D), LOW),
        ],
        [ONCHIP] * 5,
        [
            *Gather.scratch,
            *Slab.scratch,
            pltpu.VMEM((4, tokens, width), LOW),
            pltpu.VMEM((8, tokens, width), LOW),
            pltpu.VMEM((count, 5 * HD), LOW),
            pltpu.VMEM((count // 2, 3 * HD), LOW),
            pltpu.VMEM(acts.shape, LOW),
            pltpu.VMEM((count, 5 * HD), LOW),
            pltpu.VMEM((count, HD), F32),
            pltpu.VMEM((count, HD), F32),
            pltpu.VMEM((2, 4, HALF, 5 * HD), LOW),
            pltpu.VMEM((2, D // 8, D), LOW),
            pltpu.VMEM((4, HALF, 5 * HD), LOW),
            pltpu.VMEM((D // 8, D), LOW),
            pltpu.SemaphoreType.DMA((3,)),
            pltpu.SemaphoreType.DMA((2,)),
            pltpu.SemaphoreType.DMA((2,)),
            pltpu.VMEM((tokens, width), F32),
            pltpu.VMEM((QB, 3 * HD), LOW),
            *Reduce.scratch(tokens, width),
        ],
        cargo,
        name=name,
    )
    return grad, low, d_gain, d_slab.reshape(4 * HALF, 5 * HD), d_out, loads


def settle_rows(row, fulls, slots):
    kinds, layers = len(fulls), len(fulls[0])
    count, size = slots[0][0].shape[1:]
    tile = count // 5

    def kernel(row_ref, *refs):
        ins, outs = refs[: 2 * kinds * layers], refs[2 * kinds * layers :]
        for kind in range(kinds):
            for layer in range(layers):
                full, slot = ins[2 * (kind * layers + layer)], ins[2 * (kind * layers + layer) + 1]
                outs[kind][layer] = full[...].astype(F32) + slot[0].astype(F32) + slot[1].astype(F32)

    pairs = [pair for kind in range(kinds) for pair in zip(fulls[kind], slots[kind])]
    return pl.pallas_call(
        kernel,
        out_shape=[jax.ShapeDtypeStruct((layers, count, size), F32)] * kinds,
        grid_spec=pltpu.PrefetchScalarGridSpec(
            num_scalar_prefetch=1,
            grid=(count // tile,),
            in_specs=[
                pl.BlockSpec((tile, size), lambda i, row: (i, row[0])),
                pl.BlockSpec((2, tile, size), lambda i, row: (0, i, 0)),
            ]
            * (kinds * layers),
            out_specs=[pl.BlockSpec((layers, tile, size), lambda i, row: (0, i, 0))] * kinds,
        ),
        compiler_params=pltpu.CompilerParams(vmem_limit_bytes=VMEM),
        name="settle",
    )(row.reshape(1), *[array for pair in pairs for array in pair])


def backward_feed(names, block, grads_all, grad, residual, gain, acts, w_gate, w_up, w_down, gate, up, cargo, name):
    tokens, width = QB, D
    inner = w_gate.shape[0]
    apart = grads_all is not None

    def body(place, ins, outs, scratch, later, middle, start):
        head_ref, grad_ref, residual_ref, gain_ref, acts_hbm, gate_hbm, up_hbm, down_hbm, gates_hbm, ups_hbm = ins
        grad_out, low_out, gain_out, gate_out, up_out, down_out = outs
        scratch = list(scratch)
        gather_sems = [scratch.pop(0) for _ in Gather.scratch]
        full, part, acts_own, pair_w, down_w, pair, hiddens, load_sem, keep_sem, total, d_down = scratch[:11]
        gate_w, up_w, gates, ups = pair_w.at[0], pair_w.at[1], pair.at[0], pair.at[1]
        reduce = Reduce(place, part, total, scratch[11:], far=apart)
        if not apart:
            d_down = down_w
        def weights(dst, left, right, cut):
            dst[cut, :] = t_dot(left[:, cut], right()).astype(LOW)

        def grads_flat():
            return full[...].reshape(8 * tokens, width)

        def acts_flat():
            return acts_own[...]

        pairs = [(gates_hbm, gates), (ups_hbm, ups)]
        if apart:
            pairs.append((head_ref, full))
        early = len(pairs)
        pairs += [(down_hbm, down_w), (gate_hbm, gate_w), (up_hbm, up_w), (acts_hbm, acts_own)]
        loads = copy_in(pairs, load_sem)
        gather = None
        if not apart:
            gather = Gather(place, head_ref, full, gather_sems)
            gather.start(later)
        start(0)
        start(3)
        for load in loads[:early]:
            load.wait()

        def lit(rows, cut):
            gate, up = gates[rows, cut].astype(F32), ups[rows, cut].astype(F32)
            squash = jax.nn.sigmoid(gate)
            glow = gate * squash
            hiddens[rows, cut] = (glow * up).astype(LOW)
            return gate, up, squash, glow

        if apart:

            def light(i, carry):
                lit(rows_of(i * tokens, tokens), slice(None))
                return carry

            lax.fori_loop(0, 8, light, 0)
            tiles(inner, partial(weights, d_down, hiddens, grads_flat))
            start(1, d_down)
        for load in loads[early:]:
            load.wait()

        def step(p, carry):
            j = far_first(place, p) if apart else gather.chunk(p)
            pl.when(p == 2)(middle)
            rows = rows_of(j * 2 * tokens, 2 * tokens)
            grads = full[pl.ds(2 * j, 2)].reshape(2 * tokens, width)

            def columns(cut):
                d_hidden = dot_t(grads, down_w[cut, :])
                gate, up, squash, glow = lit(rows, cut)
                gates[rows, cut] = (d_hidden * up * squash * (1.0 + gate * (1.0 - squash))).astype(LOW)
                ups[rows, cut] = (d_hidden * glow).astype(LOW)

            tiles(inner, columns)

            def outputs(cut):
                sums = dot(gates[rows, :], gate_w[:, cut]) + dot(ups[rows, :], up_w[:, cut])
                part[pl.ds(2 * j, 2), :, cut] = sums.astype(LOW).reshape(2, tokens, cut.size)

            tiles(width, outputs, 512)
            reduce.made(j)
            return carry

        lax.fori_loop(0, 4, step, 0)

        if not apart:
            tiles(inner, partial(weights, d_down, hiddens, grads_flat))
            start(1, d_down)

        def both_rows(cut):
            def kind(k, carry):
                weights(pair_w.at[k], pair.at[k], acts_flat, cut)
                return carry

            lax.fori_loop(0, 2, kind, 0)

        def early(i):
            if apart:
                pl.when(i == 0)(lambda: middle(1))
            both_rows(rows_of(i * 256, 256))

        def late(i):
            @pl.when(i == 0)
            def _():
                if inner > 256 * SUB:
                    both_rows(pl.ds(256 * SUB, inner - 256 * SUB))
                if not apart:
                    middle(1)

        reduce.finish(later, early, late)
        saves = copy_in([(gate_w, gate_out), (up_w, up_out), (d_down, down_out)], keep_sem)
        after_backward(total, grad_ref, residual_ref, gain_ref, grad_out, low_out, gain_out)
        for copy in saves:
            copy.wait()

    head = grads_all.reshape(8, tokens, width) if apart else block
    (grad, low, d_gain, d_gate, d_up, d_down), loads = carry_call(
        names,
        body,
        "line",
        [head, grad, residual, gain, acts, w_gate, w_up, w_down, gate, up],
        [ANY if apart else ONCHIP, ONCHIP, ONCHIP, ONCHIP, ANY, ANY, ANY, ANY, ANY, ANY],
        [
            jax.ShapeDtypeStruct((tokens, width), F32),
            jax.ShapeDtypeStruct((tokens, width), LOW),
            jax.ShapeDtypeStruct((1, width), F32),
            jax.ShapeDtypeStruct(w_gate.shape, LOW),
            jax.ShapeDtypeStruct(w_up.shape, LOW),
            jax.ShapeDtypeStruct(w_down.shape, LOW),
        ],
        [ONCHIP, ONCHIP, ONCHIP, ANY, ANY, ANY],
        [
            *Gather.scratch,
            pltpu.VMEM((8, tokens, width), LOW),
            pltpu.VMEM((8, tokens, width), LOW),
            pltpu.VMEM((8 * tokens, width), LOW),
            pltpu.VMEM((2, *w_gate.shape), LOW),
            pltpu.VMEM(w_down.shape, LOW),
            pltpu.VMEM((2, 8 * tokens, inner), LOW),
            pltpu.VMEM((8 * tokens, inner), LOW),
            pltpu.SemaphoreType.DMA((7,)),
            pltpu.SemaphoreType.DMA((3,)),
            pltpu.VMEM((tokens, width), F32),
            pltpu.VMEM(w_down.shape if apart else (16, 128), LOW),
            *Reduce.scratch(tokens, width),
        ],
        cargo,
        name=name,
    )
    return grad, low, d_gain, d_gate, d_up, d_down, loads


eps_norm = 1e-06
rope_base = 1000000.0
neg_fill = -1e30


def row_starts(sizes, count):
    ends = jnp.cumsum(sizes)
    firsts = ends - sizes
    places = jnp.arange(count, dtype=jnp.int32)
    inside = (places[None, :] >= firsts[:, None]) & (places[None, :] < ends[:, None])
    return jnp.sum(jnp.where(inside, firsts[:, None], 0), axis=0)


def rope_tables(positions):
    half = HD // 2
    freq = rope_base ** (-(jnp.arange(half, dtype=jnp.float32) * (2.0 / HD)))
    angle = freq[:, None] * positions.astype(jnp.float32)[None, :]
    cosine = jnp.concatenate([jnp.cos(angle), jnp.cos(angle)], axis=0)
    sine = jnp.concatenate([jnp.sin(angle), jnp.sin(angle)], axis=0)
    return (cosine, sine)


def rotate(values, cosine, sine):
    half = HD // 2
    turned = jnp.concatenate([-values[:, half:], values[:, :half]], axis=1)
    return values * cosine + turned * sine


def rotate_back(grads, cosine, sine):
    half = HD // 2
    lifted = grads * sine
    turned = jnp.concatenate([lifted[:, half:], -lifted[:, :half]], axis=1)
    return grads * cosine + turned


def contract_first(left, right):
    return lax.dot_general(
        left, right, (((0,), (0,)), ((), ())), preferred_element_type=jnp.float32
    )


def contract_last(left, right):
    return lax.dot_general(
        left, right, (((1,), (1,)), ((), ())), preferred_element_type=jnp.float32
    )


def feature_total(values):
    return lax.psum(jnp.sum(values, axis=0), "col")


def spread(values):
    return lax.all_gather(values, "col", axis=0, tiled=True)


def summed_rows(make_term, rows):
    return lax.psum_scatter(
        make_term(jnp.int32(0), lax.axis_size("col") * rows), "col", scatter_dimension=0, tiled=True
    )


def to_blocks(values):
    return lax.all_to_all(values, "col", split_axis=1, concat_axis=0, tiled=True)


def to_tokens(values):
    return lax.all_to_all(values, "col", split_axis=0, concat_axis=1, tiled=True)


def by_columns(weight, acts, start, count):
    return contract_first(weight, acts)


def by_rows(weight, grads, start, count):
    return jnp.dot(weight, grads, preferred_element_type=jnp.float32)


def by_rows_pair(first_weight, first_grads, second_weight, second_grads, start, count):
    return by_rows(first_weight, first_grads, start, count) + by_rows(
        second_weight, second_grads, start, count
    )


def norm_forward(residual, gain):
    totals = feature_total(residual * residual)
    scale = lax.rsqrt(totals / D + eps_norm)
    return (scale, (residual * scale * gain[:, None]).astype(jnp.bfloat16))


def norm_backward(d_normed, residual, scale, gain):
    weighted = d_normed * gain[:, None]
    inner = feature_total(weighted * residual)
    d_residual = weighted * scale - residual * (scale * scale * scale) * inner / D
    d_gain = jnp.sum(d_normed * residual * scale, axis=1)
    return (d_residual, d_gain)


def attend_scores(queries, keys, mask):
    scores = jnp.einsum(
        "kghq,khj->kgqj", queries, keys, preferred_element_type=jnp.float32
    ) * HD ** (-0.5)
    return jnp.where(mask[None, None], scores, neg_fill)


def per_device(
    hidden_states,
    out_grad,
    lengths,
    norm_gains,
    qkv_weight,
    qkv_bias,
    out_weight,
    gate_weight,
    up_weight,
    down_weight,
):
    feat_rows, tok_row = hidden_states.shape
    col_at = lax.axis_index("col")
    starts = row_starts(lengths[0], tok_row)
    positions = jnp.arange(tok_row, dtype=jnp.int32) - starts
    cosine, sine = rope_tables(positions)
    first = col_at * QB
    block_starts = lax.dynamic_slice_in_dim(starts, first, QB)
    cos_block = lax.dynamic_slice_in_dim(cosine, first, QB, 1)
    sin_block = lax.dynamic_slice_in_dim(sine, first, QB, 1)
    reach = QB + SEQ_MAX
    window = jnp.maximum(first - SEQ_MAX, 0)
    key_places = window + jnp.arange(reach, dtype=jnp.int32)
    query_places = first + jnp.arange(QB, dtype=jnp.int32)
    mask = (key_places[None, :] >= block_starts[:, None]) & (
        key_places[None, :] <= query_places[:, None]
    )
    group = HEADS // KV_HEADS
    rotary = HEADS + KV_HEADS
    query_rows = HEADS * HD
    kv_rows = KV_HEADS * HD
    gains = norm_gains.astype(jnp.float32)
    residual = hidden_states.astype(jnp.float32)
    saved = []
    for layer in range(LAYERS):
        w_qkv, b_qkv, w_out, w_gate, w_up, w_down = (
            lax.all_gather(qkv_weight[layer], "row", axis=0, tiled=True),
            lax.all_gather(qkv_bias[layer], "row", axis=1, tiled=True),
            lax.all_gather(out_weight[layer], "row", axis=1, tiled=True),
            lax.all_gather(gate_weight[layer], "row", axis=0, tiled=True),
            lax.all_gather(up_weight[layer], "row", axis=0, tiled=True),
            lax.all_gather(down_weight[layer], "row", axis=1, tiled=True),
        )
        scale_one, normed_one = norm_forward(residual, gains[layer, 0])
        full_one = spread(normed_one)
        raw = contract_first(w_qkv, full_one) + b_qkv.reshape(-1).astype(jnp.float32)[:, None]
        local_heads = raw.shape[0] // HD
        shaped = raw.reshape(local_heads, HD, tok_row)
        head_ids = col_at * local_heads + jnp.arange(local_heads)
        turned = jnp.where((head_ids < rotary)[:, None, None], rotate(shaped, cosine, sine), shaped)
        blocked = to_blocks(turned.reshape(raw.shape).astype(jnp.bfloat16))
        kv_full = lax.all_gather(blocked[query_rows:], "col", axis=1, tiled=True)
        kv_window = lax.dynamic_slice_in_dim(kv_full, window, reach, 1)
        queries = blocked[:query_rows].reshape(KV_HEADS, group, HD, QB)
        keys = kv_window[:kv_rows].reshape(KV_HEADS, HD, reach)
        values = kv_window[kv_rows:].reshape(KV_HEADS, HD, reach)
        masked = attend_scores(queries, keys, mask)
        row_top = jnp.max(masked, axis=-1, keepdims=True)
        lifted = jnp.exp(masked - row_top)
        row_mass = jnp.sum(lifted, axis=-1, keepdims=True)
        probs = lifted / row_mass
        log_mass = row_top + jnp.log(row_mass)
        mixed = (
            jnp.einsum(
                "kgqj,khj->kghq",
                probs.astype(jnp.bfloat16),
                values,
                preferred_element_type=jnp.float32,
            )
            .reshape(query_rows, QB)
            .astype(jnp.bfloat16)
        )
        carried = to_tokens(mixed)
        attention = summed_rows(partial(by_columns, w_out, carried), feat_rows)
        residual_mid = residual + attention
        scale_two, normed_two = norm_forward(residual_mid, gains[layer, 1])
        full_two = spread(normed_two)
        gate = contract_first(w_gate, full_two)
        up = contract_first(w_up, full_two)
        hidden = (gate * jax.nn.sigmoid(gate) * up).astype(jnp.bfloat16)
        feed = summed_rows(partial(by_columns, w_down, hidden), feat_rows)
        saved.append(
            (
                residual,
                scale_one,
                full_one,
                blocked,
                kv_window,
                log_mass,
                mixed,
                carried,
                residual_mid,
                scale_two,
                full_two,
                gate,
                up,
                hidden,
                (w_qkv, w_out, w_gate, w_up, w_down),
                local_heads,
            )
        )
        residual = residual_mid + feed
    out_states = residual.astype(jnp.bfloat16)
    grad = out_grad.astype(jnp.float32)
    layer_grads = [None] * LAYERS
    gain_terms = [None] * LAYERS
    for layer in reversed(range(LAYERS)):
        (
            residual_in,
            scale_one,
            full_one,
            blocked,
            kv_window,
            log_mass,
            mixed,
            carried,
            residual_mid,
            scale_two,
            full_two,
            gate,
            up,
            hidden,
            weights_full,
            local_heads,
        ) = saved[layer]
        w_qkv, w_out, w_gate, w_up, w_down = weights_full
        grad_full = spread(grad.astype(jnp.bfloat16))
        d_down = contract_last(hidden, grad_full)
        d_hidden = jnp.dot(w_down, grad_full, preferred_element_type=jnp.float32)
        squash = jax.nn.sigmoid(gate)
        d_gate = (d_hidden * up * squash * (1.0 + gate * (1.0 - squash))).astype(jnp.bfloat16)
        d_up = (d_hidden * gate * squash).astype(jnp.bfloat16)
        d_gate_w = contract_last(full_two, d_gate)
        d_up_w = contract_last(full_two, d_up)
        d_normed_two = summed_rows(partial(by_rows_pair, w_gate, d_gate, w_up, d_up), feat_rows)
        d_residual, d_gain_two = norm_backward(
            d_normed_two, residual_mid, scale_two, gains[layer, 1]
        )
        grad = grad + d_residual
        grad_full = spread(grad.astype(jnp.bfloat16))
        d_out_w = contract_last(carried, grad_full)
        d_mixed = to_blocks(
            jnp.dot(w_out, grad_full, preferred_element_type=jnp.float32).astype(jnp.bfloat16)
        )
        queries = blocked[:query_rows].reshape(KV_HEADS, group, HD, QB)
        keys = kv_window[:kv_rows].reshape(KV_HEADS, HD, reach)
        values = kv_window[kv_rows:].reshape(KV_HEADS, HD, reach)
        masked = attend_scores(queries, keys, mask)
        probs = jnp.exp(masked - log_mass)
        low_probs = probs.astype(jnp.bfloat16)
        d_heads_mix = d_mixed.reshape(KV_HEADS, group, HD, QB)
        d_probs = jnp.einsum(
            "kghq,khj->kgqj", d_heads_mix, values, preferred_element_type=jnp.float32
        )
        inner = jnp.sum(probs * d_probs, axis=-1, keepdims=True)
        d_scores = (probs * (d_probs - inner)).astype(jnp.bfloat16)
        d_queries = (
            jnp.einsum("kgqj,khj->kghq", d_scores, keys, preferred_element_type=jnp.float32)
            * HD ** (-0.5)
        ).reshape(query_rows, QB)
        d_keys = (
            jnp.einsum("kgqj,kghq->khj", d_scores, queries, preferred_element_type=jnp.float32)
            * HD ** (-0.5)
        ).reshape(kv_rows, reach)
        d_values = jnp.einsum(
            "kgqj,kghq->khj", low_probs, d_heads_mix, preferred_element_type=jnp.float32
        ).reshape(kv_rows, reach)
        d_window = jnp.concatenate([d_keys, d_values], axis=0)
        d_placed = lax.dynamic_update_slice_in_dim(
            jnp.zeros((2 * kv_rows, tok_row), jnp.float32), d_window, window, 1
        )
        d_kv = lax.psum_scatter(d_placed, "col", scatter_dimension=1, tiled=True)
        d_heads = jnp.concatenate([d_queries, d_kv], axis=0).reshape(HEADS + 2 * KV_HEADS, HD, QB)
        d_turned = jnp.concatenate(
            [rotate_back(d_heads[:rotary], cos_block, sin_block), d_heads[rotary:]], axis=0
        )
        d_raw = to_tokens(d_turned.reshape((HEADS + 2 * KV_HEADS) * HD, QB).astype(jnp.bfloat16))
        d_bias = jnp.sum(d_raw, axis=1, dtype=jnp.float32).reshape(local_heads, HD)
        d_qkv_w = contract_last(full_one, d_raw)
        d_normed_one = summed_rows(partial(by_rows, w_qkv, d_raw), feat_rows)
        d_residual, d_gain_one = norm_backward(
            d_normed_one, residual_in, scale_one, gains[layer, 0]
        )
        grad = grad + d_residual
        layer_grads[layer] = (
            lax.psum_scatter(d_qkv_w, "row", scatter_dimension=0, tiled=True),
            lax.psum_scatter(d_bias, "row", scatter_dimension=1, tiled=True),
            lax.psum_scatter(d_out_w, "row", scatter_dimension=1, tiled=True),
            lax.psum_scatter(d_gate_w, "row", scatter_dimension=0, tiled=True),
            lax.psum_scatter(d_up_w, "row", scatter_dimension=0, tiled=True),
            lax.psum_scatter(d_down, "row", scatter_dimension=1, tiled=True),
        )
        gain_terms[layer] = jnp.stack([d_gain_one, d_gain_two])
    gain_grads = lax.psum(jnp.stack(gain_terms), "row")
    stacked = [jnp.stack([entry[member] for entry in layer_grads]) for member in range(6)]
    return (
        out_states,
        grad,
        gain_grads,
        stacked[0],
        stacked[1],
        stacked[2],
        stacked[3],
        stacked[4],
        stacked[5],
    )


def dot(a, b):
    return jnp.dot(a, b, preferred_element_type=F32)


def dot_t(a, b):
    return lax.dot_general(a, b, (((1,), (1,)), ((), ())), preferred_element_type=F32)


def t_dot(a, b):
    return lax.dot_general(a, b, (((0,), (0,)), ((), ())), preferred_element_type=F32)


def line_tables(sizes, count):
    fine = 32
    freq = rope_base ** (-(jnp.arange(HD // 2, dtype=F32) * (2.0 / HD)))
    firsts = jnp.cumsum(sizes) - sizes
    places = jnp.arange(count, dtype=jnp.int32)[:, None]
    inside = (places >= firsts[None]) & (places < (firsts + sizes)[None])
    starts = jnp.sum(jnp.where(inside, firsts[None], 0), axis=1, keepdims=True)
    points = jnp.concatenate([jnp.arange(count // fine) * fine, jnp.arange(fine), -firsts])
    angles = points.astype(F32)[:, None] * freq[None]
    cosines, sines = jnp.cos(angles), jnp.sin(angles)

    def add(one, two):
        return one[0] * two[0] - one[1] * two[1], one[1] * two[0] + one[0] * two[1]

    def pick(low, high):
        return cosines[low:high], sines[low:high]

    coarse = count // fine
    upper = [part[:, None] for part in pick(0, coarse)]
    lower = [part[None] for part in pick(coarse, coarse + fine)]
    at = [part.reshape(count, HD // 2) for part in add(upper, lower)]
    shift = [jnp.sum(jnp.where(inside[:, :, None], part[None], 0.0), axis=1) for part in pick(coarse + fine, None)]
    cosine, sine = add(at, shift)
    return starts, jnp.concatenate([cosine, cosine], axis=1), jnp.concatenate([-sine, sine], axis=1)


def per_device_line(
    hidden_states,
    out_grad,
    lengths,
    norm_gains,
    qkv_weight,
    qkv_bias,
    out_weight,
    gate_weight,
    up_weight,
    down_weight,
):
    names = Names()
    tok_row = hidden_states.shape[1]
    row_at = lax.axis_index("row")
    col_at = lax.axis_index("col")
    core = col_at % 2

    biases = jnp.zeros((LAYERS, 2, 16, HD), LOW)
    biases = lax.dynamic_update_slice(biases, qkv_bias[:, :, None], (0, 0, 0, row_at * (HD // 4)))
    gain_rows = jnp.pad(norm_gains.reshape(2 * LAYERS, D // 8), ((0, 16 - 2 * LAYERS), (0, 0)))

    def rows_load(layer):
        return (
            GatherRows(gate_weight.swapaxes(1, 2), 1, layer),
            GatherRows(up_weight.swapaxes(1, 2), 1, layer),
            GatherRows(down_weight, 1, layer),
        )

    sent = rows_load(0)
    to_chips = [HeadsToChips(qkv_weight, biases, layer) for layer in range(LAYERS)]
    slab_rows, out_rows = GatherRows(From(to_chips[0]), 0, phase=1), GatherRows(out_weight, 1, 0, phase=1)
    swap = Swap(From(slab_rows), From(out_rows), phase=2)
    sent[0].phase = 3
    states, loads = open_call(
        names, hidden_states, [*to_chips, Exchange(gain_rows, same=True), slab_rows, out_rows, swap, sent[0]]
    )
    (_,), (slab_next,), (gains,), (mine,), (out_mine,), (theirs, out_theirs), (w_gate,) = loads
    load = (mine, theirs, out_mine, out_theirs)
    gains = gains[:, : 2 * LAYERS].transpose(1, 0, 2).reshape(LAYERS, 2, D).astype(F32)
    starts, cosine, sine = line_tables(lengths[0], tok_row)

    wide = states.reshape(D, tok_row)
    residual = lax.dynamic_slice_in_dim(wide, col_at * QB, QB, 1).astype(F32).T

    def own_rows(full):
        return lax.dynamic_slice_in_dim(full, col_at * QB, QB, 0).astype(F32)

    def gain_of(layer, which):
        return gains[layer, which][None]

    saved = []
    normed = None
    for layer in range(LAYERS):
        slab = load
        sent[1].phase, sent[2].phase = 0, 3
        fixed = (residual, gain_of(layer, 1), slab, cosine, sine, starts, sent[1:])
        if layer == 0:
            mid, normed, grads_all, qkv, mixed, full_one, loads = forward_heads(
                names, out_grad, wide, gains[0, 0][:, None], *fixed, name="heads_0"
            )
        else:
            mid, normed, full_one, qkv, mixed, _, loads = forward_heads(names, normed, None, None, *fixed, name="heads_1")
        (w_up,), (w_down,) = loads
        cargo = []
        if layer == 0:
            sent = rows_load(1)
            sent[0].phase = 3
            slab_rows, out_rows = GatherRows(slab_next, 0), GatherRows(out_weight, 1, 1)
            cargo = [slab_rows, out_rows, sent[0], Swap(From(slab_rows), From(out_rows), phase=2)]
        following = gain_of(layer + 1, 0) if layer + 1 < LAYERS else None
        states, normed, full_two, gate, up, loads = forward_feed(
            names, normed, mid, following, w_gate, w_up, w_down, cargo, name=f"feed_{layer}"
        )
        saved.append((residual, full_one, slab, qkv, mixed, mid, full_two, gate, up, (w_gate, w_up, w_down)))
        residual = states
        if layer == 0:
            (mine,), (out_mine,), (w_gate,), (theirs, out_theirs) = loads
            load = (mine, theirs, out_mine, out_theirs)
    states = normed

    def own_part(full, dim):
        size = full.shape[dim] // 4
        return lax.dynamic_slice_in_dim(full, row_at * size, size, dim)

    def settle(full, dim, slots):
        return jnp.sum(slots.astype(F32), axis=0) + own_part(full, dim).astype(F32)

    def settle_heads(tiles):
        total = tiles[:, :, 0].astype(F32) + jnp.where(col_at >= 6, tiles[:, :, 1].astype(F32), 0.0)
        weight = total[:, :, : D // 8].transpose(1, 2, 0, 3).reshape(D // 4, 2 * HD)
        bias = lax.dynamic_slice_in_dim(total[:, 0, D // 8], row_at * (HD // 4), HD // 4, 1)
        return weight, bias

    grads = {}
    gain_terms = [None] * LAYERS
    grad, low = own_rows(grads_all), None
    inner = w_gate.shape[0]
    owners = []
    for layer in reversed(range(LAYERS)):
        residual_in, full_one, slab, qkv, mixed, mid, full_two, gate, up, feed_weights = saved[layer]
        last = layer == LAYERS - 1
        if last:
            cargo = [Exchange(states.T.reshape(8, D // 8, QB))]
        else:
            cargo = [ScatterRows(d_slab, 0), ScatterRows(d_out_w, 1)]
        cargo.append(ScatterRows(Inner((inner, D)), 1, phase=1))
        grad, low, d_gain_two, d_gate_w, d_up_w, d_down, loads = backward_feed(
            names,
            low,
            grads_all if last else None,
            grad,
            mid,
            gain_of(layer, 1),
            full_two,
            *feed_weights,
            gate,
            up,
            cargo,
            name=f"back_feed_{layer}",
        )
        grads["down", layer] = d_down, loads[-1][0]
        if last:
            out_states = loads[0][0]
        else:
            grads["out", layer + 1] = settle(d_out_w, 1, loads[1][0])
            owners.append(HeadsToOwners(settle(d_slab, 0, loads[0][0]).astype(LOW)))
        grad, low, d_gain_one, d_slab, d_out_w, loads = backward_heads(
            names,
            low,
            grad,
            residual_in,
            gain_of(layer, 0),
            full_one,
            layer == 0,
            slab,
            qkv,
            mixed,
            cosine,
            sine,
            starts,
            [ScatterRows(d_gate_w, 1), ScatterRows(d_up_w, 1, phase=3)],
            name=f"back_heads_{layer}",
        )
        grads["gate", layer] = d_gate_w, loads[0][0]
        grads["up", layer] = d_up_w, loads[1][0]
        gain_terms[layer] = jnp.concatenate([d_gain_one, d_gain_two], axis=0)
    gain_parts = jnp.pad(jnp.stack(gain_terms).reshape(2 * LAYERS, 8, D // 8), ((0, 8 - 2 * LAYERS), (0, 0), (0, 0)))
    for owner in owners:
        owner.phase = 3
    tiles, ((left,), (gain_all,), (out_slots,), (tiles_next,)) = close_call(
        names,
        d_slab,
        [
            Exchange(low.T.reshape(8, D // 8, QB)),
            Exchange(gain_parts.transpose(1, 0, 2), every_row=True),
            ScatterRows(d_out_w, 1, phase=3),
            *owners,
        ],
    )
    grads["qkv", 1] = settle_heads(tiles_next)
    grads["qkv", 0] = settle_heads(tiles)
    grads["out", 0] = settle(d_out_w, 1, out_slots)
    out_states = out_states.transpose(1, 0, 2).reshape(D // 8, tok_row)
    input_grad = left.transpose(1, 0, 2).reshape(D // 8, tok_row).astype(F32)
    gain_grads = jnp.sum(gain_all, axis=(0, 1))[: 2 * LAYERS].reshape(LAYERS, 2, D // 8)

    def both_layers(kind):
        return jnp.stack([grads[kind, layer] for layer in range(LAYERS)])

    kinds = ("gate", "up", "down")
    d_gate, d_up, d_down = settle_rows(
        row_at,
        [[grads[kind, layer][0] for layer in range(LAYERS)] for kind in kinds],
        [[grads[kind, layer][1] for layer in range(LAYERS)] for kind in kinds],
    )
    heads = [jnp.stack([grads["qkv", layer][i] for layer in range(LAYERS)]) for i in range(2)]
    return (
        out_states,
        input_grad,
        gain_grads,
        heads[0],
        heads[1],
        both_layers("out"),
        d_gate.swapaxes(1, 2),
        d_up.swapaxes(1, 2),
        d_down,
    )


def solution(mesh):
    placed = (
        P("col", "row"),
        P("col", "row"),
        P("row", None),
        P(None, None, "col"),
        P(None, "row", "col"),
        P(None, "col", "row"),
        P(None, "col", "row"),
        P(None, "row", "col"),
        P(None, "row", "col"),
        P(None, "col", "row"),
    )
    on_lines = mesh.shape["row"] == 4 and mesh.shape["col"] == 8
    return jax.shard_map(
        per_device_line if on_lines else per_device,
        mesh=mesh,
        in_specs=placed,
        out_specs=(
            P("col", "row"),
            P("col", "row"),
            P(None, None, "col"),
            P(None, "row", "col"),
            P(None, "col", "row"),
            P(None, "col", "row"),
            P(None, "row", "col"),
            P(None, "row", "col"),
            P(None, "col", "row"),
        ),
        check_vma=False,
    )
```
